32 devices in a mesh: row: 8 (over z, x), col: 4 (over y, core).
Axes of the slice: x: 2, y: 2, z: 4, core: 2. Of those that a mesh axis runs over, the one named last changes fastest.
Arguments:
- stream: float32 [1024, 2048], P('row', 'col'), may hold values from -6 to 6
- grad_out: float32 [1024, 2048], P('row', 'col'), may hold values from -6 to 6
- wqkv: bfloat16 [2, 2048, 4, 640], P(None, 'row', 'col'), may hold values from -0.125 to 0.125
- wo: bfloat16 [2, 2048, 2048], P(None, 'row', 'col'), may hold values from -2 to 2
- wgu: bfloat16 [2, 2048, 2, 5632], P(None, 'row', None, 'col'), may hold values from -0.125 to 0.125
- wd: bfloat16 [2, 2048, 5632], P(None, 'row', 'col'), may hold values from -0.078125 to 0.078125
- gain_attn: float32 [2, 2048], P(None, 'col'), may hold values from 0.5 to 1.5
- gain_ffn: float32 [2, 2048], P(None, 'col'), may hold values from 0.5 to 1.5
Outputs:
- out_stream: float32 [1024, 2048], P('row', 'col')
- grad_stream: float32 [1024, 2048], P('row', 'col')
- grad_wqkv: float32 [2, 2048, 4, 640], P(None, 'row', 'col')
- grad_wo: float32 [2, 2048, 2048], P(None, 'row', 'col')
- grad_wgu: float32 [2, 2048, 2, 5632], P(None, 'row', None, 'col')
- grad_wd: float32 [2, 2048, 5632], P(None, 'row', 'col')
- grad_gain_attn: float32 [2, 2048], P(None, 'col')
- grad_gain_ffn: float32 [2, 2048], P(None, 'col')
The draws below stay inside these ranges and needn't reach their ends.
All inputs are finite; a program needn't handle non-finite values.
Results may differ from the reference program's by a relative error of at most 0.028.
Values may be sent and summed in bfloat16 or wider, within the bound.
A program may use at most 256 MiB of HBM per device.

```python
import math
import jax
import jax.numpy as jnp
from jax import lax

D = 2048
FF = 5632
KVH = 4
HEAD = 64
GROUP = 8
LAYERS = 2
SEQ = 1024
HQ = 32
TOKENS = 1024


def shard_levels(stream_key, dims, split, least, high):
    level = 1.0
    for axis_at, blocks in split:
        heights = jax.random.uniform(jax.random.fold_in(jax.random.fold_in(stream_key, 6), axis_at), (blocks,), jnp.float32, least / len(split), high / len(split))
        level = level * jnp.repeat(jnp.exp(heights), dims[axis_at] // blocks).reshape((-1,) + (1,) * (len(dims) - 1 - axis_at))
    return level


def noise(stream_key, shape, width, reach, shards=(), held_as=jnp.bfloat16):
    drawn = width * jax.random.normal(stream_key, shape, jnp.float32)
    if shards:
        drawn = drawn * shard_levels(stream_key, shape, shards, -0.22, 0.18)
    return jnp.clip(drawn, -reach, reach).astype(held_as)


def setup_inputs(seed: int = 0) -> dict:
    streams_of = jax.random.split(jax.random.key(seed), 9)
    return {
        "stream": noise(streams_of[0], (TOKENS, D), 1.0, 6.0, ((0, 8), (1, 4)), jnp.float32),
        "grad_out": noise(streams_of[1], (TOKENS, D), 1.0, 6.0, ((0, 8), (1, 4)), jnp.float32),
        "wqkv": noise(streams_of[2], (LAYERS, D, KVH, (GROUP + 2) * HEAD), D ** -0.5, 0.125, ((1, 8), (2, 4))),
        "wo": noise(streams_of[3], (LAYERS, D, HQ * HEAD), (max(HQ * HEAD // 256, 1)) ** -0.5, 2.0, ((1, 8), (2, 4))),
        "wgu": noise(streams_of[4], (LAYERS, D, 2, FF), D ** -0.5, 0.125, ((1, 8), (3, 4))),
        "wd": noise(streams_of[5], (LAYERS, D, FF), FF ** -0.5, 0.078125, ((1, 8), (2, 4))),
        "gain_attn": jnp.clip(1.0 + 0.1 * jax.random.normal(streams_of[6], (LAYERS, D), jnp.float32), 0.5, 1.5),
        "gain_ffn": jnp.clip(1.0 + 0.1 * jax.random.normal(streams_of[7], (LAYERS, D), jnp.float32), 0.5, 1.5),
    }


EPS = 1e-05
THETA = 10000.0

@jax.custom_vjp
def low(v):
    return lax.optimization_barrier(v.astype(jnp.bfloat16)).astype(jnp.float32)

@jax.custom_vjp
def low_back(v):
    return v

def low_keep(v):
    return (low(v), None)

def low_pass(kept, grad):
    return (grad,)

def back_keep(v):
    return (v, None)

def back_low(kept, grad):
    return (low(grad),)
low.defvjp(low_keep, low_pass)
low_back.defvjp(back_keep, back_low)

def normalize(values, gain):
    return values * lax.rsqrt(lax.optimization_barrier(jnp.mean(values * values, axis=-1, keepdims=True)) + EPS) * gain

def rope_turn(tensor, cosine, sine):
    half = tensor.shape[-1] // 2
    first = tensor[..., :half]
    second = tensor[..., half:]
    return jnp.concatenate([first * cosine - second * sine, second * cosine + first * sine], axis=-1)

def one_head(item):
    queries, keys, values = item
    scores = jnp.dot(queries, keys.T, precision=lax.Precision.HIGHEST) * (1.0 / math.sqrt(HEAD))
    scores = low_back(scores)
    place = jnp.arange(SEQ, dtype=jnp.int32)
    scores = jnp.where(place[None, :] <= place[:, None], scores, -1e+30)
    top = lax.optimization_barrier(jnp.max(scores, axis=-1, keepdims=True))
    expo = jnp.exp(scores - top)
    probs = low(expo / lax.optimization_barrier(jnp.sum(expo, axis=-1, keepdims=True)))
    return jnp.dot(probs, values, precision=lax.Precision.HIGHEST)

def layer(stream_in, wqkv, wo, wgu, wd, gain_attn, gain_ffn, cosine, sine):
    tokens = stream_in.shape[0]
    normed = low(normalize(stream_in, gain_attn))
    qkv = low_back(jnp.einsum('td,djc->tjc', normed, wqkv, precision=lax.Precision.HIGHEST))
    qkv = qkv.reshape(tokens, KVH, GROUP + 2, HEAD)
    queries = low(rope_turn(qkv[:, :, :GROUP], cosine[:, None, None], sine[:, None, None]))
    keys = low(rope_turn(qkv[:, :, GROUP], cosine[:, None], sine[:, None]))
    values = low(qkv[:, :, GROUP + 1])
    head_q = jnp.transpose(queries, (1, 2, 0, 3)).reshape(HQ, tokens, HEAD)
    head_k = jnp.repeat(jnp.transpose(keys, (1, 0, 2)), GROUP, axis=0)
    head_v = jnp.repeat(jnp.transpose(values, (1, 0, 2)), GROUP, axis=0)
    mixed = lax.map(jax.checkpoint(one_head), (head_q, head_k, head_v))
    mixed = jnp.transpose(mixed, (1, 0, 2))
    mixed = low(low_back(mixed.reshape(tokens, HQ * HEAD)))
    hidden_in = stream_in + low_back(jnp.einsum('tj,dj->td', mixed, wo, precision=lax.Precision.HIGHEST))
    hnormed = low(normalize(hidden_in, gain_ffn))
    gate_up = low_back(jnp.einsum('td,dcf->tcf', hnormed, wgu, precision=lax.Precision.HIGHEST))
    active = low(jax.nn.silu(gate_up[:, 0]) * gate_up[:, 1])
    return hidden_in + low_back(jnp.einsum('tf,df->td', active, wd, precision=lax.Precision.HIGHEST))

def reference(stream, grad_out, wqkv, wo, wgu, wd, gain_attn, gain_ffn):
    inputs = tuple((item.astype(jnp.float32) for item in (stream, wqkv, wo, wgu, wd, gain_attn, gain_ffn)))
    position = (jnp.arange(TOKENS, dtype=jnp.int32) % SEQ).astype(jnp.float32)
    freq = THETA ** (-(jnp.arange(HEAD // 2, dtype=jnp.float32) * 2.0 / HEAD))
    angle = position[:, None] * freq[None, :]
    cosine = jnp.cos(angle)
    sine = jnp.sin(angle)

    def forward(start, wqkv_all, wo_all, wgu_all, wd_all, attn_all, ffn_all):
        current = start
        for index in range(LAYERS):
            current = layer(current, wqkv_all[index], wo_all[index], wgu_all[index], wd_all[index], attn_all[index], ffn_all[index], cosine, sine)
        return current
    result, pull = jax.vjp(forward, *inputs)
    grads = pull(grad_out.astype(jnp.float32))
    return (result, grads[0], grads[1], grads[2], grads[3], grads[4], grads[5], grads[6])
```

```python
import math

import jax
import jax.numpy as jnp
from jax import lax
from jax.sharding import Mesh
from jax.sharding import PartitionSpec as P

D = 2048
HEAD = 64
GROUP = 8


EPS = 1e-05
THETA = 10000.0


def rope_turn(tensor, cosine, sine):
    half = tensor.shape[-1] // 2
    first = tensor[..., :half]
    second = tensor[..., half:]
    return jnp.concatenate(
        [first * cosine - second * sine, second * cosine + first * sine], axis=-1
    )


def feature_sum(values):
    return lax.psum(values, "col")


def gather_features(rows_in):
    return lax.all_gather(rows_in, "col", axis=1, tiled=True)


def sum_features(partials):
    return lax.psum_scatter(
        partials.astype(jnp.bfloat16), "col", scatter_dimension=1, tiled=True
    ).astype(jnp.float32)


def add_rows(left, piece):
    return jnp.dot(left, piece, preferred_element_type=jnp.float32)


def project_in(left, shard):
    return add_rows(left, lax.all_gather(shard, "row", axis=0, tiled=True))


def columns_of(left, piece):
    return jnp.einsum("tj,dj->td", left, piece, preferred_element_type=jnp.float32)


def project_out(left, shard):
    return columns_of(left, lax.all_gather(shard, "row", axis=0, tiled=True))


def weight_grad(left, right):
    return lax.psum_scatter(
        lax.dot_general(
            left, right, (((0,), (0,)), ((), ())), preferred_element_type=jnp.float32
        ).astype(jnp.bfloat16),
        "row",
        scatter_dimension=0,
        tiled=True,
    ).astype(jnp.float32)


def norm_forward(values, gain):
    total = feature_sum(jnp.sum(values * values, axis=1))
    factor = lax.rsqrt(total / D + EPS)
    normed = values * factor[:, None]
    return (normed, factor, (normed * gain).astype(jnp.bfloat16))


def norm_backward(grad_normed, normed, factor, gain):
    scaled = grad_normed * gain
    inner = feature_sum(jnp.sum(scaled * normed, axis=1))
    grad_in = factor[:, None] * (scaled - normed * (inner / D)[:, None])
    return (grad_in, jnp.sum(grad_normed * normed, axis=0))


def masked_scores(queries, keys, query_pos, key_pos):
    scores = jnp.einsum("qgd,kd->gqk", queries, keys, preferred_element_type=jnp.float32) * (
        1.0 / math.sqrt(queries.shape[-1])
    )
    return jnp.where(key_pos[None, None, :] <= query_pos[None, :, None], scores, -1e30)


def local(stream, grad_out, wqkv, wo, wgu, wd, gain_attn, gain_ffn):
    tok = stream.shape[0]
    layers = wqkv.shape[0]
    count_rows = wqkv.shape[1]
    head = HEAD
    query_cols = GROUP * head
    seq_len = lax.axis_size("row") * tok
    query_pos = lax.axis_index("row") * tok + jnp.arange(tok, dtype=jnp.int32)
    key_pos = jnp.arange(seq_len, dtype=jnp.int32)
    freq = THETA ** (-(jnp.arange(head // 2, dtype=jnp.float32) * 2.0 / head))
    angle = query_pos.astype(jnp.float32)[:, None] * freq[None, :]
    cosine = jnp.cos(angle)
    sine = jnp.sin(angle)
    saved = []
    current = stream
    for index in range(layers):
        weight_qkv = wqkv[index].reshape(count_rows, -1)
        weight_out = wo[index]
        weight_gu = wgu[index].reshape(count_rows, -1)
        weight_down = wd[index]
        wholes = (None, None, None, None)
        normed_a, factor_a, xnormed = norm_forward(current, gain_attn[index])
        xfull = gather_features(xnormed)
        qkv = project_in(xfull, weight_qkv)
        queries = rope_turn(
            qkv[:, :query_cols].reshape(tok, GROUP, head), cosine[:, None, :], sine[:, None, :]
        ).astype(jnp.bfloat16)
        keys = rope_turn(qkv[:, query_cols : query_cols + head], cosine, sine).astype(jnp.bfloat16)
        values = qkv[:, query_cols + head :].astype(jnp.bfloat16)
        seqkv = lax.all_gather(jnp.concatenate([keys, values], axis=1), "row", axis=0, tiled=True)
        seq_keys = seqkv[:, :head]
        seq_values = seqkv[:, head:]
        scores = masked_scores(queries, seq_keys, query_pos, key_pos)
        top = jnp.max(scores, axis=2, keepdims=True)
        expo = jnp.exp(scores - top)
        denom = jnp.sum(expo, axis=2, keepdims=True)
        probs = (expo / denom).astype(jnp.bfloat16)
        log_total = top + jnp.log(denom)
        mixed = (
            jnp.einsum("gqk,kd->qgd", probs, seq_values, preferred_element_type=jnp.float32)
            .reshape(tok, query_cols)
            .astype(jnp.bfloat16)
        )
        hidden_in = current + sum_features(project_out(mixed, weight_out))
        normed_f, factor_f, hnormed = norm_forward(hidden_in, gain_ffn[index])
        hfull = gather_features(hnormed)
        gate_up = project_in(hfull, weight_gu)
        hidden_cols = gate_up.shape[1] // 2
        gate = gate_up[:, :hidden_cols]
        upper = gate_up[:, hidden_cols:]
        active = (jax.nn.silu(gate) * upper).astype(jnp.bfloat16)
        current = hidden_in + sum_features(project_out(active, weight_down))
        saved.append(
            (
                weight_qkv,
                weight_out,
                weight_gu,
                weight_down,
                wholes,
                normed_a,
                factor_a,
                xfull,
                queries,
                seq_keys,
                seq_values,
                log_total,
                mixed,
                normed_f,
                factor_f,
                hfull,
                gate,
                upper,
                active,
            )
        )
    grad_now = grad_out
    list_qkv, list_out, list_gu, list_down, list_ga, list_gf = ([], [], [], [], [], [])
    for index in reversed(range(layers)):
        (
            weight_qkv,
            weight_out,
            weight_gu,
            weight_down,
            wholes,
            normed_a,
            factor_a,
            xfull,
            queries,
            seq_keys,
            seq_values,
            log_total,
            mixed,
            normed_f,
            factor_f,
            hfull,
            gate,
            upper,
            active,
        ) = saved[index]
        grad_full = gather_features(grad_now.astype(jnp.bfloat16))
        grad_active = project_in(grad_full, weight_down)
        list_down.append(weight_grad(grad_full, active))
        sig = jax.nn.sigmoid(gate)
        grad_gate = grad_active * upper * sig * (1.0 + gate * (1.0 - sig))
        grad_up = grad_active * gate * sig
        grad_gu = jnp.concatenate([grad_gate, grad_up], axis=1).astype(jnp.bfloat16)
        grad_hn = sum_features(project_out(grad_gu, weight_gu))
        list_gu.append(weight_grad(hfull, grad_gu).reshape(count_rows, 2, -1))
        grad_mid, gain_f_grad = norm_backward(grad_hn, normed_f, factor_f, gain_ffn[index])
        list_gf.append(gain_f_grad)
        grad_hidden = grad_now + grad_mid
        hidden_full = gather_features(grad_hidden.astype(jnp.bfloat16))
        grad_mixed = project_in(hidden_full, weight_out).astype(jnp.bfloat16)
        list_out.append(weight_grad(hidden_full, mixed))
        grad_heads = grad_mixed.reshape(tok, GROUP, head)
        scores = masked_scores(queries, seq_keys, query_pos, key_pos)
        probs_full = jnp.exp(scores - log_total)
        probs = probs_full.astype(jnp.bfloat16)
        grad_probs = jnp.einsum(
            "qgd,kd->gqk", grad_heads, seq_values, preferred_element_type=jnp.float32
        )
        delta = jnp.sum(probs_full * grad_probs, axis=2, keepdims=True)
        grad_scores = (probs_full * (grad_probs - delta)).astype(jnp.bfloat16)
        inverse = 1.0 / math.sqrt(head)
        grad_queries = (
            jnp.einsum("gqk,kd->qgd", grad_scores, seq_keys, preferred_element_type=jnp.float32)
            * inverse
        )
        grad_keys = (
            jnp.einsum("gqk,qgd->kd", grad_scores, queries, preferred_element_type=jnp.float32)
            * inverse
        )
        grad_values = jnp.einsum(
            "gqk,qgd->kd", probs, grad_heads, preferred_element_type=jnp.float32
        )
        grad_kv = lax.psum_scatter(
            jnp.concatenate([grad_keys, grad_values], axis=1).astype(jnp.bfloat16),
            "row",
            scatter_dimension=0,
            tiled=True,
        ).astype(jnp.float32)
        grad_k = rope_turn(grad_kv[:, :head], cosine, -sine)
        grad_v = grad_kv[:, head:]
        grad_q = rope_turn(grad_queries, cosine[:, None, :], -sine[:, None, :]).reshape(
            tok, query_cols
        )
        grad_qkv = jnp.concatenate([grad_q, grad_k, grad_v], axis=1).astype(jnp.bfloat16)
        grad_xn = sum_features(project_out(grad_qkv, weight_qkv))
        list_qkv.append(weight_grad(xfull, grad_qkv).reshape(count_rows, 1, -1))
        grad_in, gain_a_grad = norm_backward(grad_xn, normed_a, factor_a, gain_attn[index])
        list_ga.append(gain_a_grad)
        grad_now = grad_hidden + grad_in
    gains_a, gains_f = lax.psum((jnp.stack(list_ga[::-1]), jnp.stack(list_gf[::-1])), "row")
    return (
        current,
        grad_now,
        jnp.stack(list_qkv[::-1]),
        jnp.stack(list_out[::-1]),
        jnp.stack(list_gu[::-1]),
        jnp.stack(list_down[::-1]),
        gains_a,
        gains_f,
    )


def share_out(mesh):
    rows, cols = mesh.shape["row"], mesh.shape["col"]
    return Mesh(
        mesh.devices.reshape(rows // 2, 2, cols // 2, 2), ("z", "x", "y", "c")
    )


GRID = ("y", "c")


def swap_grid(values, depth):
    width = lax.axis_size("c")
    pairs = [(z * depth + g, g * depth + z) for z in range(depth) for g in range(depth)]
    return lax.ppermute(values, ("z", "y", "c"), pairs)


def gather_grid(rows_in):
    return lax.all_gather(rows_in, GRID, axis=0, tiled=True)


def sum_grid(partials):
    return lax.psum_scatter(
        partials.astype(jnp.bfloat16), GRID, scatter_dimension=0, tiled=True
    ).astype(jnp.float32)


def gather_line(rows_in):
    return lax.all_gather(rows_in, "z", axis=0, tiled=True)


def sum_line(partials):
    return lax.psum_scatter(
        partials.astype(jnp.bfloat16), "z", scatter_dimension=0, tiled=True
    ).astype(jnp.float32)


def pair_grad(left, right):
    return lax.psum_scatter(
        lax.dot_general(
            left, right, (((0,), (0,)), ((), ())), preferred_element_type=jnp.float32
        ).astype(jnp.bfloat16),
        "x",
        scatter_dimension=0,
        tiled=True,
    ).astype(jnp.float32)


def line_norm(values, gain):
    total = lax.psum(jnp.sum(values * values, axis=1), "z")
    factor = lax.rsqrt(total / D + EPS)
    normed = values * factor[:, None]
    return (normed, factor, (normed * gain).astype(jnp.bfloat16))


def line_norm_back(grad_normed, normed, factor, gain):
    scaled = grad_normed * gain
    inner = lax.psum(jnp.sum(scaled * normed, axis=1), "z")
    grad_in = factor[:, None] * (scaled - normed * (inner / D)[:, None])
    return (grad_in, jnp.sum(grad_normed * normed, axis=0))


def times_t(left, piece):
    return jnp.einsum("tj,dj->td", left, piece, preferred_element_type=jnp.float32)


def stationary(stream, grad_out, wqkv, wo, wgu, wd, gain_attn, gain_ffn):
    tok = stream.shape[0]
    layers = wqkv.shape[0]
    count_rows = wqkv.shape[1]
    depth = lax.axis_size("z")
    head = HEAD
    query_cols = GROUP * head
    inverse = 1.0 / math.sqrt(head)
    row = lax.axis_index("z") * 2 + lax.axis_index("x")
    query_pos = row * tok + jnp.arange(tok, dtype=jnp.int32)
    key_pos = jnp.arange(2 * depth * tok, dtype=jnp.int32)
    freq = THETA ** (-(jnp.arange(head // 2, dtype=jnp.float32) * 2.0 / head))
    angle = query_pos.astype(jnp.float32)[:, None] * freq[None, :]
    cosine = jnp.cos(angle)
    sine = jnp.sin(angle)
    whole = lambda shard: lax.all_gather(shard, "x", axis=0, tiled=True)
    current = swap_grid(stream, depth)
    grad_now = swap_grid(grad_out, depth)
    gain_a = swap_grid(gain_attn, depth)
    gain_f = swap_grid(gain_ffn, depth)
    saved = []
    for index in range(layers):
        weight_qkv = whole(wqkv[index].reshape(count_rows, -1))
        weight_out = whole(wo[index])
        weight_gu = whole(wgu[index].reshape(count_rows, -1))
        weight_down = whole(wd[index])
        normed_a, factor_a, xnormed = line_norm(current, gain_a[index])
        xfull = gather_grid(xnormed)
        qkv = sum_line(add_rows(xfull, weight_qkv))
        queries = rope_turn(
            qkv[:, :query_cols].reshape(tok, GROUP, head), cosine[:, None, :], sine[:, None, :]
        ).astype(jnp.bfloat16)
        keys = rope_turn(qkv[:, query_cols : query_cols + head], cosine, sine).astype(jnp.bfloat16)
        values = qkv[:, query_cols + head :].astype(jnp.bfloat16)
        seqkv = lax.all_gather(
            jnp.concatenate([keys, values], axis=1), ("z", "x"), axis=0, tiled=True
        )
        seq_keys = seqkv[:, :head]
        seq_values = seqkv[:, head:]
        scores = masked_scores(queries, seq_keys, query_pos, key_pos)
        top = jnp.max(scores, axis=2, keepdims=True)
        expo = jnp.exp(scores - top)
        denom = jnp.sum(expo, axis=2, keepdims=True)
        probs = (expo / denom).astype(jnp.bfloat16)
        log_total = top + jnp.log(denom)
        mixed = (
            jnp.einsum("gqk,kd->qgd", probs, seq_values, preferred_element_type=jnp.float32)
            .reshape(tok, query_cols)
            .astype(jnp.bfloat16)
        )
        mixed_full = gather_line(mixed)
        hidden_in = current + sum_grid(times_t(mixed_full, weight_out))
        normed_f, factor_f, hnormed = line_norm(hidden_in, gain_f[index])
        hfull = gather_grid(hnormed)
        gate_up = sum_line(add_rows(hfull, weight_gu))
        hidden_cols = gate_up.shape[1] // 2
        gate = gate_up[:, :hidden_cols]
        upper = gate_up[:, hidden_cols:]
        active = gather_line((jax.nn.silu(gate) * upper).astype(jnp.bfloat16))
        current = hidden_in + sum_grid(times_t(active, weight_down))
        saved.append(
            (weight_qkv, weight_out, weight_gu, weight_down, normed_a, factor_a, xfull, queries,
             seq_keys, seq_values, log_total, mixed_full, normed_f, factor_f, hfull, gate, upper, active)
        )
    list_qkv, list_out, list_gu, list_down, list_ga, list_gf = ([], [], [], [], [], [])
    for index in reversed(range(layers)):
        (weight_qkv, weight_out, weight_gu, weight_down, normed_a, factor_a, xfull, queries,
         seq_keys, seq_values, log_total, mixed_full, normed_f, factor_f, hfull, gate, upper, active) = saved[index]
        grad_full = gather_grid(grad_now.astype(jnp.bfloat16))
        grad_active = sum_line(add_rows(grad_full, weight_down))
        list_down.append(pair_grad(grad_full, active))
        sig = jax.nn.sigmoid(gate)
        grad_gate = grad_active * upper * sig * (1.0 + gate * (1.0 - sig))
        grad_up = grad_active * gate * sig
        grad_gu = gather_line(jnp.concatenate([grad_gate, grad_up], axis=1).astype(jnp.bfloat16))
        grad_hn = sum_grid(times_t(grad_gu, weight_gu))
        list_gu.append(pair_grad(hfull, grad_gu).reshape(count_rows, 2, -1))
        grad_mid, gain_f_grad = line_norm_back(grad_hn, normed_f, factor_f, gain_f[index])
        list_gf.append(gain_f_grad)
        grad_hidden = grad_now + grad_mid
        hidden_full = gather_grid(grad_hidden.astype(jnp.bfloat16))
        grad_mixed = sum_line(add_rows(hidden_full, weight_out)).astype(jnp.bfloat16)
        list_out.append(pair_grad(hidden_full, mixed_full))
        grad_heads = grad_mixed.reshape(tok, GROUP, head)
        scores = masked_scores(queries, seq_keys, query_pos, key_pos)
        probs_full = jnp.exp(scores - log_total)
        probs = probs_full.astype(jnp.bfloat16)
        grad_probs = jnp.einsum(
            "qgd,kd->gqk", grad_heads, seq_values, preferred_element_type=jnp.float32
        )
        delta = jnp.sum(probs_full * grad_probs, axis=2, keepdims=True)
        grad_scores = (probs_full * (grad_probs - delta)).astype(jnp.bfloat16)
        grad_queries = (
            jnp.einsum("gqk,kd->qgd", grad_scores, seq_keys, preferred_element_type=jnp.float32)
            * inverse
        )
        grad_keys = (
            jnp.einsum("gqk,qgd->kd", grad_scores, queries, preferred_element_type=jnp.float32)
            * inverse
        )
        grad_values = jnp.einsum(
            "gqk,qgd->kd", probs, grad_heads, preferred_element_type=jnp.float32
        )
        grad_kv = lax.psum_scatter(
            jnp.concatenate([grad_keys, grad_values], axis=1).astype(jnp.bfloat16),
            ("z", "x"),
            scatter_dimension=0,
            tiled=True,
        ).astype(jnp.float32)
        grad_k = rope_turn(grad_kv[:, :head], cosine, -sine)
        grad_v = grad_kv[:, head:]
        grad_q = rope_turn(grad_queries, cosine[:, None, :], -sine[:, None, :]).reshape(
            tok, query_cols
        )
        grad_qkv = gather_line(
            jnp.concatenate([grad_q, grad_k, grad_v], axis=1).astype(jnp.bfloat16)
        )
        grad_xn = sum_grid(times_t(grad_qkv, weight_qkv))
        list_qkv.append(pair_grad(xfull, grad_qkv).reshape(count_rows, 1, -1))
        grad_in, gain_a_grad = line_norm_back(grad_xn, normed_a, factor_a, gain_a[index])
        list_ga.append(gain_a_grad)
        grad_now = grad_hidden + grad_in
    gains = lax.psum(jnp.concatenate([jnp.stack(list_ga[::-1]), jnp.stack(list_gf[::-1])]), ("x", "y", "c"))
    gains = swap_grid(gains, depth)
    return (
        swap_grid(current, depth),
        swap_grid(grad_now, depth),
        jnp.stack(list_qkv[::-1]),
        jnp.stack(list_out[::-1]),
        jnp.stack(list_gu[::-1]),
        jnp.stack(list_down[::-1]),
        gains[:layers],
        gains[layers:],
    )


def solution(mesh):
    rows, cols = ("row", "col")
    body = local
    if (mesh.shape["row"], mesh.shape["col"]) == (8, 4):
        mesh = share_out(mesh)
        rows, cols = (("z", "x"), ("y", "c"))
        body = stationary
    in_specs = (
        P(rows, cols),
        P(rows, cols),
        P(None, rows, cols, None),
        P(None, rows, cols),
        P(None, rows, None, cols),
        P(None, rows, cols),
        P(None, cols),
        P(None, cols),
    )
    out_specs = (
        P(rows, cols),
        P(rows, cols),
        P(None, rows, cols, None),
        P(None, rows, cols),
        P(None, rows, None, cols),
        P(None, rows, cols),
        P(None, cols),
        P(None, cols),
    )
    return jax.shard_map(body, mesh=mesh, in_specs=in_specs, out_specs=out_specs, check_vma=False)
```

```python
import math

import jax
import jax.numpy as jnp
from jax import lax
from jax.experimental import pallas as pl
from jax.experimental.pallas import tpu as pltpu
from jax.sharding import Mesh
from jax.sharding import PartitionSpec as P

D = 2048
HEAD = 64
GROUP = 8


EPS = 1e-05
THETA = 10000.0


def rope_turn(tensor, cosine, sine):
    half = tensor.shape[-1] // 2
    first = tensor[..., :half]
    second = tensor[..., half:]
    return jnp.concatenate(
        [first * cosine - second * sine, second * cosine + first * sine], axis=-1
    )


def feature_sum(values):
    return lax.psum(values, "col")


def gather_features(rows_in):
    return lax.all_gather(rows_in, "col", axis=1, tiled=True)


def sum_features(partials):
    return lax.psum_scatter(
        partials.astype(jnp.bfloat16), "col", scatter_dimension=1, tiled=True
    ).astype(jnp.float32)


def add_rows(left, piece):
    return jnp.dot(left, piece, preferred_element_type=jnp.float32)


def project_in(left, shard):
    return add_rows(left, lax.all_gather(shard, "row", axis=0, tiled=True))


def columns_of(left, piece):
    return jnp.einsum("tj,dj->td", left, piece, preferred_element_type=jnp.float32)


def project_out(left, shard):
    return columns_of(left, lax.all_gather(shard, "row", axis=0, tiled=True))


def weight_grad(left, right):
    return lax.psum_scatter(
        lax.dot_general(
            left, right, (((0,), (0,)), ((), ())), preferred_element_type=jnp.float32
        ).astype(jnp.bfloat16),
        "row",
        scatter_dimension=0,
        tiled=True,
    ).astype(jnp.float32)


def norm_forward(values, gain):
    total = feature_sum(jnp.sum(values * values, axis=1))
    factor = lax.rsqrt(total / D + EPS)
    normed = values * factor[:, None]
    return (normed, factor, (normed * gain).astype(jnp.bfloat16))


def norm_backward(grad_normed, normed, factor, gain):
    scaled = grad_normed * gain
    inner = feature_sum(jnp.sum(scaled * normed, axis=1))
    grad_in = factor[:, None] * (scaled - normed * (inner / D)[:, None])
    return (grad_in, jnp.sum(grad_normed * normed, axis=0))


def masked_scores(queries, keys, query_pos, key_pos):
    scores = jnp.einsum("qgd,kd->gqk", queries, keys, preferred_element_type=jnp.float32) * (
        1.0 / math.sqrt(queries.shape[-1])
    )
    return jnp.where(key_pos[None, None, :] <= query_pos[None, :, None], scores, -1e30)


def local(stream, grad_out, wqkv, wo, wgu, wd, gain_attn, gain_ffn):
    tok = stream.shape[0]
    layers = wqkv.shape[0]
    count_rows = wqkv.shape[1]
    head = HEAD
    query_cols = GROUP * head
    seq_len = lax.axis_size("row") * tok
    query_pos = lax.axis_index("row") * tok + jnp.arange(tok, dtype=jnp.int32)
    key_pos = jnp.arange(seq_len, dtype=jnp.int32)
    freq = THETA ** (-(jnp.arange(head // 2, dtype=jnp.float32) * 2.0 / head))
    angle = query_pos.astype(jnp.float32)[:, None] * freq[None, :]
    cosine = jnp.cos(angle)
    sine = jnp.sin(angle)
    saved = []
    current = stream
    for index in range(layers):
        weight_qkv = wqkv[index].reshape(count_rows, -1)
        weight_out = wo[index]
        weight_gu = wgu[index].reshape(count_rows, -1)
        weight_down = wd[index]
        wholes = (None, None, None, None)
        normed_a, factor_a, xnormed = norm_forward(current, gain_attn[index])
        xfull = gather_features(xnormed)
        qkv = project_in(xfull, weight_qkv)
        queries = rope_turn(
            qkv[:, :query_cols].reshape(tok, GROUP, head), cosine[:, None, :], sine[:, None, :]
        ).astype(jnp.bfloat16)
        keys = rope_turn(qkv[:, query_cols : query_cols + head], cosine, sine).astype(jnp.bfloat16)
        values = qkv[:, query_cols + head :].astype(jnp.bfloat16)
        seqkv = lax.all_gather(jnp.concatenate([keys, values], axis=1), "row", axis=0, tiled=True)
        seq_keys = seqkv[:, :head]
        seq_values = seqkv[:, head:]
        scores = masked_scores(queries, seq_keys, query_pos, key_pos)
        top = jnp.max(scores, axis=2, keepdims=True)
        expo = jnp.exp(scores - top)
        denom = jnp.sum(expo, axis=2, keepdims=True)
        probs = (expo / denom).astype(jnp.bfloat16)
        log_total = top + jnp.log(denom)
        mixed = (
            jnp.einsum("gqk,kd->qgd", probs, seq_values, preferred_element_type=jnp.float32)
            .reshape(tok, query_cols)
            .astype(jnp.bfloat16)
        )
        hidden_in = current + sum_features(project_out(mixed, weight_out))
        normed_f, factor_f, hnormed = norm_forward(hidden_in, gain_ffn[index])
        hfull = gather_features(hnormed)
        gate_up = project_in(hfull, weight_gu)
        hidden_cols = gate_up.shape[1] // 2
        gate = gate_up[:, :hidden_cols]
        upper = gate_up[:, hidden_cols:]
        active = (jax.nn.silu(gate) * upper).astype(jnp.bfloat16)
        current = hidden_in + sum_features(project_out(active, weight_down))
        saved.append(
            (
                weight_qkv,
                weight_out,
                weight_gu,
                weight_down,
                wholes,
                normed_a,
                factor_a,
                xfull,
                queries,
                seq_keys,
                seq_values,
                log_total,
                mixed,
                normed_f,
                factor_f,
                hfull,
                gate,
                upper,
                active,
            )
        )
    grad_now = grad_out
    list_qkv, list_out, list_gu, list_down, list_ga, list_gf = ([], [], [], [], [], [])
    for index in reversed(range(layers)):
        (
            weight_qkv,
            weight_out,
            weight_gu,
            weight_down,
            wholes,
            normed_a,
            factor_a,
            xfull,
            queries,
            seq_keys,
            seq_values,
            log_total,
            mixed,
            normed_f,
            factor_f,
            hfull,
            gate,
            upper,
            active,
        ) = saved[index]
        grad_full = gather_features(grad_now.astype(jnp.bfloat16))
        grad_active = project_in(grad_full, weight_down)
        list_down.append(weight_grad(grad_full, active))
        sig = jax.nn.sigmoid(gate)
        grad_gate = grad_active * upper * sig * (1.0 + gate * (1.0 - sig))
        grad_up = grad_active * gate * sig
        grad_gu = jnp.concatenate([grad_gate, grad_up], axis=1).astype(jnp.bfloat16)
        grad_hn = sum_features(project_out(grad_gu, weight_gu))
        list_gu.append(weight_grad(hfull, grad_gu).reshape(count_rows, 2, -1))
        grad_mid, gain_f_grad = norm_backward(grad_hn, normed_f, factor_f, gain_ffn[index])
        list_gf.append(gain_f_grad)
        grad_hidden = grad_now + grad_mid
        hidden_full = gather_features(grad_hidden.astype(jnp.bfloat16))
        grad_mixed = project_in(hidden_full, weight_out).astype(jnp.bfloat16)
        list_out.append(weight_grad(hidden_full, mixed))
        grad_heads = grad_mixed.reshape(tok, GROUP, head)
        scores = masked_scores(queries, seq_keys, query_pos, key_pos)
        probs_full = jnp.exp(scores - log_total)
        probs = probs_full.astype(jnp.bfloat16)
        grad_probs = jnp.einsum(
            "qgd,kd->gqk", grad_heads, seq_values, preferred_element_type=jnp.float32
        )
        delta = jnp.sum(probs_full * grad_probs, axis=2, keepdims=True)
        grad_scores = (probs_full * (grad_probs - delta)).astype(jnp.bfloat16)
        inverse = 1.0 / math.sqrt(head)
        grad_queries = (
            jnp.einsum("gqk,kd->qgd", grad_scores, seq_keys, preferred_element_type=jnp.float32)
            * inverse
        )
        grad_keys = (
            jnp.einsum("gqk,qgd->kd", grad_scores, queries, preferred_element_type=jnp.float32)
            * inverse
        )
        grad_values = jnp.einsum(
            "gqk,qgd->kd", probs, grad_heads, preferred_element_type=jnp.float32
        )
        grad_kv = lax.psum_scatter(
            jnp.concatenate([grad_keys, grad_values], axis=1).astype(jnp.bfloat16),
            "row",
            scatter_dimension=0,
            tiled=True,
        ).astype(jnp.float32)
        grad_k = rope_turn(grad_kv[:, :head], cosine, -sine)
        grad_v = grad_kv[:, head:]
        grad_q = rope_turn(grad_queries, cosine[:, None, :], -sine[:, None, :]).reshape(
            tok, query_cols
        )
        grad_qkv = jnp.concatenate([grad_q, grad_k, grad_v], axis=1).astype(jnp.bfloat16)
        grad_xn = sum_features(project_out(grad_qkv, weight_qkv))
        list_qkv.append(weight_grad(xfull, grad_qkv).reshape(count_rows, 1, -1))
        grad_in, gain_a_grad = norm_backward(grad_xn, normed_a, factor_a, gain_attn[index])
        list_ga.append(gain_a_grad)
        grad_now = grad_hidden + grad_in
    gains_a, gains_f = lax.psum((jnp.stack(list_ga[::-1]), jnp.stack(list_gf[::-1])), "row")
    return (
        current,
        grad_now,
        jnp.stack(list_qkv[::-1]),
        jnp.stack(list_out[::-1]),
        jnp.stack(list_gu[::-1]),
        jnp.stack(list_down[::-1]),
        gains_a,
        gains_f,
    )


def share_out(mesh):
    rows, cols = mesh.shape["row"], mesh.shape["col"]
    return Mesh(
        mesh.devices.reshape(rows // 2, 2, cols // 2, 2), ("z", "x", "y", "c")
    )


GRID = ("y", "c")


def swap_grid(values, depth):
    width = lax.axis_size("c")
    pairs = [(z * depth + g, g * depth + z) for z in range(depth) for g in range(depth)]
    return lax.ppermute(values, ("z", "y", "c"), pairs)


def gather_grid(rows_in):
    return lax.all_gather(rows_in, GRID, axis=0, tiled=True)


def sum_grid(partials):
    return lax.psum_scatter(
        partials.astype(jnp.bfloat16), GRID, scatter_dimension=0, tiled=True
    ).astype(jnp.float32)


def gather_line(rows_in):
    return lax.all_gather(rows_in, "z", axis=0, tiled=True)


def sum_line(partials):
    return lax.psum_scatter(
        partials.astype(jnp.bfloat16), "z", scatter_dimension=0, tiled=True
    ).astype(jnp.float32)


def pair_grad(left, right):
    return lax.psum_scatter(
        lax.dot_general(
            left, right, (((0,), (0,)), ((), ())), preferred_element_type=jnp.float32
        ).astype(jnp.bfloat16),
        "x",
        scatter_dimension=0,
        tiled=True,
    ).astype(jnp.float32)


def line_norm(values, gain):
    total = lax.psum(jnp.sum(values * values, axis=1), "z")
    factor = lax.rsqrt(total / D + EPS)
    normed = values * factor[:, None]
    return (normed, factor, (normed * gain).astype(jnp.bfloat16))


def line_norm_back(grad_normed, normed, factor, gain):
    scaled = grad_normed * gain
    inner = lax.psum(jnp.sum(scaled * normed, axis=1), "z")
    grad_in = factor[:, None] * (scaled - normed * (inner / D)[:, None])
    return (grad_in, jnp.sum(grad_normed * normed, axis=0))


def times_t(left, piece):
    return jnp.einsum("tj,dj->td", left, piece, preferred_element_type=jnp.float32)


MESH_ID = pl.DeviceIdType.MESH
ROWS = 16
SKEW = 2
GROUP_CHUNKS = 4
EXTRA = 128


def spread(column):
    high = column.astype(jnp.bfloat16)
    low = (column - high.astype(jnp.float32)).astype(jnp.bfloat16)
    lane = lax.broadcasted_iota(jnp.int32, (column.shape[0], EXTRA), 1)
    wide = jnp.where(lane == 0, high.astype(jnp.float32), jnp.where(lane == 1, low.astype(jnp.float32), 0.0))
    return wide.astype(jnp.bfloat16)


def unspread(block):
    return jnp.sum(block.astype(jnp.float32), axis=1, keepdims=True)


def transposed_dot(left, right):
    return lax.dot_general(left, right, (((1,), (1,)), ((), ())), preferred_element_type=jnp.float32)


class Line:
    def __init__(self, tok, depth):
        self.z, self.x = lax.axis_index("z"), lax.axis_index("x")
        self.y, self.c = lax.axis_index("y"), lax.axis_index("c")
        self.tok, self.depth = tok, depth
        self.half = 2 * tok
        self.chunks = self.half // ROWS
        self.own = pl.multiple_of((2 * self.y + self.c) * tok, tok)
        self.peers = (
            {"y": self.y, "c": 1 - self.c},
            {"y": 1 - self.y, "c": self.c},
            {"y": 1 - self.y, "c": 1 - self.c},
        )

    def greet(self):
        barrier = pltpu.get_barrier_semaphore()
        for peer in self.peers:
            pl.semaphore_signal(barrier, 1, device_id=peer, device_id_type=MESH_ID)

        @pl.when(self.z > 0)
        def _():
            pl.semaphore_signal(barrier, 1, device_id={"z": self.z - 1}, device_id_type=MESH_ID)

        @pl.when(self.z < self.depth - 1)
        def _():
            pl.semaphore_signal(barrier, 1, device_id={"z": self.z + 1}, device_id_type=MESH_ID)

        inner = jnp.where(self.z > 0, 1, 0) + jnp.where(self.z < self.depth - 1, 1, 0)
        pl.semaphore_wait(barrier, 3 + inner)

    def place(self, stream):
        return self.z if stream == 0 else self.depth - 1 - self.z

    def onward(self, stream):
        return {"z": self.z + 1} if stream == 0 else {"z": self.z - 1}

    def backward(self, stream):
        return {"z": self.z - 1} if stream == 0 else {"z": self.z + 1}

    def row_of(self, stream, chunk):
        per = self.chunks // 2
        far = chunk // per
        y = self.y + far * (1 - 2 * self.y)
        return pl.multiple_of((2 * y + stream) * self.tok + lax.rem(chunk, per) * ROWS, ROWS)


def make_line(tok, depth, width_in, width_out, carry_in, carry_out, features):
    chunks = 2 * tok // ROWS
    groups = chunks // GROUP_CHUNKS
    span = GROUP_CHUNKS * ROWS
    half_groups = groups // 2

    def run(line, taken, prepare, finish, second, close, product, carried, chain_out, chain_in, wide, own_part, rs_out, rs_in,
            ag_s, ag_r, ch_s, ch_r, bc_s, bc_r, rs_s, rs_r):
        line.greet()
        gather = [
            pltpu.make_async_remote_copy(
                src_ref=taken.at[pl.ds(line.own, tok)],
                dst_ref=taken.at[pl.ds(line.own, tok)],
                send_sem=ag_s.at[at],
                recv_sem=ag_r.at[at],
                device_id=peer,
                device_id_type=MESH_ID,
            )
            for at, peer in enumerate(line.peers)
        ]
        for copy in gather:
            copy.start()
        gather[0].wait_recv()
        prepare(pl.multiple_of(line.y * 2 * tok, 2 * tok))

        def chain_copy(stream, chunk):
            return pltpu.make_async_remote_copy(
                src_ref=chain_out.at[stream, chunk],
                dst_ref=chain_in.at[stream, chunk],
                send_sem=ch_s.at[stream, chunk],
                recv_sem=ch_r.at[stream, chunk],
                device_id=line.onward(stream),
                device_id_type=MESH_ID,
            )

        def wide_copy(stream, chunk):
            rows = pl.ds(line.row_of(stream, chunk), ROWS)
            return pltpu.make_async_remote_copy(
                src_ref=wide.at[rows],
                dst_ref=wide.at[rows],
                send_sem=bc_s.at[stream, chunk],
                recv_sem=bc_r.at[stream, chunk],
                device_id=line.backward(stream),
                device_id_type=MESH_ID,
            )

        def sum_copy(stream, group):
            far = group // half_groups
            y = line.y + far * (1 - 2 * line.y)
            other = stream + line.c - 2 * stream * line.c
            slot = 2 * far + other - 1
            part = lax.rem(group, half_groups)
            return (slot >= 0, part, pltpu.make_async_remote_copy(
                src_ref=rs_out.at[stream, group],
                dst_ref=rs_in.at[jnp.maximum(slot, 0), pl.ds(pl.multiple_of(part * span, span), span)],
                send_sem=rs_s.at[stream, group],
                recv_sem=rs_r.at[jnp.maximum(slot, 0), part],
                device_id={"y": y, "c": stream},
                device_id_type=MESH_ID,
            ))

        def step(i, _):
            @pl.when(i == SKEW)
            def _():
                gather[1].wait_recv()
                gather[2].wait_recv()
                prepare(pl.multiple_of((1 - line.y) * 2 * tok, 2 * tok))

            for stream in (0, 1):
                place = line.place(stream)
                chunk = i - SKEW * place

                @pl.when((chunk >= 0) & (chunk < chunks))
                def _():
                    row = line.row_of(stream, chunk)

                    @pl.when(place > 0)
                    def _():
                        chain_copy(stream, chunk).wait_recv()

                    @pl.when(place == 0)
                    def _():
                        chain_out[stream, chunk, :, :width_in] = product[pl.ds(row, ROWS), :].astype(jnp.bfloat16)
                        if carry_in:
                            chain_out[stream, chunk, :, width_in:] = spread(carried[pl.ds(row, ROWS), :1])

                    @pl.when((place > 0) & (place < depth - 1))
                    def _():
                        chain_out[stream, chunk, :, :width_in] = (
                            product[pl.ds(row, ROWS), :] + chain_in[stream, chunk, :, :width_in].astype(jnp.float32)
                        ).astype(jnp.bfloat16)
                        if carry_in:
                            chain_out[stream, chunk, :, width_in:] = spread(
                                carried[pl.ds(row, ROWS), :1] + unspread(chain_in[stream, chunk, :, width_in:])
                            )

                    @pl.when(place < depth - 1)
                    def _():
                        chain_copy(stream, chunk).start()

                    @pl.when(place == depth - 1)
                    def _():
                        total = product[pl.ds(row, ROWS), :] + chain_in[stream, chunk, :, :width_in].astype(jnp.float32)
                        extra = None
                        if carry_in:
                            extra = carried[pl.ds(row, ROWS), :1] + unspread(chain_in[stream, chunk, :, width_in:])
                        finish(row, pl.multiple_of(chunk * ROWS, ROWS), total, extra)
                        wide_copy(stream, chunk).start()

                ready = i - SKEW * (2 * (depth - 1) - place)

                @pl.when((ready >= 0) & (ready < chunks))
                def _():
                    @pl.when(place < depth - 1)
                    def _():
                        wide_copy(stream, ready).wait_recv()

                        @pl.when(place > 0)
                        def _():
                            wide_copy(stream, ready).start()

                    @pl.when(lax.rem(ready, GROUP_CHUNKS) == GROUP_CHUNKS - 1)
                    def _():
                        group = ready // GROUP_CHUNKS
                        row = pl.multiple_of(line.row_of(stream, ready) - (span - ROWS), span)
                        away, part, copy = sum_copy(stream, group)
                        value = second(row, span)

                        @pl.when(away)
                        def _():
                            rs_out[stream, group, :, :features] = value.astype(jnp.bfloat16)
                            if carry_out:
                                rs_out[stream, group, :, features:] = wide[pl.ds(row, span), width_out:]
                            copy.start()

                        @pl.when(jnp.logical_not(away))
                        def _():
                            own_part[pl.ds(pl.multiple_of(part * span, span), span), :] = value

            return 0

        lax.fori_loop(0, chunks + 2 * SKEW * (depth - 1), step, 0)

        def drain(i, _):
            for stream in (0, 1):
                place = line.place(stream)

                @pl.when(place < depth - 1)
                def _():
                    chain_copy(stream, i).wait_send()

                @pl.when(place > 0)
                def _():
                    wide_copy(stream, i).wait_send()

            return 0

        def drain_sums(i, _):
            for stream in (0, 1):
                away, part, copy = sum_copy(stream, i)

                @pl.when(away)
                def _():
                    copy.wait_send()
            return 0

        for slot in range(3):
            for part in range(half_groups):
                pltpu.make_async_remote_copy(
                    src_ref=rs_out.at[0, 0],
                    dst_ref=rs_in.at[slot, pl.ds(part * span, span)],
                    send_sem=rs_s.at[0, 0],
                    recv_sem=rs_r.at[slot, part],
                    device_id=line.peers[slot],
                    device_id_type=MESH_ID,
                ).wait_recv()
        close()
        for copy in gather:
            copy.wait_send()
        lax.fori_loop(0, chunks, drain, 0)
        lax.fori_loop(0, groups, drain_sums, 0)

    wide_in = width_in + (EXTRA if carry_in else 0)
    scratch = [
        pltpu.VMEM((4 * tok, width_in), jnp.float32),
        pltpu.VMEM((4 * tok, EXTRA), jnp.float32),
        pltpu.VMEM((2, chunks, ROWS, wide_in), jnp.bfloat16),
        pltpu.VMEM((2, chunks, ROWS, wide_in), jnp.bfloat16),
        pltpu.VMEM((tok, features), jnp.float32),
        pltpu.VMEM((2, groups, span, features + (EXTRA if carry_out else 0)), jnp.bfloat16),
        pltpu.VMEM((3, tok, features + (EXTRA if carry_out else 0)), jnp.bfloat16),
        pltpu.SemaphoreType.DMA((3,)),
        pltpu.SemaphoreType.DMA((3,)),
        pltpu.SemaphoreType.DMA((2, chunks)),
        pltpu.SemaphoreType.DMA((2, chunks)),
        pltpu.SemaphoreType.DMA((2, chunks)),
        pltpu.SemaphoreType.DMA((2, chunks)),
        pltpu.SemaphoreType.DMA((2, groups)),
        pltpu.SemaphoreType.DMA((3, half_groups)),
    ]
    return run, scratch


TILE = 256


def ffn_forward(hidden, gain, weight_gu, weight_down, depth):
    tok, features = hidden.shape
    width = weight_down.shape[1]
    run, scratch = make_line(tok, depth, 2 * width, width, True, False, features)

    def kernel(h_ref, gain_ref, w1_ref, w2_ref, out_ref, taken, kept, wide, scaled, product, carried, chain_out, chain_in,
               own_part, rs_out, rs_in, *sems):
        line = Line(tok, depth)
        taken[pl.ds(line.own, tok), :] = h_ref[...].astype(jnp.bfloat16)

        def prepare(row):
            rows = pl.ds(row, 2 * tok)
            block = taken[rows, :].astype(jnp.float32)
            carried[rows, :] = jnp.broadcast_to(jnp.sum(block * block, axis=1, keepdims=True), (2 * tok, EXTRA))
            scaled[...] = (block * gain_ref[...]).astype(jnp.bfloat16)

            def tile(j, _):
                cols = pl.ds(pl.multiple_of(j * TILE, TILE), TILE)
                product[rows, cols] = jnp.dot(scaled[...], w1_ref[:, cols], preferred_element_type=jnp.float32)
                return 0

            lax.fori_loop(0, 2 * width // TILE, tile, 0)

        def finish(row, at, total, extra):
            factor = lax.rsqrt(extra / D + EPS)
            gate = total[:, :width] * factor
            upper = total[:, width:] * factor
            kept[pl.ds(at, ROWS), :width] = gate
            kept[pl.ds(at, ROWS), width:] = upper
            active = gate * jax.nn.sigmoid(gate) * upper
            wide[pl.ds(row, ROWS), :width] = active.astype(jnp.bfloat16)
            wide[pl.ds(row, ROWS), width:] = spread(factor)

        def second(row, span):
            return transposed_dot(wide[pl.ds(row, span), :width], w2_ref[...])

        def close():
            total = own_part[...]
            for slot in range(3):
                total = total + rs_in[slot].astype(jnp.float32)
            out_ref[...] = h_ref[...] + total

        run(line, taken, prepare, finish, second, close, product, carried, chain_out, chain_in, wide, own_part, rs_out, rs_in,
            *sems)

    shapes = (
        jax.ShapeDtypeStruct((tok, features), jnp.float32),
        jax.ShapeDtypeStruct((4 * tok, features), jnp.bfloat16),
        jax.ShapeDtypeStruct((2 * tok, 2 * width), jnp.float32),
        jax.ShapeDtypeStruct((4 * tok, width + EXTRA), jnp.bfloat16),
    )
    return pl.pallas_call(
        kernel,
        out_shape=shapes,
        in_specs=[pl.BlockSpec(memory_space=pltpu.VMEM)] * 4,
        out_specs=[pl.BlockSpec(memory_space=pltpu.VMEM)] * 4,
        scratch_shapes=[pltpu.VMEM((2 * tok, features), jnp.bfloat16)] + scratch,
        compiler_params=pltpu.CompilerParams(collective_id=1, has_side_effects=True, vmem_limit_bytes=60 << 20),
        cost_estimate=pl.CostEstimate(flops=60_000_000_000, bytes_accessed=8_000_000, transcendentals=0),
        name="ffn_forward",
    )(hidden, gain.reshape(1, -1), weight_gu, weight_down)


def ffn_backward(grad, hidden, gain, kept, wide_forward, weight_gu, weight_down, depth):
    tok, features = hidden.shape
    width = weight_down.shape[1]
    run, scratch = make_line(tok, depth, width, 2 * width, False, True, features)

    def kernel(dy_ref, h_ref, gain_ref, kept_ref, before_ref, w1_ref, w2_ref, out_ref, taken, wide, gain_out, product, carried,
               chain_out, chain_in, own_part, rs_out, rs_in, *sems):
        line = Line(tok, depth)
        taken[pl.ds(line.own, tok), :] = dy_ref[...].astype(jnp.bfloat16)

        def prepare(row):
            rows = pl.ds(row, 2 * tok)

            def tile(j, _):
                cols = pl.ds(pl.multiple_of(j * 128, 128), 128)
                product[rows, cols] = jnp.dot(taken[rows, :], w2_ref[:, cols], preferred_element_type=jnp.float32)
                return 0

            lax.fori_loop(0, width // 128, tile, 0)

        def finish(row, at, total, extra):
            gate = kept_ref[pl.ds(at, ROWS), :width]
            upper = kept_ref[pl.ds(at, ROWS), width:]
            sig = jax.nn.sigmoid(gate)
            silu = gate * sig
            grad_gate = total * upper * (sig + silu * (1.0 - sig))
            grad_up = total * silu
            wide[pl.ds(row, ROWS), :width] = grad_gate.astype(jnp.bfloat16)
            wide[pl.ds(row, ROWS), width : 2 * width] = grad_up.astype(jnp.bfloat16)
            inner = jnp.sum(grad_gate * gate + grad_up * upper, axis=1, keepdims=True)
            wide[pl.ds(row, ROWS), 2 * width :] = spread(inner)

        def second(row, span):
            return transposed_dot(wide[pl.ds(row, span), : 2 * width], w1_ref[...])

        def close():
            total = own_part[...]
            inner = unspread(wide[pl.ds(line.own, tok), 2 * width :])
            for slot in range(3):
                total = total + rs_in[slot, :, :features].astype(jnp.float32)
                inner = inner + unspread(rs_in[slot, :, features:])
            factor = unspread(before_ref[pl.ds(line.own, tok), width:])
            normed = h_ref[...] * factor
            gain_out[...] = jnp.broadcast_to(jnp.sum(total * normed, axis=0, keepdims=True), gain_out.shape)
            out_ref[...] = dy_ref[...] + factor * (total * gain_ref[...] - normed * (inner / D))

        run(line, taken, prepare, finish, second, close, product, carried, chain_out, chain_in, wide, own_part, rs_out, rs_in,
            *sems)

    shapes = (
        jax.ShapeDtypeStruct((tok, features), jnp.float32),
        jax.ShapeDtypeStruct((4 * tok, features), jnp.bfloat16),
        jax.ShapeDtypeStruct((4 * tok, 2 * width + EXTRA), jnp.bfloat16),
        jax.ShapeDtypeStruct((8, features), jnp.float32),
    )
    return pl.pallas_call(
        kernel,
        out_shape=shapes,
        in_specs=[pl.BlockSpec(memory_space=pltpu.VMEM)] * 7,
        out_specs=[pl.BlockSpec(memory_space=pltpu.VMEM)] * 4,
        scratch_shapes=scratch,
        compiler_params=pltpu.CompilerParams(collective_id=2, has_side_effects=True, vmem_limit_bytes=60 << 20),
        cost_estimate=pl.CostEstimate(flops=60_000_000_000, bytes_accessed=8_000_000, transcendentals=0),
        name="ffn_backward",
    )(grad, hidden, gain.reshape(1, -1), kept, wide_forward, weight_gu, weight_down)


def stationary(stream, grad_out, wqkv, wo, wgu, wd, gain_attn, gain_ffn):
    tok = stream.shape[0]
    layers = wqkv.shape[0]
    count_rows = wqkv.shape[1]
    depth = lax.axis_size("z")
    head = HEAD
    query_cols = GROUP * head
    inverse = 1.0 / math.sqrt(head)
    row = lax.axis_index("z") * 2 + lax.axis_index("x")
    query_pos = row * tok + jnp.arange(tok, dtype=jnp.int32)
    key_pos = jnp.arange(2 * depth * tok, dtype=jnp.int32)
    freq = THETA ** (-(jnp.arange(head // 2, dtype=jnp.float32) * 2.0 / head))
    angle = query_pos.astype(jnp.float32)[:, None] * freq[None, :]
    cosine = jnp.cos(angle)
    sine = jnp.sin(angle)
    whole = lambda shard: lax.all_gather(shard, "x", axis=0, tiled=True)
    current = swap_grid(stream, depth)
    grad_now = swap_grid(grad_out, depth)
    gain_a = swap_grid(gain_attn, depth)
    gain_f = swap_grid(gain_ffn, depth)
    saved = []
    for index in range(layers):
        weight_qkv = whole(wqkv[index].reshape(count_rows, -1))
        weight_out = whole(wo[index])
        weight_gu = whole(wgu[index].reshape(count_rows, -1))
        weight_down = whole(wd[index])
        normed_a, factor_a, xnormed = line_norm(current, gain_a[index])
        xfull = gather_grid(xnormed)
        qkv = sum_line(add_rows(xfull, weight_qkv))
        queries = rope_turn(
            qkv[:, :query_cols].reshape(tok, GROUP, head), cosine[:, None, :], sine[:, None, :]
        ).astype(jnp.bfloat16)
        keys = rope_turn(qkv[:, query_cols : query_cols + head], cosine, sine).astype(jnp.bfloat16)
        values = qkv[:, query_cols + head :].astype(jnp.bfloat16)
        seqkv = lax.all_gather(
            jnp.concatenate([keys, values], axis=1), ("z", "x"), axis=0, tiled=True
        )
        seq_keys = seqkv[:, :head]
        seq_values = seqkv[:, head:]
        scores = masked_scores(queries, seq_keys, query_pos, key_pos)
        top = jnp.max(scores, axis=2, keepdims=True)
        expo = jnp.exp(scores - top)
        denom = jnp.sum(expo, axis=2, keepdims=True)
        probs = (expo / denom).astype(jnp.bfloat16)
        log_total = top + jnp.log(denom)
        mixed = (
            jnp.einsum("gqk,kd->qgd", probs, seq_values, preferred_element_type=jnp.float32)
            .reshape(tok, query_cols)
            .astype(jnp.bfloat16)
        )
        mixed_full = gather_line(mixed)
        hidden_in = current + sum_grid(times_t(mixed_full, weight_out))
        current, hfull, kept, active = ffn_forward(hidden_in, gain_f[index], weight_gu, weight_down, depth)
        saved.append(
            (weight_qkv, weight_out, weight_gu, weight_down, normed_a, factor_a, xfull, queries,
             seq_keys, seq_values, log_total, mixed_full, hidden_in, hfull, kept, active)
        )
    list_qkv, list_out, list_gu, list_down, list_ga, list_gf = ([], [], [], [], [], [])
    for index in reversed(range(layers)):
        (weight_qkv, weight_out, weight_gu, weight_down, normed_a, factor_a, xfull, queries,
         seq_keys, seq_values, log_total, mixed_full, hidden_in, hfull, kept, active) = saved[index]
        width = weight_down.shape[1]
        grad_hidden, grad_full, grad_gu, gain_f_grad = ffn_backward(
            grad_now, hidden_in, gain_f[index], kept, active, weight_gu, weight_down, depth
        )
        list_down.append(pair_grad(grad_full, active[:, :width]))
        factor_f = jnp.sum(active[:, width:].astype(jnp.float32), axis=1, keepdims=True)
        hnormed = (hfull.astype(jnp.float32) * factor_f * gain_f[index]).astype(jnp.bfloat16)
        list_gu.append(pair_grad(hnormed, grad_gu[:, : 2 * width]).reshape(count_rows, 2, -1))
        list_gf.append(gain_f_grad[0])
        hidden_full = gather_grid(grad_hidden.astype(jnp.bfloat16))
        grad_mixed = sum_line(add_rows(hidden_full, weight_out)).astype(jnp.bfloat16)
        list_out.append(pair_grad(hidden_full, mixed_full))
        grad_heads = grad_mixed.reshape(tok, GROUP, head)
        scores = masked_scores(queries, seq_keys, query_pos, key_pos)
        probs_full = jnp.exp(scores - log_total)
        probs = probs_full.astype(jnp.bfloat16)
        grad_probs = jnp.einsum(
            "qgd,kd->gqk", grad_heads, seq_values, preferred_element_type=jnp.float32
        )
        delta = jnp.sum(probs_full * grad_probs, axis=2, keepdims=True)
        grad_scores = (probs_full * (grad_probs - delta)).astype(jnp.bfloat16)
        grad_queries = (
            jnp.einsum("gqk,kd->qgd", grad_scores, seq_keys, preferred_element_type=jnp.float32)
            * inverse
        )
        grad_keys = (
            jnp.einsum("gqk,qgd->kd", grad_scores, queries, preferred_element_type=jnp.float32)
            * inverse
        )
        grad_values = jnp.einsum(
            "gqk,qgd->kd", probs, grad_heads, preferred_element_type=jnp.float32
        )
        grad_kv = lax.psum_scatter(
            jnp.concatenate([grad_keys, grad_values], axis=1).astype(jnp.bfloat16),
            ("z", "x"),
            scatter_dimension=0,
            tiled=True,
        ).astype(jnp.float32)
        grad_k = rope_turn(grad_kv[:, :head], cosine, -sine)
        grad_v = grad_kv[:, head:]
        grad_q = rope_turn(grad_queries, cosine[:, None, :], -sine[:, None, :]).reshape(
            tok, query_cols
        )
        grad_qkv = gather_line(
            jnp.concatenate([grad_q, grad_k, grad_v], axis=1).astype(jnp.bfloat16)
        )
        grad_xn = sum_grid(times_t(grad_qkv, weight_qkv))
        list_qkv.append(pair_grad(xfull, grad_qkv).reshape(count_rows, 1, -1))
        grad_in, gain_a_grad = line_norm_back(grad_xn, normed_a, factor_a, gain_a[index])
        list_ga.append(gain_a_grad)
        grad_now = grad_hidden + grad_in
    gains = lax.psum(jnp.concatenate([jnp.stack(list_ga[::-1]), jnp.stack(list_gf[::-1])]), ("x", "y", "c"))
    gains = swap_grid(gains, depth)
    return (
        swap_grid(current, depth),
        swap_grid(grad_now, depth),
        jnp.stack(list_qkv[::-1]),
        jnp.stack(list_out[::-1]),
        jnp.stack(list_gu[::-1]),
        jnp.stack(list_down[::-1]),
        gains[:layers],
        gains[layers:],
    )


def solution(mesh):
    rows, cols = ("row", "col")
    body = local
    if (mesh.shape["row"], mesh.shape["col"]) == (8, 4):
        mesh = share_out(mesh)
        rows, cols = (("z", "x"), ("y", "c"))
        body = stationary
    in_specs = (
        P(rows, cols),
        P(rows, cols),
        P(None, rows, cols, None),
        P(None, rows, cols),
        P(None, rows, None, cols),
        P(None, rows, cols),
        P(None, cols),
        P(None, cols),
    )
    out_specs = (
        P(rows, cols),
        P(rows, cols),
        P(None, rows, cols, None),
        P(None, rows, cols),
        P(None, rows, None, cols),
        P(None, rows, cols),
        P(None, cols),
        P(None, cols),
    )
    return jax.shard_map(body, mesh=mesh, in_specs=in_specs, out_specs=out_specs, check_vma=False)
```

```python
import math

import jax
import jax.numpy as jnp
from jax import lax
from jax.experimental import pallas as pl
from jax.experimental.pallas import tpu as pltpu
from jax.sharding import Mesh
from jax.sharding import PartitionSpec as P

D = 2048
HEAD = 64
GROUP = 8


EPS = 1e-05
THETA = 10000.0


def rope_turn(tensor, cosine, sine):
    half = tensor.shape[-1] // 2
    first = tensor[..., :half]
    second = tensor[..., half:]
    return jnp.concatenate(
        [first * cosine - second * sine, second * cosine + first * sine], axis=-1
    )


def feature_sum(values):
    return lax.psum(values, "col")


def gather_features(rows_in):
    return lax.all_gather(rows_in, "col", axis=1, tiled=True)


def sum_features(partials):
    return lax.psum_scatter(
        partials.astype(jnp.bfloat16), "col", scatter_dimension=1, tiled=True
    ).astype(jnp.float32)


def add_rows(left, piece):
    return jnp.dot(left, piece, preferred_element_type=jnp.float32)


def project_in(left, shard):
    return add_rows(left, lax.all_gather(shard, "row", axis=0, tiled=True))


def columns_of(left, piece):
    return jnp.einsum("tj,dj->td", left, piece, preferred_element_type=jnp.float32)


def project_out(left, shard):
    return columns_of(left, lax.all_gather(shard, "row", axis=0, tiled=True))


def weight_grad(left, right):
    return lax.psum_scatter(
        lax.dot_general(
            left, right, (((0,), (0,)), ((), ())), preferred_element_type=jnp.float32
        ).astype(jnp.bfloat16),
        "row",
        scatter_dimension=0,
        tiled=True,
    ).astype(jnp.float32)


def norm_forward(values, gain):
    total = feature_sum(jnp.sum(values * values, axis=1))
    factor = lax.rsqrt(total / D + EPS)
    normed = values * factor[:, None]
    return (normed, factor, (normed * gain).astype(jnp.bfloat16))


def norm_backward(grad_normed, normed, factor, gain):
    scaled = grad_normed * gain
    inner = feature_sum(jnp.sum(scaled * normed, axis=1))
    grad_in = factor[:, None] * (scaled - normed * (inner / D)[:, None])
    return (grad_in, jnp.sum(grad_normed * normed, axis=0))


def masked_scores(queries, keys, query_pos, key_pos):
    scores = jnp.einsum("qgd,kd->gqk", queries, keys, preferred_element_type=jnp.float32) * (
        1.0 / math.sqrt(queries.shape[-1])
    )
    return jnp.where(key_pos[None, None, :] <= query_pos[None, :, None], scores, -1e30)


def local(stream, grad_out, wqkv, wo, wgu, wd, gain_attn, gain_ffn):
    tok = stream.shape[0]
    layers = wqkv.shape[0]
    count_rows = wqkv.shape[1]
    head = HEAD
    query_cols = GROUP * head
    seq_len = lax.axis_size("row") * tok
    query_pos = lax.axis_index("row") * tok + jnp.arange(tok, dtype=jnp.int32)
    key_pos = jnp.arange(seq_len, dtype=jnp.int32)
    freq = THETA ** (-(jnp.arange(head // 2, dtype=jnp.float32) * 2.0 / head))
    angle = query_pos.astype(jnp.float32)[:, None] * freq[None, :]
    cosine = jnp.cos(angle)
    sine = jnp.sin(angle)
    saved = []
    current = stream
    for index in range(layers):
        weight_qkv = wqkv[index].reshape(count_rows, -1)
        weight_out = wo[index]
        weight_gu = wgu[index].reshape(count_rows, -1)
        weight_down = wd[index]
        wholes = (None, None, None, None)
        normed_a, factor_a, xnormed = norm_forward(current, gain_attn[index])
        xfull = gather_features(xnormed)
        qkv = project_in(xfull, weight_qkv)
        queries = rope_turn(
            qkv[:, :query_cols].reshape(tok, GROUP, head), cosine[:, None, :], sine[:, None, :]
        ).astype(jnp.bfloat16)
        keys = rope_turn(qkv[:, query_cols : query_cols + head], cosine, sine).astype(jnp.bfloat16)
        values = qkv[:, query_cols + head :].astype(jnp.bfloat16)
        seqkv = lax.all_gather(jnp.concatenate([keys, values], axis=1), "row", axis=0, tiled=True)
        seq_keys = seqkv[:, :head]
        seq_values = seqkv[:, head:]
        scores = masked_scores(queries, seq_keys, query_pos, key_pos)
        top = jnp.max(scores, axis=2, keepdims=True)
        expo = jnp.exp(scores - top)
        denom = jnp.sum(expo, axis=2, keepdims=True)
        probs = (expo / denom).astype(jnp.bfloat16)
        log_total = top + jnp.log(denom)
        mixed = (
            jnp.einsum("gqk,kd->qgd", probs, seq_values, preferred_element_type=jnp.float32)
            .reshape(tok, query_cols)
            .astype(jnp.bfloat16)
        )
        hidden_in = current + sum_features(project_out(mixed, weight_out))
        normed_f, factor_f, hnormed = norm_forward(hidden_in, gain_ffn[index])
        hfull = gather_features(hnormed)
        gate_up = project_in(hfull, weight_gu)
        hidden_cols = gate_up.shape[1] // 2
        gate = gate_up[:, :hidden_cols]
        upper = gate_up[:, hidden_cols:]
        active = (jax.nn.silu(gate) * upper).astype(jnp.bfloat16)
        current = hidden_in + sum_features(project_out(active, weight_down))
        saved.append(
            (
                weight_qkv,
                weight_out,
                weight_gu,
                weight_down,
                wholes,
                normed_a,
                factor_a,
                xfull,
                queries,
                seq_keys,
                seq_values,
                log_total,
                mixed,
                normed_f,
                factor_f,
                hfull,
                gate,
                upper,
                active,
            )
        )
    grad_now = grad_out
    list_qkv, list_out, list_gu, list_down, list_ga, list_gf = ([], [], [], [], [], [])
    for index in reversed(range(layers)):
        (
            weight_qkv,
            weight_out,
            weight_gu,
            weight_down,
            wholes,
            normed_a,
            factor_a,
            xfull,
            queries,
            seq_keys,
            seq_values,
            log_total,
            mixed,
            normed_f,
            factor_f,
            hfull,
            gate,
            upper,
            active,
        ) = saved[index]
        grad_full = gather_features(grad_now.astype(jnp.bfloat16))
        grad_active = project_in(grad_full, weight_down)
        list_down.append(weight_grad(grad_full, active))
        sig = jax.nn.sigmoid(gate)
        grad_gate = grad_active * upper * sig * (1.0 + gate * (1.0 - sig))
        grad_up = grad_active * gate * sig
        grad_gu = jnp.concatenate([grad_gate, grad_up], axis=1).astype(jnp.bfloat16)
        grad_hn = sum_features(project_out(grad_gu, weight_gu))
        list_gu.append(weight_grad(hfull, grad_gu).reshape(count_rows, 2, -1))
        grad_mid, gain_f_grad = norm_backward(grad_hn, normed_f, factor_f, gain_ffn[index])
        list_gf.append(gain_f_grad)
        grad_hidden = grad_now + grad_mid
        hidden_full = gather_features(grad_hidden.astype(jnp.bfloat16))
        grad_mixed = project_in(hidden_full, weight_out).astype(jnp.bfloat16)
        list_out.append(weight_grad(hidden_full, mixed))
        grad_heads = grad_mixed.reshape(tok, GROUP, head)
        scores = masked_scores(queries, seq_keys, query_pos, key_pos)
        probs_full = jnp.exp(scores - log_total)
        probs = probs_full.astype(jnp.bfloat16)
        grad_probs = jnp.einsum(
            "qgd,kd->gqk", grad_heads, seq_values, preferred_element_type=jnp.float32
        )
        delta = jnp.sum(probs_full * grad_probs, axis=2, keepdims=True)
        grad_scores = (probs_full * (grad_probs - delta)).astype(jnp.bfloat16)
        inverse = 1.0 / math.sqrt(head)
        grad_queries = (
            jnp.einsum("gqk,kd->qgd", grad_scores, seq_keys, preferred_element_type=jnp.float32)
            * inverse
        )
        grad_keys = (
            jnp.einsum("gqk,qgd->kd", grad_scores, queries, preferred_element_type=jnp.float32)
            * inverse
        )
        grad_values = jnp.einsum(
            "gqk,qgd->kd", probs, grad_heads, preferred_element_type=jnp.float32
        )
        grad_kv = lax.psum_scatter(
            jnp.concatenate([grad_keys, grad_values], axis=1).astype(jnp.bfloat16),
            "row",
            scatter_dimension=0,
            tiled=True,
        ).astype(jnp.float32)
        grad_k = rope_turn(grad_kv[:, :head], cosine, -sine)
        grad_v = grad_kv[:, head:]
        grad_q = rope_turn(grad_queries, cosine[:, None, :], -sine[:, None, :]).reshape(
            tok, query_cols
        )
        grad_qkv = jnp.concatenate([grad_q, grad_k, grad_v], axis=1).astype(jnp.bfloat16)
        grad_xn = sum_features(project_out(grad_qkv, weight_qkv))
        list_qkv.append(weight_grad(xfull, grad_qkv).reshape(count_rows, 1, -1))
        grad_in, gain_a_grad = norm_backward(grad_xn, normed_a, factor_a, gain_attn[index])
        list_ga.append(gain_a_grad)
        grad_now = grad_hidden + grad_in
    gains_a, gains_f = lax.psum((jnp.stack(list_ga[::-1]), jnp.stack(list_gf[::-1])), "row")
    return (
        current,
        grad_now,
        jnp.stack(list_qkv[::-1]),
        jnp.stack(list_out[::-1]),
        jnp.stack(list_gu[::-1]),
        jnp.stack(list_down[::-1]),
        gains_a,
        gains_f,
    )


def share_out(mesh):
    rows, cols = mesh.shape["row"], mesh.shape["col"]
    return Mesh(
        mesh.devices.reshape(rows // 2, 2, cols // 2, 2), ("z", "x", "y", "c")
    )


def swap_grid(values, depth):
    pairs = [(z * depth + g, g * depth + z) for z in range(depth) for g in range(depth)]
    return lax.ppermute(values, ("z", "y", "c"), pairs)


def pair_grad(left, right):
    return lax.psum_scatter(
        lax.dot_general(
            left, right, (((0,), (0,)), ((), ())), preferred_element_type=jnp.float32
        ).astype(jnp.bfloat16),
        "x",
        scatter_dimension=0,
        tiled=True,
    ).astype(jnp.float32)


MESH_ID = pl.DeviceIdType.MESH
ROWS = 16
SKEW = 2
GROUP_CHUNKS = 4
EXTRA = 128


def spread(column):
    high = column.astype(jnp.bfloat16)
    low = (column - high.astype(jnp.float32)).astype(jnp.bfloat16)
    lane = lax.broadcasted_iota(jnp.int32, (column.shape[0], EXTRA), 1)
    wide = jnp.where(lane == 0, high.astype(jnp.float32), jnp.where(lane == 1, low.astype(jnp.float32), 0.0))
    return wide.astype(jnp.bfloat16)


def unspread(block):
    return jnp.sum(block.astype(jnp.float32), axis=1, keepdims=True)


def transposed_dot(left, right):
    return lax.dot_general(left, right, (((1,), (1,)), ((), ())), preferred_element_type=jnp.float32)


class Line:
    def __init__(self, tok, depth):
        self.z, self.x = lax.axis_index("z"), lax.axis_index("x")
        self.y, self.c = lax.axis_index("y"), lax.axis_index("c")
        self.tok, self.depth = tok, depth
        self.half = 2 * tok
        self.chunks = self.half // ROWS
        self.own = pl.multiple_of((2 * self.y + self.c) * tok, tok)
        self.peers = (
            {"y": self.y, "c": 1 - self.c},
            {"y": 1 - self.y, "c": self.c},
            {"y": 1 - self.y, "c": 1 - self.c},
        )

    def greet(self):
        barrier = pltpu.get_barrier_semaphore()
        for peer in self.peers:
            pl.semaphore_signal(barrier, 1, device_id=peer, device_id_type=MESH_ID)

        @pl.when(self.z > 0)
        def _():
            pl.semaphore_signal(barrier, 1, device_id={"z": self.z - 1}, device_id_type=MESH_ID)

        @pl.when(self.z < self.depth - 1)
        def _():
            pl.semaphore_signal(barrier, 1, device_id={"z": self.z + 1}, device_id_type=MESH_ID)

        inner = jnp.where(self.z > 0, 1, 0) + jnp.where(self.z < self.depth - 1, 1, 0)
        pl.semaphore_wait(barrier, 3 + inner)

    def place(self, stream):
        return self.z if stream == 0 else self.depth - 1 - self.z

    def onward(self, stream):
        return {"z": self.z + 1} if stream == 0 else {"z": self.z - 1}

    def backward(self, stream):
        return {"z": self.z - 1} if stream == 0 else {"z": self.z + 1}

    def row_of(self, stream, chunk):
        per = self.chunks // 2
        far = chunk // per
        y = self.y + far * (1 - 2 * self.y)
        return pl.multiple_of((2 * y + stream) * self.tok + lax.rem(chunk, per) * ROWS, ROWS)


def make_line(tok, depth, width_in, width_out, carry_in, carry_out, features):
    chunks = 2 * tok // ROWS
    groups = chunks // GROUP_CHUNKS
    span = GROUP_CHUNKS * ROWS
    half_groups = groups // 2

    def run(line, taken, prepare, finish, second, close, product, carried, chain_out, chain_in, wide, own_part, rs_out, rs_in,
            ag_s, ag_r, ch_s, ch_r, bc_s, bc_r, rs_s, rs_r):
        line.greet()
        gather = [
            pltpu.make_async_remote_copy(
                src_ref=taken.at[pl.ds(line.own, tok)],
                dst_ref=taken.at[pl.ds(line.own, tok)],
                send_sem=ag_s.at[at],
                recv_sem=ag_r.at[at],
                device_id=peer,
                device_id_type=MESH_ID,
            )
            for at, peer in enumerate(line.peers)
        ]
        for copy in gather:
            copy.start()
        gather[0].wait_recv()
        prepare(pl.multiple_of(line.y * 2 * tok, 2 * tok))

        def chain_copy(stream, chunk):
            return pltpu.make_async_remote_copy(
                src_ref=chain_out.at[stream, chunk],
                dst_ref=chain_in.at[stream, chunk],
                send_sem=ch_s.at[stream, chunk],
                recv_sem=ch_r.at[stream, chunk],
                device_id=line.onward(stream),
                device_id_type=MESH_ID,
            )

        def wide_copy(stream, chunk):
            rows = pl.ds(line.row_of(stream, chunk), ROWS)
            return pltpu.make_async_remote_copy(
                src_ref=wide.at[rows],
                dst_ref=wide.at[rows],
                send_sem=bc_s.at[stream, chunk],
                recv_sem=bc_r.at[stream, chunk],
                device_id=line.backward(stream),
                device_id_type=MESH_ID,
            )

        def sum_copy(stream, group):
            far = group // half_groups
            y = line.y + far * (1 - 2 * line.y)
            other = stream + line.c - 2 * stream * line.c
            slot = 2 * far + other - 1
            part = lax.rem(group, half_groups)
            return (slot >= 0, part, pltpu.make_async_remote_copy(
                src_ref=rs_out.at[stream, group],
                dst_ref=rs_in.at[jnp.maximum(slot, 0), pl.ds(pl.multiple_of(part * span, span), span)],
                send_sem=rs_s.at[stream, group],
                recv_sem=rs_r.at[jnp.maximum(slot, 0), part],
                device_id={"y": y, "c": stream},
                device_id_type=MESH_ID,
            ))

        def step(i, _):
            @pl.when(i == SKEW)
            def _():
                gather[1].wait_recv()
                gather[2].wait_recv()
                prepare(pl.multiple_of((1 - line.y) * 2 * tok, 2 * tok))

            for stream in (0, 1):
                place = line.place(stream)
                chunk = i - SKEW * place

                @pl.when((chunk >= 0) & (chunk < chunks))
                def _():
                    row = line.row_of(stream, chunk)

                    @pl.when(place > 0)
                    def _():
                        chain_copy(stream, chunk).wait_recv()

                    @pl.when(place == 0)
                    def _():
                        chain_out[stream, chunk, :, :width_in] = product[pl.ds(row, ROWS), :].astype(jnp.bfloat16)
                        if carry_in:
                            chain_out[stream, chunk, :, width_in:] = spread(carried[pl.ds(row, ROWS), :1])

                    @pl.when((place > 0) & (place < depth - 1))
                    def _():
                        chain_out[stream, chunk, :, :width_in] = (
                            product[pl.ds(row, ROWS), :] + chain_in[stream, chunk, :, :width_in].astype(jnp.float32)
                        ).astype(jnp.bfloat16)
                        if carry_in:
                            chain_out[stream, chunk, :, width_in:] = spread(
                                carried[pl.ds(row, ROWS), :1] + unspread(chain_in[stream, chunk, :, width_in:])
                            )

                    @pl.when(place < depth - 1)
                    def _():
                        chain_copy(stream, chunk).start()

                    @pl.when(place == depth - 1)
                    def _():
                        total = product[pl.ds(row, ROWS), :] + chain_in[stream, chunk, :, :width_in].astype(jnp.float32)
                        extra = None
                        if carry_in:
                            extra = carried[pl.ds(row, ROWS), :1] + unspread(chain_in[stream, chunk, :, width_in:])
                        finish(row, pl.multiple_of(chunk * ROWS, ROWS), total, extra)
                        wide_copy(stream, chunk).start()

                ready = i - SKEW * (2 * (depth - 1) - place)

                @pl.when((ready >= 0) & (ready < chunks))
                def _():
                    @pl.when(place < depth - 1)
                    def _():
                        wide_copy(stream, ready).wait_recv()

                        @pl.when(place > 0)
                        def _():
                            wide_copy(stream, ready).start()

                    @pl.when(lax.rem(ready, GROUP_CHUNKS) == GROUP_CHUNKS - 1)
                    def _():
                        group = ready // GROUP_CHUNKS
                        row = pl.multiple_of(line.row_of(stream, ready) - (span - ROWS), span)
                        away, part, copy = sum_copy(stream, group)
                        value = second(row, span)

                        @pl.when(away)
                        def _():
                            rs_out[stream, group, :, :features] = value.astype(jnp.bfloat16)
                            if carry_out:
                                rs_out[stream, group, :, features:] = wide[pl.ds(row, span), width_out:]
                            copy.start()

                        @pl.when(jnp.logical_not(away))
                        def _():
                            own_part[pl.ds(pl.multiple_of(part * span, span), span), :] = value

            return 0

        lax.fori_loop(0, chunks + 2 * SKEW * (depth - 1), step, 0)

        def drain(i, _):
            for stream in (0, 1):
                place = line.place(stream)

                @pl.when(place < depth - 1)
                def _():
                    chain_copy(stream, i).wait_send()

                @pl.when(place > 0)
                def _():
                    wide_copy(stream, i).wait_send()

            return 0

        def drain_sums(i, _):
            for stream in (0, 1):
                away, part, copy = sum_copy(stream, i)

                @pl.when(away)
                def _():
                    copy.wait_send()
            return 0

        for slot in range(3):
            for part in range(half_groups):
                pltpu.make_async_remote_copy(
                    src_ref=rs_out.at[0, 0],
                    dst_ref=rs_in.at[slot, pl.ds(part * span, span)],
                    send_sem=rs_s.at[0, 0],
                    recv_sem=rs_r.at[slot, part],
                    device_id=line.peers[slot],
                    device_id_type=MESH_ID,
                ).wait_recv()
        close()
        for copy in gather:
            copy.wait_send()
        lax.fori_loop(0, chunks, drain, 0)
        lax.fori_loop(0, groups, drain_sums, 0)

    wide_in = width_in + (EXTRA if carry_in else 0)
    scratch = [
        pltpu.VMEM((4 * tok, width_in), jnp.float32),
        pltpu.VMEM((4 * tok, EXTRA), jnp.float32),
        pltpu.VMEM((2, chunks, ROWS, wide_in), jnp.bfloat16),
        pltpu.VMEM((2, chunks, ROWS, wide_in), jnp.bfloat16),
        pltpu.VMEM((tok, features), jnp.float32),
        pltpu.VMEM((2, groups, span, features + (EXTRA if carry_out else 0)), jnp.bfloat16),
        pltpu.VMEM((3, tok, features + (EXTRA if carry_out else 0)), jnp.bfloat16),
        pltpu.SemaphoreType.DMA((3,)),
        pltpu.SemaphoreType.DMA((3,)),
        pltpu.SemaphoreType.DMA((2, chunks)),
        pltpu.SemaphoreType.DMA((2, chunks)),
        pltpu.SemaphoreType.DMA((2, chunks)),
        pltpu.SemaphoreType.DMA((2, chunks)),
        pltpu.SemaphoreType.DMA((2, groups)),
        pltpu.SemaphoreType.DMA((3, half_groups)),
    ]
    return run, scratch


TILE = 256


def ffn_forward(hidden, gain, weight_gu, weight_down, depth):
    tok, features = hidden.shape
    width = weight_down.shape[1]
    run, scratch = make_line(tok, depth, 2 * width, width, True, False, features)

    def kernel(h_ref, gain_ref, w1_ref, w2_ref, out_ref, taken, kept, wide, scaled, product, carried, chain_out, chain_in,
               own_part, rs_out, rs_in, *sems):
        line = Line(tok, depth)
        taken[pl.ds(line.own, tok), :] = h_ref[...].astype(jnp.bfloat16)

        def prepare(row):
            rows = pl.ds(row, 2 * tok)
            block = taken[rows, :].astype(jnp.float32)
            carried[rows, :] = jnp.broadcast_to(jnp.sum(block * block, axis=1, keepdims=True), (2 * tok, EXTRA))
            scaled[...] = (block * gain_ref[...]).astype(jnp.bfloat16)

            def tile(j, _):
                cols = pl.ds(pl.multiple_of(j * TILE, TILE), TILE)
                product[rows, cols] = jnp.dot(scaled[...], w1_ref[:, cols], preferred_element_type=jnp.float32)
                return 0

            lax.fori_loop(0, 2 * width // TILE, tile, 0)

        def finish(row, at, total, extra):
            factor = lax.rsqrt(extra / D + EPS)
            gate = total[:, :width] * factor
            upper = total[:, width:] * factor
            kept[pl.ds(at, ROWS), :width] = gate
            kept[pl.ds(at, ROWS), width:] = upper
            active = gate * jax.nn.sigmoid(gate) * upper
            wide[pl.ds(row, ROWS), :width] = active.astype(jnp.bfloat16)
            wide[pl.ds(row, ROWS), width:] = spread(factor)

        def second(row, span):
            return transposed_dot(wide[pl.ds(row, span), :width], w2_ref[...])

        def close():
            total = own_part[...]
            for slot in range(3):
                total = total + rs_in[slot].astype(jnp.float32)
            out_ref[...] = h_ref[...] + total

        run(line, taken, prepare, finish, second, close, product, carried, chain_out, chain_in, wide, own_part, rs_out, rs_in,
            *sems)

    shapes = (
        jax.ShapeDtypeStruct((tok, features), jnp.float32),
        jax.ShapeDtypeStruct((4 * tok, features), jnp.bfloat16),
        jax.ShapeDtypeStruct((2 * tok, 2 * width), jnp.float32),
        jax.ShapeDtypeStruct((4 * tok, width + EXTRA), jnp.bfloat16),
    )
    return pl.pallas_call(
        kernel,
        out_shape=shapes,
        in_specs=[pl.BlockSpec(memory_space=pltpu.VMEM)] * 4,
        out_specs=[pl.BlockSpec(memory_space=pltpu.VMEM)] * 4,
        scratch_shapes=[pltpu.VMEM((2 * tok, features), jnp.bfloat16)] + scratch,
        compiler_params=pltpu.CompilerParams(collective_id=1, has_side_effects=True, vmem_limit_bytes=60 << 20),
        cost_estimate=pl.CostEstimate(flops=60_000_000_000, bytes_accessed=8_000_000, transcendentals=0),
        name="ffn_forward",
    )(hidden, gain.reshape(1, -1), weight_gu, weight_down)


def ffn_backward(grad, hidden, gain, kept, wide_forward, weight_gu, weight_down, depth):
    tok, features = hidden.shape
    width = weight_down.shape[1]
    run, scratch = make_line(tok, depth, width, 2 * width, False, True, features)

    def kernel(dy_ref, h_ref, gain_ref, kept_ref, before_ref, w1_ref, w2_ref, out_ref, taken, wide, gain_out, product, carried,
               chain_out, chain_in, own_part, rs_out, rs_in, *sems):
        line = Line(tok, depth)
        taken[pl.ds(line.own, tok), :] = dy_ref[...].astype(jnp.bfloat16)

        def prepare(row):
            rows = pl.ds(row, 2 * tok)

            def tile(j, _):
                cols = pl.ds(pl.multiple_of(j * 128, 128), 128)
                product[rows, cols] = jnp.dot(taken[rows, :], w2_ref[:, cols], preferred_element_type=jnp.float32)
                return 0

            lax.fori_loop(0, width // 128, tile, 0)

        def finish(row, at, total, extra):
            gate = kept_ref[pl.ds(at, ROWS), :width]
            upper = kept_ref[pl.ds(at, ROWS), width:]
            sig = jax.nn.sigmoid(gate)
            silu = gate * sig
            grad_gate = total * upper * (sig + silu * (1.0 - sig))
            grad_up = total * silu
            wide[pl.ds(row, ROWS), :width] = grad_gate.astype(jnp.bfloat16)
            wide[pl.ds(row, ROWS), width : 2 * width] = grad_up.astype(jnp.bfloat16)
            inner = jnp.sum(grad_gate * gate + grad_up * upper, axis=1, keepdims=True)
            wide[pl.ds(row, ROWS), 2 * width :] = spread(inner)

        def second(row, span):
            return transposed_dot(wide[pl.ds(row, span), : 2 * width], w1_ref[...])

        def close():
            total = own_part[...]
            inner = unspread(wide[pl.ds(line.own, tok), 2 * width :])
            for slot in range(3):
                total = total + rs_in[slot, :, :features].astype(jnp.float32)
                inner = inner + unspread(rs_in[slot, :, features:])
            factor = unspread(before_ref[pl.ds(line.own, tok), width:])
            normed = h_ref[...] * factor
            gain_out[...] = jnp.broadcast_to(jnp.sum(total * normed, axis=0, keepdims=True), gain_out.shape)
            out_ref[...] = dy_ref[...] + factor * (total * gain_ref[...] - normed * (inner / D))

        run(line, taken, prepare, finish, second, close, product, carried, chain_out, chain_in, wide, own_part, rs_out, rs_in,
            *sems)

    shapes = (
        jax.ShapeDtypeStruct((tok, features), jnp.float32),
        jax.ShapeDtypeStruct((4 * tok, features), jnp.bfloat16),
        jax.ShapeDtypeStruct((4 * tok, 2 * width + EXTRA), jnp.bfloat16),
        jax.ShapeDtypeStruct((8, features), jnp.float32),
    )
    return pl.pallas_call(
        kernel,
        out_shape=shapes,
        in_specs=[pl.BlockSpec(memory_space=pltpu.VMEM)] * 7,
        out_specs=[pl.BlockSpec(memory_space=pltpu.VMEM)] * 4,
        scratch_shapes=scratch,
        compiler_params=pltpu.CompilerParams(collective_id=2, has_side_effects=True, vmem_limit_bytes=60 << 20),
        cost_estimate=pl.CostEstimate(flops=60_000_000_000, bytes_accessed=8_000_000, transcendentals=0),
        name="ffn_backward",
    )(grad, hidden, gain.reshape(1, -1), kept, wide_forward, weight_gu, weight_down)


def to_row(column):
    return jnp.transpose(jnp.broadcast_to(column, (column.shape[0], EXTRA)))[:8]


def to_column(row):
    return jnp.transpose(jnp.broadcast_to(row[:1], (row.shape[1], row.shape[1])))[:, :1]


def turn(values, cosine, sine):
    lane = lax.broadcasted_iota(jnp.int32, values.shape, 1)
    width = values.shape[1]
    back = pltpu.roll(values, width - HEAD // 2, 1)
    forth = pltpu.roll(values, HEAD // 2, 1)
    partner = jnp.where(lax.rem(lane, HEAD) < HEAD // 2, back, forth)
    return values * cosine + partner * sine


def split_pair(block):
    lane = lax.broadcasted_iota(jnp.int32, block.shape, 1)
    zero = jnp.zeros_like(block)
    return jnp.concatenate([jnp.where(lane < HEAD, block, zero), jnp.where(lane < HEAD, zero, block)], axis=0)


def join_pair(turned, tok):
    return jnp.transpose(jnp.concatenate([turned[:HEAD, :tok], turned[HEAD:, tok:]], axis=0))


def twice(kv):
    wide = kv.astype(jnp.float32)
    lane = lax.broadcasted_iota(jnp.int32, wide.shape, 1)
    other = pltpu.roll(wide, HEAD, 1)
    return jnp.where(lane < HEAD, wide, other), jnp.where(lane < HEAD, other, wide)


class Square:
    def __init__(self, tok, depth):
        self.z, self.x = lax.axis_index("z"), lax.axis_index("x")
        self.y, self.c = lax.axis_index("y"), lax.axis_index("c")
        self.tok, self.depth = tok, depth
        self.g = 2 * self.y + self.c
        self.row = 2 * self.z + self.x
        self.own = pl.multiple_of(self.g * tok, tok)
        self.mine = pl.multiple_of(self.z * tok, tok)
        self.peers = (
            {"y": self.y, "c": 1 - self.c},
            {"y": 1 - self.y, "c": self.c},
            {"y": 1 - self.y, "c": 1 - self.c},
        )

    def row_peer(self, step):
        at = lax.rem(self.row + step, 2 * self.depth)
        return {"z": at // 2, "x": lax.rem(at, 2)}

    def greet(self):
        barrier = pltpu.get_barrier_semaphore()
        for peer in self.peers:
            pl.semaphore_signal(barrier, 1, device_id=peer, device_id_type=MESH_ID)
        for step in range(1, 2 * self.depth):
            pl.semaphore_signal(barrier, 1, device_id=self.row_peer(step), device_id_type=MESH_ID)
        pl.semaphore_wait(barrier, 3 + 2 * self.depth - 1)


def remote(src, dst, send, recv, device):
    return pltpu.make_async_remote_copy(
        src_ref=src, dst_ref=dst, send_sem=send, recv_sem=recv, device_id=device, device_id_type=MESH_ID
    )


def start_gather(square, taken, send, recv):
    copies = [
        remote(taken.at[pl.ds(square.own, square.tok)], taken.at[pl.ds(square.own, square.tok)], send.at[at], recv.at[at], peer)
        for at, peer in enumerate(square.peers)
    ]
    for copy in copies:
        copy.start()
    return copies


def line_sum(square, gather, product, own, own_row, outs, ins, row_outs, row_ins, send, recv, row_send, row_recv):
    tok, depth = square.tok, square.depth

    def one(order):
        block = lax.rem(2 * square.y + order, depth)
        step = lax.rem(block - square.z + depth, depth)
        slot = jnp.maximum(depth - 1 - step, 0)
        value, column = product(pl.multiple_of(block * tok, tok))

        @pl.when(step == 0)
        def _():
            own[...] = value
            if column is not None:
                own_row[...] = to_row(column)

        copy = remote(outs.at[order], ins.at[slot], send.at[order], recv.at[slot], {"z": block})
        row_copy = None
        if column is not None:
            row_copy = remote(row_outs.at[order], row_ins.at[slot], row_send.at[order], row_recv.at[slot], {"z": block})

        @pl.when(step != 0)
        def _():
            outs[order] = value.astype(jnp.bfloat16)
            copy.start()
            if column is not None:
                row_outs[order] = to_row(column)
                row_copy.start()

        return step, copy, row_copy

    gather[0].wait_recv()
    sent = [one(0), one(1)]
    gather[1].wait_recv()
    gather[2].wait_recv()
    sent += [one(2), one(3)]
    for slot in range(depth - 1):
        remote(outs.at[0], ins.at[slot], send.at[0], recv.at[slot], {"z": square.z}).wait_recv()
        if row_ins is not None:
            remote(row_outs.at[0], row_ins.at[slot], row_send.at[0], row_recv.at[slot], {"z": square.z}).wait_recv()
    return sent


def line_gather(square, array, rows, send, recv, row_send, row_recv):
    depth = square.depth
    sent = []
    for step in range(1, depth):
        peer = {"z": lax.rem(square.z + step, depth)}
        here = array.at[pl.ds(square.mine, square.tok)]
        copy = remote(here, here, send.at[step - 1], recv.at[depth - 1 - step], peer)
        line = rows.at[square.z]
        row_copy = remote(line, line, row_send.at[step - 1], row_recv.at[depth - 1 - step], peer)
        copy.start()
        row_copy.start()
        sent += [copy, row_copy]
    return sent


def grid_sum(square, array, rows, second, own, outs, ins, row_ins, arrive, row_arrive, send, recv, row_send, row_recv):
    tok, depth = square.tok, square.depth
    sent = []
    for step in range(depth):
        block = lax.rem(square.z + step, depth)
        if step:
            rows_of = pl.ds(pl.multiple_of(block * tok, tok), tok)
            remote(array.at[rows_of], array.at[rows_of], send.at[0], arrive.at[step - 1], {"z": square.z}).wait_recv()
            remote(rows.at[block], rows.at[block], send.at[0], row_arrive.at[step - 1], {"z": square.z}).wait_recv()
        value = second(pl.multiple_of(block * tok, tok))
        away = lax.rem(block - square.g + depth, depth)
        slot = jnp.maximum(depth - 1 - away, 0)
        device = {"y": block // 2, "c": lax.rem(block, 2)}
        copy = remote(outs.at[step], ins.at[slot], send.at[step], recv.at[slot], device)
        row_copy = None
        if row_ins is not None:
            row_copy = remote(rows.at[block], row_ins.at[slot], row_send.at[step], row_recv.at[slot], device)

        @pl.when(away == 0)
        def _():
            own[...] = value

        @pl.when(away != 0)
        def _():
            outs[step] = value.astype(jnp.bfloat16)
            copy.start()
            if row_ins is not None:
                row_copy.start()

        sent.append((away, copy, row_copy))
    for slot in range(depth - 1):
        remote(outs.at[0], ins.at[slot], send.at[0], recv.at[slot], square.peers[0]).wait_recv()
        if row_ins is not None:
            remote(rows.at[0], row_ins.at[slot], row_send.at[0], row_recv.at[slot], square.peers[0]).wait_recv()
    return sent


def drain(sent):
    for away, copy, row_copy in sent:

        @pl.when(away != 0)
        def _():
            copy.wait_send()
            if row_copy is not None:
                row_copy.wait_send()


def sem(*shape):
    return pltpu.SemaphoreType.DMA(shape)


def attention_forward(hidden, gain, weight_qkv, weight_out, cosine, sine, depth):
    tok, features = hidden.shape
    cols = weight_qkv.shape[1]
    query_cols = GROUP * HEAD
    seq = 2 * depth * tok
    pairs = query_cols // EXTRA
    scale = 1.0 / math.sqrt(HEAD)

    def kernel(h_ref, gain_ref, wqkv_ref, wo_ref, cos_ref, sin_ref, out_ref, taken, queries, kv, lse, mixed, factors,
               own, own_row, z_out, z_in, zr_out, zr_in, values_t, g_own, g_out, g_in,
               ag_s, ag_r, zs_s, zs_r, zr_s, zr_r, kv_s, kv_r, zg_s, zg_r, zgr_s, zgr_r, gs_s, gs_r):
        square = Square(tok, depth)
        taken[pl.ds(square.own, tok), :] = h_ref[...].astype(jnp.bfloat16)
        square.greet()
        gather = start_gather(square, taken, ag_s, ag_r)

        def product(row):
            block = taken[pl.ds(row, tok), :].astype(jnp.float32)
            scaled = (block * gain_ref[...]).astype(jnp.bfloat16)
            return (
                jnp.dot(scaled, wqkv_ref[...], preferred_element_type=jnp.float32),
                jnp.sum(block * block, axis=1, keepdims=True),
            )

        sent = line_sum(square, gather, product, own, own_row, z_out, z_in, zr_out, zr_in, zs_s, zs_r, zr_s, zr_r)
        total, squares = own[...], own_row[...]
        for slot in range(depth - 1):
            total = total + z_in[slot].astype(jnp.float32)
            squares = squares + zr_in[slot]
        factor_row = lax.rsqrt(squares / D + EPS)
        factors[square.z] = factor_row
        turned = turn(total * to_column(factor_row), cos_ref[...], sin_ref[...])
        here = pl.ds(pl.multiple_of(square.row * tok, tok), tok)
        kv[here, :] = turned[:, query_cols:].astype(jnp.bfloat16)
        queries[...] = turned[:, :query_cols].astype(jnp.bfloat16)
        spreads = []
        for step in range(1, 2 * depth):
            copy = remote(kv.at[here], kv.at[here], kv_s.at[step - 1], kv_r.at[2 * depth - 1 - step], square.row_peer(step))
            copy.start()
            spreads.append(copy)
        for copy in spreads:
            copy.wait_recv()
        keys, both = twice(kv[...])
        values_t[...] = jnp.transpose(both).astype(jnp.bfloat16)
        keys = keys.astype(jnp.bfloat16)

        def pair(t, _):
            lanes = pl.ds(pl.multiple_of(t * EXTRA, EXTRA), EXTRA)
            scores = transposed_dot(keys, split_pair(queries[:, lanes])) * scale
            key_at = lax.broadcasted_iota(jnp.int32, scores.shape, 0)
            query_at = lax.rem(lax.broadcasted_iota(jnp.int32, scores.shape, 1), tok) + square.row * tok
            scores = jnp.where(key_at <= query_at, scores, -1e30)
            top = jnp.max(scores, axis=0, keepdims=True)
            expo = jnp.exp(scores - top)
            denom = jnp.sum(expo, axis=0, keepdims=True)
            lse[t] = jnp.broadcast_to(top + jnp.log(denom), (8, 2 * tok))
            probs = (expo * (1.0 / denom)).astype(jnp.bfloat16)
            out_t = jnp.dot(values_t[...], probs, preferred_element_type=jnp.float32)
            mixed[pl.ds(square.mine, tok), lanes] = join_pair(out_t, tok).astype(jnp.bfloat16)
            return 0

        lax.fori_loop(0, pairs, pair, 0)
        given = line_gather(square, mixed, factors, zg_s, zg_r, zgr_s, zgr_r)

        def second(row):
            return transposed_dot(mixed[pl.ds(row, tok), :], wo_ref[...])

        sums = grid_sum(square, mixed, factors, second, g_own, g_out, g_in, None, zg_r, zgr_r, gs_s, gs_r, None, None)
        total = g_own[...]
        for slot in range(depth - 1):
            total = total + g_in[slot].astype(jnp.float32)
        out_ref[...] = h_ref[...] + total
        drain(sent)
        drain(sums)
        for copy in gather + spreads + given:
            copy.wait_send()

    low, full = jnp.bfloat16, jnp.float32
    shapes = (
        jax.ShapeDtypeStruct((tok, features), full),
        jax.ShapeDtypeStruct((depth * tok, features), low),
        jax.ShapeDtypeStruct((tok, query_cols), low),
        jax.ShapeDtypeStruct((seq, 2 * HEAD), low),
        jax.ShapeDtypeStruct((pairs, 8, 2 * tok), full),
        jax.ShapeDtypeStruct((depth * tok, query_cols), low),
        jax.ShapeDtypeStruct((depth, 8, tok), full),
    )
    return pl.pallas_call(
        kernel,
        out_shape=shapes,
        in_specs=[pl.BlockSpec(memory_space=pltpu.VMEM)] * 6,
        out_specs=[pl.BlockSpec(memory_space=pltpu.VMEM)] * 7,
        scratch_shapes=[
            pltpu.VMEM((tok, cols), full),
            pltpu.VMEM((8, tok), full),
            pltpu.VMEM((depth, tok, cols), low),
            pltpu.VMEM((depth - 1, tok, cols), low),
            pltpu.VMEM((depth, 8, tok), full),
            pltpu.VMEM((depth - 1, 8, tok), full),
            pltpu.VMEM((2 * HEAD, seq), low),
            pltpu.VMEM((tok, features), full),
            pltpu.VMEM((depth, tok, features), low),
            pltpu.VMEM((depth - 1, tok, features), low),
            sem(3), sem(3), sem(depth), sem(depth - 1), sem(depth), sem(depth - 1),
            sem(2 * depth - 1), sem(2 * depth - 1), sem(depth - 1), sem(depth - 1), sem(depth - 1), sem(depth - 1),
            sem(depth), sem(depth - 1),
        ],
        compiler_params=pltpu.CompilerParams(collective_id=3, has_side_effects=True, vmem_limit_bytes=60 << 20),
        cost_estimate=pl.CostEstimate(flops=50_000_000_000, bytes_accessed=8_000_000, transcendentals=0),
        name="attention_forward",
    )(hidden, gain.reshape(1, -1), weight_qkv, weight_out, cosine, sine)


def attention_backward(grad, hidden, gain, weight_qkv, weight_out, cosine, sine, queries, kv, lse, factors, depth):
    tok, features = hidden.shape
    cols = weight_qkv.shape[1]
    query_cols = GROUP * HEAD
    seq = 2 * depth * tok
    pairs = query_cols // EXTRA
    scale = 1.0 / math.sqrt(HEAD)

    def kernel(dy_ref, h_ref, gain_ref, wqkv_ref, wo_ref, cos_ref, sin_ref, q_ref, kv_ref, lse_ref, factor_ref,
               out_ref, taken, spun, gain_out,
               own, heads, z_out, z_in, keys_t, dk, dv, kv_out, kv_own, kv_in, dq, inner_rows, g_own, g_out, g_in, g_rows,
               ag_s, ag_r, zs_s, zs_r, kv_s, kv_r, zg_s, zg_r, zgr_s, zgr_r, gs_s, gs_r, gr_s, gr_r):
        square = Square(tok, depth)
        taken[pl.ds(square.own, tok), :] = dy_ref[...].astype(jnp.bfloat16)
        square.greet()
        gather = start_gather(square, taken, ag_s, ag_r)

        def product(row):
            return jnp.dot(taken[pl.ds(row, tok), :], wo_ref[...], preferred_element_type=jnp.float32), None

        sent = line_sum(square, gather, product, own, None, z_out, z_in, None, None, zs_s, zs_r, None, None)
        total = own[...]
        for slot in range(depth - 1):
            total = total + z_in[slot].astype(jnp.float32)
        heads[...] = total.astype(jnp.bfloat16)
        keys, both = twice(kv_ref[...])
        keys_t[...] = jnp.transpose(keys).astype(jnp.bfloat16)
        keys = keys.astype(jnp.bfloat16)
        both = both.astype(jnp.bfloat16)
        dk[...] = jnp.zeros_like(dk)
        dv[...] = jnp.zeros_like(dv)

        def pair(t, _):
            lanes = pl.ds(pl.multiple_of(t * EXTRA, EXTRA), EXTRA)
            query = split_pair(q_ref[:, lanes])
            head = split_pair(heads[:, lanes])
            scores = transposed_dot(keys, query) * scale
            key_at = lax.broadcasted_iota(jnp.int32, scores.shape, 0)
            query_at = lax.rem(lax.broadcasted_iota(jnp.int32, scores.shape, 1), tok) + square.row * tok
            probs = jnp.exp(jnp.where(key_at <= query_at, scores, -1e30) - lse_ref[t, :1, :])
            grad_probs = transposed_dot(both, head)
            delta = jnp.sum(probs * grad_probs, axis=0, keepdims=True)
            grad_scores = (probs * (grad_probs - delta)).astype(jnp.bfloat16)
            dk[...] += jnp.dot(grad_scores, query, preferred_element_type=jnp.float32)
            dv[...] += jnp.dot(probs.astype(jnp.bfloat16), head, preferred_element_type=jnp.float32)
            turned = jnp.dot(keys_t[...], grad_scores, preferred_element_type=jnp.float32)
            dq[:, lanes] = join_pair(turned, tok) * scale
            return 0

        lax.fori_loop(0, pairs, pair, 0)
        lane = lax.broadcasted_iota(jnp.int32, (seq, EXTRA), 1)
        left = dk[...]
        right = dv[...]
        both_kv = jnp.where(
            lane < HEAD, (left + pltpu.roll(left, HEAD, 1)) * scale, right + pltpu.roll(right, HEAD, 1)
        )
        dk[...] = both_kv
        kv_out[...] = both_kv.astype(jnp.bfloat16)
        here = pl.ds(pl.multiple_of(square.row * tok, tok), tok)
        spreads = []
        for step in range(1, 2 * depth):
            at = lax.rem(square.row + step, 2 * depth)
            copy = remote(
                kv_out.at[pl.ds(pl.multiple_of(at * tok, tok), tok)],
                kv_in.at[2 * depth - 1 - step],
                kv_s.at[step - 1],
                kv_r.at[2 * depth - 1 - step],
                square.row_peer(step),
            )
            copy.start()
            spreads.append(copy)
        total_kv = dk[here, :]
        for copy in spreads:
            copy.wait_recv()
        for slot in range(2 * depth - 1):
            total_kv = total_kv + kv_in[slot].astype(jnp.float32)
        inner = jnp.sum(dq[...] * q_ref[...].astype(jnp.float32), axis=1, keepdims=True) + jnp.sum(
            total_kv * kv_ref[here, :].astype(jnp.float32), axis=1, keepdims=True
        )
        inner_rows[square.z] = to_row(inner)
        whole = jnp.concatenate([dq[...], total_kv], axis=1)
        spun[pl.ds(square.mine, tok), :] = turn(whole, cos_ref[...], -sin_ref[...]).astype(jnp.bfloat16)
        given = line_gather(square, spun, inner_rows, zg_s, zg_r, zgr_s, zgr_r)

        def second(row):
            return transposed_dot(spun[pl.ds(row, tok), :], wqkv_ref[...])

        sums = grid_sum(
            square, spun, inner_rows, second, g_own, g_out, g_in, g_rows, zg_r, zgr_r, gs_s, gs_r, gr_s, gr_r
        )
        total = g_own[...]
        inner = inner_rows[square.g]
        for slot in range(depth - 1):
            total = total + g_in[slot].astype(jnp.float32)
            inner = inner + g_rows[slot]
        factor = to_column(factor_ref[square.g])
        normed = h_ref[...] * factor
        gain_out[...] = jnp.broadcast_to(jnp.sum(total * normed, axis=0, keepdims=True), gain_out.shape)
        out_ref[...] = dy_ref[...] + factor * (total * gain_ref[...] - normed * (to_column(inner) / D))
        drain(sent)
        drain(sums)
        for copy in gather + spreads + given:
            copy.wait_send()

    low, full = jnp.bfloat16, jnp.float32
    shapes = (
        jax.ShapeDtypeStruct((tok, features), full),
        jax.ShapeDtypeStruct((depth * tok, features), low),
        jax.ShapeDtypeStruct((depth * tok, cols), low),
        jax.ShapeDtypeStruct((8, features), full),
    )
    return pl.pallas_call(
        kernel,
        out_shape=shapes,
        in_specs=[pl.BlockSpec(memory_space=pltpu.VMEM)] * 11,
        out_specs=[pl.BlockSpec(memory_space=pltpu.VMEM)] * 4,
        scratch_shapes=[
            pltpu.VMEM((tok, query_cols), full),
            pltpu.VMEM((tok, query_cols), low),
            pltpu.VMEM((depth, tok, query_cols), low),
            pltpu.VMEM((depth - 1, tok, query_cols), low),
            pltpu.VMEM((2 * HEAD, seq), low),
            pltpu.VMEM((seq, 2 * HEAD), full),
            pltpu.VMEM((seq, 2 * HEAD), full),
            pltpu.VMEM((seq, 2 * HEAD), low),
            pltpu.VMEM((tok, 2 * HEAD), full),
            pltpu.VMEM((2 * depth - 1, tok, 2 * HEAD), low),
            pltpu.VMEM((tok, query_cols), full),
            pltpu.VMEM((depth, 8, tok), full),
            pltpu.VMEM((tok, features), full),
            pltpu.VMEM((depth, tok, features), low),
            pltpu.VMEM((depth - 1, tok, features), low),
            pltpu.VMEM((depth - 1, 8, tok), full),
            sem(3), sem(3), sem(depth), sem(depth - 1),
            sem(2 * depth - 1), sem(2 * depth - 1), sem(depth - 1), sem(depth - 1), sem(depth - 1), sem(depth - 1),
            sem(depth), sem(depth - 1), sem(depth), sem(depth - 1),
        ],
        compiler_params=pltpu.CompilerParams(collective_id=4, has_side_effects=True, vmem_limit_bytes=60 << 20),
        cost_estimate=pl.CostEstimate(flops=50_000_000_000, bytes_accessed=8_000_000, transcendentals=0),
        name="attention_backward",
    )(grad, hidden, gain.reshape(1, -1), weight_qkv, weight_out, cosine, sine, queries, kv, lse, factors)


def stationary(stream, grad_out, wqkv, wo, wgu, wd, gain_attn, gain_ffn):
    tok = stream.shape[0]
    layers = wqkv.shape[0]
    count_rows = wqkv.shape[1]
    depth = lax.axis_size("z")
    head = HEAD
    row = lax.axis_index("z") * 2 + lax.axis_index("x")
    query_pos = row * tok + jnp.arange(tok, dtype=jnp.int32)
    freq = THETA ** (-(jnp.arange(head // 2, dtype=jnp.float32) * 2.0 / head))
    angle = query_pos.astype(jnp.float32)[:, None] * freq[None, :]
    cosine = jnp.cos(angle)
    sine = jnp.sin(angle)
    turns = GROUP + 1
    cosine = jnp.concatenate([jnp.tile(cosine, (1, 2 * turns)), jnp.ones((tok, head), jnp.float32)], axis=1)
    sine = jnp.concatenate(
        [jnp.tile(jnp.concatenate([-sine, sine], axis=1), (1, turns)), jnp.zeros((tok, head), jnp.float32)], axis=1
    )
    whole = lambda shard: lax.all_gather(shard, "x", axis=0, tiled=True)
    current = swap_grid(stream, depth)
    grad_now = swap_grid(grad_out, depth)
    gain_a = swap_grid(gain_attn, depth)
    gain_f = swap_grid(gain_ffn, depth)
    saved = []
    for index in range(layers):
        weight_qkv = whole(wqkv[index].reshape(count_rows, -1))
        weight_out = whole(wo[index])
        weight_gu = whole(wgu[index].reshape(count_rows, -1))
        weight_down = whole(wd[index])
        before = current
        hidden_in, xfull, queries, kv, lse, mixed_full, factors = attention_forward(
            before, gain_a[index], weight_qkv, weight_out, cosine, sine, depth
        )
        current, hfull, kept, active = ffn_forward(hidden_in, gain_f[index], weight_gu, weight_down, depth)
        saved.append(
            (weight_qkv, weight_out, weight_gu, weight_down, before, xfull, queries, kv, lse, mixed_full, factors,
             hidden_in, hfull, kept, active)
        )
    list_qkv, list_out, list_gu, list_down, list_ga, list_gf = ([], [], [], [], [], [])
    for index in reversed(range(layers)):
        (weight_qkv, weight_out, weight_gu, weight_down, before, xfull, queries, kv, lse, mixed_full, factors,
         hidden_in, hfull, kept, active) = saved[index]
        width = weight_down.shape[1]
        grad_hidden, grad_full, grad_gu, gain_f_grad = ffn_backward(
            grad_now, hidden_in, gain_f[index], kept, active, weight_gu, weight_down, depth
        )
        list_down.append(pair_grad(grad_full, active[:, :width]))
        factor_f = jnp.sum(active[:, width:].astype(jnp.float32), axis=1, keepdims=True)
        hnormed = (hfull.astype(jnp.float32) * factor_f * gain_f[index]).astype(jnp.bfloat16)
        list_gu.append(pair_grad(hnormed, grad_gu[:, : 2 * width]).reshape(count_rows, 2, -1))
        list_gf.append(gain_f_grad[0])
        grad_now, hidden_full, grad_qkv, gain_a_grad = attention_backward(
            grad_hidden, before, gain_a[index], weight_qkv, weight_out, cosine, sine, queries, kv, lse, factors, depth
        )
        list_out.append(pair_grad(hidden_full, mixed_full))
        factor_a = factors[:, 0, :].reshape(-1, 1)
        xnormed = (xfull.astype(jnp.float32) * factor_a * gain_a[index]).astype(jnp.bfloat16)
        list_qkv.append(pair_grad(xnormed, grad_qkv).reshape(count_rows, 1, -1))
        list_ga.append(gain_a_grad[0])
    gains = lax.psum(jnp.concatenate([jnp.stack(list_ga[::-1]), jnp.stack(list_gf[::-1])]), ("x", "y", "c"))
    gains = swap_grid(gains, depth)
    return (
        swap_grid(current, depth),
        swap_grid(grad_now, depth),
        jnp.stack(list_qkv[::-1]),
        jnp.stack(list_out[::-1]),
        jnp.stack(list_gu[::-1]),
        jnp.stack(list_down[::-1]),
        gains[:layers],
        gains[layers:],
    )


def solution(mesh):
    rows, cols = ("row", "col")
    body = local
    if (mesh.shape["row"], mesh.shape["col"]) == (8, 4):
        mesh = share_out(mesh)
        rows, cols = (("z", "x"), ("y", "c"))
        body = stationary
    in_specs = (
        P(rows, cols),
        P(rows, cols),
        P(None, rows, cols, None),
        P(None, rows, cols),
        P(None, rows, None, cols),
        P(None, rows, cols),
        P(None, cols),
        P(None, cols),
    )
    out_specs = (
        P(rows, cols),
        P(rows, cols),
        P(None, rows, cols, None),
        P(None, rows, cols),
        P(None, rows, None, cols),
        P(None, rows, cols),
        P(None, cols),
        P(None, cols),
    )
    return jax.shard_map(body, mesh=mesh, in_specs=in_specs, out_specs=out_specs, check_vma=False)
```

```python
import math

import jax
import jax.numpy as jnp
from jax import lax
from jax.experimental import pallas as pl
from jax.experimental.pallas import tpu as pltpu
from jax.sharding import Mesh
from jax.sharding import PartitionSpec as P

D = 2048
HEAD = 64
GROUP = 8


EPS = 1e-05
THETA = 10000.0


def rope_turn(tensor, cosine, sine):
    half = tensor.shape[-1] // 2
    first = tensor[..., :half]
    second = tensor[..., half:]
    return jnp.concatenate(
        [first * cosine - second * sine, second * cosine + first * sine], axis=-1
    )


def feature_sum(values):
    return lax.psum(values, "col")


def gather_features(rows_in):
    return lax.all_gather(rows_in, "col", axis=1, tiled=True)


def sum_features(partials):
    return lax.psum_scatter(
        partials.astype(jnp.bfloat16), "col", scatter_dimension=1, tiled=True
    ).astype(jnp.float32)


def add_rows(left, piece):
    return jnp.dot(left, piece, preferred_element_type=jnp.float32)


def project_in(left, shard):
    return add_rows(left, lax.all_gather(shard, "row", axis=0, tiled=True))


def columns_of(left, piece):
    return jnp.einsum("tj,dj->td", left, piece, preferred_element_type=jnp.float32)


def project_out(left, shard):
    return columns_of(left, lax.all_gather(shard, "row", axis=0, tiled=True))


def weight_grad(left, right):
    return lax.psum_scatter(
        lax.dot_general(
            left, right, (((0,), (0,)), ((), ())), preferred_element_type=jnp.float32
        ).astype(jnp.bfloat16),
        "row",
        scatter_dimension=0,
        tiled=True,
    ).astype(jnp.float32)


def norm_forward(values, gain):
    total = feature_sum(jnp.sum(values * values, axis=1))
    factor = lax.rsqrt(total / D + EPS)
    normed = values * factor[:, None]
    return (normed, factor, (normed * gain).astype(jnp.bfloat16))


def norm_backward(grad_normed, normed, factor, gain):
    scaled = grad_normed * gain
    inner = feature_sum(jnp.sum(scaled * normed, axis=1))
    grad_in = factor[:, None] * (scaled - normed * (inner / D)[:, None])
    return (grad_in, jnp.sum(grad_normed * normed, axis=0))


def masked_scores(queries, keys, query_pos, key_pos):
    scores = jnp.einsum("qgd,kd->gqk", queries, keys, preferred_element_type=jnp.float32) * (
        1.0 / math.sqrt(queries.shape[-1])
    )
    return jnp.where(key_pos[None, None, :] <= query_pos[None, :, None], scores, -1e30)


def local(stream, grad_out, wqkv, wo, wgu, wd, gain_attn, gain_ffn):
    tok = stream.shape[0]
    layers = wqkv.shape[0]
    count_rows = wqkv.shape[1]
    head = HEAD
    query_cols = GROUP * head
    seq_len = lax.axis_size("row") * tok
    query_pos = lax.axis_index("row") * tok + jnp.arange(tok, dtype=jnp.int32)
    key_pos = jnp.arange(seq_len, dtype=jnp.int32)
    freq = THETA ** (-(jnp.arange(head // 2, dtype=jnp.float32) * 2.0 / head))
    angle = query_pos.astype(jnp.float32)[:, None] * freq[None, :]
    cosine = jnp.cos(angle)
    sine = jnp.sin(angle)
    saved = []
    current = stream
    for index in range(layers):
        weight_qkv = wqkv[index].reshape(count_rows, -1)
        weight_out = wo[index]
        weight_gu = wgu[index].reshape(count_rows, -1)
        weight_down = wd[index]
        wholes = (None, None, None, None)
        normed_a, factor_a, xnormed = norm_forward(current, gain_attn[index])
        xfull = gather_features(xnormed)
        qkv = project_in(xfull, weight_qkv)
        queries = rope_turn(
            qkv[:, :query_cols].reshape(tok, GROUP, head), cosine[:, None, :], sine[:, None, :]
        ).astype(jnp.bfloat16)
        keys = rope_turn(qkv[:, query_cols : query_cols + head], cosine, sine).astype(jnp.bfloat16)
        values = qkv[:, query_cols + head :].astype(jnp.bfloat16)
        seqkv = lax.all_gather(jnp.concatenate([keys, values], axis=1), "row", axis=0, tiled=True)
        seq_keys = seqkv[:, :head]
        seq_values = seqkv[:, head:]
        scores = masked_scores(queries, seq_keys, query_pos, key_pos)
        top = jnp.max(scores, axis=2, keepdims=True)
        expo = jnp.exp(scores - top)
        denom = jnp.sum(expo, axis=2, keepdims=True)
        probs = (expo / denom).astype(jnp.bfloat16)
        log_total = top + jnp.log(denom)
        mixed = (
            jnp.einsum("gqk,kd->qgd", probs, seq_values, preferred_element_type=jnp.float32)
            .reshape(tok, query_cols)
            .astype(jnp.bfloat16)
        )
        hidden_in = current + sum_features(project_out(mixed, weight_out))
        normed_f, factor_f, hnormed = norm_forward(hidden_in, gain_ffn[index])
        hfull = gather_features(hnormed)
        gate_up = project_in(hfull, weight_gu)
        hidden_cols = gate_up.shape[1] // 2
        gate = gate_up[:, :hidden_cols]
        upper = gate_up[:, hidden_cols:]
        active = (jax.nn.silu(gate) * upper).astype(jnp.bfloat16)
        current = hidden_in + sum_features(project_out(active, weight_down))
        saved.append(
            (
                weight_qkv,
                weight_out,
                weight_gu,
                weight_down,
                wholes,
                normed_a,
                factor_a,
                xfull,
                queries,
                seq_keys,
                seq_values,
                log_total,
                mixed,
                normed_f,
                factor_f,
                hfull,
                gate,
                upper,
                active,
            )
        )
    grad_now = grad_out
    list_qkv, list_out, list_gu, list_down, list_ga, list_gf = ([], [], [], [], [], [])
    for index in reversed(range(layers)):
        (
            weight_qkv,
            weight_out,
            weight_gu,
            weight_down,
            wholes,
            normed_a,
            factor_a,
            xfull,
            queries,
            seq_keys,
            seq_values,
            log_total,
            mixed,
            normed_f,
            factor_f,
            hfull,
            gate,
            upper,
            active,
        ) = saved[index]
        grad_full = gather_features(grad_now.astype(jnp.bfloat16))
        grad_active = project_in(grad_full, weight_down)
        list_down.append(weight_grad(grad_full, active))
        sig = jax.nn.sigmoid(gate)
        grad_gate = grad_active * upper * sig * (1.0 + gate * (1.0 - sig))
        grad_up = grad_active * gate * sig
        grad_gu = jnp.concatenate([grad_gate, grad_up], axis=1).astype(jnp.bfloat16)
        grad_hn = sum_features(project_out(grad_gu, weight_gu))
        list_gu.append(weight_grad(hfull, grad_gu).reshape(count_rows, 2, -1))
        grad_mid, gain_f_grad = norm_backward(grad_hn, normed_f, factor_f, gain_ffn[index])
        list_gf.append(gain_f_grad)
        grad_hidden = grad_now + grad_mid
        hidden_full = gather_features(grad_hidden.astype(jnp.bfloat16))
        grad_mixed = project_in(hidden_full, weight_out).astype(jnp.bfloat16)
        list_out.append(weight_grad(hidden_full, mixed))
        grad_heads = grad_mixed.reshape(tok, GROUP, head)
        scores = masked_scores(queries, seq_keys, query_pos, key_pos)
        probs_full = jnp.exp(scores - log_total)
        probs = probs_full.astype(jnp.bfloat16)
        grad_probs = jnp.einsum(
            "qgd,kd->gqk", grad_heads, seq_values, preferred_element_type=jnp.float32
        )
        delta = jnp.sum(probs_full * grad_probs, axis=2, keepdims=True)
        grad_scores = (probs_full * (grad_probs - delta)).astype(jnp.bfloat16)
        inverse = 1.0 / math.sqrt(head)
        grad_queries = (
            jnp.einsum("gqk,kd->qgd", grad_scores, seq_keys, preferred_element_type=jnp.float32)
            * inverse
        )
        grad_keys = (
            jnp.einsum("gqk,qgd->kd", grad_scores, queries, preferred_element_type=jnp.float32)
            * inverse
        )
        grad_values = jnp.einsum(
            "gqk,qgd->kd", probs, grad_heads, preferred_element_type=jnp.float32
        )
        grad_kv = lax.psum_scatter(
            jnp.concatenate([grad_keys, grad_values], axis=1).astype(jnp.bfloat16),
            "row",
            scatter_dimension=0,
            tiled=True,
        ).astype(jnp.float32)
        grad_k = rope_turn(grad_kv[:, :head], cosine, -sine)
        grad_v = grad_kv[:, head:]
        grad_q = rope_turn(grad_queries, cosine[:, None, :], -sine[:, None, :]).reshape(
            tok, query_cols
        )
        grad_qkv = jnp.concatenate([grad_q, grad_k, grad_v], axis=1).astype(jnp.bfloat16)
        grad_xn = sum_features(project_out(grad_qkv, weight_qkv))
        list_qkv.append(weight_grad(xfull, grad_qkv).reshape(count_rows, 1, -1))
        grad_in, gain_a_grad = norm_backward(grad_xn, normed_a, factor_a, gain_attn[index])
        list_ga.append(gain_a_grad)
        grad_now = grad_hidden + grad_in
    gains_a, gains_f = lax.psum((jnp.stack(list_ga[::-1]), jnp.stack(list_gf[::-1])), "row")
    return (
        current,
        grad_now,
        jnp.stack(list_qkv[::-1]),
        jnp.stack(list_out[::-1]),
        jnp.stack(list_gu[::-1]),
        jnp.stack(list_down[::-1]),
        gains_a,
        gains_f,
    )


def share_out(mesh):
    rows, cols = mesh.shape["row"], mesh.shape["col"]
    return Mesh(
        mesh.devices.reshape(rows // 2, 2, cols // 2, 2), ("z", "x", "y", "c")
    )


def swap_grid(values, depth):
    pairs = [(z * depth + g, g * depth + z) for z in range(depth) for g in range(depth)]
    return lax.ppermute(values, ("z", "y", "c"), pairs)


MESH_ID = pl.DeviceIdType.MESH
ROWS = 16
SKEW = 2
GROUP_CHUNKS = 4
EXTRA = 128


def spread(column):
    high = column.astype(jnp.bfloat16)
    low = (column - high.astype(jnp.float32)).astype(jnp.bfloat16)
    lane = lax.broadcasted_iota(jnp.int32, (column.shape[0], EXTRA), 1)
    wide = jnp.where(lane == 0, high.astype(jnp.float32), jnp.where(lane == 1, low.astype(jnp.float32), 0.0))
    return wide.astype(jnp.bfloat16)


def unspread(block):
    return jnp.sum(block.astype(jnp.float32), axis=1, keepdims=True)


def transposed_dot(left, right):
    return lax.dot_general(left, right, (((1,), (1,)), ((), ())), preferred_element_type=jnp.float32)


class Side:
    def __init__(self, send, recv):
        self.peer = {"x": 1 - lax.axis_index("x")}
        self.send, self.recv, self.copies = send, recv, []

    def start(self, source, target):
        at = len(self.copies)
        copy = remote(source, target, self.send.at[at], self.recv.at[at], self.peer)
        copy.start()
        self.copies.append(copy)
        return copy

    def later(self, source, target):
        at = len(self.copies)
        copy = remote(source, target, self.send.at[at], self.recv.at[at], self.peer)
        self.copies.append(copy)
        return copy

    def finish(self, taken=()):
        for copy in self.copies:
            copy.wait_send()
            if not any(copy is item for item in taken):
                copy.wait_recv()


def remote(src, dst, send, recv, device):
    return pltpu.make_async_remote_copy(
        src_ref=src, dst_ref=dst, send_sem=send, recv_sem=recv, device_id=device, device_id_type=MESH_ID
    )


def halves(features):
    half = features // 2
    x = lax.axis_index("x")
    own = pl.ds(pl.multiple_of(x * half, half), half)
    other = pl.ds(pl.multiple_of((1 - x) * half, half), half)
    return own, other


def flip(block):
    return jnp.transpose(block.astype(jnp.float32)).astype(jnp.bfloat16)


def grad_tile(turned, features, right, cols, kept, given):
    own, other = halves(features)
    value = right[:, cols]
    kept[:, cols] = jnp.dot(turned[own, :], value, preferred_element_type=jnp.float32).astype(jnp.bfloat16)
    given[:, cols] = jnp.dot(turned[other, :], value, preferred_element_type=jnp.float32).astype(jnp.bfloat16)


def sem(*shape):
    return pltpu.SemaphoreType.DMA(shape)


class Line:
    def __init__(self, tok, depth):
        self.z, self.x = lax.axis_index("z"), lax.axis_index("x")
        self.y, self.c = lax.axis_index("y"), lax.axis_index("c")
        self.tok, self.depth = tok, depth
        self.half = 2 * tok
        self.chunks = self.half // ROWS
        self.own = pl.multiple_of((2 * self.y + self.c) * tok, tok)
        self.peers = (
            {"y": self.y, "c": 1 - self.c},
            {"y": 1 - self.y, "c": self.c},
            {"y": 1 - self.y, "c": 1 - self.c},
        )

    def greet(self):
        barrier = pltpu.get_barrier_semaphore()
        for peer in self.peers:
            pl.semaphore_signal(barrier, 1, device_id=peer, device_id_type=MESH_ID)

        @pl.when(self.z > 0)
        def _():
            pl.semaphore_signal(barrier, 1, device_id={"z": self.z - 1}, device_id_type=MESH_ID)

        @pl.when(self.z < self.depth - 1)
        def _():
            pl.semaphore_signal(barrier, 1, device_id={"z": self.z + 1}, device_id_type=MESH_ID)

        pl.semaphore_signal(barrier, 1, device_id={"x": 1 - self.x}, device_id_type=MESH_ID)
        inner = jnp.where(self.z > 0, 1, 0) + jnp.where(self.z < self.depth - 1, 1, 0)
        pl.semaphore_wait(barrier, 4 + inner)

    def place(self, stream):
        return self.z if stream == 0 else self.depth - 1 - self.z

    def onward(self, stream):
        return {"z": self.z + 1} if stream == 0 else {"z": self.z - 1}

    def backward(self, stream):
        return {"z": self.z - 1} if stream == 0 else {"z": self.z + 1}

    def row_of(self, stream, chunk):
        per = self.chunks // 2
        far = chunk // per
        y = self.y + far * (1 - 2 * self.y)
        return pl.multiple_of((2 * y + stream) * self.tok + lax.rem(chunk, per) * ROWS, ROWS)


def make_line(tok, depth, width_in, width_out, carry_in, carry_out, features):
    chunks = 2 * tok // ROWS
    groups = chunks // GROUP_CHUNKS
    span = GROUP_CHUNKS * ROWS
    half_groups = groups // 2

    def run(line, taken, begin, prepare, beside, finish, second, settle, close, product, carried, chain_out, chain_in, wide, own_part, rs_out, rs_in,
            ag_s, ag_r, ch_s, ch_r, bc_s, bc_r, rs_s, rs_r):
        line.greet()
        gather = [
            pltpu.make_async_remote_copy(
                src_ref=taken.at[pl.ds(line.own, tok)],
                dst_ref=taken.at[pl.ds(line.own, tok)],
                send_sem=ag_s.at[at],
                recv_sem=ag_r.at[at],
                device_id=peer,
                device_id_type=MESH_ID,
            )
            for at, peer in enumerate(line.peers)
        ]
        for copy in gather:
            copy.start()
        begin()
        gather[0].wait_recv()
        prepare(pl.multiple_of(line.y * 2 * tok, 2 * tok))

        def chain_copy(stream, chunk):
            return pltpu.make_async_remote_copy(
                src_ref=chain_out.at[stream, chunk],
                dst_ref=chain_in.at[stream, chunk],
                send_sem=ch_s.at[stream, chunk],
                recv_sem=ch_r.at[stream, chunk],
                device_id=line.onward(stream),
                device_id_type=MESH_ID,
            )

        def wide_copy(stream, chunk):
            rows = pl.ds(line.row_of(stream, chunk), ROWS)
            return pltpu.make_async_remote_copy(
                src_ref=wide.at[rows],
                dst_ref=wide.at[rows],
                send_sem=bc_s.at[stream, chunk],
                recv_sem=bc_r.at[stream, chunk],
                device_id=line.backward(stream),
                device_id_type=MESH_ID,
            )

        def sum_copy(stream, group):
            far = group // half_groups
            y = line.y + far * (1 - 2 * line.y)
            other = stream + line.c - 2 * stream * line.c
            slot = 2 * far + other - 1
            part = lax.rem(group, half_groups)
            return (slot >= 0, part, pltpu.make_async_remote_copy(
                src_ref=rs_out.at[stream, group],
                dst_ref=rs_in.at[jnp.maximum(slot, 0), pl.ds(pl.multiple_of(part * span, span), span)],
                send_sem=rs_s.at[stream, group],
                recv_sem=rs_r.at[jnp.maximum(slot, 0), part],
                device_id={"y": y, "c": stream},
                device_id_type=MESH_ID,
            ))

        def step(i, _):
            @pl.when(i == SKEW)
            def _():
                gather[1].wait_recv()
                gather[2].wait_recv()
                prepare(pl.multiple_of((1 - line.y) * 2 * tok, 2 * tok))

            beside(i)
            for stream in (0, 1):
                place = line.place(stream)
                chunk = i - SKEW * place

                @pl.when((chunk >= 0) & (chunk < chunks))
                def _():
                    row = line.row_of(stream, chunk)

                    @pl.when(place > 0)
                    def _():
                        chain_copy(stream, chunk).wait_recv()

                    @pl.when(place == 0)
                    def _():
                        chain_out[stream, chunk, :, :width_in] = product[pl.ds(row, ROWS), :].astype(jnp.bfloat16)
                        if carry_in:
                            chain_out[stream, chunk, :, width_in:] = spread(carried[pl.ds(row, ROWS), :1])

                    @pl.when((place > 0) & (place < depth - 1))
                    def _():
                        chain_out[stream, chunk, :, :width_in] = (
                            product[pl.ds(row, ROWS), :] + chain_in[stream, chunk, :, :width_in].astype(jnp.float32)
                        ).astype(jnp.bfloat16)
                        if carry_in:
                            chain_out[stream, chunk, :, width_in:] = spread(
                                carried[pl.ds(row, ROWS), :1] + unspread(chain_in[stream, chunk, :, width_in:])
                            )

                    @pl.when(place < depth - 1)
                    def _():
                        chain_copy(stream, chunk).start()

                    @pl.when(place == depth - 1)
                    def _():
                        total = product[pl.ds(row, ROWS), :] + chain_in[stream, chunk, :, :width_in].astype(jnp.float32)
                        extra = None
                        if carry_in:
                            extra = carried[pl.ds(row, ROWS), :1] + unspread(chain_in[stream, chunk, :, width_in:])
                        finish(row, pl.multiple_of(chunk * ROWS, ROWS), total, extra)
                        wide_copy(stream, chunk).start()

                ready = i - SKEW * (2 * (depth - 1) - place)

                @pl.when((ready >= 0) & (ready < chunks))
                def _():
                    @pl.when(place < depth - 1)
                    def _():
                        wide_copy(stream, ready).wait_recv()

                        @pl.when(place > 0)
                        def _():
                            wide_copy(stream, ready).start()

                    @pl.when(lax.rem(ready, GROUP_CHUNKS) == GROUP_CHUNKS - 1)
                    def _():
                        group = ready // GROUP_CHUNKS
                        row = pl.multiple_of(line.row_of(stream, ready) - (span - ROWS), span)
                        away, part, copy = sum_copy(stream, group)
                        value = second(row, span)

                        @pl.when(away)
                        def _():
                            rs_out[stream, group, :, :features] = value.astype(jnp.bfloat16)
                            if carry_out:
                                rs_out[stream, group, :, features:] = wide[pl.ds(row, span), width_out:]
                            copy.start()

                        @pl.when(jnp.logical_not(away))
                        def _():
                            own_part[pl.ds(pl.multiple_of(part * span, span), span), :] = value

            return 0

        lax.fori_loop(0, chunks + 2 * SKEW * (depth - 1), step, 0)

        def drain(i, _):
            for stream in (0, 1):
                place = line.place(stream)

                @pl.when(place < depth - 1)
                def _():
                    chain_copy(stream, i).wait_send()

                @pl.when(place > 0)
                def _():
                    wide_copy(stream, i).wait_send()

            return 0

        def drain_sums(i, _):
            for stream in (0, 1):
                away, part, copy = sum_copy(stream, i)

                @pl.when(away)
                def _():
                    copy.wait_send()
            return 0

        settle()
        for slot in range(3):
            for part in range(half_groups):
                pltpu.make_async_remote_copy(
                    src_ref=rs_out.at[0, 0],
                    dst_ref=rs_in.at[slot, pl.ds(part * span, span)],
                    send_sem=rs_s.at[0, 0],
                    recv_sem=rs_r.at[slot, part],
                    device_id=line.peers[slot],
                    device_id_type=MESH_ID,
                ).wait_recv()
        close()
        for copy in gather:
            copy.wait_send()
        lax.fori_loop(0, chunks, drain, 0)
        lax.fori_loop(0, groups, drain_sums, 0)

    wide_in = width_in + (EXTRA if carry_in else 0)
    scratch = [
        pltpu.VMEM((4 * tok, width_in), jnp.float32),
        pltpu.VMEM((4 * tok, EXTRA), jnp.float32),
        pltpu.VMEM((2, chunks, ROWS, wide_in), jnp.bfloat16),
        pltpu.VMEM((2, chunks, ROWS, wide_in), jnp.bfloat16),
        pltpu.VMEM((tok, features), jnp.float32),
        pltpu.VMEM((2, groups, span, features + (EXTRA if carry_out else 0)), jnp.bfloat16),
        pltpu.VMEM((3, tok, features + (EXTRA if carry_out else 0)), jnp.bfloat16),
        pltpu.SemaphoreType.DMA((3,)),
        pltpu.SemaphoreType.DMA((3,)),
        pltpu.SemaphoreType.DMA((2, chunks)),
        pltpu.SemaphoreType.DMA((2, chunks)),
        pltpu.SemaphoreType.DMA((2, chunks)),
        pltpu.SemaphoreType.DMA((2, chunks)),
        pltpu.SemaphoreType.DMA((2, groups)),
        pltpu.SemaphoreType.DMA((3, half_groups)),
    ]
    return run, scratch


TILE = 256


def ffn_forward(hidden, gain, gu_own, gu_peer, down_own, shipped, depth):
    tok, features = hidden.shape
    width = down_own.shape[1]
    run, scratch = make_line(tok, depth, 2 * width, width, True, False, features)
    count = len(shipped)

    def kernel(h_ref, gain_ref, w1_own, w1_peer, w2_own, *rest):
        leave, rest = rest[:count], rest[count:]
        (out_ref, normed_t, kept, wide, w2_peer), rest = rest[:5], rest[5:]
        landed, rest = rest[:count], rest[count:]
        (taken, scaled, pieces, side_s, side_r, product, carried, chain_out, chain_in, own_part, rs_out, rs_in), sems = (
            rest[:12], rest[12:])
        line = Line(tok, depth)
        side = Side(side_s, side_r)
        own, other = halves(features)
        taken[pl.ds(line.own, tok), :] = h_ref[...].astype(jnp.bfloat16)

        def begin():
            side.start(w2_own, w2_peer)
            for source, target in zip(leave, landed):
                side.start(source, target)

        def prepare(row):
            rows = pl.ds(row, 2 * tok)
            block = taken[rows, :].astype(jnp.float32)
            carried[rows, :] = jnp.broadcast_to(jnp.sum(block * block, axis=1, keepdims=True), (2 * tok, EXTRA))
            scaled[...] = (block * gain_ref[...]).astype(jnp.bfloat16)

            def tile(j, _):
                cols = pl.ds(pl.multiple_of(j * TILE, TILE), TILE)
                product[rows, cols] = jnp.dot(
                    scaled[:, own], w1_own[:, cols], preferred_element_type=jnp.float32
                ) + jnp.dot(scaled[:, other], w1_peer[:, cols], preferred_element_type=jnp.float32)
                return 0

            lax.fori_loop(0, 2 * width // TILE, tile, 0)

        def beside(i):
            @pl.when(i == SKEW * (depth - 1))
            def _():
                side.copies[0].wait_recv()

        def finish(row, at, total, extra):
            factor = lax.rsqrt(extra / D + EPS)
            gate = total[:, :width] * factor
            upper = total[:, width:] * factor
            kept[pl.ds(at, ROWS), :width] = gate
            kept[pl.ds(at, ROWS), width:] = upper
            active = gate * jax.nn.sigmoid(gate) * upper
            wide[pl.ds(row, ROWS), :width] = active.astype(jnp.bfloat16)
            wide[pl.ds(row, ROWS), width:] = spread(factor)

        def second(row, span):
            value = wide[pl.ds(row, span), :width]
            pieces[:, own] = transposed_dot(value, w2_own[...])
            pieces[:, other] = transposed_dot(value, w2_peer[...])
            return pieces[...]

        def settle():
            normed = taken[...].astype(jnp.float32) * unspread(wide[:, width:]) * gain_ref[...]
            normed_t[...] = jnp.transpose(normed).astype(jnp.bfloat16)

        def close():
            total = own_part[...]
            for slot in range(3):
                total = total + rs_in[slot].astype(jnp.float32)
            out_ref[...] = h_ref[...] + total
            side.finish(side.copies[:1])

        run(line, taken, begin, prepare, beside, finish, second, settle, close, product, carried, chain_out, chain_in, wide,
            own_part, rs_out, rs_in, *sems)

    low, full = jnp.bfloat16, jnp.float32
    shapes = (
        jax.ShapeDtypeStruct((tok, features), full),
        jax.ShapeDtypeStruct((features, 4 * tok), low),
        jax.ShapeDtypeStruct((2 * tok, 2 * width), full),
        jax.ShapeDtypeStruct((4 * tok, width + EXTRA), low),
        jax.ShapeDtypeStruct(down_own.shape, low),
    ) + tuple(jax.ShapeDtypeStruct(item.shape, item.dtype) for item in shipped)
    inside, outside = pl.BlockSpec(memory_space=pltpu.VMEM), pl.BlockSpec(memory_space=pl.ANY)
    out = pl.pallas_call(
        kernel,
        out_shape=shapes,
        in_specs=[inside] * 5 + [outside] * count,
        out_specs=[inside] * 5 + [outside] * count,
        scratch_shapes=[
            pltpu.VMEM((4 * tok, features), low),
            pltpu.VMEM((2 * tok, features), low),
            pltpu.VMEM((GROUP_CHUNKS * ROWS, features), full),
            sem(1 + count), sem(1 + count),
        ] + scratch,
        compiler_params=pltpu.CompilerParams(
            collective_id=1 if count else 5, has_side_effects=True, vmem_limit_bytes=60 << 20
        ),
        cost_estimate=pl.CostEstimate(flops=60_000_000_000, bytes_accessed=8_000_000, transcendentals=0),
        name="ffn_forward",
    )(hidden, gain.reshape(1, -1), gu_own, gu_peer, down_own, *shipped)
    return out[:5], out[5:]


def ffn_backward(grad, hidden, gain, kept, wide_forward, gu_own, gu_peer, down_own, down_peer, shipped, depth):
    tok, features = hidden.shape
    width = down_own.shape[1]
    run, scratch = make_line(tok, depth, width, 2 * width, False, True, features)
    count = len(shipped)
    first_tile = SKEW + 1
    tiles = width // EXTRA

    def kernel(dy_ref, h_ref, gain_ref, kept_ref, before_ref, w1_own, w1_peer, w2_own, w2_peer, *rest):
        leave, rest = rest[:count], rest[count:]
        (out_ref, wide, gain_out, down_kept, down_got), rest = rest[:5], rest[5:]
        landed, rest = rest[:count], rest[count:]
        (taken, turned, down_given, pieces, side_s, side_r, product, carried, chain_out, chain_in, own_part, rs_out,
         rs_in), sems = rest[:13], rest[13:]
        line = Line(tok, depth)
        side = Side(side_s, side_r)
        own, other = halves(features)
        taken[pl.ds(line.own, tok), :] = dy_ref[...].astype(jnp.bfloat16)
        give = side.later(down_given, down_got)

        def begin():
            for source, target in zip(leave, landed):
                side.start(source, target)

        def prepare(row):
            rows = pl.ds(row, 2 * tok)

            def tile(j, _):
                cols = pl.ds(pl.multiple_of(j * EXTRA, EXTRA), EXTRA)
                product[rows, cols] = jnp.dot(
                    taken[rows, own], w2_own[:, cols], preferred_element_type=jnp.float32
                ) + jnp.dot(taken[rows, other], w2_peer[:, cols], preferred_element_type=jnp.float32)
                return 0

            lax.fori_loop(0, width // EXTRA, tile, 0)

        def beside(i):
            @pl.when(i == first_tile)
            def _():
                turned[...] = flip(taken[...])

            @pl.when((i >= first_tile) & (i < first_tile + tiles))
            def _():
                cols = pl.ds(pl.multiple_of((i - first_tile) * EXTRA, EXTRA), EXTRA)
                grad_tile(turned, features, before_ref, cols, down_kept, down_given)

            @pl.when(i == first_tile + tiles)
            def _():
                give.start()

        def finish(row, at, total, extra):
            gate = kept_ref[pl.ds(at, ROWS), :width]
            upper = kept_ref[pl.ds(at, ROWS), width:]
            sig = jax.nn.sigmoid(gate)
            silu = gate * sig
            grad_gate = total * upper * (sig + silu * (1.0 - sig))
            grad_up = total * silu
            wide[pl.ds(row, ROWS), :width] = grad_gate.astype(jnp.bfloat16)
            wide[pl.ds(row, ROWS), width : 2 * width] = grad_up.astype(jnp.bfloat16)
            inner = jnp.sum(grad_gate * gate + grad_up * upper, axis=1, keepdims=True)
            wide[pl.ds(row, ROWS), 2 * width :] = spread(inner)

        def second(row, span):
            value = wide[pl.ds(row, span), : 2 * width]
            pieces[:, own] = transposed_dot(value, w1_own[...])
            pieces[:, other] = transposed_dot(value, w1_peer[...])
            return pieces[...]

        def close():
            total = own_part[...]
            inner = unspread(wide[pl.ds(line.own, tok), 2 * width :])
            for slot in range(3):
                total = total + rs_in[slot, :, :features].astype(jnp.float32)
                inner = inner + unspread(rs_in[slot, :, features:])
            factor = unspread(before_ref[pl.ds(line.own, tok), width:])
            normed = h_ref[...] * factor
            gain_out[...] = jnp.broadcast_to(jnp.sum(total * normed, axis=0, keepdims=True), gain_out.shape)
            out_ref[...] = dy_ref[...] + factor * (total * gain_ref[...] - normed * (inner / D))
            side.finish()

        run(line, taken, begin, prepare, beside, finish, second, lambda: None, close, product, carried, chain_out, chain_in,
            wide, own_part, rs_out, rs_in, *sems)

    low, full = jnp.bfloat16, jnp.float32
    shapes = (
        jax.ShapeDtypeStruct((tok, features), full),
        jax.ShapeDtypeStruct((4 * tok, 2 * width + EXTRA), low),
        jax.ShapeDtypeStruct((8, features), full),
        jax.ShapeDtypeStruct(down_own.shape, low),
        jax.ShapeDtypeStruct(down_own.shape, low),
    ) + tuple(jax.ShapeDtypeStruct(item.shape, item.dtype) for item in shipped)
    inside, outside = pl.BlockSpec(memory_space=pltpu.VMEM), pl.BlockSpec(memory_space=pl.ANY)
    out = pl.pallas_call(
        kernel,
        out_shape=shapes,
        in_specs=[inside] * 9 + [outside] * count,
        out_specs=[inside] * 5 + [outside] * count,
        scratch_shapes=[
            pltpu.VMEM((4 * tok, features), low),
            pltpu.VMEM((features, 4 * tok), low),
            pltpu.VMEM(down_own.shape, low),
            pltpu.VMEM((GROUP_CHUNKS * ROWS, features), full),
            sem(1 + count), sem(1 + count),
        ] + scratch,
        compiler_params=pltpu.CompilerParams(
            collective_id=2 if count else 6, has_side_effects=True, vmem_limit_bytes=60 << 20
        ),
        cost_estimate=pl.CostEstimate(flops=60_000_000_000, bytes_accessed=8_000_000, transcendentals=0),
        name="ffn_backward",
    )(grad, hidden, gain.reshape(1, -1), kept, wide_forward, gu_own, gu_peer, down_own, down_peer, *shipped)
    return out[:5], out[5:]


def to_row(column):
    return jnp.transpose(jnp.broadcast_to(column, (column.shape[0], EXTRA)))[:8]


def to_column(row):
    return jnp.transpose(jnp.broadcast_to(row[:1], (row.shape[1], row.shape[1])))[:, :1]


def turn(values, cosine, sine):
    lane = lax.broadcasted_iota(jnp.int32, values.shape, 1)
    width = values.shape[1]
    back = pltpu.roll(values, width - HEAD // 2, 1)
    forth = pltpu.roll(values, HEAD // 2, 1)
    partner = jnp.where(lax.rem(lane, HEAD) < HEAD // 2, back, forth)
    return values * cosine + partner * sine


def split_pair(block):
    lane = lax.broadcasted_iota(jnp.int32, block.shape, 1)
    zero = jnp.zeros_like(block)
    return jnp.concatenate([jnp.where(lane < HEAD, block, zero), jnp.where(lane < HEAD, zero, block)], axis=0)


def join_pair(turned, tok):
    return jnp.transpose(jnp.concatenate([turned[:HEAD, :tok], turned[HEAD:, tok:]], axis=0))


def twice(kv):
    wide = kv.astype(jnp.float32)
    lane = lax.broadcasted_iota(jnp.int32, wide.shape, 1)
    other = pltpu.roll(wide, HEAD, 1)
    return jnp.where(lane < HEAD, wide, other), jnp.where(lane < HEAD, other, wide)


class Square:
    def __init__(self, tok, depth):
        self.z, self.x = lax.axis_index("z"), lax.axis_index("x")
        self.y, self.c = lax.axis_index("y"), lax.axis_index("c")
        self.tok, self.depth = tok, depth
        self.g = 2 * self.y + self.c
        self.row = 2 * self.z + self.x
        self.own = pl.multiple_of(self.g * tok, tok)
        self.mine = pl.multiple_of(self.z * tok, tok)
        self.peers = (
            {"y": self.y, "c": 1 - self.c},
            {"y": 1 - self.y, "c": self.c},
            {"y": 1 - self.y, "c": 1 - self.c},
        )

    def row_peer(self, step):
        at = lax.rem(self.row + step, 2 * self.depth)
        return {"z": at // 2, "x": lax.rem(at, 2)}

    def greet(self):
        barrier = pltpu.get_barrier_semaphore()
        for peer in self.peers:
            pl.semaphore_signal(barrier, 1, device_id=peer, device_id_type=MESH_ID)
        for step in range(1, 2 * self.depth):
            pl.semaphore_signal(barrier, 1, device_id=self.row_peer(step), device_id_type=MESH_ID)
        pl.semaphore_wait(barrier, 3 + 2 * self.depth - 1)


def start_gather(square, taken, send, recv):
    copies = [
        remote(taken.at[pl.ds(square.own, square.tok)], taken.at[pl.ds(square.own, square.tok)], send.at[at], recv.at[at], peer)
        for at, peer in enumerate(square.peers)
    ]
    for copy in copies:
        copy.start()
    return copies


def line_sum(square, gather, product, own, own_row, outs, ins, row_outs, row_ins, send, recv, row_send, row_recv, between):
    tok, depth = square.tok, square.depth

    def one(order):
        block = lax.rem(2 * square.y + order, depth)
        step = lax.rem(block - square.z + depth, depth)
        slot = jnp.maximum(depth - 1 - step, 0)
        value, column = product(pl.multiple_of(block * tok, tok))

        @pl.when(step == 0)
        def _():
            own[...] = value
            if column is not None:
                own_row[...] = to_row(column)

        copy = remote(outs.at[order], ins.at[slot], send.at[order], recv.at[slot], {"z": block})
        row_copy = None
        if column is not None:
            row_copy = remote(row_outs.at[order], row_ins.at[slot], row_send.at[order], row_recv.at[slot], {"z": block})

        @pl.when(step != 0)
        def _():
            outs[order] = value.astype(jnp.bfloat16)
            copy.start()
            if column is not None:
                row_outs[order] = to_row(column)
                row_copy.start()

        return step, copy, row_copy

    gather[0].wait_recv()
    sent = [one(0), one(1)]
    gather[1].wait_recv()
    gather[2].wait_recv()
    sent += [one(2), one(3)]
    between()
    for slot in range(depth - 1):
        remote(outs.at[0], ins.at[slot], send.at[0], recv.at[slot], {"z": square.z}).wait_recv()
        if row_ins is not None:
            remote(row_outs.at[0], row_ins.at[slot], row_send.at[0], row_recv.at[slot], {"z": square.z}).wait_recv()
    return sent


def line_gather(square, array, rows, send, recv, row_send, row_recv):
    depth = square.depth
    sent = []
    for step in range(1, depth):
        peer = {"z": lax.rem(square.z + step, depth)}
        here = array.at[pl.ds(square.mine, square.tok)]
        copy = remote(here, here, send.at[step - 1], recv.at[depth - 1 - step], peer)
        line = rows.at[square.z]
        row_copy = remote(line, line, row_send.at[step - 1], row_recv.at[depth - 1 - step], peer)
        copy.start()
        row_copy.start()
        sent += [copy, row_copy]
    return sent


def grid_sum(square, array, rows, second, settle, own, outs, ins, row_ins, arrive, row_arrive, send, recv, row_send, row_recv):
    tok, depth = square.tok, square.depth
    sent = []
    for step in range(depth):
        block = lax.rem(square.z + step, depth)
        if step:
            rows_of = pl.ds(pl.multiple_of(block * tok, tok), tok)
            remote(array.at[rows_of], array.at[rows_of], send.at[0], arrive.at[step - 1], {"z": square.z}).wait_recv()
            remote(rows.at[block], rows.at[block], send.at[0], row_arrive.at[step - 1], {"z": square.z}).wait_recv()
        value = second(pl.multiple_of(block * tok, tok))
        away = lax.rem(block - square.g + depth, depth)
        slot = jnp.maximum(depth - 1 - away, 0)
        device = {"y": block // 2, "c": lax.rem(block, 2)}
        copy = remote(outs.at[step], ins.at[slot], send.at[step], recv.at[slot], device)
        row_copy = None
        if row_ins is not None:
            row_copy = remote(rows.at[block], row_ins.at[slot], row_send.at[step], row_recv.at[slot], device)

        @pl.when(away == 0)
        def _():
            own[...] = value

        @pl.when(away != 0)
        def _():
            outs[step] = value.astype(jnp.bfloat16)
            copy.start()
            if row_ins is not None:
                row_copy.start()

        sent.append((away, copy, row_copy))
    settle()
    for slot in range(depth - 1):
        remote(outs.at[0], ins.at[slot], send.at[0], recv.at[slot], square.peers[0]).wait_recv()
        if row_ins is not None:
            remote(rows.at[0], row_ins.at[slot], row_send.at[0], row_recv.at[slot], square.peers[0]).wait_recv()
    return sent


def drain(sent):
    for away, copy, row_copy in sent:

        @pl.when(away != 0)
        def _():
            copy.wait_send()
            if row_copy is not None:
                row_copy.wait_send()


def attention_forward(hidden, gain, qkv_own, out_own, qkv_peer, out_peer, shipped, cosine, sine, depth):
    tok, features = hidden.shape
    cols = qkv_own.shape[1]
    fetch = qkv_peer is None
    extra = 2 if fetch else 0
    count = len(shipped)
    sides = extra + 2 * count
    query_cols = GROUP * HEAD
    seq = 2 * depth * tok
    pairs = query_cols // EXTRA
    scale = 1.0 / math.sqrt(HEAD)

    def kernel(h_ref, gain_ref, wqkv_own, wo_own, cos_ref, sin_ref, *rest):
        if not fetch:
            (wqkv_peer, wo_peer), rest = rest[:2], rest[2:]
        leave, rest = rest[:count], rest[count:]
        (out_ref, normed_t, queries, kv, lse, mixed, factors), rest = rest[:7], rest[7:]
        if fetch:
            (wqkv_peer, wo_peer), rest = rest[:2], rest[2:]
        landed, rest = rest[:count], rest[count:]
        (taken, scaled, pieces, own, own_row, z_out, z_in, zr_out, zr_in, values_t, g_own, g_out, g_in,
         ag_s, ag_r, zs_s, zs_r, zr_s, zr_r, kv_s, kv_r, zg_s, zg_r, zgr_s, zgr_r, gs_s, gs_r), rest = rest[:27], rest[27:]
        square = Square(tok, depth)
        side = Side(*rest) if sides else None
        mine, other = halves(features)
        taken[pl.ds(square.own, tok), :] = h_ref[...].astype(jnp.bfloat16)
        square.greet()
        gather = start_gather(square, taken, ag_s, ag_r)
        urgent = []
        if fetch:
            urgent = [side.start(wqkv_own, wqkv_peer), side.start(wo_own, wo_peer)]
        held = []
        for source, target in zip(leave, landed):
            half = source.shape[0] // 2
            side.start(source.at[pl.ds(0, half)], target.at[pl.ds(0, half)])
            held.append(side.later(source.at[pl.ds(half, half)], target.at[pl.ds(half, half)]))
        for copy in urgent[:1]:
            copy.wait_recv()

        def product(row):
            block = taken[pl.ds(row, tok), :].astype(jnp.float32)
            scaled[...] = (block * gain_ref[...]).astype(jnp.bfloat16)
            return (
                jnp.dot(scaled[:, mine], wqkv_own[...], preferred_element_type=jnp.float32)
                + jnp.dot(scaled[:, other], wqkv_peer[...], preferred_element_type=jnp.float32),
                jnp.sum(block * block, axis=1, keepdims=True),
            )

        sent = line_sum(square, gather, product, own, own_row, z_out, z_in, zr_out, zr_in, zs_s, zs_r, zr_s, zr_r, lambda: None)
        total, squares = own[...], own_row[...]
        for slot in range(depth - 1):
            total = total + z_in[slot].astype(jnp.float32)
            squares = squares + zr_in[slot]
        factor_row = lax.rsqrt(squares / D + EPS)
        factors[square.z] = factor_row
        turned = turn(total * to_column(factor_row), cos_ref[...], sin_ref[...])
        here = pl.ds(pl.multiple_of(square.row * tok, tok), tok)
        kv[here, :] = turned[:, query_cols:].astype(jnp.bfloat16)
        queries[...] = turned[:, :query_cols].astype(jnp.bfloat16)
        spreads = []
        for step in range(1, 2 * depth):
            copy = remote(kv.at[here], kv.at[here], kv_s.at[step - 1], kv_r.at[2 * depth - 1 - step], square.row_peer(step))
            copy.start()
            spreads.append(copy)
        for copy in spreads:
            copy.wait_recv()
        for copy in held:
            copy.start()
        keys, both = twice(kv[...])
        values_t[...] = jnp.transpose(both).astype(jnp.bfloat16)
        keys = keys.astype(jnp.bfloat16)

        def pair(t, _):
            lanes = pl.ds(pl.multiple_of(t * EXTRA, EXTRA), EXTRA)
            scores = transposed_dot(keys, split_pair(queries[:, lanes])) * scale
            key_at = lax.broadcasted_iota(jnp.int32, scores.shape, 0)
            query_at = lax.rem(lax.broadcasted_iota(jnp.int32, scores.shape, 1), tok) + square.row * tok
            scores = jnp.where(key_at <= query_at, scores, -1e30)
            top = jnp.max(scores, axis=0, keepdims=True)
            expo = jnp.exp(scores - top)
            denom = jnp.sum(expo, axis=0, keepdims=True)
            lse[t] = jnp.broadcast_to(top + jnp.log(denom), (8, 2 * tok))
            probs = (expo * (1.0 / denom)).astype(jnp.bfloat16)
            out_t = jnp.dot(values_t[...], probs, preferred_element_type=jnp.float32)
            mixed[pl.ds(square.mine, tok), lanes] = join_pair(out_t, tok).astype(jnp.bfloat16)
            return 0

        lax.fori_loop(0, pairs, pair, 0)
        given = line_gather(square, mixed, factors, zg_s, zg_r, zgr_s, zgr_r)

        for copy in urgent[1:]:
            copy.wait_recv()

        def second(row):
            value = mixed[pl.ds(row, tok), :]
            pieces[:, mine] = transposed_dot(value, wo_own[...])
            pieces[:, other] = transposed_dot(value, wo_peer[...])
            return pieces[...]

        def settle():
            for block in range(depth):
                rows = pl.ds(block * tok, tok)
                normed = taken[rows, :].astype(jnp.float32) * to_column(factors[block]) * gain_ref[...]
                normed_t[:, rows] = jnp.transpose(normed).astype(jnp.bfloat16)

        sums = grid_sum(square, mixed, factors, second, settle, g_own, g_out, g_in, None, zg_r, zgr_r, gs_s, gs_r, None, None)
        total = g_own[...]
        for slot in range(depth - 1):
            total = total + g_in[slot].astype(jnp.float32)
        out_ref[...] = h_ref[...] + total
        drain(sent)
        drain(sums)
        for copy in gather + spreads + given:
            copy.wait_send()
        if side:
            side.finish(urgent)

    low, full = jnp.bfloat16, jnp.float32
    shapes = (
        jax.ShapeDtypeStruct((tok, features), full),
        jax.ShapeDtypeStruct((features, depth * tok), low),
        jax.ShapeDtypeStruct((tok, query_cols), low),
        jax.ShapeDtypeStruct((seq, 2 * HEAD), low),
        jax.ShapeDtypeStruct((pairs, 8, 2 * tok), full),
        jax.ShapeDtypeStruct((depth * tok, query_cols), low),
        jax.ShapeDtypeStruct((depth, 8, tok), full),
    )
    if fetch:
        shapes += (jax.ShapeDtypeStruct(qkv_own.shape, low), jax.ShapeDtypeStruct(out_own.shape, low))
    shapes += tuple(jax.ShapeDtypeStruct(item.shape, item.dtype) for item in shipped)
    inside, outside = pl.BlockSpec(memory_space=pltpu.VMEM), pl.BlockSpec(memory_space=pl.ANY)
    peers = () if fetch else (qkv_peer, out_peer)
    out = pl.pallas_call(
        kernel,
        out_shape=shapes,
        in_specs=[inside] * (6 + len(peers)) + [outside] * count,
        out_specs=[inside] * (7 + extra) + [outside] * count,
        scratch_shapes=[
            pltpu.VMEM((depth * tok, features), low),
            pltpu.VMEM((tok, features), low),
            pltpu.VMEM((tok, features), full),
            pltpu.VMEM((tok, cols), full),
            pltpu.VMEM((8, tok), full),
            pltpu.VMEM((depth, tok, cols), low),
            pltpu.VMEM((depth - 1, tok, cols), low),
            pltpu.VMEM((depth, 8, tok), full),
            pltpu.VMEM((depth - 1, 8, tok), full),
            pltpu.VMEM((2 * HEAD, seq), low),
            pltpu.VMEM((tok, features), full),
            pltpu.VMEM((depth, tok, features), low),
            pltpu.VMEM((depth - 1, tok, features), low),
            sem(3), sem(3), sem(depth), sem(depth - 1), sem(depth), sem(depth - 1),
            sem(2 * depth - 1), sem(2 * depth - 1), sem(depth - 1), sem(depth - 1), sem(depth - 1), sem(depth - 1),
            sem(depth), sem(depth - 1),
        ] + ([sem(sides), sem(sides)] if sides else []),
        compiler_params=pltpu.CompilerParams(
            collective_id=3 if fetch else 7, has_side_effects=True, vmem_limit_bytes=60 << 20
        ),
        cost_estimate=pl.CostEstimate(flops=50_000_000_000, bytes_accessed=8_000_000, transcendentals=0),
        name="attention_forward",
    )(hidden, gain.reshape(1, -1), qkv_own, out_own, cosine, sine, *peers, *shipped)
    peers = out[7:9] if fetch else peers
    return out[:7], peers, out[7 + extra :]


def attention_backward(
    grad, hidden, gain, qkv_own, qkv_peer, out_own, out_peer, cosine, sine, queries, kv, lse, factors, mixed, normed_a, normed_f,
    grad_gu, depth,
):
    tok, features = hidden.shape
    cols = qkv_own.shape[1]
    wide = grad_gu.shape[1] - EXTRA
    query_cols = GROUP * HEAD
    seq = 2 * depth * tok
    pairs = query_cols // EXTRA
    scale = 1.0 / math.sqrt(HEAD)

    def kernel(dy_ref, h_ref, gain_ref, wqkv_own, wqkv_peer, wo_own, wo_peer, cos_ref, sin_ref, q_ref, kv_ref, lse_ref,
               factor_ref, mixed_ref, normed_a_ref, normed_f_ref, gu_ref,
               out_ref, gain_out, gu_kept, gu_got, out_kept, out_got, qkv_kept, qkv_given,
               taken, spun, turned, pieces, gu_given, out_given,
               own, heads, z_out, z_in, keys_t, dk, dv, kv_out, kv_in, dq, inner_rows, g_own, g_out, g_in, g_rows,
               ag_s, ag_r, zs_s, zs_r, kv_s, kv_r, zg_s, zg_r, zgr_s, zgr_r, gs_s, gs_r, gr_s, gr_r, side_s, side_r):
        square = Square(tok, depth)
        side = Side(side_s, side_r)
        mine, other = halves(features)
        taken[pl.ds(square.own, tok), :] = dy_ref[...].astype(jnp.bfloat16)
        square.greet()
        gather = start_gather(square, taken, ag_s, ag_r)

        def gu_tiles(start, stop):
            def tile(j, _):
                grad_tile(normed_f_ref, features, gu_ref, pl.ds(pl.multiple_of(j * EXTRA, EXTRA), EXTRA), gu_kept, gu_given)
                return 0

            lax.fori_loop(start, stop, tile, 0)

        middle = wide // EXTRA // 2
        gu_tiles(0, middle)
        front, rest = pl.ds(0, middle * EXTRA), pl.ds(middle * EXTRA, wide - middle * EXTRA)
        side.start(gu_given.at[:, front], gu_got.at[:, front])

        def between():
            turned[...] = flip(taken[...])
            for t in range(query_cols // EXTRA):
                grad_tile(turned, features, mixed_ref, pl.ds(t * EXTRA, EXTRA), out_kept, out_given)
            side.start(out_given, out_got)
            gu_tiles(middle, wide // EXTRA)

        def product(row):
            rows = pl.ds(row, tok)
            value = jnp.dot(taken[rows, mine], wo_own[...], preferred_element_type=jnp.float32) + jnp.dot(
                taken[rows, other], wo_peer[...], preferred_element_type=jnp.float32
            )
            return value, None

        sent = line_sum(square, gather, product, own, None, z_out, z_in, None, None, zs_s, zs_r, None, None, between)
        total = own[...]
        for slot in range(depth - 1):
            total = total + z_in[slot].astype(jnp.float32)
        heads[...] = total.astype(jnp.bfloat16)
        keys, both = twice(kv_ref[...])
        keys_t[...] = jnp.transpose(keys).astype(jnp.bfloat16)
        keys = keys.astype(jnp.bfloat16)
        both = both.astype(jnp.bfloat16)
        dk[...] = jnp.zeros_like(dk)
        dv[...] = jnp.zeros_like(dv)

        def pair(t, _):
            lanes = pl.ds(pl.multiple_of(t * EXTRA, EXTRA), EXTRA)
            query = split_pair(q_ref[:, lanes])
            head = split_pair(heads[:, lanes])
            scores = transposed_dot(keys, query) * scale
            key_at = lax.broadcasted_iota(jnp.int32, scores.shape, 0)
            query_at = lax.rem(lax.broadcasted_iota(jnp.int32, scores.shape, 1), tok) + square.row * tok
            probs = jnp.exp(jnp.where(key_at <= query_at, scores, -1e30) - lse_ref[t, :1, :])
            grad_probs = transposed_dot(both, head)
            delta = jnp.sum(probs * grad_probs, axis=0, keepdims=True)
            grad_scores = (probs * (grad_probs - delta)).astype(jnp.bfloat16)
            dk[...] += jnp.dot(grad_scores, query, preferred_element_type=jnp.float32)
            dv[...] += jnp.dot(probs.astype(jnp.bfloat16), head, preferred_element_type=jnp.float32)
            turned = jnp.dot(keys_t[...], grad_scores, preferred_element_type=jnp.float32)
            dq[:, lanes] = join_pair(turned, tok) * scale
            return 0

        lax.fori_loop(0, pairs, pair, 0)
        lane = lax.broadcasted_iota(jnp.int32, (seq, EXTRA), 1)
        left = dk[...]
        right = dv[...]
        both_kv = jnp.where(
            lane < HEAD, (left + pltpu.roll(left, HEAD, 1)) * scale, right + pltpu.roll(right, HEAD, 1)
        )
        dk[...] = both_kv
        kv_out[...] = both_kv.astype(jnp.bfloat16)
        here = pl.ds(pl.multiple_of(square.row * tok, tok), tok)
        spreads = []
        for step in range(1, 2 * depth):
            at = lax.rem(square.row + step, 2 * depth)
            copy = remote(
                kv_out.at[pl.ds(pl.multiple_of(at * tok, tok), tok)],
                kv_in.at[2 * depth - 1 - step],
                kv_s.at[step - 1],
                kv_r.at[2 * depth - 1 - step],
                square.row_peer(step),
            )
            copy.start()
            spreads.append(copy)
        total_kv = dk[here, :]
        for copy in spreads:
            copy.wait_recv()
        side.start(gu_given.at[:, rest], gu_got.at[:, rest])
        for slot in range(2 * depth - 1):
            total_kv = total_kv + kv_in[slot].astype(jnp.float32)
        inner = jnp.sum(dq[...] * q_ref[...].astype(jnp.float32), axis=1, keepdims=True) + jnp.sum(
            total_kv * kv_ref[here, :].astype(jnp.float32), axis=1, keepdims=True
        )
        inner_rows[square.z] = to_row(inner)
        whole = jnp.concatenate([dq[...], total_kv], axis=1)
        spun[pl.ds(square.mine, tok), :] = turn(whole, cos_ref[...], -sin_ref[...]).astype(jnp.bfloat16)
        given = line_gather(square, spun, inner_rows, zg_s, zg_r, zgr_s, zgr_r)

        def second(row):
            value = spun[pl.ds(row, tok), :]
            pieces[:, mine] = transposed_dot(value, wqkv_own[...])
            pieces[:, other] = transposed_dot(value, wqkv_peer[...])
            return pieces[...]

        def settle():
            for t in range(cols // EXTRA):
                grad_tile(normed_a_ref, features, spun, pl.ds(t * EXTRA, EXTRA), qkv_kept, qkv_given)

        sums = grid_sum(
            square, spun, inner_rows, second, settle, g_own, g_out, g_in, g_rows, zg_r, zgr_r, gs_s, gs_r, gr_s, gr_r
        )
        total = g_own[...]
        inner = inner_rows[square.g]
        for slot in range(depth - 1):
            total = total + g_in[slot].astype(jnp.float32)
            inner = inner + g_rows[slot]
        factor = to_column(factor_ref[square.g])
        normed = h_ref[...] * factor
        gain_out[...] = jnp.broadcast_to(jnp.sum(total * normed, axis=0, keepdims=True), gain_out.shape)
        out_ref[...] = dy_ref[...] + factor * (total * gain_ref[...] - normed * (to_column(inner) / D))
        drain(sent)
        drain(sums)
        for copy in gather + spreads + given:
            copy.wait_send()
        side.finish()

    low, full = jnp.bfloat16, jnp.float32
    shapes = (
        jax.ShapeDtypeStruct((tok, features), full),
        jax.ShapeDtypeStruct((8, features), full),
        jax.ShapeDtypeStruct((features // 2, wide), low),
        jax.ShapeDtypeStruct((features // 2, wide), low),
        jax.ShapeDtypeStruct(out_own.shape, low),
        jax.ShapeDtypeStruct(out_own.shape, low),
        jax.ShapeDtypeStruct(qkv_own.shape, low),
        jax.ShapeDtypeStruct(qkv_own.shape, low),
    )
    return pl.pallas_call(
        kernel,
        out_shape=shapes,
        in_specs=[pl.BlockSpec(memory_space=pltpu.VMEM)] * 17,
        out_specs=[pl.BlockSpec(memory_space=pltpu.VMEM)] * 8,
        scratch_shapes=[
            pltpu.VMEM((depth * tok, features), low),
            pltpu.VMEM((depth * tok, cols), low),
            pltpu.VMEM((features, depth * tok), low),
            pltpu.VMEM((tok, features), full),
            pltpu.VMEM((features // 2, wide), low),
            pltpu.VMEM(out_own.shape, low),
            pltpu.VMEM((tok, query_cols), full),
            pltpu.VMEM((tok, query_cols), low),
            pltpu.VMEM((depth, tok, query_cols), low),
            pltpu.VMEM((depth - 1, tok, query_cols), low),
            pltpu.VMEM((2 * HEAD, seq), low),
            pltpu.VMEM((seq, 2 * HEAD), full),
            pltpu.VMEM((seq, 2 * HEAD), full),
            pltpu.VMEM((seq, 2 * HEAD), low),
            pltpu.VMEM((2 * depth - 1, tok, 2 * HEAD), low),
            pltpu.VMEM((tok, query_cols), full),
            pltpu.VMEM((depth, 8, tok), full),
            pltpu.VMEM((tok, features), full),
            pltpu.VMEM((depth, tok, features), low),
            pltpu.VMEM((depth - 1, tok, features), low),
            pltpu.VMEM((depth - 1, 8, tok), full),
            sem(3), sem(3), sem(depth), sem(depth - 1),
            sem(2 * depth - 1), sem(2 * depth - 1), sem(depth - 1), sem(depth - 1), sem(depth - 1), sem(depth - 1),
            sem(depth), sem(depth - 1), sem(depth), sem(depth - 1), sem(3), sem(3),
        ],
        compiler_params=pltpu.CompilerParams(collective_id=4, has_side_effects=True, vmem_limit_bytes=60 << 20),
        cost_estimate=pl.CostEstimate(flops=50_000_000_000, bytes_accessed=8_000_000, transcendentals=0),
        name="attention_backward",
    )(grad, hidden, gain.reshape(1, -1), qkv_own, qkv_peer, out_own, out_peer, cosine, sine, queries, kv, lse, factors, mixed,
      normed_a, normed_f, grad_gu)


def stationary(stream, grad_out, wqkv, wo, wgu, wd, gain_attn, gain_ffn):
    tok = stream.shape[0]
    layers = wqkv.shape[0]
    count_rows = wqkv.shape[1]
    depth = lax.axis_size("z")
    head = HEAD
    row = lax.axis_index("z") * 2 + lax.axis_index("x")
    query_pos = row * tok + jnp.arange(tok, dtype=jnp.int32)
    freq = THETA ** (-(jnp.arange(head // 2, dtype=jnp.float32) * 2.0 / head))
    angle = query_pos.astype(jnp.float32)[:, None] * freq[None, :]
    cosine = jnp.cos(angle)
    sine = jnp.sin(angle)
    turns = GROUP + 1
    cosine = jnp.concatenate([jnp.tile(cosine, (1, 2 * turns)), jnp.ones((tok, head), jnp.float32)], axis=1)
    sine = jnp.concatenate(
        [jnp.tile(jnp.concatenate([-sine, sine], axis=1), (1, turns)), jnp.zeros((tok, head), jnp.float32)], axis=1
    )
    current = swap_grid(stream, depth)
    grad_now = swap_grid(grad_out, depth)
    gain_a = swap_grid(gain_attn, depth)
    gain_f = swap_grid(gain_ffn, depth)
    own_qkv = [wqkv[index].reshape(count_rows, -1) for index in range(layers)]
    own_out = [wo[index] for index in range(layers)]
    own_gu = [wgu[index].reshape(count_rows, -1) for index in range(layers)]
    own_down = [wd[index] for index in range(layers)]
    peer_qkv, peer_out, peer_gu, peer_down = ([None] * layers for _ in range(4))
    saved = []
    for index in range(layers):
        before = current
        (hidden_in, normed_a, queries, kv, lse, mixed, factors), (peer_qkv[index], peer_out[index]), landed = attention_forward(
            before, gain_a[index], own_qkv[index], own_out[index], peer_qkv[index], peer_out[index],
            [] if index else own_gu[:1], cosine, sine, depth
        )
        if landed:
            peer_gu[0] = landed[0]
        follow = index + 1
        shipped = [own_qkv[follow], own_out[follow], own_gu[follow]] if follow < layers else []
        (current, normed_f, kept, active, peer_down[index]), landed = ffn_forward(
            hidden_in, gain_f[index], own_gu[index], peer_gu[index], own_down[index], shipped, depth
        )
        if landed:
            peer_qkv[follow], peer_out[follow], peer_gu[follow] = landed
        saved.append((before, normed_a, queries, kv, lse, mixed, factors, hidden_in, normed_f, kept, active))
    list_qkv, list_out, list_gu, list_down, list_ga, list_gf = ([], [], [], [], [], [])
    pending = []
    add = lambda kept, got: kept.astype(jnp.float32) + got.astype(jnp.float32)
    for index in reversed(range(layers)):
        before, normed_a, queries, kv, lse, mixed, factors, hidden_in, normed_f, kept, active = saved[index]
        (grad_hidden, grad_gu, gain_f_grad, down_kept, down_got), landed = ffn_backward(
            grad_now, hidden_in, gain_f[index], kept, active, own_gu[index], peer_gu[index], own_down[index],
            peer_down[index], pending[-1:], depth
        )
        if landed:
            list_qkv.append(add(qkv_kept, landed[0]))
        list_down.append(add(down_kept, down_got))
        list_gf.append(gain_f_grad[0])
        (grad_now, gain_a_grad, gu_kept, gu_got, out_kept, out_got, qkv_kept, qkv_given) = attention_backward(
            grad_hidden, before, gain_a[index], own_qkv[index], peer_qkv[index], own_out[index], peer_out[index],
            cosine, sine, queries, kv, lse, factors, mixed, normed_a, normed_f, grad_gu, depth
        )
        pending.append(qkv_given)
        list_gu.append(add(gu_kept, gu_got).reshape(count_rows, 2, -1))
        list_out.append(add(out_kept, out_got))
        list_ga.append(gain_a_grad[0])
    list_qkv.append(add(qkv_kept, lax.ppermute(qkv_given, "x", [(0, 1), (1, 0)])))
    list_qkv = [item.reshape(count_rows, 1, -1) for item in list_qkv]
    gains = lax.psum(jnp.concatenate([jnp.stack(list_ga[::-1]), jnp.stack(list_gf[::-1])]), ("x", "y", "c"))
    gains = swap_grid(gains, depth)
    return (
        swap_grid(current, depth),
        swap_grid(grad_now, depth),
        jnp.stack(list_qkv[::-1]),
        jnp.stack(list_out[::-1]),
        jnp.stack(list_gu[::-1]),
        jnp.stack(list_down[::-1]),
        gains[:layers],
        gains[layers:],
    )


def solution(mesh):
    rows, cols = ("row", "col")
    body = local
    if (mesh.shape["row"], mesh.shape["col"]) == (8, 4):
        mesh = share_out(mesh)
        rows, cols = (("z", "x"), ("y", "c"))
        body = stationary
    in_specs = (
        P(rows, cols),
        P(rows, cols),
        P(None, rows, cols, None),
        P(None, rows, cols),
        P(None, rows, None, cols),
        P(None, rows, cols),
        P(None, cols),
        P(None, cols),
    )
    out_specs = (
        P(rows, cols),
        P(rows, cols),
        P(None, rows, cols, None),
        P(None, rows, cols),
        P(None, rows, None, cols),
        P(None, rows, cols),
        P(None, cols),
        P(None, cols),
    )
    return jax.shard_map(body, mesh=mesh, in_specs=in_specs, out_specs=out_specs, check_vma=False)
```

```python
import math

import jax
import jax.numpy as jnp
from jax import lax
from jax.experimental import pallas as pl
from jax.experimental.pallas import tpu as pltpu
from jax.sharding import Mesh
from jax.sharding import PartitionSpec as P

D = 2048
HEAD = 64
GROUP = 8


EPS = 1e-05
THETA = 10000.0


def rope_turn(tensor, cosine, sine):
    half = tensor.shape[-1] // 2
    first = tensor[..., :half]
    second = tensor[..., half:]
    return jnp.concatenate(
        [first * cosine - second * sine, second * cosine + first * sine], axis=-1
    )


def feature_sum(values):
    return lax.psum(values, "col")


def gather_features(rows_in):
    return lax.all_gather(rows_in, "col", axis=1, tiled=True)


def sum_features(partials):
    return lax.psum_scatter(
        partials.astype(jnp.bfloat16), "col", scatter_dimension=1, tiled=True
    ).astype(jnp.float32)


def add_rows(left, piece):
    return jnp.dot(left, piece, preferred_element_type=jnp.float32)


def project_in(left, shard):
    return add_rows(left, lax.all_gather(shard, "row", axis=0, tiled=True))


def columns_of(left, piece):
    return jnp.einsum("tj,dj->td", left, piece, preferred_element_type=jnp.float32)


def project_out(left, shard):
    return columns_of(left, lax.all_gather(shard, "row", axis=0, tiled=True))


def weight_grad(left, right):
    return lax.psum_scatter(
        lax.dot_general(
            left, right, (((0,), (0,)), ((), ())), preferred_element_type=jnp.float32
        ).astype(jnp.bfloat16),
        "row",
        scatter_dimension=0,
        tiled=True,
    ).astype(jnp.float32)


def norm_forward(values, gain):
    total = feature_sum(jnp.sum(values * values, axis=1))
    factor = lax.rsqrt(total / D + EPS)
    normed = values * factor[:, None]
    return (normed, factor, (normed * gain).astype(jnp.bfloat16))


def norm_backward(grad_normed, normed, factor, gain):
    scaled = grad_normed * gain
    inner = feature_sum(jnp.sum(scaled * normed, axis=1))
    grad_in = factor[:, None] * (scaled - normed * (inner / D)[:, None])
    return (grad_in, jnp.sum(grad_normed * normed, axis=0))


def masked_scores(queries, keys, query_pos, key_pos):
    scores = jnp.einsum("qgd,kd->gqk", queries, keys, preferred_element_type=jnp.float32) * (
        1.0 / math.sqrt(queries.shape[-1])
    )
    return jnp.where(key_pos[None, None, :] <= query_pos[None, :, None], scores, -1e30)


def local(stream, grad_out, wqkv, wo, wgu, wd, gain_attn, gain_ffn):
    tok = stream.shape[0]
    layers = wqkv.shape[0]
    count_rows = wqkv.shape[1]
    head = HEAD
    query_cols = GROUP * head
    seq_len = lax.axis_size("row") * tok
    query_pos = lax.axis_index("row") * tok + jnp.arange(tok, dtype=jnp.int32)
    key_pos = jnp.arange(seq_len, dtype=jnp.int32)
    freq = THETA ** (-(jnp.arange(head // 2, dtype=jnp.float32) * 2.0 / head))
    angle = query_pos.astype(jnp.float32)[:, None] * freq[None, :]
    cosine = jnp.cos(angle)
    sine = jnp.sin(angle)
    saved = []
    current = stream
    for index in range(layers):
        weight_qkv = wqkv[index].reshape(count_rows, -1)
        weight_out = wo[index]
        weight_gu = wgu[index].reshape(count_rows, -1)
        weight_down = wd[index]
        wholes = (None, None, None, None)
        normed_a, factor_a, xnormed = norm_forward(current, gain_attn[index])
        xfull = gather_features(xnormed)
        qkv = project_in(xfull, weight_qkv)
        queries = rope_turn(
            qkv[:, :query_cols].reshape(tok, GROUP, head), cosine[:, None, :], sine[:, None, :]
        ).astype(jnp.bfloat16)
        keys = rope_turn(qkv[:, query_cols : query_cols + head], cosine, sine).astype(jnp.bfloat16)
        values = qkv[:, query_cols + head :].astype(jnp.bfloat16)
        seqkv = lax.all_gather(jnp.concatenate([keys, values], axis=1), "row", axis=0, tiled=True)
        seq_keys = seqkv[:, :head]
        seq_values = seqkv[:, head:]
        scores = masked_scores(queries, seq_keys, query_pos, key_pos)
        top = jnp.max(scores, axis=2, keepdims=True)
        expo = jnp.exp(scores - top)
        denom = jnp.sum(expo, axis=2, keepdims=True)
        probs = (expo / denom).astype(jnp.bfloat16)
        log_total = top + jnp.log(denom)
        mixed = (
            jnp.einsum("gqk,kd->qgd", probs, seq_values, preferred_element_type=jnp.float32)
            .reshape(tok, query_cols)
            .astype(jnp.bfloat16)
        )
        hidden_in = current + sum_features(project_out(mixed, weight_out))
        normed_f, factor_f, hnormed = norm_forward(hidden_in, gain_ffn[index])
        hfull = gather_features(hnormed)
        gate_up = project_in(hfull, weight_gu)
        hidden_cols = gate_up.shape[1] // 2
        gate = gate_up[:, :hidden_cols]
        upper = gate_up[:, hidden_cols:]
        active = (jax.nn.silu(gate) * upper).astype(jnp.bfloat16)
        current = hidden_in + sum_features(project_out(active, weight_down))
        saved.append(
            (
                weight_qkv,
                weight_out,
                weight_gu,
                weight_down,
                wholes,
                normed_a,
                factor_a,
                xfull,
                queries,
                seq_keys,
                seq_values,
                log_total,
                mixed,
                normed_f,
                factor_f,
                hfull,
                gate,
                upper,
                active,
            )
        )
    grad_now = grad_out
    list_qkv, list_out, list_gu, list_down, list_ga, list_gf = ([], [], [], [], [], [])
    for index in reversed(range(layers)):
        (
            weight_qkv,
            weight_out,
            weight_gu,
            weight_down,
            wholes,
            normed_a,
            factor_a,
            xfull,
            queries,
            seq_keys,
            seq_values,
            log_total,
            mixed,
            normed_f,
            factor_f,
            hfull,
            gate,
            upper,
            active,
        ) = saved[index]
        grad_full = gather_features(grad_now.astype(jnp.bfloat16))
        grad_active = project_in(grad_full, weight_down)
        list_down.append(weight_grad(grad_full, active))
        sig = jax.nn.sigmoid(gate)
        grad_gate = grad_active * upper * sig * (1.0 + gate * (1.0 - sig))
        grad_up = grad_active * gate * sig
        grad_gu = jnp.concatenate([grad_gate, grad_up], axis=1).astype(jnp.bfloat16)
        grad_hn = sum_features(project_out(grad_gu, weight_gu))
        list_gu.append(weight_grad(hfull, grad_gu).reshape(count_rows, 2, -1))
        grad_mid, gain_f_grad = norm_backward(grad_hn, normed_f, factor_f, gain_ffn[index])
        list_gf.append(gain_f_grad)
        grad_hidden = grad_now + grad_mid
        hidden_full = gather_features(grad_hidden.astype(jnp.bfloat16))
        grad_mixed = project_in(hidden_full, weight_out).astype(jnp.bfloat16)
        list_out.append(weight_grad(hidden_full, mixed))
        grad_heads = grad_mixed.reshape(tok, GROUP, head)
        scores = masked_scores(queries, seq_keys, query_pos, key_pos)
        probs_full = jnp.exp(scores - log_total)
        probs = probs_full.astype(jnp.bfloat16)
        grad_probs = jnp.einsum(
            "qgd,kd->gqk", grad_heads, seq_values, preferred_element_type=jnp.float32
        )
        delta = jnp.sum(probs_full * grad_probs, axis=2, keepdims=True)
        grad_scores = (probs_full * (grad_probs - delta)).astype(jnp.bfloat16)
        inverse = 1.0 / math.sqrt(head)
        grad_queries = (
            jnp.einsum("gqk,kd->qgd", grad_scores, seq_keys, preferred_element_type=jnp.float32)
            * inverse
        )
        grad_keys = (
            jnp.einsum("gqk,qgd->kd", grad_scores, queries, preferred_element_type=jnp.float32)
            * inverse
        )
        grad_values = jnp.einsum(
            "gqk,qgd->kd", probs, grad_heads, preferred_element_type=jnp.float32
        )
        grad_kv = lax.psum_scatter(
            jnp.concatenate([grad_keys, grad_values], axis=1).astype(jnp.bfloat16),
            "row",
            scatter_dimension=0,
            tiled=True,
        ).astype(jnp.float32)
        grad_k = rope_turn(grad_kv[:, :head], cosine, -sine)
        grad_v = grad_kv[:, head:]
        grad_q = rope_turn(grad_queries, cosine[:, None, :], -sine[:, None, :]).reshape(
            tok, query_cols
        )
        grad_qkv = jnp.concatenate([grad_q, grad_k, grad_v], axis=1).astype(jnp.bfloat16)
        grad_xn = sum_features(project_out(grad_qkv, weight_qkv))
        list_qkv.append(weight_grad(xfull, grad_qkv).reshape(count_rows, 1, -1))
        grad_in, gain_a_grad = norm_backward(grad_xn, normed_a, factor_a, gain_attn[index])
        list_ga.append(gain_a_grad)
        grad_now = grad_hidden + grad_in
    gains_a, gains_f = lax.psum((jnp.stack(list_ga[::-1]), jnp.stack(list_gf[::-1])), "row")
    return (
        current,
        grad_now,
        jnp.stack(list_qkv[::-1]),
        jnp.stack(list_out[::-1]),
        jnp.stack(list_gu[::-1]),
        jnp.stack(list_down[::-1]),
        gains_a,
        gains_f,
    )


def share_out(mesh):
    rows, cols = mesh.shape["row"], mesh.shape["col"]
    return Mesh(
        mesh.devices.reshape(rows // 2, 2, cols // 2, 2), ("z", "x", "y", "c")
    )


def swap_grid(values, depth):
    pairs = [(z * depth + g, g * depth + z) for z in range(depth) for g in range(depth)]
    return lax.ppermute(values, ("z", "y", "c"), pairs)


MESH_ID = pl.DeviceIdType.MESH
ROWS = 16
SKEW = 3
GROUP_CHUNKS = 4
EXTRA = 128


def spread(column):
    high = column.astype(jnp.bfloat16)
    low = (column - high.astype(jnp.float32)).astype(jnp.bfloat16)
    lane = lax.broadcasted_iota(jnp.int32, (column.shape[0], EXTRA), 1)
    wide = jnp.where(lane == 0, high.astype(jnp.float32), jnp.where(lane == 1, low.astype(jnp.float32), 0.0))
    return wide.astype(jnp.bfloat16)


def unspread(block):
    return jnp.sum(block.astype(jnp.float32), axis=1, keepdims=True)


def transposed_dot(left, right):
    return lax.dot_general(left, right, (((1,), (1,)), ((), ())), preferred_element_type=jnp.float32)


class Side:
    def __init__(self, send, recv):
        self.peer = {"x": 1 - lax.axis_index("x")}
        self.send, self.recv, self.copies = send, recv, []

    def start(self, source, target):
        at = len(self.copies)
        copy = remote(source, target, self.send.at[at], self.recv.at[at], self.peer)
        copy.start()
        self.copies.append(copy)
        return copy

    def later(self, source, target):
        at = len(self.copies)
        copy = remote(source, target, self.send.at[at], self.recv.at[at], self.peer)
        self.copies.append(copy)
        return copy

    def finish(self, taken=()):
        for copy in self.copies:
            copy.wait_send()
            if not any(copy is item for item in taken):
                copy.wait_recv()


def remote(src, dst, send, recv, device):
    return pltpu.make_async_remote_copy(
        src_ref=src, dst_ref=dst, send_sem=send, recv_sem=recv, device_id=device, device_id_type=MESH_ID
    )


def halves(features):
    half = features // 2
    x = lax.axis_index("x")
    own = pl.ds(pl.multiple_of(x * half, half), half)
    other = pl.ds(pl.multiple_of((1 - x) * half, half), half)
    return own, other


def flip(block):
    return jnp.transpose(block.astype(jnp.float32)).astype(jnp.bfloat16)


def grad_tile(turned, features, right, cols, kept, given):
    own, other = halves(features)
    value = right[:, cols]
    kept[:, cols] = jnp.dot(turned[own, :], value, preferred_element_type=jnp.float32).astype(jnp.bfloat16)
    given[:, cols] = jnp.dot(turned[other, :], value, preferred_element_type=jnp.float32).astype(jnp.bfloat16)


def sem(*shape):
    return pltpu.SemaphoreType.DMA(shape)


class Line:
    def __init__(self, tok, depth):
        self.z, self.x = lax.axis_index("z"), lax.axis_index("x")
        self.y, self.c = lax.axis_index("y"), lax.axis_index("c")
        self.tok, self.depth = tok, depth
        self.half = 2 * tok
        self.chunks = self.half // ROWS
        self.own = pl.multiple_of((2 * self.y + self.c) * tok, tok)
        self.peers = (
            {"y": self.y, "c": 1 - self.c},
            {"y": 1 - self.y, "c": self.c},
            {"y": 1 - self.y, "c": 1 - self.c},
        )

    def greet(self):
        barrier = pltpu.get_barrier_semaphore()
        for peer in self.peers:
            pl.semaphore_signal(barrier, 1, device_id=peer, device_id_type=MESH_ID)

        @pl.when(self.z > 0)
        def _():
            pl.semaphore_signal(barrier, 1, device_id={"z": self.z - 1}, device_id_type=MESH_ID)

        @pl.when(self.z < self.depth - 1)
        def _():
            pl.semaphore_signal(barrier, 1, device_id={"z": self.z + 1}, device_id_type=MESH_ID)

        pl.semaphore_signal(barrier, 1, device_id={"x": 1 - self.x}, device_id_type=MESH_ID)
        inner = jnp.where(self.z > 0, 1, 0) + jnp.where(self.z < self.depth - 1, 1, 0)
        pl.semaphore_wait(barrier, 4 + inner)

    def place(self, stream):
        return self.z if stream == 0 else self.depth - 1 - self.z

    def onward(self, stream):
        return {"z": self.z + 1} if stream == 0 else {"z": self.z - 1}

    def backward(self, stream):
        return {"z": self.z - 1} if stream == 0 else {"z": self.z + 1}

    def row_of(self, stream, chunk):
        per = self.chunks // 2
        far = chunk // per
        y = self.y + far * (1 - 2 * self.y)
        return pl.multiple_of((2 * y + stream) * self.tok + lax.rem(chunk, per) * ROWS, ROWS)


def make_line(tok, depth, width_in, width_out, carry_in, carry_out, features):
    chunks = 2 * tok // ROWS
    groups = chunks // GROUP_CHUNKS
    span = GROUP_CHUNKS * ROWS
    half_groups = groups // 2

    def run(line, taken, begin, prepare, beside, finish, second, settle, close, product, carried, chain_out, chain_in, wide, own_part, rs_out, rs_in,
            ag_s, ag_r, ch_s, ch_r, bc_s, bc_r, rs_s, rs_r):
        line.greet()
        gather = [
            pltpu.make_async_remote_copy(
                src_ref=taken.at[pl.ds(line.own, tok)],
                dst_ref=taken.at[pl.ds(line.own, tok)],
                send_sem=ag_s.at[at],
                recv_sem=ag_r.at[at],
                device_id=peer,
                device_id_type=MESH_ID,
            )
            for at, peer in enumerate(line.peers)
        ]
        for copy in gather:
            copy.start()
        begin()
        gather[0].wait_recv()
        prepare(pl.multiple_of(line.y * 2 * tok, 2 * tok))

        def chain_copy(stream, chunk):
            return pltpu.make_async_remote_copy(
                src_ref=chain_out.at[stream, chunk],
                dst_ref=chain_in.at[stream, chunk],
                send_sem=ch_s.at[stream, chunk],
                recv_sem=ch_r.at[stream, chunk],
                device_id=line.onward(stream),
                device_id_type=MESH_ID,
            )

        def wide_copy(stream, chunk):
            rows = pl.ds(line.row_of(stream, chunk), ROWS)
            return pltpu.make_async_remote_copy(
                src_ref=wide.at[rows],
                dst_ref=wide.at[rows],
                send_sem=bc_s.at[stream, chunk],
                recv_sem=bc_r.at[stream, chunk],
                device_id=line.backward(stream),
                device_id_type=MESH_ID,
            )

        def sum_copy(stream, group):
            far = group // half_groups
            y = line.y + far * (1 - 2 * line.y)
            other = stream + line.c - 2 * stream * line.c
            slot = 2 * far + other - 1
            part = lax.rem(group, half_groups)
            return (slot >= 0, part, pltpu.make_async_remote_copy(
                src_ref=rs_out.at[stream, group],
                dst_ref=rs_in.at[jnp.maximum(slot, 0), pl.ds(pl.multiple_of(part * span, span), span)],
                send_sem=rs_s.at[stream, group],
                recv_sem=rs_r.at[jnp.maximum(slot, 0), part],
                device_id={"y": y, "c": stream},
                device_id_type=MESH_ID,
            ))

        def step(i, _):
            @pl.when(i == SKEW)
            def _():
                gather[1].wait_recv()
                gather[2].wait_recv()
                prepare(pl.multiple_of((1 - line.y) * 2 * tok, 2 * tok))

            beside(i)
            for stream in (0, 1):
                place = line.place(stream)
                chunk = i - SKEW * place

                @pl.when((chunk >= 0) & (chunk < chunks))
                def _():
                    row = line.row_of(stream, chunk)

                    @pl.when(place > 0)
                    def _():
                        chain_copy(stream, chunk).wait_recv()

                    @pl.when(place == 0)
                    def _():
                        chain_out[stream, chunk, :, :width_in] = product[pl.ds(row, ROWS), :].astype(jnp.bfloat16)
                        if carry_in:
                            chain_out[stream, chunk, :, width_in:] = spread(carried[pl.ds(row, ROWS), :1])

                    @pl.when((place > 0) & (place < depth - 1))
                    def _():
                        chain_out[stream, chunk, :, :width_in] = (
                            product[pl.ds(row, ROWS), :] + chain_in[stream, chunk, :, :width_in].astype(jnp.float32)
                        ).astype(jnp.bfloat16)
                        if carry_in:
                            chain_out[stream, chunk, :, width_in:] = spread(
                                carried[pl.ds(row, ROWS), :1] + unspread(chain_in[stream, chunk, :, width_in:])
                            )

                    @pl.when(place < depth - 1)
                    def _():
                        chain_copy(stream, chunk).start()

                    @pl.when(place == depth - 1)
                    def _():
                        total = product[pl.ds(row, ROWS), :] + chain_in[stream, chunk, :, :width_in].astype(jnp.float32)
                        extra = None
                        if carry_in:
                            extra = carried[pl.ds(row, ROWS), :1] + unspread(chain_in[stream, chunk, :, width_in:])
                        finish(row, pl.multiple_of(chunk * ROWS, ROWS), total, extra)
                        wide_copy(stream, chunk).start()

                ready = i - SKEW * (2 * (depth - 1) - place)

                @pl.when((ready >= 0) & (ready < chunks))
                def _():
                    @pl.when(place < depth - 1)
                    def _():
                        wide_copy(stream, ready).wait_recv()

                        @pl.when(place > 0)
                        def _():
                            wide_copy(stream, ready).start()

                    @pl.when(lax.rem(ready, GROUP_CHUNKS) == GROUP_CHUNKS - 1)
                    def _():
                        group = ready // GROUP_CHUNKS
                        row = pl.multiple_of(line.row_of(stream, ready) - (span - ROWS), span)
                        away, part, copy = sum_copy(stream, group)
                        value = second(row, span)

                        @pl.when(away)
                        def _():
                            rs_out[stream, group, :, :features] = value.astype(jnp.bfloat16)
                            if carry_out:
                                rs_out[stream, group, :, features:] = wide[pl.ds(row, span), width_out:]
                            copy.start()

                        @pl.when(jnp.logical_not(away))
                        def _():
                            own_part[pl.ds(pl.multiple_of(part * span, span), span), :] = value

            return 0

        lax.fori_loop(0, chunks + 2 * SKEW * (depth - 1), step, 0)

        def drain(i, _):
            for stream in (0, 1):
                place = line.place(stream)

                @pl.when(place < depth - 1)
                def _():
                    chain_copy(stream, i).wait_send()

                @pl.when(place > 0)
                def _():
                    wide_copy(stream, i).wait_send()

            return 0

        def drain_sums(i, _):
            for stream in (0, 1):
                away, part, copy = sum_copy(stream, i)

                @pl.when(away)
                def _():
                    copy.wait_send()
            return 0

        settle()
        for slot in range(3):
            for part in range(half_groups):
                pltpu.make_async_remote_copy(
                    src_ref=rs_out.at[0, 0],
                    dst_ref=rs_in.at[slot, pl.ds(part * span, span)],
                    send_sem=rs_s.at[0, 0],
                    recv_sem=rs_r.at[slot, part],
                    device_id=line.peers[slot],
                    device_id_type=MESH_ID,
                ).wait_recv()
        close()
        for copy in gather:
            copy.wait_send()
        lax.fori_loop(0, chunks, drain, 0)
        lax.fori_loop(0, groups, drain_sums, 0)

    wide_in = width_in + (EXTRA if carry_in else 0)
    scratch = [
        pltpu.VMEM((4 * tok, width_in), jnp.float32),
        pltpu.VMEM((4 * tok, EXTRA), jnp.float32),
        pltpu.VMEM((2, chunks, ROWS, wide_in), jnp.bfloat16),
        pltpu.VMEM((2, chunks, ROWS, wide_in), jnp.bfloat16),
        pltpu.VMEM((tok, features), jnp.float32),
        pltpu.VMEM((2, groups, span, features + (EXTRA if carry_out else 0)), jnp.bfloat16),
        pltpu.VMEM((3, tok, features + (EXTRA if carry_out else 0)), jnp.bfloat16),
        pltpu.SemaphoreType.DMA((3,)),
        pltpu.SemaphoreType.DMA((3,)),
        pltpu.SemaphoreType.DMA((2, chunks)),
        pltpu.SemaphoreType.DMA((2, chunks)),
        pltpu.SemaphoreType.DMA((2, chunks)),
        pltpu.SemaphoreType.DMA((2, chunks)),
        pltpu.SemaphoreType.DMA((2, groups)),
        pltpu.SemaphoreType.DMA((3, half_groups)),
    ]
    return run, scratch


TILE = 256


def ffn_forward(hidden, gain, gu_own, gu_peer, down_own, shipped, depth, ident):
    tok, features = hidden.shape
    width = down_own.shape[1]
    run, scratch = make_line(tok, depth, 2 * width, width, True, False, features)
    count = len(shipped)

    def kernel(h_ref, gain_ref, w1_own, w1_peer, w2_own, *rest):
        leave, rest = rest[:count], rest[count:]
        (out_ref, normed_t, kept, wide, w2_peer), rest = rest[:5], rest[5:]
        landed, rest = rest[:count], rest[count:]
        (taken, scaled, pieces, side_s, side_r, product, carried, chain_out, chain_in, own_part, rs_out, rs_in), sems = (
            rest[:12], rest[12:])
        line = Line(tok, depth)
        side = Side(side_s, side_r)
        own, other = halves(features)
        taken[pl.ds(line.own, tok), :] = h_ref[...].astype(jnp.bfloat16)

        def begin():
            side.start(w2_own, w2_peer)
            for source, target in zip(leave, landed):
                side.start(source, target)

        def prepare(row):
            rows = pl.ds(row, 2 * tok)
            block = taken[rows, :].astype(jnp.float32)
            carried[rows, :] = jnp.broadcast_to(jnp.sum(block * block, axis=1, keepdims=True), (2 * tok, EXTRA))
            scaled[...] = (block * gain_ref[...]).astype(jnp.bfloat16)

            def tile(j, _):
                cols = pl.ds(pl.multiple_of(j * TILE, TILE), TILE)
                product[rows, cols] = jnp.dot(
                    scaled[:, own], w1_own[:, cols], preferred_element_type=jnp.float32
                ) + jnp.dot(scaled[:, other], w1_peer[:, cols], preferred_element_type=jnp.float32)
                return 0

            lax.fori_loop(0, 2 * width // TILE, tile, 0)

        def beside(i):
            @pl.when(i == SKEW * (depth - 1))
            def _():
                side.copies[0].wait_recv()

        def finish(row, at, total, extra):
            factor = lax.rsqrt(extra / D + EPS)
            gate = total[:, :width] * factor
            upper = total[:, width:] * factor
            kept[pl.ds(at, ROWS), :width] = gate
            kept[pl.ds(at, ROWS), width:] = upper
            active = gate * jax.nn.sigmoid(gate) * upper
            wide[pl.ds(row, ROWS), :width] = active.astype(jnp.bfloat16)
            wide[pl.ds(row, ROWS), width:] = spread(factor)

        def second(row, span):
            value = wide[pl.ds(row, span), :width]
            pieces[:, own] = transposed_dot(value, w2_own[...])
            pieces[:, other] = transposed_dot(value, w2_peer[...])
            return pieces[...]

        def settle():
            normed = taken[...].astype(jnp.float32) * unspread(wide[:, width:]) * gain_ref[...]
            normed_t[...] = jnp.transpose(normed).astype(jnp.bfloat16)

        def close():
            total = own_part[...]
            for slot in range(3):
                total = total + rs_in[slot].astype(jnp.float32)
            out_ref[...] = h_ref[...] + total
            side.finish(side.copies[:1])

        run(line, taken, begin, prepare, beside, finish, second, settle, close, product, carried, chain_out, chain_in, wide,
            own_part, rs_out, rs_in, *sems)

    low, full = jnp.bfloat16, jnp.float32
    shapes = (
        jax.ShapeDtypeStruct((tok, features), full),
        jax.ShapeDtypeStruct((features, 4 * tok), low),
        jax.ShapeDtypeStruct((2 * tok, 2 * width), full),
        jax.ShapeDtypeStruct((4 * tok, width + EXTRA), low),
        jax.ShapeDtypeStruct(down_own.shape, low),
    ) + tuple(jax.ShapeDtypeStruct(item.shape, item.dtype) for item in shipped)
    inside, outside = pl.BlockSpec(memory_space=pltpu.VMEM), pl.BlockSpec(memory_space=pl.ANY)
    out = pl.pallas_call(
        kernel,
        out_shape=shapes,
        in_specs=[inside] * 5 + [outside] * count,
        out_specs=[inside] * 5 + [outside] * count,
        scratch_shapes=[
            pltpu.VMEM((4 * tok, features), low),
            pltpu.VMEM((2 * tok, features), low),
            pltpu.VMEM((GROUP_CHUNKS * ROWS, features), full),
            sem(1 + count), sem(1 + count),
        ] + scratch,
        compiler_params=pltpu.CompilerParams(
            collective_id=ident, has_side_effects=True, vmem_limit_bytes=60 << 20
        ),
        cost_estimate=pl.CostEstimate(flops=60_000_000_000, bytes_accessed=8_000_000, transcendentals=0),
        name="ffn_forward",
    )(hidden, gain.reshape(1, -1), gu_own, gu_peer, down_own, *shipped)
    return out[:5], out[5:]


def ffn_backward(
    grad, hidden, gain, kept, wide_forward, gu_own, gu_peer, down_own, down_peer, shipped, stacks, index, layers, depth, ident
):
    tok, features = hidden.shape
    width = down_own.shape[1]
    run, scratch = make_line(tok, depth, width, 2 * width, False, True, features)
    count = len(shipped)
    first_tile = SKEW + 1
    tiles = width // EXTRA

    def kernel(dy_ref, h_ref, gain_ref, kept_ref, before_ref, w1_own, w1_peer, w2_own, w2_peer, *rest):
        leave, rest = rest[:count], rest[count:]
        rest = rest[len(stacks):]
        (out_ref, wide, gain_out, kept_all, got_all), rest = rest[:5], rest[5:]
        landed, rest = rest[:count], rest[count:]
        (taken, turned, down_kept, down_given, keep_s, pieces, side_s, side_r, product, carried, chain_out, chain_in, own_part,
         rs_out, rs_in), sems = rest[:15], rest[15:]
        line = Line(tok, depth)
        side = Side(side_s, side_r)
        own, other = halves(features)
        taken[pl.ds(line.own, tok), :] = dy_ref[...].astype(jnp.bfloat16)
        give = side.later(down_given, got_all.at[index])
        keep = pltpu.make_async_copy(down_kept, kept_all.at[index], keep_s)

        def begin():
            for source, target in zip(leave, landed):
                side.start(source, target)

        def prepare(row):
            rows = pl.ds(row, 2 * tok)

            def tile(j, _):
                cols = pl.ds(pl.multiple_of(j * EXTRA, EXTRA), EXTRA)
                product[rows, cols] = jnp.dot(
                    taken[rows, own], w2_own[:, cols], preferred_element_type=jnp.float32
                ) + jnp.dot(taken[rows, other], w2_peer[:, cols], preferred_element_type=jnp.float32)
                return 0

            lax.fori_loop(0, width // EXTRA, tile, 0)

        def beside(i):
            @pl.when(i == first_tile)
            def _():
                turned[...] = flip(taken[...])

            @pl.when((i >= first_tile) & (i < first_tile + tiles))
            def _():
                cols = pl.ds(pl.multiple_of((i - first_tile) * EXTRA, EXTRA), EXTRA)
                grad_tile(turned, features, before_ref, cols, down_kept, down_given)

            @pl.when(i == first_tile + tiles)
            def _():
                give.start()
                keep.start()

        def finish(row, at, total, extra):
            gate = kept_ref[pl.ds(at, ROWS), :width]
            upper = kept_ref[pl.ds(at, ROWS), width:]
            sig = jax.nn.sigmoid(gate)
            silu = gate * sig
            grad_gate = total * upper * (sig + silu * (1.0 - sig))
            grad_up = total * silu
            wide[pl.ds(row, ROWS), :width] = grad_gate.astype(jnp.bfloat16)
            wide[pl.ds(row, ROWS), width : 2 * width] = grad_up.astype(jnp.bfloat16)
            inner = jnp.sum(grad_gate * gate + grad_up * upper, axis=1, keepdims=True)
            wide[pl.ds(row, ROWS), 2 * width :] = spread(inner)

        def second(row, span):
            value = wide[pl.ds(row, span), : 2 * width]
            pieces[:, own] = transposed_dot(value, w1_own[...])
            pieces[:, other] = transposed_dot(value, w1_peer[...])
            return pieces[...]

        def close():
            total = own_part[...]
            inner = unspread(wide[pl.ds(line.own, tok), 2 * width :])
            for slot in range(3):
                total = total + rs_in[slot, :, :features].astype(jnp.float32)
                inner = inner + unspread(rs_in[slot, :, features:])
            factor = unspread(before_ref[pl.ds(line.own, tok), width:])
            normed = h_ref[...] * factor
            gain_out[...] = jnp.broadcast_to(jnp.sum(total * normed, axis=0, keepdims=True), gain_out.shape)
            out_ref[...] = dy_ref[...] + factor * (total * gain_ref[...] - normed * (inner / D))
            keep.wait()
            side.finish()

        run(line, taken, begin, prepare, beside, finish, second, lambda: None, close, product, carried, chain_out, chain_in,
            wide, own_part, rs_out, rs_in, *sems)

    low, full = jnp.bfloat16, jnp.float32
    shapes = (
        jax.ShapeDtypeStruct((tok, features), full),
        jax.ShapeDtypeStruct((4 * tok, 2 * width + EXTRA), low),
        jax.ShapeDtypeStruct((8, features), full),
        jax.ShapeDtypeStruct((layers,) + down_own.shape, low),
        jax.ShapeDtypeStruct((layers,) + down_own.shape, low),
    ) + tuple(jax.ShapeDtypeStruct(item.shape, item.dtype) for item in shipped)
    inside, outside = pl.BlockSpec(memory_space=pltpu.VMEM), pl.BlockSpec(memory_space=pl.ANY)
    out = pl.pallas_call(
        kernel,
        out_shape=shapes,
        in_specs=[inside] * 9 + [outside] * (count + len(stacks)),
        out_specs=[inside] * 3 + [outside] * (2 + count),
        input_output_aliases={9 + count + at: 3 + at for at in range(len(stacks))},
        scratch_shapes=[
            pltpu.VMEM((4 * tok, features), low),
            pltpu.VMEM((features, 4 * tok), low),
            pltpu.VMEM(down_own.shape, low),
            pltpu.VMEM(down_own.shape, low),
            pltpu.SemaphoreType.DMA,
            pltpu.VMEM((GROUP_CHUNKS * ROWS, features), full),
            sem(1 + count), sem(1 + count),
        ] + scratch,
        compiler_params=pltpu.CompilerParams(
            collective_id=ident, has_side_effects=True, vmem_limit_bytes=60 << 20
        ),
        cost_estimate=pl.CostEstimate(flops=60_000_000_000, bytes_accessed=8_000_000, transcendentals=0),
        name="ffn_backward",
    )(grad, hidden, gain.reshape(1, -1), kept, wide_forward, gu_own, gu_peer, down_own, down_peer, *shipped, *stacks)
    return out[:5], out[5:]


def to_row(column):
    return jnp.transpose(jnp.broadcast_to(column, (column.shape[0], EXTRA)))[:8]


def to_column(row):
    return jnp.transpose(jnp.broadcast_to(row[:1], (row.shape[1], row.shape[1])))[:, :1]


def turn(values, cosine, sine):
    lane = lax.broadcasted_iota(jnp.int32, values.shape, 1)
    width = values.shape[1]
    back = pltpu.roll(values, width - HEAD // 2, 1)
    forth = pltpu.roll(values, HEAD // 2, 1)
    partner = jnp.where(lax.rem(lane, HEAD) < HEAD // 2, back, forth)
    return values * cosine + partner * sine


def split_pair(block):
    lane = lax.broadcasted_iota(jnp.int32, block.shape, 1)
    zero = jnp.zeros_like(block)
    return jnp.concatenate([jnp.where(lane < HEAD, block, zero), jnp.where(lane < HEAD, zero, block)], axis=0)


def join_pair(turned, tok):
    return jnp.transpose(jnp.concatenate([turned[:HEAD, :tok], turned[HEAD:, tok:]], axis=0))


def twice(kv):
    wide = kv.astype(jnp.float32)
    lane = lax.broadcasted_iota(jnp.int32, wide.shape, 1)
    other = pltpu.roll(wide, HEAD, 1)
    return jnp.where(lane < HEAD, wide, other), jnp.where(lane < HEAD, other, wide)


class Square:
    def __init__(self, tok, depth):
        self.z, self.x = lax.axis_index("z"), lax.axis_index("x")
        self.y, self.c = lax.axis_index("y"), lax.axis_index("c")
        self.tok, self.depth = tok, depth
        self.g = 2 * self.y + self.c
        self.row = 2 * self.z + self.x
        self.own = pl.multiple_of(self.g * tok, tok)
        self.mine = pl.multiple_of(self.z * tok, tok)
        self.peers = (
            {"y": self.y, "c": 1 - self.c},
            {"y": 1 - self.y, "c": self.c},
            {"y": 1 - self.y, "c": 1 - self.c},
        )

    def row_peer(self, step):
        at = lax.rem(self.row + step, 2 * self.depth)
        return {"z": at // 2, "x": lax.rem(at, 2)}

    def greet(self):
        barrier = pltpu.get_barrier_semaphore()
        for peer in self.peers:
            pl.semaphore_signal(barrier, 1, device_id=peer, device_id_type=MESH_ID)
        for step in range(1, 2 * self.depth):
            pl.semaphore_signal(barrier, 1, device_id=self.row_peer(step), device_id_type=MESH_ID)
        pl.semaphore_wait(barrier, 3 + 2 * self.depth - 1)


def start_gather(square, taken, send, recv):
    copies = [
        remote(taken.at[pl.ds(square.own, square.tok)], taken.at[pl.ds(square.own, square.tok)], send.at[at], recv.at[at], peer)
        for at, peer in enumerate(square.peers)
    ]
    for copy in copies:
        copy.start()
    return copies


def line_sum(square, gather, product, own, own_row, outs, ins, row_outs, row_ins, send, recv, row_send, row_recv, between):
    tok, depth = square.tok, square.depth

    def one(order):
        block = lax.rem(2 * square.y + order, depth)
        step = lax.rem(block - square.z + depth, depth)
        slot = jnp.maximum(depth - 1 - step, 0)
        value, column = product(pl.multiple_of(block * tok, tok))

        @pl.when(step == 0)
        def _():
            own[...] = value
            if column is not None:
                own_row[...] = to_row(column)

        copy = remote(outs.at[order], ins.at[slot], send.at[order], recv.at[slot], {"z": block})
        row_copy = None
        if column is not None:
            row_copy = remote(row_outs.at[order], row_ins.at[slot], row_send.at[order], row_recv.at[slot], {"z": block})

        @pl.when(step != 0)
        def _():
            outs[order] = value.astype(jnp.bfloat16)
            copy.start()
            if column is not None:
                row_outs[order] = to_row(column)
                row_copy.start()

        return step, copy, row_copy

    gather[0].wait_recv()
    sent = [one(0), one(1)]
    gather[1].wait_recv()
    gather[2].wait_recv()
    sent += [one(2), one(3)]
    between()
    for slot in range(depth - 1):
        remote(outs.at[0], ins.at[slot], send.at[0], recv.at[slot], {"z": square.z}).wait_recv()
        if row_ins is not None:
            remote(row_outs.at[0], row_ins.at[slot], row_send.at[0], row_recv.at[slot], {"z": square.z}).wait_recv()
    return sent


def send_part(square, array, part, send, recv):
    lanes = pl.ds(pl.multiple_of(part * EXTRA, EXTRA), EXTRA)
    here = array.at[pl.ds(square.mine, square.tok), lanes]
    depth = square.depth
    return [
        remote(here, here, send.at[step - 1, part], recv.at[depth - 1 - step, part], {"z": lax.rem(square.z + step, depth)})
        for step in range(1, depth)
    ]


def send_row(square, rows, send, recv):
    line = rows.at[square.z]
    depth = square.depth
    return [
        remote(line, line, send.at[step - 1], recv.at[depth - 1 - step], {"z": lax.rem(square.z + step, depth)})
        for step in range(1, depth)
    ]


def grid_sum(square, array, rows, second, settle, own, outs, ins, row_ins, arrive, row_arrive, send, recv, row_send, row_recv):
    tok, depth = square.tok, square.depth
    sent = []
    for step in range(depth):
        block = lax.rem(square.z + step, depth)
        if step:
            for part in range(array.shape[1] // EXTRA):
                rows_of = array.at[pl.ds(pl.multiple_of(block * tok, tok), tok), pl.ds(part * EXTRA, EXTRA)]
                remote(rows_of, rows_of, send.at[0], arrive.at[step - 1, part], {"z": square.z}).wait_recv()
            remote(rows.at[block], rows.at[block], send.at[0], row_arrive.at[step - 1], {"z": square.z}).wait_recv()
        value = second(pl.multiple_of(block * tok, tok))
        away = lax.rem(block - square.g + depth, depth)
        slot = jnp.maximum(depth - 1 - away, 0)
        device = {"y": block // 2, "c": lax.rem(block, 2)}
        copy = remote(outs.at[step], ins.at[slot], send.at[step], recv.at[slot], device)
        row_copy = None
        if row_ins is not None:
            row_copy = remote(rows.at[block], row_ins.at[slot], row_send.at[step], row_recv.at[slot], device)

        @pl.when(away == 0)
        def _():
            own[...] = value

        @pl.when(away != 0)
        def _():
            outs[step] = value.astype(jnp.bfloat16)
            copy.start()
            if row_ins is not None:
                row_copy.start()

        sent.append((away, copy, row_copy))
    settle()
    for slot in range(depth - 1):
        remote(outs.at[0], ins.at[slot], send.at[0], recv.at[slot], square.peers[0]).wait_recv()
        if row_ins is not None:
            remote(rows.at[0], row_ins.at[slot], row_send.at[0], row_recv.at[slot], square.peers[0]).wait_recv()
    return sent


def drain(sent):
    for away, copy, row_copy in sent:

        @pl.when(away != 0)
        def _():
            copy.wait_send()
            if row_copy is not None:
                row_copy.wait_send()


def attention_forward(hidden, gain, qkv_own, out_own, qkv_peer, out_peer, shipped, cosine, sine, depth, ident):
    tok, features = hidden.shape
    cols = qkv_own.shape[1]
    fetch = qkv_peer is None
    extra = 2 if fetch else 0
    count = len(shipped)
    sides = extra + 2 * count
    query_cols = GROUP * HEAD
    seq = 2 * depth * tok
    pairs = query_cols // EXTRA
    scale = 1.0 / math.sqrt(HEAD)

    def kernel(h_ref, gain_ref, wqkv_own, wo_own, cos_ref, sin_ref, *rest):
        if not fetch:
            (wqkv_peer, wo_peer), rest = rest[:2], rest[2:]
        leave, rest = rest[:count], rest[count:]
        (out_ref, normed_t, queries, kv, lse, mixed, factors), rest = rest[:7], rest[7:]
        if fetch:
            (wqkv_peer, wo_peer), rest = rest[:2], rest[2:]
        landed, rest = rest[:count], rest[count:]
        (taken, scaled, pieces, own, own_row, z_out, z_in, zr_out, zr_in, values_t, g_own, g_out, g_in,
         ag_s, ag_r, zs_s, zs_r, zr_s, zr_r, kv_s, kv_r, zg_s, zg_r, zgr_s, zgr_r, gs_s, gs_r), rest = rest[:27], rest[27:]
        square = Square(tok, depth)
        side = Side(*rest) if sides else None
        mine, other = halves(features)
        taken[pl.ds(square.own, tok), :] = h_ref[...].astype(jnp.bfloat16)
        square.greet()
        gather = start_gather(square, taken, ag_s, ag_r)
        urgent = []
        if fetch:
            urgent = [side.start(wqkv_own, wqkv_peer), side.start(wo_own, wo_peer)]
        held = []
        for source, target in zip(leave, landed):
            half = source.shape[0] // 2
            side.start(source.at[pl.ds(0, half)], target.at[pl.ds(0, half)])
            held.append(side.later(source.at[pl.ds(half, half)], target.at[pl.ds(half, half)]))
        for copy in urgent[:1]:
            copy.wait_recv()

        def product(row):
            block = taken[pl.ds(row, tok), :].astype(jnp.float32)
            scaled[...] = (block * gain_ref[...]).astype(jnp.bfloat16)
            return (
                jnp.dot(scaled[:, mine], wqkv_own[...], preferred_element_type=jnp.float32)
                + jnp.dot(scaled[:, other], wqkv_peer[...], preferred_element_type=jnp.float32),
                jnp.sum(block * block, axis=1, keepdims=True),
            )

        sent = line_sum(square, gather, product, own, own_row, z_out, z_in, zr_out, zr_in, zs_s, zs_r, zr_s, zr_r, lambda: None)
        total, squares = own[...], own_row[...]
        for slot in range(depth - 1):
            total = total + z_in[slot].astype(jnp.float32)
            squares = squares + zr_in[slot]
        factor_row = lax.rsqrt(squares / D + EPS)
        factors[square.z] = factor_row
        given = send_row(square, factors, zgr_s, zgr_r)
        for copy in given:
            copy.start()
        turned = turn(total * to_column(factor_row), cos_ref[...], sin_ref[...])
        here = pl.ds(pl.multiple_of(square.row * tok, tok), tok)
        kv[here, :] = turned[:, query_cols:].astype(jnp.bfloat16)
        queries[...] = turned[:, :query_cols].astype(jnp.bfloat16)
        spreads = []
        for step in range(1, 2 * depth):
            copy = remote(kv.at[here], kv.at[here], kv_s.at[step - 1], kv_r.at[2 * depth - 1 - step], square.row_peer(step))
            copy.start()
            spreads.append(copy)
        for copy in spreads:
            copy.wait_recv()
        for copy in held:
            copy.start()
        keys, both = twice(kv[...])
        values_t[...] = jnp.transpose(both).astype(jnp.bfloat16)
        keys = keys.astype(jnp.bfloat16)

        def pair(t, _):
            lanes = pl.ds(pl.multiple_of(t * EXTRA, EXTRA), EXTRA)
            scores = transposed_dot(keys, split_pair(queries[:, lanes])) * scale
            key_at = lax.broadcasted_iota(jnp.int32, scores.shape, 0)
            query_at = lax.rem(lax.broadcasted_iota(jnp.int32, scores.shape, 1), tok) + square.row * tok
            scores = jnp.where(key_at <= query_at, scores, -1e30)
            top = jnp.max(scores, axis=0, keepdims=True)
            expo = jnp.exp(scores - top)
            denom = jnp.sum(expo, axis=0, keepdims=True)
            lse[t] = jnp.broadcast_to(top + jnp.log(denom), (8, 2 * tok))
            probs = (expo * (1.0 / denom)).astype(jnp.bfloat16)
            out_t = jnp.dot(values_t[...], probs, preferred_element_type=jnp.float32)
            mixed[pl.ds(square.mine, tok), lanes] = join_pair(out_t, tok).astype(jnp.bfloat16)
            for copy in send_part(square, mixed, t, zg_s, zg_r):
                copy.start()
            return 0

        lax.fori_loop(0, pairs, pair, 0)
        given += [copy for part in range(pairs) for copy in send_part(square, mixed, part, zg_s, zg_r)]

        for copy in urgent[1:]:
            copy.wait_recv()

        def second(row):
            value = mixed[pl.ds(row, tok), :]
            pieces[:, mine] = transposed_dot(value, wo_own[...])
            pieces[:, other] = transposed_dot(value, wo_peer[...])
            return pieces[...]

        def settle():
            for block in range(depth):
                rows = pl.ds(block * tok, tok)
                normed = taken[rows, :].astype(jnp.float32) * to_column(factors[block]) * gain_ref[...]
                normed_t[:, rows] = jnp.transpose(normed).astype(jnp.bfloat16)

        sums = grid_sum(square, mixed, factors, second, settle, g_own, g_out, g_in, None, zg_r, zgr_r, gs_s, gs_r, None, None)
        total = g_own[...]
        for slot in range(depth - 1):
            total = total + g_in[slot].astype(jnp.float32)
        out_ref[...] = h_ref[...] + total
        drain(sent)
        drain(sums)
        for copy in gather + spreads + given:
            copy.wait_send()
        if side:
            side.finish(urgent)

    low, full = jnp.bfloat16, jnp.float32
    shapes = (
        jax.ShapeDtypeStruct((tok, features), full),
        jax.ShapeDtypeStruct((features, depth * tok), low),
        jax.ShapeDtypeStruct((tok, query_cols), low),
        jax.ShapeDtypeStruct((seq, 2 * HEAD), low),
        jax.ShapeDtypeStruct((pairs, 8, 2 * tok), full),
        jax.ShapeDtypeStruct((depth * tok, query_cols), low),
        jax.ShapeDtypeStruct((depth, 8, tok), full),
    )
    if fetch:
        shapes += (jax.ShapeDtypeStruct(qkv_own.shape, low), jax.ShapeDtypeStruct(out_own.shape, low))
    shapes += tuple(jax.ShapeDtypeStruct(item.shape, item.dtype) for item in shipped)
    inside, outside = pl.BlockSpec(memory_space=pltpu.VMEM), pl.BlockSpec(memory_space=pl.ANY)
    peers = () if fetch else (qkv_peer, out_peer)
    out = pl.pallas_call(
        kernel,
        out_shape=shapes,
        in_specs=[inside] * (6 + len(peers)) + [outside] * count,
        out_specs=[inside] * (7 + extra) + [outside] * count,
        scratch_shapes=[
            pltpu.VMEM((depth * tok, features), low),
            pltpu.VMEM((tok, features), low),
            pltpu.VMEM((tok, features), full),
            pltpu.VMEM((tok, cols), full),
            pltpu.VMEM((8, tok), full),
            pltpu.VMEM((depth, tok, cols), low),
            pltpu.VMEM((depth - 1, tok, cols), low),
            pltpu.VMEM((depth, 8, tok), full),
            pltpu.VMEM((depth - 1, 8, tok), full),
            pltpu.VMEM((2 * HEAD, seq), low),
            pltpu.VMEM((tok, features), full),
            pltpu.VMEM((depth, tok, features), low),
            pltpu.VMEM((depth - 1, tok, features), low),
            sem(3), sem(3), sem(depth), sem(depth - 1), sem(depth), sem(depth - 1),
            sem(2 * depth - 1), sem(2 * depth - 1), sem(depth - 1, pairs), sem(depth - 1, pairs), sem(depth - 1), sem(depth - 1),
            sem(depth), sem(depth - 1),
        ] + ([sem(sides), sem(sides)] if sides else []),
        compiler_params=pltpu.CompilerParams(
            collective_id=ident, has_side_effects=True, vmem_limit_bytes=60 << 20
        ),
        cost_estimate=pl.CostEstimate(flops=50_000_000_000, bytes_accessed=8_000_000, transcendentals=0),
        name="attention_forward",
    )(hidden, gain.reshape(1, -1), qkv_own, out_own, cosine, sine, *peers, *shipped)
    peers = out[7:9] if fetch else peers
    return out[:7], peers, out[7 + extra :]


def attention_backward(
    grad, hidden, gain, qkv_own, qkv_peer, out_own, out_peer, cosine, sine, queries, kv, lse, factors, mixed, normed_a, normed_f,
    grad_gu, stacks, index, layers, depth, ident,
):
    tok, features = hidden.shape
    cols = qkv_own.shape[1]
    wide = grad_gu.shape[1] - EXTRA
    query_cols = GROUP * HEAD
    seq = 2 * depth * tok
    pairs = query_cols // EXTRA
    scale = 1.0 / math.sqrt(HEAD)

    def kernel(dy_ref, h_ref, gain_ref, wqkv_own, wqkv_peer, wo_own, wo_peer, cos_ref, sin_ref, q_ref, kv_ref, lse_ref,
               factor_ref, mixed_ref, normed_a_ref, normed_f_ref, gu_ref, *rest_refs):
        (out_ref, gain_out, qkv_given, gu_kept_all, gu_got_all, out_kept_all, out_got_all, qkv_kept_all,
               taken, spun, turned, pieces, gu_kept, gu_given, out_kept, out_given, qkv_kept, keep_s,
               own, heads, z_out, z_in, keys_t, dk, dv, kv_out, kv_in, dq, inner_rows, g_own, g_out, g_in, g_rows,
               ag_s, ag_r, zs_s, zs_r, kv_s, kv_r, zg_s, zg_r, zgr_s, zgr_r, gs_s, gs_r, gr_s, gr_r, side_s, side_r) = rest_refs[len(stacks):]
        square = Square(tok, depth)
        side = Side(side_s, side_r)
        mine, other = halves(features)
        taken[pl.ds(square.own, tok), :] = dy_ref[...].astype(jnp.bfloat16)
        square.greet()
        gather = start_gather(square, taken, ag_s, ag_r)

        def gu_tiles(start, stop):
            def tile(j, _):
                grad_tile(normed_f_ref, features, gu_ref, pl.ds(pl.multiple_of(j * EXTRA, EXTRA), EXTRA), gu_kept, gu_given)
                return 0

            lax.fori_loop(start, stop, tile, 0)

        gu_got = gu_got_all.at[index]
        keeps = [
            pltpu.make_async_copy(gu_kept, gu_kept_all.at[index], keep_s.at[0]),
            pltpu.make_async_copy(out_kept, out_kept_all.at[index], keep_s.at[1]),
            pltpu.make_async_copy(qkv_kept, qkv_kept_all.at[index], keep_s.at[2]),
        ]
        every = wide // EXTRA
        middle, late = every // 2, every * 3 // 4
        gu_tiles(0, middle)
        front, rest = pl.ds(0, middle * EXTRA), pl.ds(late * EXTRA, wide - late * EXTRA)
        inner_part = pl.ds(middle * EXTRA, (late - middle) * EXTRA)
        side.start(gu_given.at[:, front], gu_got.at[:, front])

        def between():
            turned[...] = flip(taken[...])
            for t in range(query_cols // EXTRA):
                grad_tile(turned, features, mixed_ref, pl.ds(t * EXTRA, EXTRA), out_kept, out_given)
            side.start(out_given, out_got_all.at[index])
            gu_tiles(middle, late)
            side.start(gu_given.at[:, inner_part], gu_got.at[:, inner_part])
            gu_tiles(late, every)
            keeps[0].start()
            keeps[1].start()

        def product(row):
            rows = pl.ds(row, tok)
            value = jnp.dot(taken[rows, mine], wo_own[...], preferred_element_type=jnp.float32) + jnp.dot(
                taken[rows, other], wo_peer[...], preferred_element_type=jnp.float32
            )
            return value, None

        sent = line_sum(square, gather, product, own, None, z_out, z_in, None, None, zs_s, zs_r, None, None, between)
        total = own[...]
        for slot in range(depth - 1):
            total = total + z_in[slot].astype(jnp.float32)
        heads[...] = total.astype(jnp.bfloat16)
        keys, both = twice(kv_ref[...])
        keys_t[...] = jnp.transpose(keys).astype(jnp.bfloat16)
        keys = keys.astype(jnp.bfloat16)
        both = both.astype(jnp.bfloat16)
        dk[...] = jnp.zeros_like(dk)
        dv[...] = jnp.zeros_like(dv)

        def pair(t, _):
            lanes = pl.ds(pl.multiple_of(t * EXTRA, EXTRA), EXTRA)
            query = split_pair(q_ref[:, lanes])
            head = split_pair(heads[:, lanes])
            scores = transposed_dot(keys, query) * scale
            key_at = lax.broadcasted_iota(jnp.int32, scores.shape, 0)
            query_at = lax.rem(lax.broadcasted_iota(jnp.int32, scores.shape, 1), tok) + square.row * tok
            probs = jnp.exp(jnp.where(key_at <= query_at, scores, -1e30) - lse_ref[t, :1, :])
            grad_probs = transposed_dot(both, head)
            delta = jnp.sum(probs * grad_probs, axis=0, keepdims=True)
            grad_scores = (probs * (grad_probs - delta)).astype(jnp.bfloat16)
            dk[...] += jnp.dot(grad_scores, query, preferred_element_type=jnp.float32)
            dv[...] += jnp.dot(probs.astype(jnp.bfloat16), head, preferred_element_type=jnp.float32)
            back = jnp.dot(keys_t[...], grad_scores, preferred_element_type=jnp.float32)
            value = join_pair(back, tok) * scale
            dq[...] += jnp.broadcast_to(
                jnp.sum(value * q_ref[:, lanes].astype(jnp.float32), axis=1, keepdims=True), dq.shape
            )
            spun[pl.ds(square.mine, tok), lanes] = turn(value, cos_ref[:, lanes], -sin_ref[:, lanes]).astype(jnp.bfloat16)
            for copy in send_part(square, spun, t, zg_s, zg_r):
                copy.start()
            return 0

        dq[...] = jnp.zeros_like(dq)
        lax.fori_loop(0, pairs, pair, 0)
        lane = lax.broadcasted_iota(jnp.int32, (seq, EXTRA), 1)
        left = dk[...]
        right = dv[...]
        both_kv = jnp.where(
            lane < HEAD, (left + pltpu.roll(left, HEAD, 1)) * scale, right + pltpu.roll(right, HEAD, 1)
        )
        dk[...] = both_kv
        kv_out[...] = both_kv.astype(jnp.bfloat16)
        here = pl.ds(pl.multiple_of(square.row * tok, tok), tok)
        spreads = []
        for step in range(1, 2 * depth):
            at = lax.rem(square.row + step, 2 * depth)
            copy = remote(
                kv_out.at[pl.ds(pl.multiple_of(at * tok, tok), tok)],
                kv_in.at[2 * depth - 1 - step],
                kv_s.at[step - 1],
                kv_r.at[2 * depth - 1 - step],
                square.row_peer(step),
            )
            copy.start()
            spreads.append(copy)
        total_kv = dk[here, :]
        for copy in spreads:
            copy.wait_recv()
        side.start(gu_given.at[:, rest], gu_got.at[:, rest])
        for slot in range(2 * depth - 1):
            total_kv = total_kv + kv_in[slot].astype(jnp.float32)
        spun[pl.ds(square.mine, tok), query_cols:] = turn(
            total_kv, cos_ref[:, query_cols:], -sin_ref[:, query_cols:]
        ).astype(jnp.bfloat16)
        inner = dq[:, :1] + jnp.sum(total_kv * kv_ref[here, :].astype(jnp.float32), axis=1, keepdims=True)
        inner_rows[square.z] = to_row(inner)
        given = send_part(square, spun, pairs, zg_s, zg_r) + send_row(square, inner_rows, zgr_s, zgr_r)
        for copy in given:
            copy.start()
        given += [copy for part in range(pairs) for copy in send_part(square, spun, part, zg_s, zg_r)]

        def second(row):
            value = spun[pl.ds(row, tok), :]
            pieces[:, mine] = transposed_dot(value, wqkv_own[...])
            pieces[:, other] = transposed_dot(value, wqkv_peer[...])
            return pieces[...]

        def settle():
            for t in range(cols // EXTRA):
                grad_tile(normed_a_ref, features, spun, pl.ds(t * EXTRA, EXTRA), qkv_kept, qkv_given)
            keeps[2].start()

        sums = grid_sum(
            square, spun, inner_rows, second, settle, g_own, g_out, g_in, g_rows, zg_r, zgr_r, gs_s, gs_r, gr_s, gr_r
        )
        total = g_own[...]
        inner = inner_rows[square.g]
        for slot in range(depth - 1):
            total = total + g_in[slot].astype(jnp.float32)
            inner = inner + g_rows[slot]
        factor = to_column(factor_ref[square.g])
        normed = h_ref[...] * factor
        gain_out[...] = jnp.broadcast_to(jnp.sum(total * normed, axis=0, keepdims=True), gain_out.shape)
        out_ref[...] = dy_ref[...] + factor * (total * gain_ref[...] - normed * (to_column(inner) / D))
        drain(sent)
        drain(sums)
        for copy in gather + spreads + given:
            copy.wait_send()
        for copy in keeps:
            copy.wait()
        side.finish()

    low, full = jnp.bfloat16, jnp.float32
    shapes = (
        jax.ShapeDtypeStruct((tok, features), full),
        jax.ShapeDtypeStruct((8, features), full),
        jax.ShapeDtypeStruct(qkv_own.shape, low),
        jax.ShapeDtypeStruct((layers, features // 2, wide), low),
        jax.ShapeDtypeStruct((layers, features // 2, wide), low),
        jax.ShapeDtypeStruct((layers,) + out_own.shape, low),
        jax.ShapeDtypeStruct((layers,) + out_own.shape, low),
        jax.ShapeDtypeStruct((layers,) + qkv_own.shape, low),
    )
    inside, outside = pl.BlockSpec(memory_space=pltpu.VMEM), pl.BlockSpec(memory_space=pl.ANY)
    return pl.pallas_call(
        kernel,
        out_shape=shapes,
        in_specs=[inside] * 17 + [outside] * len(stacks),
        out_specs=[inside] * 3 + [outside] * 5,
        input_output_aliases={17 + at: 3 + at for at in range(len(stacks))},
        scratch_shapes=[
            pltpu.VMEM((depth * tok, features), low),
            pltpu.VMEM((depth * tok, cols), low),
            pltpu.VMEM((features, depth * tok), low),
            pltpu.VMEM((tok, features), full),
            pltpu.VMEM((features // 2, wide), low),
            pltpu.VMEM((features // 2, wide), low),
            pltpu.VMEM(out_own.shape, low),
            pltpu.VMEM(out_own.shape, low),
            pltpu.VMEM(qkv_own.shape, low),
            sem(3),
            pltpu.VMEM((tok, query_cols), full),
            pltpu.VMEM((tok, query_cols), low),
            pltpu.VMEM((depth, tok, query_cols), low),
            pltpu.VMEM((depth - 1, tok, query_cols), low),
            pltpu.VMEM((2 * HEAD, seq), low),
            pltpu.VMEM((seq, 2 * HEAD), full),
            pltpu.VMEM((seq, 2 * HEAD), full),
            pltpu.VMEM((seq, 2 * HEAD), low),
            pltpu.VMEM((2 * depth - 1, tok, 2 * HEAD), low),
            pltpu.VMEM((tok, EXTRA), full),
            pltpu.VMEM((depth, 8, tok), full),
            pltpu.VMEM((tok, features), full),
            pltpu.VMEM((depth, tok, features), low),
            pltpu.VMEM((depth - 1, tok, features), low),
            pltpu.VMEM((depth - 1, 8, tok), full),
            sem(3), sem(3), sem(depth), sem(depth - 1),
            sem(2 * depth - 1), sem(2 * depth - 1), sem(depth - 1, pairs + 1), sem(depth - 1, pairs + 1), sem(depth - 1),
            sem(depth - 1), sem(depth), sem(depth - 1), sem(depth), sem(depth - 1), sem(4), sem(4),
        ],
        compiler_params=pltpu.CompilerParams(collective_id=ident, has_side_effects=True, vmem_limit_bytes=60 << 20),
        cost_estimate=pl.CostEstimate(flops=50_000_000_000, bytes_accessed=8_000_000, transcendentals=0),
        name="attention_backward",
    )(grad, hidden, gain.reshape(1, -1), qkv_own, qkv_peer, out_own, out_peer, cosine, sine, queries, kv, lse, factors, mixed,
      normed_a, normed_f, grad_gu, *stacks)


def finish(grad, gains, qkv_given, depth, ident):
    tok, features = grad.shape
    count = len(gains)
    members = 2 * depth

    def kernel(grad_ref, *rest):
        gain_refs, rest = rest[:count], rest[count:]
        (given, out_ref, gain_out, got, packed, parts, sent, home, part_s, part_r, move_s, move_r, side_s, side_r) = rest
        z, x = lax.axis_index("z"), lax.axis_index("x")
        y, c = lax.axis_index("y"), lax.axis_index("c")
        g = 2 * y + c
        barrier = pltpu.get_barrier_semaphore()
        self_at = x * depth + g

        def source(slot):
            return {"z": g, "x": slot // depth, "y": (slot % depth) // 2, "c": slot % 2}

        def target(at):
            return {"z": at // 2, "x": at % 2, "y": z // 2, "c": lax.rem(z, 2)}

        def is_source_me(slot):
            return (z == g) & (slot == self_at)

        def is_target_me(at):
            return (z == g) & (at == 2 * z + x)

        for slot in range(members):

            @pl.when(jnp.logical_not(is_source_me(slot)))
            def _():
                pl.semaphore_signal(barrier, 1, device_id=source(slot), device_id_type=MESH_ID)

        pl.semaphore_signal(barrier, 1, device_id={"x": 1 - x}, device_id_type=MESH_ID)
        for at, ref in enumerate(gain_refs):
            packed[at : at + 1, :] = ref[:1, :]
        sent[...] = grad_ref[...].astype(jnp.bfloat16)
        pl.semaphore_wait(barrier, members + 1 - jnp.where(z == g, 1, 0))
        side = Side(side_s, side_r)
        side.start(given, got)
        move = remote(sent, home, move_s, move_r, {"z": g, "y": z // 2, "c": lax.rem(z, 2)})

        @pl.when(z != g)
        def _():
            move.start()

        def part(at):
            return remote(packed, parts.at[self_at], part_s.at[at], part_r.at[self_at], target(at))

        for at in range(members):

            @pl.when(jnp.logical_not(is_target_me(at)))
            def _():
                part(at).start()

        @pl.when(z == g)
        def _():
            parts[self_at] = packed[...]

        for slot in range(members):

            @pl.when(jnp.logical_not(is_source_me(slot)))
            def _():
                remote(packed, parts.at[slot], part_s.at[0], part_r.at[slot], target(0)).wait_recv()

        total = parts[0]
        for slot in range(1, members):
            total = total + parts[slot]
        gain_out[...] = total

        @pl.when(z == g)
        def _():
            out_ref[...] = grad_ref[...]

        @pl.when(z != g)
        def _():
            move.wait_recv()
            out_ref[...] = home[...].astype(jnp.float32)
            move.wait_send()

        for at in range(members):

            @pl.when(jnp.logical_not(is_target_me(at)))
            def _():
                part(at).wait_send()

        side.finish()

    low, full = jnp.bfloat16, jnp.float32
    inside, outside = pl.BlockSpec(memory_space=pltpu.VMEM), pl.BlockSpec(memory_space=pl.ANY)
    return pl.pallas_call(
        kernel,
        out_shape=(
            jax.ShapeDtypeStruct((tok, features), full),
            jax.ShapeDtypeStruct((count, features), full),
            jax.ShapeDtypeStruct(qkv_given.shape, low),
        ),
        in_specs=[inside] * (1 + count) + [outside],
        out_specs=[inside, inside, outside],
        scratch_shapes=[
            pltpu.VMEM((count, features), full),
            pltpu.VMEM((members, count, features), full),
            pltpu.VMEM((tok, features), low),
            pltpu.VMEM((tok, features), low),
            sem(members), sem(members),
            pltpu.SemaphoreType.DMA, pltpu.SemaphoreType.DMA,
            sem(1), sem(1),
        ],
        compiler_params=pltpu.CompilerParams(collective_id=ident, has_side_effects=True),
        cost_estimate=pl.CostEstimate(flops=5_000_000_000, bytes_accessed=1_000_000, transcendentals=0),
        name="finish",
    )(grad, *gains, qkv_given)


def stationary(stream, grad_out, wqkv, wo, wgu, wd, gain_attn, gain_ffn):
    tok = stream.shape[0]
    layers = wqkv.shape[0]
    count_rows = wqkv.shape[1]
    depth = lax.axis_size("z")
    head = HEAD
    row = lax.axis_index("z") * 2 + lax.axis_index("x")
    query_pos = row * tok + jnp.arange(tok, dtype=jnp.int32)
    lane = jnp.arange((GROUP + 2) * head, dtype=jnp.int32)
    half = head // 2
    freq = THETA ** (-((lane % half).astype(jnp.float32) * 2.0 / head))
    angle = query_pos.astype(jnp.float32)[:, None] * freq[None, :]
    rotated = (lane < (GROUP + 1) * head)[None, :]
    cosine = jnp.where(rotated, jnp.cos(angle), 1.0)
    sine = jnp.where(rotated, jnp.where((lane % head < half)[None, :], -1.0, 1.0) * jnp.sin(angle), 0.0)
    current = swap_grid(stream, depth)
    grad_now = swap_grid(grad_out, depth)
    gain_a = swap_grid(gain_attn, depth)
    gain_f = swap_grid(gain_ffn, depth)
    own_qkv = [wqkv[index].reshape(count_rows, -1) for index in range(layers)]
    own_out = [wo[index] for index in range(layers)]
    own_gu = [wgu[index].reshape(count_rows, -1) for index in range(layers)]
    own_down = [wd[index] for index in range(layers)]
    peer_qkv, peer_out, peer_gu, peer_down = ([None] * layers for _ in range(4))
    saved = []
    for index in range(layers):
        before = current
        (hidden_in, normed_a, queries, kv, lse, mixed, factors), (peer_qkv[index], peer_out[index]), landed = attention_forward(
            before, gain_a[index], own_qkv[index], own_out[index], peer_qkv[index], peer_out[index],
            [] if index else own_gu[:1], cosine, sine, depth, 4 * index
        )
        if landed:
            peer_gu[0] = landed[0]
        follow = index + 1
        shipped = [own_qkv[follow], own_out[follow], own_gu[follow]] if follow < layers else []
        (current, normed_f, kept, active, peer_down[index]), landed = ffn_forward(
            hidden_in, gain_f[index], own_gu[index], peer_gu[index], own_down[index], shipped, depth, 4 * index + 1
        )
        if landed:
            peer_qkv[follow], peer_out[follow], peer_gu[follow] = landed
        saved.append((before, normed_a, queries, kv, lse, mixed, factors, hidden_in, normed_f, kept, active))
    list_ga, list_gf, got_qkv, pending, down_stack, rest_stack = ([], [], [], [], [], [])
    for index in reversed(range(layers)):
        before, normed_a, queries, kv, lse, mixed, factors, hidden_in, normed_f, kept, active = saved[index]
        (grad_hidden, grad_gu, gain_f_grad, *down_stack), landed = ffn_backward(
            grad_now, hidden_in, gain_f[index], kept, active, own_gu[index], peer_gu[index], own_down[index],
            peer_down[index], pending[-1:], down_stack, index, layers, depth, 4 * index + 2
        )
        got_qkv.extend(landed)
        list_gf.append(gain_f_grad)
        (grad_now, gain_a_grad, qkv_given, *rest_stack) = attention_backward(
            grad_hidden, before, gain_a[index], own_qkv[index], peer_qkv[index], own_out[index], peer_out[index],
            cosine, sine, queries, kv, lse, factors, mixed, normed_a, normed_f, grad_gu, rest_stack, index, layers, depth,
            4 * index + 3
        )
        pending.append(qkv_given)
        list_ga.append(gain_a_grad)
    grad_in, gains, last_qkv = finish(grad_now, list_ga[::-1] + list_gf[::-1], qkv_given, depth, 4 * layers)
    got_qkv.append(last_qkv)
    gu_kept, gu_got, out_kept, out_got, qkv_kept = rest_stack
    add = lambda kept, got: kept.astype(jnp.float32) + got.astype(jnp.float32)
    return (
        swap_grid(current, depth),
        grad_in,
        add(qkv_kept, jnp.stack(got_qkv[::-1])).reshape(layers, count_rows, 1, -1),
        add(out_kept, out_got),
        add(gu_kept, gu_got).reshape(layers, count_rows, 2, -1),
        add(*down_stack),
        gains[:layers],
        gains[layers:],
    )


def solution(mesh):
    rows, cols = ("row", "col")
    body = local
    if (mesh.shape["row"], mesh.shape["col"]) == (8, 4):
        mesh = share_out(mesh)
        rows, cols = (("z", "x"), ("y", "c"))
        body = stationary
    in_specs = (
        P(rows, cols),
        P(rows, cols),
        P(None, rows, cols, None),
        P(None, rows, cols),
        P(None, rows, None, cols),
        P(None, rows, cols),
        P(None, cols),
        P(None, cols),
    )
    out_specs = (
        P(rows, cols),
        P(rows, cols),
        P(None, rows, cols, None),
        P(None, rows, cols),
        P(None, rows, None, cols),
        P(None, rows, cols),
        P(None, cols),
        P(None, cols),
    )
    return jax.shard_map(body, mesh=mesh, in_specs=in_specs, out_specs=out_specs, check_vma=False)
```

```python
import math

import jax
import jax.numpy as jnp
from jax import lax
from jax.experimental import pallas as pl
from jax.experimental.pallas import tpu as pltpu
from jax.sharding import Mesh
from jax.sharding import PartitionSpec as P

D = 2048
HEAD = 64
GROUP = 8


EPS = 1e-05
THETA = 10000.0


def rope_turn(tensor, cosine, sine):
    half = tensor.shape[-1] // 2
    first = tensor[..., :half]
    second = tensor[..., half:]
    return jnp.concatenate(
        [first * cosine - second * sine, second * cosine + first * sine], axis=-1
    )


def feature_sum(values):
    return lax.psum(values, "col")


def gather_features(rows_in):
    return lax.all_gather(rows_in, "col", axis=1, tiled=True)


def sum_features(partials):
    return lax.psum_scatter(
        partials.astype(jnp.bfloat16), "col", scatter_dimension=1, tiled=True
    ).astype(jnp.float32)


def add_rows(left, piece):
    return jnp.dot(left, piece, preferred_element_type=jnp.float32)


def project_in(left, shard):
    return add_rows(left, lax.all_gather(shard, "row", axis=0, tiled=True))


def columns_of(left, piece):
    return jnp.einsum("tj,dj->td", left, piece, preferred_element_type=jnp.float32)


def project_out(left, shard):
    return columns_of(left, lax.all_gather(shard, "row", axis=0, tiled=True))


def weight_grad(left, right):
    return lax.psum_scatter(
        lax.dot_general(
            left, right, (((0,), (0,)), ((), ())), preferred_element_type=jnp.float32
        ).astype(jnp.bfloat16),
        "row",
        scatter_dimension=0,
        tiled=True,
    ).astype(jnp.float32)


def norm_forward(values, gain):
    total = feature_sum(jnp.sum(values * values, axis=1))
    factor = lax.rsqrt(total / D + EPS)
    normed = values * factor[:, None]
    return (normed, factor, (normed * gain).astype(jnp.bfloat16))


def norm_backward(grad_normed, normed, factor, gain):
    scaled = grad_normed * gain
    inner = feature_sum(jnp.sum(scaled * normed, axis=1))
    grad_in = factor[:, None] * (scaled - normed * (inner / D)[:, None])
    return (grad_in, jnp.sum(grad_normed * normed, axis=0))


def masked_scores(queries, keys, query_pos, key_pos):
    scores = jnp.einsum("qgd,kd->gqk", queries, keys, preferred_element_type=jnp.float32) * (
        1.0 / math.sqrt(queries.shape[-1])
    )
    return jnp.where(key_pos[None, None, :] <= query_pos[None, :, None], scores, -1e30)


def local(stream, grad_out, wqkv, wo, wgu, wd, gain_attn, gain_ffn):
    tok = stream.shape[0]
    layers = wqkv.shape[0]
    count_rows = wqkv.shape[1]
    head = HEAD
    query_cols = GROUP * head
    seq_len = lax.axis_size("row") * tok
    query_pos = lax.axis_index("row") * tok + jnp.arange(tok, dtype=jnp.int32)
    key_pos = jnp.arange(seq_len, dtype=jnp.int32)
    freq = THETA ** (-(jnp.arange(head // 2, dtype=jnp.float32) * 2.0 / head))
    angle = query_pos.astype(jnp.float32)[:, None] * freq[None, :]
    cosine = jnp.cos(angle)
    sine = jnp.sin(angle)
    saved = []
    current = stream
    for index in range(layers):
        weight_qkv = wqkv[index].reshape(count_rows, -1)
        weight_out = wo[index]
        weight_gu = wgu[index].reshape(count_rows, -1)
        weight_down = wd[index]
        wholes = (None, None, None, None)
        normed_a, factor_a, xnormed = norm_forward(current, gain_attn[index])
        xfull = gather_features(xnormed)
        qkv = project_in(xfull, weight_qkv)
        queries = rope_turn(
            qkv[:, :query_cols].reshape(tok, GROUP, head), cosine[:, None, :], sine[:, None, :]
        ).astype(jnp.bfloat16)
        keys = rope_turn(qkv[:, query_cols : query_cols + head], cosine, sine).astype(jnp.bfloat16)
        values = qkv[:, query_cols + head :].astype(jnp.bfloat16)
        seqkv = lax.all_gather(jnp.concatenate([keys, values], axis=1), "row", axis=0, tiled=True)
        seq_keys = seqkv[:, :head]
        seq_values = seqkv[:, head:]
        scores = masked_scores(queries, seq_keys, query_pos, key_pos)
        top = jnp.max(scores, axis=2, keepdims=True)
        expo = jnp.exp(scores - top)
        denom = jnp.sum(expo, axis=2, keepdims=True)
        probs = (expo / denom).astype(jnp.bfloat16)
        log_total = top + jnp.log(denom)
        mixed = (
            jnp.einsum("gqk,kd->qgd", probs, seq_values, preferred_element_type=jnp.float32)
            .reshape(tok, query_cols)
            .astype(jnp.bfloat16)
        )
        hidden_in = current + sum_features(project_out(mixed, weight_out))
        normed_f, factor_f, hnormed = norm_forward(hidden_in, gain_ffn[index])
        hfull = gather_features(hnormed)
        gate_up = project_in(hfull, weight_gu)
        hidden_cols = gate_up.shape[1] // 2
        gate = gate_up[:, :hidden_cols]
        upper = gate_up[:, hidden_cols:]
        active = (jax.nn.silu(gate) * upper).astype(jnp.bfloat16)
        current = hidden_in + sum_features(project_out(active, weight_down))
        saved.append(
            (
                weight_qkv,
                weight_out,
                weight_gu,
                weight_down,
                wholes,
                normed_a,
                factor_a,
                xfull,
                queries,
                seq_keys,
                seq_values,
                log_total,
                mixed,
                normed_f,
                factor_f,
                hfull,
                gate,
                upper,
                active,
            )
        )
    grad_now = grad_out
    list_qkv, list_out, list_gu, list_down, list_ga, list_gf = ([], [], [], [], [], [])
    for index in reversed(range(layers)):
        (
            weight_qkv,
            weight_out,
            weight_gu,
            weight_down,
            wholes,
            normed_a,
            factor_a,
            xfull,
            queries,
            seq_keys,
            seq_values,
            log_total,
            mixed,
            normed_f,
            factor_f,
            hfull,
            gate,
            upper,
            active,
        ) = saved[index]
        grad_full = gather_features(grad_now.astype(jnp.bfloat16))
        grad_active = project_in(grad_full, weight_down)
        list_down.append(weight_grad(grad_full, active))
        sig = jax.nn.sigmoid(gate)
        grad_gate = grad_active * upper * sig * (1.0 + gate * (1.0 - sig))
        grad_up = grad_active * gate * sig
        grad_gu = jnp.concatenate([grad_gate, grad_up], axis=1).astype(jnp.bfloat16)
        grad_hn = sum_features(project_out(grad_gu, weight_gu))
        list_gu.append(weight_grad(hfull, grad_gu).reshape(count_rows, 2, -1))
        grad_mid, gain_f_grad = norm_backward(grad_hn, normed_f, factor_f, gain_ffn[index])
        list_gf.append(gain_f_grad)
        grad_hidden = grad_now + grad_mid
        hidden_full = gather_features(grad_hidden.astype(jnp.bfloat16))
        grad_mixed = project_in(hidden_full, weight_out).astype(jnp.bfloat16)
        list_out.append(weight_grad(hidden_full, mixed))
        grad_heads = grad_mixed.reshape(tok, GROUP, head)
        scores = masked_scores(queries, seq_keys, query_pos, key_pos)
        probs_full = jnp.exp(scores - log_total)
        probs = probs_full.astype(jnp.bfloat16)
        grad_probs = jnp.einsum(
            "qgd,kd->gqk", grad_heads, seq_values, preferred_element_type=jnp.float32
        )
        delta = jnp.sum(probs_full * grad_probs, axis=2, keepdims=True)
        grad_scores = (probs_full * (grad_probs - delta)).astype(jnp.bfloat16)
        inverse = 1.0 / math.sqrt(head)
        grad_queries = (
            jnp.einsum("gqk,kd->qgd", grad_scores, seq_keys, preferred_element_type=jnp.float32)
            * inverse
        )
        grad_keys = (
            jnp.einsum("gqk,qgd->kd", grad_scores, queries, preferred_element_type=jnp.float32)
            * inverse
        )
        grad_values = jnp.einsum(
            "gqk,qgd->kd", probs, grad_heads, preferred_element_type=jnp.float32
        )
        grad_kv = lax.psum_scatter(
            jnp.concatenate([grad_keys, grad_values], axis=1).astype(jnp.bfloat16),
            "row",
            scatter_dimension=0,
            tiled=True,
        ).astype(jnp.float32)
        grad_k = rope_turn(grad_kv[:, :head], cosine, -sine)
        grad_v = grad_kv[:, head:]
        grad_q = rope_turn(grad_queries, cosine[:, None, :], -sine[:, None, :]).reshape(
            tok, query_cols
        )
        grad_qkv = jnp.concatenate([grad_q, grad_k, grad_v], axis=1).astype(jnp.bfloat16)
        grad_xn = sum_features(project_out(grad_qkv, weight_qkv))
        list_qkv.append(weight_grad(xfull, grad_qkv).reshape(count_rows, 1, -1))
        grad_in, gain_a_grad = norm_backward(grad_xn, normed_a, factor_a, gain_attn[index])
        list_ga.append(gain_a_grad)
        grad_now = grad_hidden + grad_in
    gains_a, gains_f = lax.psum((jnp.stack(list_ga[::-1]), jnp.stack(list_gf[::-1])), "row")
    return (
        current,
        grad_now,
        jnp.stack(list_qkv[::-1]),
        jnp.stack(list_out[::-1]),
        jnp.stack(list_gu[::-1]),
        jnp.stack(list_down[::-1]),
        gains_a,
        gains_f,
    )


def share_out(mesh):
    rows, cols = mesh.shape["row"], mesh.shape["col"]
    return Mesh(
        mesh.devices.reshape(rows // 2, 2, cols // 2, 2), ("z", "x", "y", "c")
    )


def swap_grid(values, depth):
    pairs = [(z * depth + g, g * depth + z) for z in range(depth) for g in range(depth)]
    return lax.ppermute(values, ("z", "y", "c"), pairs)


MESH_ID = pl.DeviceIdType.MESH
ROWS = 16
SKEW = 3
GROUP_CHUNKS = 4
EXTRA = 128


def spread(column):
    high = column.astype(jnp.bfloat16)
    low = (column - high.astype(jnp.float32)).astype(jnp.bfloat16)
    lane = lax.broadcasted_iota(jnp.int32, (column.shape[0], EXTRA), 1)
    wide = jnp.where(lane == 0, high.astype(jnp.float32), jnp.where(lane == 1, low.astype(jnp.float32), 0.0))
    return wide.astype(jnp.bfloat16)


def unspread(block):
    return jnp.sum(block.astype(jnp.float32), axis=1, keepdims=True)


def transposed_dot(left, right):
    return lax.dot_general(left, right, (((1,), (1,)), ((), ())), preferred_element_type=jnp.float32)


class Side:
    def __init__(self, send, recv):
        self.peer = {"x": 1 - lax.axis_index("x")}
        self.send, self.recv, self.copies = send, recv, []

    def start(self, source, target):
        at = len(self.copies)
        copy = remote(source, target, self.send.at[at], self.recv.at[at], self.peer)
        copy.start()
        self.copies.append(copy)
        return copy

    def later(self, source, target):
        at = len(self.copies)
        copy = remote(source, target, self.send.at[at], self.recv.at[at], self.peer)
        self.copies.append(copy)
        return copy

    def finish(self, taken=()):
        for copy in self.copies:
            copy.wait_send()
            if not any(copy is item for item in taken):
                copy.wait_recv()


def remote(src, dst, send, recv, device):
    return pltpu.make_async_remote_copy(
        src_ref=src, dst_ref=dst, send_sem=send, recv_sem=recv, device_id=device, device_id_type=MESH_ID
    )


def halves(features):
    half = features // 2
    x = lax.axis_index("x")
    own = pl.ds(pl.multiple_of(x * half, half), half)
    other = pl.ds(pl.multiple_of((1 - x) * half, half), half)
    return own, other


def flip(block):
    return jnp.transpose(block.astype(jnp.float32)).astype(jnp.bfloat16)


def grad_tile(turned, features, right, cols, kept, given):
    own, other = halves(features)
    value = right[:, cols]
    kept[:, cols] = jnp.dot(turned[own, :], value, preferred_element_type=jnp.float32).astype(jnp.bfloat16)
    given[:, cols] = jnp.dot(turned[other, :], value, preferred_element_type=jnp.float32).astype(jnp.bfloat16)


def sem(*shape):
    return pltpu.SemaphoreType.DMA(shape)


class Link:
    def __init__(self, part, at, shape, dtype):
        self.part, self.at, self.shape, self.dtype = part, at, shape, dtype


class Part:
    def __init__(self, kernel, operands, shapes, staged_in, staged_out, scratch, aliases, flops, name):
        self.kernel, self.operands, self.shapes = kernel, operands, shapes
        self.staged_in, self.staged_out, self.scratch = staged_in, staged_out, scratch
        self.aliases, self.flops, self.name = aliases, flops, name

    def link(self, at, part=0):
        return Link(part, at, self.shapes[at].shape, self.shapes[at].dtype)


class Done:
    def start(self):
        pass

    def wait(self):
        pass


class Later:
    def __init__(self, copy):
        self.start = copy.start

    def wait(self):
        pass


def launch(parts, greet, ident):
    operands, aliases, shapes, scratch = [], {}, [], []
    for part in parts:
        base = len(shapes)
        for at, item in enumerate(part.operands):
            if not isinstance(item, Link):
                if at in part.aliases:
                    aliases[len(operands)] = base + part.aliases[at]
                operands.append(item)
        shapes += part.shapes
        for item in part.operands[: part.staged_in]:
            if not (isinstance(item, Link) and item.at < parts[item.part].staged_out):
                scratch.append(pltpu.VMEM(item.shape, item.dtype))
        scratch += [pltpu.VMEM(item.shape, item.dtype) for item in part.shapes[: part.staged_out]]
        scratch += [sem(part.staged_in), sem(part.staged_out)] + part.scratch

    def body(*refs):
        given, made, rest = refs[: len(operands)], refs[len(operands) : len(operands) + len(shapes)], list(
            refs[len(operands) + len(shapes) :]
        )
        given, made = list(given), list(made)
        ready, results, held = [], [], []
        for part in parts:
            outs = [made.pop(0) for _ in part.shapes]
            inner, sources, late = [], [], []
            for at, item in enumerate(part.operands):
                if isinstance(item, Link):
                    staged, whole = results[item.part]
                    near = item.at < parts[item.part].staged_out
                    source = None if near else whole[item.at]
                    late.append(at)
                else:
                    near, source = False, given.pop(0)
                if at >= part.staged_in:
                    inner.append(source)
                elif near:
                    inner.append(staged[item.at])
                    source = None
                else:
                    inner.append(rest.pop(0))
                sources.append(source)
            results_in = [rest.pop(0) for _ in range(part.staged_out)]
            load_s, store_s = rest.pop(0), rest.pop(0)
            own = [rest.pop(0) for _ in part.scratch]
            loads = [
                Done() if sources[k] is None else pltpu.make_async_copy(sources[k], inner[k], load_s.at[k])
                for k in range(part.staged_in)
            ]
            stores = [pltpu.make_async_copy(results_in[k], outs[k], store_s.at[k]) for k in range(part.staged_out)]
            for k, copy in enumerate(loads):
                if k not in late:
                    copy.start()
            results.append((results_in, outs))
            ready.append((loads, stores, late, inner, results_in + outs[part.staged_out :], own))
        for at, part in enumerate(parts):
            loads, stores, late, inner, outs, own = ready[at]
            for k in late:
                if k < part.staged_in:
                    loads[k].start()
            last = at == len(parts) - 1
            if not last:
                held += stores
                stores = [Later(copy) for copy in stores]
            part.kernel(loads, stores, greet if at == 0 else lambda: None, *inner, *outs, *own)
        for copy in held:
            copy.wait()

    outside = pl.BlockSpec(memory_space=pl.ANY)
    out = pl.pallas_call(
        body,
        out_shape=tuple(shapes),
        in_specs=[outside] * len(operands),
        out_specs=[outside] * len(shapes),
        input_output_aliases=aliases,
        scratch_shapes=scratch,
        compiler_params=pltpu.CompilerParams(collective_id=ident, has_side_effects=True, vmem_limit_bytes=62 << 20),
        cost_estimate=pl.CostEstimate(
            flops=sum(part.flops for part in parts), bytes_accessed=8_000_000, transcendentals=0
        ),
        name="_".join(part.name for part in parts),
    )(*operands)
    out = list(out)
    return [[out.pop(0) for _ in part.shapes] for part in parts]


class Line:
    def __init__(self, tok, depth):
        self.z, self.x = lax.axis_index("z"), lax.axis_index("x")
        self.y, self.c = lax.axis_index("y"), lax.axis_index("c")
        self.tok, self.depth = tok, depth
        self.half = 2 * tok
        self.chunks = self.half // ROWS
        self.own = pl.multiple_of((2 * self.y + self.c) * tok, tok)
        self.peers = (
            {"y": self.y, "c": 1 - self.c},
            {"y": 1 - self.y, "c": self.c},
            {"y": 1 - self.y, "c": 1 - self.c},
        )

    def place(self, stream):
        return self.z if stream == 0 else self.depth - 1 - self.z

    def onward(self, stream):
        return {"z": self.z + 1} if stream == 0 else {"z": self.z - 1}

    def backward(self, stream):
        return {"z": self.z - 1} if stream == 0 else {"z": self.z + 1}

    def row_of(self, stream, chunk):
        per = self.chunks // 2
        far = chunk // per
        y = self.y + far * (1 - 2 * self.y)
        return pl.multiple_of((2 * y + stream) * self.tok + lax.rem(chunk, per) * ROWS, ROWS)


def make_line(tok, depth, width_in, width_out, carry_in, carry_out, features):
    chunks = 2 * tok // ROWS
    groups = chunks // GROUP_CHUNKS
    span = GROUP_CHUNKS * ROWS
    half_groups = groups // 2

    def run(line, greet, taken, begin, prepare, beside, finish, second, settle, close, product, carried, chain_out, chain_in, wide, own_part, rs_out, rs_in,
            ag_s, ag_r, ch_s, ch_r, bc_s, bc_r, rs_s, rs_r):
        greet()
        gather = [
            pltpu.make_async_remote_copy(
                src_ref=taken.at[pl.ds(line.own, tok)],
                dst_ref=taken.at[pl.ds(line.own, tok)],
                send_sem=ag_s.at[at],
                recv_sem=ag_r.at[at],
                device_id=peer,
                device_id_type=MESH_ID,
            )
            for at, peer in enumerate(line.peers)
        ]
        for copy in gather:
            copy.start()
        begin()
        gather[0].wait_recv()
        prepare(pl.multiple_of(line.y * 2 * tok, 2 * tok))

        def chain_copy(stream, chunk):
            return pltpu.make_async_remote_copy(
                src_ref=chain_out.at[stream, chunk],
                dst_ref=chain_in.at[stream, chunk],
                send_sem=ch_s.at[stream, chunk],
                recv_sem=ch_r.at[stream, chunk],
                device_id=line.onward(stream),
                device_id_type=MESH_ID,
            )

        def wide_copy(stream, chunk):
            rows = pl.ds(line.row_of(stream, chunk), ROWS)
            return pltpu.make_async_remote_copy(
                src_ref=wide.at[rows],
                dst_ref=wide.at[rows],
                send_sem=bc_s.at[stream, chunk],
                recv_sem=bc_r.at[stream, chunk],
                device_id=line.backward(stream),
                device_id_type=MESH_ID,
            )

        def sum_copy(stream, group):
            far = group // half_groups
            y = line.y + far * (1 - 2 * line.y)
            other = stream + line.c - 2 * stream * line.c
            slot = 2 * far + other - 1
            part = lax.rem(group, half_groups)
            return (slot >= 0, part, pltpu.make_async_remote_copy(
                src_ref=rs_out.at[stream, group],
                dst_ref=rs_in.at[jnp.maximum(slot, 0), pl.ds(pl.multiple_of(part * span, span), span)],
                send_sem=rs_s.at[stream, group],
                recv_sem=rs_r.at[jnp.maximum(slot, 0), part],
                device_id={"y": y, "c": stream},
                device_id_type=MESH_ID,
            ))

        def step(i, _):
            @pl.when(i == SKEW)
            def _():
                gather[1].wait_recv()
                gather[2].wait_recv()
                prepare(pl.multiple_of((1 - line.y) * 2 * tok, 2 * tok))

            beside(i)
            for stream in (0, 1):
                place = line.place(stream)
                chunk = i - SKEW * place

                @pl.when((chunk >= 0) & (chunk < chunks))
                def _():
                    row = line.row_of(stream, chunk)

                    @pl.when(place > 0)
                    def _():
                        chain_copy(stream, chunk).wait_recv()

                    @pl.when(place == 0)
                    def _():
                        chain_out[stream, chunk, :, :width_in] = product[pl.ds(row, ROWS), :].astype(jnp.bfloat16)
                        if carry_in:
                            chain_out[stream, chunk, :, width_in:] = spread(carried[pl.ds(row, ROWS), :1])

                    @pl.when((place > 0) & (place < depth - 1))
                    def _():
                        chain_out[stream, chunk, :, :width_in] = (
                            product[pl.ds(row, ROWS), :] + chain_in[stream, chunk, :, :width_in].astype(jnp.float32)
                        ).astype(jnp.bfloat16)
                        if carry_in:
                            chain_out[stream, chunk, :, width_in:] = spread(
                                carried[pl.ds(row, ROWS), :1] + unspread(chain_in[stream, chunk, :, width_in:])
                            )

                    @pl.when(place < depth - 1)
                    def _():
                        chain_copy(stream, chunk).start()

                    @pl.when(place == depth - 1)
                    def _():
                        total = product[pl.ds(row, ROWS), :] + chain_in[stream, chunk, :, :width_in].astype(jnp.float32)
                        extra = None
                        if carry_in:
                            extra = carried[pl.ds(row, ROWS), :1] + unspread(chain_in[stream, chunk, :, width_in:])
                        finish(row, pl.multiple_of(chunk * ROWS, ROWS), total, extra)
                        wide_copy(stream, chunk).start()

                ready = i - SKEW * (2 * (depth - 1) - place)

                @pl.when((ready >= 0) & (ready < chunks))
                def _():
                    @pl.when(place < depth - 1)
                    def _():
                        wide_copy(stream, ready).wait_recv()

                        @pl.when(place > 0)
                        def _():
                            wide_copy(stream, ready).start()

                    @pl.when(lax.rem(ready, GROUP_CHUNKS) == GROUP_CHUNKS - 1)
                    def _():
                        group = ready // GROUP_CHUNKS
                        row = pl.multiple_of(line.row_of(stream, ready) - (span - ROWS), span)
                        away, part, copy = sum_copy(stream, group)
                        value = second(row, span)

                        @pl.when(away)
                        def _():
                            rs_out[stream, group, :, :features] = value.astype(jnp.bfloat16)
                            if carry_out:
                                rs_out[stream, group, :, features:] = wide[pl.ds(row, span), width_out:]
                            copy.start()

                        @pl.when(jnp.logical_not(away))
                        def _():
                            own_part[pl.ds(pl.multiple_of(part * span, span), span), :] = value

            return 0

        lax.fori_loop(0, chunks + 2 * SKEW * (depth - 1), step, 0)

        def drain(i, _):
            for stream in (0, 1):
                place = line.place(stream)

                @pl.when(place < depth - 1)
                def _():
                    chain_copy(stream, i).wait_send()

                @pl.when(place > 0)
                def _():
                    wide_copy(stream, i).wait_send()

            return 0

        def drain_sums(i, _):
            for stream in (0, 1):
                away, part, copy = sum_copy(stream, i)

                @pl.when(away)
                def _():
                    copy.wait_send()
            return 0

        settle()
        for slot in range(3):
            for part in range(half_groups):
                pltpu.make_async_remote_copy(
                    src_ref=rs_out.at[0, 0],
                    dst_ref=rs_in.at[slot, pl.ds(part * span, span)],
                    send_sem=rs_s.at[0, 0],
                    recv_sem=rs_r.at[slot, part],
                    device_id=line.peers[slot],
                    device_id_type=MESH_ID,
                ).wait_recv()
        close()
        for copy in gather:
            copy.wait_send()
        lax.fori_loop(0, chunks, drain, 0)
        lax.fori_loop(0, groups, drain_sums, 0)

    wide_in = width_in + (EXTRA if carry_in else 0)
    scratch = [
        pltpu.VMEM((4 * tok, width_in), jnp.float32),
        pltpu.VMEM((4 * tok, EXTRA), jnp.float32),
        pltpu.VMEM((2, chunks, ROWS, wide_in), jnp.bfloat16),
        pltpu.VMEM((2, chunks, ROWS, wide_in), jnp.bfloat16),
        pltpu.VMEM((tok, features), jnp.float32),
        pltpu.VMEM((2, groups, span, features + (EXTRA if carry_out else 0)), jnp.bfloat16),
        pltpu.VMEM((3, tok, features + (EXTRA if carry_out else 0)), jnp.bfloat16),
        pltpu.SemaphoreType.DMA((3,)),
        pltpu.SemaphoreType.DMA((3,)),
        pltpu.SemaphoreType.DMA((2, chunks)),
        pltpu.SemaphoreType.DMA((2, chunks)),
        pltpu.SemaphoreType.DMA((2, chunks)),
        pltpu.SemaphoreType.DMA((2, chunks)),
        pltpu.SemaphoreType.DMA((2, groups)),
        pltpu.SemaphoreType.DMA((3, half_groups)),
    ]
    return run, scratch


TILE = 256


def ffn_forward(hidden, gain, gu_own, gu_peer, down_own, shipped, depth):
    tok, features = hidden.shape
    width = down_own.shape[1]
    run, scratch = make_line(tok, depth, 2 * width, width, True, False, features)
    count = len(shipped)

    def kernel(loads, stores, greet, h_ref, gain_ref, w1_own, w1_peer, w2_own, *rest):
        leave, rest = rest[:count], rest[count:]
        (out_ref, normed_t, kept, wide, w2_peer), rest = rest[:5], rest[5:]
        landed, rest = rest[:count], rest[count:]
        (taken, scaled, pieces, side_s, side_r, product, carried, chain_out, chain_in, own_part, rs_out, rs_in), sems = (
            rest[:12], rest[12:])
        line = Line(tok, depth)
        side = Side(side_s, side_r)
        own, other = halves(features)
        loads[0].wait()
        taken[pl.ds(line.own, tok), :] = h_ref[...].astype(jnp.bfloat16)
        at_end = (line.z == 0) | (line.z == depth - 1)

        def begin():
            for copy in loads[1:]:
                copy.wait()
            side.start(w2_own, w2_peer)
            for source, target in zip(leave, landed):
                side.start(source, target)

        def prepare(row):
            rows = pl.ds(row, 2 * tok)
            block = taken[rows, :].astype(jnp.float32)
            carried[rows, :] = jnp.broadcast_to(jnp.sum(block * block, axis=1, keepdims=True), (2 * tok, EXTRA))
            scaled[...] = (block * gain_ref[...]).astype(jnp.bfloat16)

            def tile(j, _):
                cols = pl.ds(pl.multiple_of(j * TILE, TILE), TILE)
                product[rows, cols] = jnp.dot(
                    scaled[:, own], w1_own[:, cols], preferred_element_type=jnp.float32
                ) + jnp.dot(scaled[:, other], w1_peer[:, cols], preferred_element_type=jnp.float32)
                return 0

            lax.fori_loop(0, 2 * width // TILE, tile, 0)

        def beside(i):
            @pl.when(i == SKEW * (depth - 1))
            def _():
                side.copies[0].wait_recv()
                stores[4].start()

        def finish(row, at, total, extra):
            factor = lax.rsqrt(extra / D + EPS)
            gate = total[:, :width] * factor
            upper = total[:, width:] * factor
            kept[pl.ds(at, ROWS), :width] = gate
            kept[pl.ds(at, ROWS), width:] = upper
            active = gate * jax.nn.sigmoid(gate) * upper
            wide[pl.ds(row, ROWS), :width] = active.astype(jnp.bfloat16)
            wide[pl.ds(row, ROWS), width:] = spread(factor)

        def second(row, span):
            value = wide[pl.ds(row, span), :width]
            pieces[:, own] = transposed_dot(value, w2_own[...])
            pieces[:, other] = transposed_dot(value, w2_peer[...])
            return pieces[...]

        def settle():
            stores[3].start()

            @pl.when(at_end)
            def _():
                stores[2].start()

            normed = taken[...].astype(jnp.float32) * unspread(wide[:, width:]) * gain_ref[...]
            normed_t[...] = jnp.transpose(normed).astype(jnp.bfloat16)
            stores[1].start()

        def close():
            total = own_part[...]
            for slot in range(3):
                total = total + rs_in[slot].astype(jnp.float32)
            out_ref[...] = h_ref[...] + total
            stores[0].start()
            side.finish(side.copies[:1])
            for at in (0, 1, 3, 4):
                stores[at].wait()

            @pl.when(at_end)
            def _():
                stores[2].wait()

        run(line, greet, taken, begin, prepare, beside, finish, second, settle, close, product, carried, chain_out, chain_in, wide,
            own_part, rs_out, rs_in, *sems)

    low, full = jnp.bfloat16, jnp.float32
    shapes = (
        jax.ShapeDtypeStruct((tok, features), full),
        jax.ShapeDtypeStruct((features, 4 * tok), low),
        jax.ShapeDtypeStruct((2 * tok, 2 * width), full),
        jax.ShapeDtypeStruct((4 * tok, width + EXTRA), low),
        jax.ShapeDtypeStruct(down_own.shape, low),
    ) + tuple(jax.ShapeDtypeStruct(item.shape, item.dtype) for item in shipped)
    return Part(
        kernel, (hidden, gain.reshape(1, -1), gu_own, gu_peer, down_own, *shipped), shapes, 5, 5,
        [
            pltpu.VMEM((4 * tok, features), low),
            pltpu.VMEM((2 * tok, features), low),
            pltpu.VMEM((GROUP_CHUNKS * ROWS, features), full),
            sem(1 + count), sem(1 + count),
        ] + scratch,
        {}, 60_000_000_000, "ffn_forward",
    )


def ffn_backward(
    grad, hidden, gain, kept, wide_forward, gu_own, gu_peer, down_own, down_peer, shipped, stacks, index, layers, depth
):
    tok, features = hidden.shape
    width = down_own.shape[1]
    run, scratch = make_line(tok, depth, width, 2 * width, False, True, features)
    count = len(shipped)
    first_tile = SKEW + 1
    tiles = width // EXTRA

    def kernel(loads, stores, greet, dy_ref, h_ref, gain_ref, kept_ref, before_ref, w1_own, w1_peer, w2_own, w2_peer, *rest):
        leave, rest = rest[:count], rest[count:]
        rest = rest[len(stacks):]
        (out_ref, wide, gain_out, kept_all, got_all), rest = rest[:5], rest[5:]
        landed, rest = rest[:count], rest[count:]
        (taken, turned, down_kept, down_given, keep_s, pieces, side_s, side_r, product, carried, chain_out, chain_in, own_part,
         rs_out, rs_in), sems = rest[:15], rest[15:]
        line = Line(tok, depth)
        side = Side(side_s, side_r)
        own, other = halves(features)
        loads[0].wait()
        taken[pl.ds(line.own, tok), :] = dy_ref[...].astype(jnp.bfloat16)
        give = side.later(down_given, got_all.at[index])
        keep = pltpu.make_async_copy(down_kept, kept_all.at[index], keep_s)

        def begin():
            for source, target in zip(leave, landed):
                side.start(source, target)
            loads[7].wait()
            loads[8].wait()

        def prepare(row):
            rows = pl.ds(row, 2 * tok)

            def tile(j, _):
                cols = pl.ds(pl.multiple_of(j * EXTRA, EXTRA), EXTRA)
                product[rows, cols] = jnp.dot(
                    taken[rows, own], w2_own[:, cols], preferred_element_type=jnp.float32
                ) + jnp.dot(taken[rows, other], w2_peer[:, cols], preferred_element_type=jnp.float32)
                return 0

            lax.fori_loop(0, width // EXTRA, tile, 0)

        def beside(i):
            @pl.when(i == 1)
            def _():
                for copy in loads[1:7]:
                    copy.wait()

            @pl.when(i == first_tile)
            def _():
                turned[...] = flip(taken[...])

            @pl.when((i >= first_tile) & (i < first_tile + tiles))
            def _():
                cols = pl.ds(pl.multiple_of((i - first_tile) * EXTRA, EXTRA), EXTRA)
                grad_tile(turned, features, before_ref, cols, down_kept, down_given)

            @pl.when(i == first_tile + tiles)
            def _():
                give.start()
                keep.start()

        def finish(row, at, total, extra):
            gate = kept_ref[pl.ds(at, ROWS), :width]
            upper = kept_ref[pl.ds(at, ROWS), width:]
            sig = jax.nn.sigmoid(gate)
            silu = gate * sig
            grad_gate = total * upper * (sig + silu * (1.0 - sig))
            grad_up = total * silu
            wide[pl.ds(row, ROWS), :width] = grad_gate.astype(jnp.bfloat16)
            wide[pl.ds(row, ROWS), width : 2 * width] = grad_up.astype(jnp.bfloat16)
            inner = jnp.sum(grad_gate * gate + grad_up * upper, axis=1, keepdims=True)
            wide[pl.ds(row, ROWS), 2 * width :] = spread(inner)

        def second(row, span):
            value = wide[pl.ds(row, span), : 2 * width]
            pieces[:, own] = transposed_dot(value, w1_own[...])
            pieces[:, other] = transposed_dot(value, w1_peer[...])
            return pieces[...]

        def settle():
            stores[1].start()

        def close():
            total = own_part[...]
            inner = unspread(wide[pl.ds(line.own, tok), 2 * width :])
            for slot in range(3):
                total = total + rs_in[slot, :, :features].astype(jnp.float32)
                inner = inner + unspread(rs_in[slot, :, features:])
            factor = unspread(before_ref[pl.ds(line.own, tok), width:])
            normed = h_ref[...] * factor
            gain_out[...] = jnp.broadcast_to(jnp.sum(total * normed, axis=0, keepdims=True), gain_out.shape)
            out_ref[...] = dy_ref[...] + factor * (total * gain_ref[...] - normed * (inner / D))
            stores[2].start()
            stores[0].start()
            keep.wait()
            side.finish()
            for copy in stores:
                copy.wait()

        run(line, greet, taken, begin, prepare, beside, finish, second, settle, close, product, carried, chain_out, chain_in,
            wide, own_part, rs_out, rs_in, *sems)

    low, full = jnp.bfloat16, jnp.float32
    shapes = (
        jax.ShapeDtypeStruct((tok, features), full),
        jax.ShapeDtypeStruct((4 * tok, 2 * width + EXTRA), low),
        jax.ShapeDtypeStruct((8, features), full),
        jax.ShapeDtypeStruct((layers,) + down_own.shape, low),
        jax.ShapeDtypeStruct((layers,) + down_own.shape, low),
    ) + tuple(jax.ShapeDtypeStruct(item.shape, item.dtype) for item in shipped)
    return Part(
        kernel,
        (grad, hidden, gain.reshape(1, -1), kept, wide_forward, gu_own, gu_peer, down_own, down_peer, *shipped, *stacks),
        shapes, 9, 3,
        [
            pltpu.VMEM((4 * tok, features), low),
            pltpu.VMEM((features, 4 * tok), low),
            pltpu.VMEM(down_own.shape, low),
            pltpu.VMEM(down_own.shape, low),
            pltpu.SemaphoreType.DMA,
            pltpu.VMEM((GROUP_CHUNKS * ROWS, features), full),
            sem(1 + count), sem(1 + count),
        ] + scratch,
        {9 + count + at: 3 + at for at in range(len(stacks))}, 60_000_000_000, "ffn_backward",
    )


def to_row(column):
    return jnp.transpose(jnp.broadcast_to(column, (column.shape[0], EXTRA)))[:8]


def to_column(row):
    return jnp.transpose(jnp.broadcast_to(row[:1], (row.shape[1], row.shape[1])))[:, :1]


def turn(values, cosine, sine):
    lane = lax.broadcasted_iota(jnp.int32, values.shape, 1)
    width = values.shape[1]
    back = pltpu.roll(values, width - HEAD // 2, 1)
    forth = pltpu.roll(values, HEAD // 2, 1)
    partner = jnp.where(lax.rem(lane, HEAD) < HEAD // 2, back, forth)
    return values * cosine + partner * sine


def split_pair(block):
    lane = lax.broadcasted_iota(jnp.int32, block.shape, 1)
    zero = jnp.zeros_like(block)
    return jnp.concatenate([jnp.where(lane < HEAD, block, zero), jnp.where(lane < HEAD, zero, block)], axis=0)


def join_pair(turned, tok):
    return jnp.transpose(jnp.concatenate([turned[:HEAD, :tok], turned[HEAD:, tok:]], axis=0))


def twice(kv):
    wide = kv.astype(jnp.float32)
    lane = lax.broadcasted_iota(jnp.int32, wide.shape, 1)
    other = pltpu.roll(wide, HEAD, 1)
    return jnp.where(lane < HEAD, wide, other), jnp.where(lane < HEAD, other, wide)


class Square:
    def __init__(self, tok, depth):
        self.z, self.x = lax.axis_index("z"), lax.axis_index("x")
        self.y, self.c = lax.axis_index("y"), lax.axis_index("c")
        self.tok, self.depth = tok, depth
        self.g = 2 * self.y + self.c
        self.row = 2 * self.z + self.x
        self.own = pl.multiple_of(self.g * tok, tok)
        self.mine = pl.multiple_of(self.z * tok, tok)
        self.peers = (
            {"y": self.y, "c": 1 - self.c},
            {"y": 1 - self.y, "c": self.c},
            {"y": 1 - self.y, "c": 1 - self.c},
        )

    def row_peer(self, step):
        at = lax.rem(self.row + step, 2 * self.depth)
        return {"z": at // 2, "x": lax.rem(at, 2)}

    def greet(self):
        barrier = pltpu.get_barrier_semaphore()
        for peer in self.peers:
            pl.semaphore_signal(barrier, 1, device_id=peer, device_id_type=MESH_ID)
        for step in range(1, 2 * self.depth):
            pl.semaphore_signal(barrier, 1, device_id=self.row_peer(step), device_id_type=MESH_ID)
        pl.semaphore_wait(barrier, 3 + 2 * self.depth - 1)


def start_gather(square, taken, send, recv):
    copies = [
        remote(taken.at[pl.ds(square.own, square.tok)], taken.at[pl.ds(square.own, square.tok)], send.at[at], recv.at[at], peer)
        for at, peer in enumerate(square.peers)
    ]
    for copy in copies:
        copy.start()
    return copies


def line_sum(square, gather, product, own, own_row, outs, ins, row_outs, row_ins, send, recv, row_send, row_recv, between):
    tok, depth = square.tok, square.depth

    def one(order):
        block = lax.rem(2 * square.y + order, depth)
        step = lax.rem(block - square.z + depth, depth)
        slot = jnp.maximum(depth - 1 - step, 0)
        value, column = product(pl.multiple_of(block * tok, tok))

        @pl.when(step == 0)
        def _():
            own[...] = value
            if column is not None:
                own_row[...] = to_row(column)

        copy = remote(outs.at[order], ins.at[slot], send.at[order], recv.at[slot], {"z": block})
        row_copy = None
        if column is not None:
            row_copy = remote(row_outs.at[order], row_ins.at[slot], row_send.at[order], row_recv.at[slot], {"z": block})

        @pl.when(step != 0)
        def _():
            outs[order] = value.astype(jnp.bfloat16)
            copy.start()
            if column is not None:
                row_outs[order] = to_row(column)
                row_copy.start()

        return step, copy, row_copy

    gather[0].wait_recv()
    sent = [one(0), one(1)]
    gather[1].wait_recv()
    gather[2].wait_recv()
    sent += [one(2), one(3)]
    between()
    for slot in range(depth - 1):
        remote(outs.at[0], ins.at[slot], send.at[0], recv.at[slot], {"z": square.z}).wait_recv()
        if row_ins is not None:
            remote(row_outs.at[0], row_ins.at[slot], row_send.at[0], row_recv.at[slot], {"z": square.z}).wait_recv()
    return sent


def send_part(square, array, part, send, recv):
    lanes = pl.ds(pl.multiple_of(part * EXTRA, EXTRA), EXTRA)
    here = array.at[pl.ds(square.mine, square.tok), lanes]
    depth = square.depth
    return [
        remote(here, here, send.at[step - 1, part], recv.at[depth - 1 - step, part], {"z": lax.rem(square.z + step, depth)})
        for step in range(1, depth)
    ]


def send_row(square, rows, send, recv):
    line = rows.at[square.z]
    depth = square.depth
    return [
        remote(line, line, send.at[step - 1], recv.at[depth - 1 - step], {"z": lax.rem(square.z + step, depth)})
        for step in range(1, depth)
    ]


def grid_sum(square, array, rows, second, settle, own, outs, ins, row_ins, arrive, row_arrive, send, recv, row_send, row_recv):
    tok, depth = square.tok, square.depth
    sent = []
    for step in range(depth):
        block = lax.rem(square.z + step, depth)
        if step:
            for part in range(array.shape[1] // EXTRA):
                rows_of = array.at[pl.ds(pl.multiple_of(block * tok, tok), tok), pl.ds(part * EXTRA, EXTRA)]
                remote(rows_of, rows_of, send.at[0], arrive.at[step - 1, part], {"z": square.z}).wait_recv()
            remote(rows.at[block], rows.at[block], send.at[0], row_arrive.at[step - 1], {"z": square.z}).wait_recv()
        value = second(pl.multiple_of(block * tok, tok))
        away = lax.rem(block - square.g + depth, depth)
        slot = jnp.maximum(depth - 1 - away, 0)
        device = {"y": block // 2, "c": lax.rem(block, 2)}
        copy = remote(outs.at[step], ins.at[slot], send.at[step], recv.at[slot], device)
        row_copy = None
        if row_ins is not None:
            row_copy = remote(rows.at[block], row_ins.at[slot], row_send.at[step], row_recv.at[slot], device)

        @pl.when(away == 0)
        def _():
            own[...] = value

        @pl.when(away != 0)
        def _():
            outs[step] = value.astype(jnp.bfloat16)
            copy.start()
            if row_ins is not None:
                row_copy.start()

        sent.append((away, copy, row_copy))
    settle()
    for slot in range(depth - 1):
        remote(outs.at[0], ins.at[slot], send.at[0], recv.at[slot], square.peers[0]).wait_recv()
        if row_ins is not None:
            remote(rows.at[0], row_ins.at[slot], row_send.at[0], row_recv.at[slot], square.peers[0]).wait_recv()
    return sent


def drain(sent):
    for away, copy, row_copy in sent:

        @pl.when(away != 0)
        def _():
            copy.wait_send()
            if row_copy is not None:
                row_copy.wait_send()


def attention_forward(hidden, gain, qkv_own, out_own, qkv_peer, out_peer, shipped, cosine, sine, depth):
    tok, features = hidden.shape
    cols = qkv_own.shape[1]
    fetch = qkv_peer is None
    extra = 2 if fetch else 0
    count = len(shipped)
    sides = extra + 2 * count
    query_cols = GROUP * HEAD
    seq = 2 * depth * tok
    pairs = query_cols // EXTRA
    scale = 1.0 / math.sqrt(HEAD)

    def kernel(loads, stores, greet, h_ref, gain_ref, wqkv_own, wo_own, cos_ref, sin_ref, *rest):
        if not fetch:
            (wqkv_peer, wo_peer), rest = rest[:2], rest[2:]
        leave, rest = rest[:count], rest[count:]
        (out_ref, normed_t, queries, kv, lse, mixed, factors), rest = rest[:7], rest[7:]
        if fetch:
            (wqkv_peer, wo_peer), rest = rest[:2], rest[2:]
        landed, rest = rest[:count], rest[count:]
        (taken, scaled, pieces, own, own_row, z_out, z_in, zr_out, zr_in, values_t, g_own, g_out, g_in,
         ag_s, ag_r, zs_s, zs_r, zr_s, zr_r, kv_s, kv_r, zg_s, zg_r, zgr_s, zgr_r, gs_s, gs_r), rest = rest[:27], rest[27:]
        square = Square(tok, depth)
        side = Side(*rest) if sides else None
        mine, other = halves(features)
        loads[0].wait()
        taken[pl.ds(square.own, tok), :] = h_ref[...].astype(jnp.bfloat16)
        greet()
        gather = start_gather(square, taken, ag_s, ag_r)
        for copy in loads[1:]:
            copy.wait()
        urgent = []
        if fetch:
            urgent = [side.start(wqkv_own, wqkv_peer), side.start(wo_own, wo_peer)]
        held = []
        for source, target in zip(leave, landed):
            most = source.shape[0] // 2
            rest_of = pl.ds(most, source.shape[0] - most)
            side.start(source.at[pl.ds(0, most)], target.at[pl.ds(0, most)])
            held.append(side.later(source.at[rest_of], target.at[rest_of]))
        for copy in urgent[:1]:
            copy.wait_recv()
            stores[7].start()

        def product(row):
            block = taken[pl.ds(row, tok), :].astype(jnp.float32)
            scaled[...] = (block * gain_ref[...]).astype(jnp.bfloat16)
            return (
                jnp.dot(scaled[:, mine], wqkv_own[...], preferred_element_type=jnp.float32)
                + jnp.dot(scaled[:, other], wqkv_peer[...], preferred_element_type=jnp.float32),
                jnp.sum(block * block, axis=1, keepdims=True),
            )

        sent = line_sum(square, gather, product, own, own_row, z_out, z_in, zr_out, zr_in, zs_s, zs_r, zr_s, zr_r, lambda: None)
        total, squares = own[...], own_row[...]
        for slot in range(depth - 1):
            total = total + z_in[slot].astype(jnp.float32)
            squares = squares + zr_in[slot]
        factor_row = lax.rsqrt(squares / D + EPS)
        factors[square.z] = factor_row
        given = send_row(square, factors, zgr_s, zgr_r)
        for copy in given:
            copy.start()
        first = lax.broadcasted_iota(jnp.int32, (tok, EXTRA), 1) < HEAD
        cosine_row, sine_row = cos_ref[...], sin_ref[...]
        turned = turn(
            total * to_column(factor_row),
            jnp.concatenate([cosine_row] * pairs + [jnp.where(first, cosine_row, 1.0)], axis=1),
            jnp.concatenate([sine_row] * pairs + [jnp.where(first, sine_row, 0.0)], axis=1),
        )
        here = pl.ds(pl.multiple_of(square.row * tok, tok), tok)
        kv[here, :] = turned[:, query_cols:].astype(jnp.bfloat16)
        queries[...] = turned[:, :query_cols].astype(jnp.bfloat16)
        stores[2].start()
        spreads = []
        for step in range(1, 2 * depth):
            copy = remote(kv.at[here], kv.at[here], kv_s.at[step - 1], kv_r.at[2 * depth - 1 - step], square.row_peer(step))
            copy.start()
            spreads.append(copy)
        for copy in spreads:
            copy.wait_recv()
        stores[3].start()
        for copy in held:
            copy.start()
        keys, both = twice(kv[...])
        values_t[...] = jnp.transpose(both).astype(jnp.bfloat16)
        keys = keys.astype(jnp.bfloat16)

        def pair(t, _):
            lanes = pl.ds(pl.multiple_of(t * EXTRA, EXTRA), EXTRA)
            scores = transposed_dot(keys, split_pair(queries[:, lanes])) * scale
            key_at = lax.broadcasted_iota(jnp.int32, scores.shape, 0)
            query_at = lax.rem(lax.broadcasted_iota(jnp.int32, scores.shape, 1), tok) + square.row * tok
            scores = jnp.where(key_at <= query_at, scores, -1e30)
            top = jnp.max(scores, axis=0, keepdims=True)
            expo = jnp.exp(scores - top)
            denom = jnp.sum(expo, axis=0, keepdims=True)
            lse[t] = jnp.broadcast_to(top + jnp.log(denom), (8, 2 * tok))
            probs = (expo * (1.0 / denom)).astype(jnp.bfloat16)
            out_t = jnp.dot(values_t[...], probs, preferred_element_type=jnp.float32)
            mixed[pl.ds(square.mine, tok), lanes] = join_pair(out_t, tok).astype(jnp.bfloat16)
            for copy in send_part(square, mixed, t, zg_s, zg_r):
                copy.start()
            return 0

        lax.fori_loop(0, pairs, pair, 0)
        given += [copy for part in range(pairs) for copy in send_part(square, mixed, part, zg_s, zg_r)]

        stores[4].start()
        for copy in urgent[1:]:
            copy.wait_recv()
            stores[8].start()

        def second(row):
            value = mixed[pl.ds(row, tok), :]
            pieces[:, mine] = transposed_dot(value, wo_own[...])
            pieces[:, other] = transposed_dot(value, wo_peer[...])
            return pieces[...]

        def settle():
            stores[5].start()
            stores[6].start()
            for block in range(depth):
                rows = pl.ds(block * tok, tok)
                normed = taken[rows, :].astype(jnp.float32) * to_column(factors[block]) * gain_ref[...]
                normed_t[:, rows] = jnp.transpose(normed).astype(jnp.bfloat16)
            stores[1].start()

        sums = grid_sum(square, mixed, factors, second, settle, g_own, g_out, g_in, None, zg_r, zgr_r, gs_s, gs_r, None, None)
        total = g_own[...]
        for slot in range(depth - 1):
            total = total + g_in[slot].astype(jnp.float32)
        out_ref[...] = h_ref[...] + total
        stores[0].start()
        drain(sent)
        drain(sums)
        for copy in gather + spreads + given:
            copy.wait_send()
        if side:
            side.finish(urgent)
        for copy in stores:
            copy.wait()

    low, full = jnp.bfloat16, jnp.float32
    shapes = (
        jax.ShapeDtypeStruct((tok, features), full),
        jax.ShapeDtypeStruct((features, depth * tok), low),
        jax.ShapeDtypeStruct((tok, query_cols), low),
        jax.ShapeDtypeStruct((seq, 2 * HEAD), low),
        jax.ShapeDtypeStruct((pairs, 8, 2 * tok), full),
        jax.ShapeDtypeStruct((depth * tok, query_cols), low),
        jax.ShapeDtypeStruct((depth, 8, tok), full),
    )
    if fetch:
        shapes += (jax.ShapeDtypeStruct(qkv_own.shape, low), jax.ShapeDtypeStruct(out_own.shape, low))
    shapes += tuple(jax.ShapeDtypeStruct(item.shape, item.dtype) for item in shipped)
    peers = () if fetch else (qkv_peer, out_peer)
    operands = (hidden, gain.reshape(1, -1), qkv_own, out_own, cosine, sine, *peers, *shipped)
    return Part(
        kernel, operands, shapes, 6 + len(peers), 7 + extra,
        [
            pltpu.VMEM((depth * tok, features), low),
            pltpu.VMEM((tok, features), low),
            pltpu.VMEM((tok, features), full),
            pltpu.VMEM((tok, cols), full),
            pltpu.VMEM((8, tok), full),
            pltpu.VMEM((depth, tok, cols), low),
            pltpu.VMEM((depth - 1, tok, cols), low),
            pltpu.VMEM((depth, 8, tok), full),
            pltpu.VMEM((depth - 1, 8, tok), full),
            pltpu.VMEM((2 * HEAD, seq), low),
            pltpu.VMEM((tok, features), full),
            pltpu.VMEM((depth, tok, features), low),
            pltpu.VMEM((depth - 1, tok, features), low),
            sem(3), sem(3), sem(depth), sem(depth - 1), sem(depth), sem(depth - 1),
            sem(2 * depth - 1), sem(2 * depth - 1), sem(depth - 1, pairs), sem(depth - 1, pairs), sem(depth - 1), sem(depth - 1),
            sem(depth), sem(depth - 1),
        ] + ([sem(sides), sem(sides)] if sides else []),
        {}, 50_000_000_000, "attention_forward",
    )


def attention_backward(
    grad, hidden, gain, qkv_own, qkv_peer, out_own, out_peer, cosine, sine, queries, kv, lse, factors, mixed, normed_a, normed_f,
    grad_gu, stacks, index, layers, depth,
):
    tok, features = hidden.shape
    cols = qkv_own.shape[1]
    wide = grad_gu.shape[1] - EXTRA
    query_cols = GROUP * HEAD
    seq = 2 * depth * tok
    pairs = query_cols // EXTRA
    scale = 1.0 / math.sqrt(HEAD)

    def kernel(loads, stores, greet, dy_ref, h_ref, gain_ref, wqkv_own, wqkv_peer, wo_own, wo_peer, cos_ref, sin_ref, q_ref, kv_ref, lse_ref,
               factor_ref, mixed_ref, normed_a_ref, normed_f_ref, gu_ref, *rest_refs):
        (out_ref, gain_out, qkv_given, gu_kept_all, gu_got_all, out_kept_all, out_got_all, qkv_kept_all,
               taken, spun, turned, pieces, gu_kept, gu_given, out_kept, out_given, qkv_kept, keep_s,
               own, heads, z_out, z_in, keys_t, dk, dv, kv_out, kv_in, dq, inner_rows, g_own, g_out, g_in, g_rows,
               ag_s, ag_r, zs_s, zs_r, kv_s, kv_r, zg_s, zg_r, zgr_s, zgr_r, gs_s, gs_r, gr_s, gr_r, side_s, side_r) = rest_refs[len(stacks):]
        square = Square(tok, depth)
        side = Side(side_s, side_r)
        mine, other = halves(features)
        loads[0].wait()
        taken[pl.ds(square.own, tok), :] = dy_ref[...].astype(jnp.bfloat16)
        greet()
        gather = start_gather(square, taken, ag_s, ag_r)
        for copy in loads[1:]:
            copy.wait()

        def gu_tiles(start, stop):
            def tile(j, _):
                grad_tile(normed_f_ref, features, gu_ref, pl.ds(pl.multiple_of(j * EXTRA, EXTRA), EXTRA), gu_kept, gu_given)
                return 0

            lax.fori_loop(start, stop, tile, 0)

        gu_got = gu_got_all.at[index]
        keeps = [
            pltpu.make_async_copy(gu_kept, gu_kept_all.at[index], keep_s.at[0]),
            pltpu.make_async_copy(out_kept, out_kept_all.at[index], keep_s.at[1]),
            pltpu.make_async_copy(qkv_kept, qkv_kept_all.at[index], keep_s.at[2]),
        ]
        every = wide // EXTRA
        middle, late = every // 2, every * 3 // 4
        gu_tiles(0, middle)
        front, rest = pl.ds(0, middle * EXTRA), pl.ds(late * EXTRA, wide - late * EXTRA)
        inner_part = pl.ds(middle * EXTRA, (late - middle) * EXTRA)
        side.start(gu_given.at[:, front], gu_got.at[:, front])

        def between():
            turned[...] = flip(taken[...])
            for t in range(query_cols // EXTRA):
                grad_tile(turned, features, mixed_ref, pl.ds(t * EXTRA, EXTRA), out_kept, out_given)
            side.start(out_given, out_got_all.at[index])
            gu_tiles(middle, late)
            side.start(gu_given.at[:, inner_part], gu_got.at[:, inner_part])
            gu_tiles(late, every)
            keeps[0].start()
            keeps[1].start()

        def product(row):
            rows = pl.ds(row, tok)
            value = jnp.dot(taken[rows, mine], wo_own[...], preferred_element_type=jnp.float32) + jnp.dot(
                taken[rows, other], wo_peer[...], preferred_element_type=jnp.float32
            )
            return value, None

        sent = line_sum(square, gather, product, own, None, z_out, z_in, None, None, zs_s, zs_r, None, None, between)
        total = own[...]
        for slot in range(depth - 1):
            total = total + z_in[slot].astype(jnp.float32)
        heads[...] = total.astype(jnp.bfloat16)
        keys, both = twice(kv_ref[...])
        keys_t[...] = jnp.transpose(keys).astype(jnp.bfloat16)
        keys = keys.astype(jnp.bfloat16)
        both = both.astype(jnp.bfloat16)
        dk[...] = jnp.zeros_like(dk)
        dv[...] = jnp.zeros_like(dv)

        def pair(t, _):
            lanes = pl.ds(pl.multiple_of(t * EXTRA, EXTRA), EXTRA)
            query = split_pair(q_ref[:, lanes])
            head = split_pair(heads[:, lanes])
            scores = transposed_dot(keys, query) * scale
            key_at = lax.broadcasted_iota(jnp.int32, scores.shape, 0)
            query_at = lax.rem(lax.broadcasted_iota(jnp.int32, scores.shape, 1), tok) + square.row * tok
            probs = jnp.exp(jnp.where(key_at <= query_at, scores, -1e30) - lse_ref[t, :1, :])
            grad_probs = transposed_dot(both, head)
            delta = jnp.sum(probs * grad_probs, axis=0, keepdims=True)
            grad_scores = (probs * (grad_probs - delta)).astype(jnp.bfloat16)
            dk[...] += jnp.dot(grad_scores, query, preferred_element_type=jnp.float32)
            dv[...] += jnp.dot(probs.astype(jnp.bfloat16), head, preferred_element_type=jnp.float32)
            back = jnp.dot(keys_t[...], grad_scores, preferred_element_type=jnp.float32)
            value = join_pair(back, tok) * scale
            dq[...] += jnp.broadcast_to(
                jnp.sum(value * q_ref[:, lanes].astype(jnp.float32), axis=1, keepdims=True), dq.shape
            )
            spun[pl.ds(square.mine, tok), lanes] = turn(value, cos_ref[...], -sin_ref[...]).astype(jnp.bfloat16)
            for copy in send_part(square, spun, t, zg_s, zg_r):
                copy.start()
            return 0

        dq[...] = jnp.zeros_like(dq)
        lax.fori_loop(0, pairs, pair, 0)
        lane = lax.broadcasted_iota(jnp.int32, (seq, EXTRA), 1)
        left = dk[...]
        right = dv[...]
        both_kv = jnp.where(
            lane < HEAD, (left + pltpu.roll(left, HEAD, 1)) * scale, right + pltpu.roll(right, HEAD, 1)
        )
        dk[...] = both_kv
        kv_out[...] = both_kv.astype(jnp.bfloat16)
        here = pl.ds(pl.multiple_of(square.row * tok, tok), tok)
        spreads = []
        for step in range(1, 2 * depth):
            at = lax.rem(square.row + step, 2 * depth)
            copy = remote(
                kv_out.at[pl.ds(pl.multiple_of(at * tok, tok), tok)],
                kv_in.at[2 * depth - 1 - step],
                kv_s.at[step - 1],
                kv_r.at[2 * depth - 1 - step],
                square.row_peer(step),
            )
            copy.start()
            spreads.append(copy)
        total_kv = dk[here, :]
        for copy in spreads:
            copy.wait_recv()
        side.start(gu_given.at[:, rest], gu_got.at[:, rest])
        for slot in range(2 * depth - 1):
            total_kv = total_kv + kv_in[slot].astype(jnp.float32)
        first = lax.broadcasted_iota(jnp.int32, (tok, EXTRA), 1) < HEAD
        spun[pl.ds(square.mine, tok), query_cols:] = turn(
            total_kv, jnp.where(first, cos_ref[...], 1.0), jnp.where(first, -sin_ref[...], 0.0)
        ).astype(jnp.bfloat16)
        inner = dq[:, :1] + jnp.sum(total_kv * kv_ref[here, :].astype(jnp.float32), axis=1, keepdims=True)
        inner_rows[square.z] = to_row(inner)
        given = send_part(square, spun, pairs, zg_s, zg_r) + send_row(square, inner_rows, zgr_s, zgr_r)
        for copy in given:
            copy.start()
        given += [copy for part in range(pairs) for copy in send_part(square, spun, part, zg_s, zg_r)]

        def second(row):
            value = spun[pl.ds(row, tok), :]
            pieces[:, mine] = transposed_dot(value, wqkv_own[...])
            pieces[:, other] = transposed_dot(value, wqkv_peer[...])
            return pieces[...]

        def settle():
            for t in range(cols // EXTRA):
                grad_tile(normed_a_ref, features, spun, pl.ds(t * EXTRA, EXTRA), qkv_kept, qkv_given)
            keeps[2].start()
            stores[2].start()

        sums = grid_sum(
            square, spun, inner_rows, second, settle, g_own, g_out, g_in, g_rows, zg_r, zgr_r, gs_s, gs_r, gr_s, gr_r
        )
        total = g_own[...]
        inner = inner_rows[square.g]
        for slot in range(depth - 1):
            total = total + g_in[slot].astype(jnp.float32)
            inner = inner + g_rows[slot]
        factor = to_column(factor_ref[square.g])
        normed = h_ref[...] * factor
        gain_out[...] = jnp.broadcast_to(jnp.sum(total * normed, axis=0, keepdims=True), gain_out.shape)
        out_ref[...] = dy_ref[...] + factor * (total * gain_ref[...] - normed * (to_column(inner) / D))
        stores[0].start()
        stores[1].start()
        drain(sent)
        drain(sums)
        for copy in gather + spreads + given:
            copy.wait_send()
        for copy in keeps + stores:
            copy.wait()
        side.finish()

    low, full = jnp.bfloat16, jnp.float32
    shapes = (
        jax.ShapeDtypeStruct((tok, features), full),
        jax.ShapeDtypeStruct((8, features), full),
        jax.ShapeDtypeStruct(qkv_own.shape, low),
        jax.ShapeDtypeStruct((layers, features // 2, wide), low),
        jax.ShapeDtypeStruct((layers, features // 2, wide), low),
        jax.ShapeDtypeStruct((layers,) + out_own.shape, low),
        jax.ShapeDtypeStruct((layers,) + out_own.shape, low),
        jax.ShapeDtypeStruct((layers,) + qkv_own.shape, low),
    )
    operands = (
        grad, hidden, gain.reshape(1, -1), qkv_own, qkv_peer, out_own, out_peer, cosine, sine, queries, kv, lse, factors,
        mixed, normed_a, normed_f, grad_gu, *stacks,
    )
    return Part(
        kernel, operands, shapes, 17, 3,
        [
            pltpu.VMEM((depth * tok, features), low),
            pltpu.VMEM((depth * tok, cols), low),
            pltpu.VMEM((features, depth * tok), low),
            pltpu.VMEM((tok, features), full),
            pltpu.VMEM((features // 2, wide), low),
            pltpu.VMEM((features // 2, wide), low),
            pltpu.VMEM(out_own.shape, low),
            pltpu.VMEM(out_own.shape, low),
            pltpu.VMEM(qkv_own.shape, low),
            sem(3),
            pltpu.VMEM((tok, query_cols), full),
            pltpu.VMEM((tok, query_cols), low),
            pltpu.VMEM((depth, tok, query_cols), low),
            pltpu.VMEM((depth - 1, tok, query_cols), low),
            pltpu.VMEM((2 * HEAD, seq), low),
            pltpu.VMEM((seq, 2 * HEAD), full),
            pltpu.VMEM((seq, 2 * HEAD), full),
            pltpu.VMEM((seq, 2 * HEAD), low),
            pltpu.VMEM((2 * depth - 1, tok, 2 * HEAD), low),
            pltpu.VMEM((tok, EXTRA), full),
            pltpu.VMEM((depth, 8, tok), full),
            pltpu.VMEM((tok, features), full),
            pltpu.VMEM((depth, tok, features), low),
            pltpu.VMEM((depth - 1, tok, features), low),
            pltpu.VMEM((depth - 1, 8, tok), full),
            sem(3), sem(3), sem(depth), sem(depth - 1),
            sem(2 * depth - 1), sem(2 * depth - 1), sem(depth - 1, pairs + 1), sem(depth - 1, pairs + 1), sem(depth - 1),
            sem(depth - 1), sem(depth), sem(depth - 1), sem(depth), sem(depth - 1), sem(4), sem(4),
        ],
        {17 + at: 3 + at for at in range(len(stacks))}, 50_000_000_000, "attention_backward",
    )


def finish(grad, gains, qkv_given, depth):
    tok, features = grad.shape
    count = len(gains)
    members = 2 * depth

    def kernel(loads, stores, greet, grad_ref, *rest):
        gain_refs, rest = rest[:count], rest[count:]
        (given, out_ref, gain_out, got, packed, parts, sent, home, part_s, part_r, move_s, move_r, side_s, side_r) = rest
        z, x = lax.axis_index("z"), lax.axis_index("x")
        y, c = lax.axis_index("y"), lax.axis_index("c")
        g = 2 * y + c
        barrier = pltpu.get_barrier_semaphore()
        self_at = x * depth + g

        def source(slot):
            return {"z": g, "x": slot // depth, "y": (slot % depth) // 2, "c": slot % 2}

        def target(at):
            return {"z": at // 2, "x": at % 2, "y": z // 2, "c": lax.rem(z, 2)}

        def is_source_me(slot):
            return (z == g) & (slot == self_at)

        def is_target_me(at):
            return (z == g) & (at == 2 * z + x)

        for slot in range(members):

            @pl.when(jnp.logical_not(is_source_me(slot)))
            def _():
                pl.semaphore_signal(barrier, 1, device_id=source(slot), device_id_type=MESH_ID)

        pl.semaphore_signal(barrier, 1, device_id={"x": 1 - x}, device_id_type=MESH_ID)
        for copy in loads:
            copy.wait()
        for at, ref in enumerate(gain_refs):
            packed[at : at + 1, :] = ref[:1, :]
        sent[...] = grad_ref[...].astype(jnp.bfloat16)
        pl.semaphore_wait(barrier, members + 1 - jnp.where(z == g, 1, 0))
        side = Side(side_s, side_r)
        side.start(given, got)
        move = remote(sent, home, move_s, move_r, {"z": g, "y": z // 2, "c": lax.rem(z, 2)})

        @pl.when(z != g)
        def _():
            move.start()

        def part(at):
            return remote(packed, parts.at[self_at], part_s.at[at], part_r.at[self_at], target(at))

        for at in range(members):

            @pl.when(jnp.logical_not(is_target_me(at)))
            def _():
                part(at).start()

        @pl.when(z == g)
        def _():
            parts[self_at] = packed[...]

        for slot in range(members):

            @pl.when(jnp.logical_not(is_source_me(slot)))
            def _():
                remote(packed, parts.at[slot], part_s.at[0], part_r.at[slot], target(0)).wait_recv()

        total = parts[0]
        for slot in range(1, members):
            total = total + parts[slot]
        gain_out[...] = total
        stores[1].start()

        @pl.when(z == g)
        def _():
            out_ref[...] = grad_ref[...]

        @pl.when(z != g)
        def _():
            move.wait_recv()
            out_ref[...] = home[...].astype(jnp.float32)
            move.wait_send()

        stores[0].start()
        for at in range(members):

            @pl.when(jnp.logical_not(is_target_me(at)))
            def _():
                part(at).wait_send()

        side.finish()
        for copy in stores:
            copy.wait()

    low, full = jnp.bfloat16, jnp.float32
    shapes = (
        jax.ShapeDtypeStruct((tok, features), full),
        jax.ShapeDtypeStruct((count, features), full),
        jax.ShapeDtypeStruct(qkv_given.shape, low),
    )
    return Part(
        kernel, (grad, *gains, qkv_given), shapes, 1 + count, 2,
        [
            pltpu.VMEM((count, features), full),
            pltpu.VMEM((members, count, features), full),
            pltpu.VMEM((tok, features), low),
            pltpu.VMEM((tok, features), low),
            sem(members), sem(members),
            pltpu.SemaphoreType.DMA, pltpu.SemaphoreType.DMA,
            sem(1), sem(1),
        ],
        {}, 5_000_000_000, "finish",
    )


def stationary(stream, grad_out, wqkv, wo, wgu, wd, gain_attn, gain_ffn):
    tok = stream.shape[0]
    layers = wqkv.shape[0]
    count_rows = wqkv.shape[1]
    depth = lax.axis_size("z")
    head = HEAD
    row = lax.axis_index("z") * 2 + lax.axis_index("x")
    query_pos = row * tok + jnp.arange(tok, dtype=jnp.int32)
    lane = jnp.arange(EXTRA, dtype=jnp.int32)
    half = head // 2
    freq = THETA ** (-((lane % half).astype(jnp.float32) * 2.0 / head))
    angle = query_pos.astype(jnp.float32)[:, None] * freq[None, :]
    cosine = jnp.cos(angle)
    sine = jnp.where((lane % head < half)[None, :], -1.0, 1.0) * jnp.sin(angle)
    current = swap_grid(stream, depth)
    grad_now = swap_grid(grad_out, depth)
    gains = swap_grid(jnp.concatenate([gain_attn, gain_ffn]), depth)
    gain_a, gain_f = gains[:layers], gains[layers:]
    greet = lambda: Square(tok, depth).greet()
    own_qkv = [wqkv[index].reshape(count_rows, -1) for index in range(layers)]
    own_out = [wo[index] for index in range(layers)]
    own_gu = [wgu[index].reshape(count_rows, -1) for index in range(layers)]
    own_down = [wd[index] for index in range(layers)]
    peer_qkv, peer_out, peer_gu, peer_down = ([None] * layers for _ in range(4))
    saved = []
    for index in range(layers):
        before = current
        first = index == 0
        follow = index + 1
        shipped = [own_qkv[follow], own_out[follow], own_gu[follow]] if follow < layers else []
        attend = attention_forward(
            before, gain_a[index], own_qkv[index], own_out[index], peer_qkv[index], peer_out[index],
            own_gu[:1] if first else [], cosine, sine, depth
        )
        feed = ffn_forward(
            attend.link(0), gain_f[index], own_gu[index], attend.link(len(attend.shapes) - 1) if first else peer_gu[index],
            own_down[index], shipped, depth
        )
        made, fed = launch([attend, feed], greet, 2 * index)
        hidden_in, normed_a, queries, kv, lse, mixed, factors = made[:7]
        if first:
            peer_qkv[0], peer_out[0], peer_gu[0] = made[7:]
        current, normed_f, kept, active, peer_down[index] = fed[:5]
        if shipped:
            peer_qkv[follow], peer_out[follow], peer_gu[follow] = fed[5:]
        saved.append((before, normed_a, queries, kv, lse, mixed, factors, hidden_in, normed_f, kept, active))
    list_ga, list_gf, got_qkv, pending, down_stack, rest_stack = ([], [], [], [], [], [])
    for index in reversed(range(layers)):
        before, normed_a, queries, kv, lse, mixed, factors, hidden_in, normed_f, kept, active = saved[index]
        feed = ffn_backward(
            grad_now, hidden_in, gain_f[index], kept, active, own_gu[index], peer_gu[index], own_down[index],
            peer_down[index], pending[-1:], down_stack, index, layers, depth
        )
        attend = attention_backward(
            feed.link(0), before, gain_a[index], own_qkv[index], peer_qkv[index], own_out[index], peer_out[index],
            cosine, sine, queries, kv, lse, factors, mixed, normed_a, normed_f, feed.link(1), rest_stack, index, layers,
            depth
        )
        fed, made = launch([feed, attend], greet, 2 * index + 1)
        down_stack = fed[3:5]
        got_qkv.extend(fed[5:])
        list_gf.append(fed[2])
        (grad_now, gain_a_grad, qkv_given, *rest_stack) = made
        pending.append(qkv_given)
        list_ga.append(gain_a_grad)
    ((grad_in, gains, last_qkv),) = launch(
        [finish(grad_now, list_ga[::-1] + list_gf[::-1], qkv_given, depth)], None, 2 * layers
    )
    got_qkv.append(last_qkv)
    gu_kept, gu_got, out_kept, out_got, qkv_kept = rest_stack
    add = lambda kept, got: kept.astype(jnp.float32) + got.astype(jnp.float32)
    return (
        swap_grid(current, depth),
        grad_in,
        add(qkv_kept, jnp.stack(got_qkv[::-1])).reshape(layers, count_rows, 1, -1),
        add(out_kept, out_got),
        add(gu_kept, gu_got).reshape(layers, count_rows, 2, -1),
        add(*down_stack),
        gains[:layers],
        gains[layers:],
    )


def solution(mesh):
    rows, cols = ("row", "col")
    body = local
    if (mesh.shape["row"], mesh.shape["col"]) == (8, 4):
        mesh = share_out(mesh)
        rows, cols = (("z", "x"), ("y", "c"))
        body = stationary
    in_specs = (
        P(rows, cols),
        P(rows, cols),
        P(None, rows, cols, None),
        P(None, rows, cols),
        P(None, rows, None, cols),
        P(None, rows, cols),
        P(None, cols),
        P(None, cols),
    )
    out_specs = (
        P(rows, cols),
        P(rows, cols),
        P(None, rows, cols, None),
        P(None, rows, cols),
        P(None, rows, None, cols),
        P(None, rows, cols),
        P(None, cols),
        P(None, cols),
    )
    return jax.shard_map(body, mesh=mesh, in_specs=in_specs, out_specs=out_specs, check_vma=False)
```

```python
import math

import jax
import jax.numpy as jnp
from jax import lax
from jax.experimental import pallas as pl
from jax.experimental.pallas import tpu as pltpu
from jax.sharding import Mesh
from jax.sharding import PartitionSpec as P

D = 2048
HEAD = 64
GROUP = 8


EPS = 1e-05
THETA = 10000.0


def rope_turn(tensor, cosine, sine):
    half = tensor.shape[-1] // 2
    first = tensor[..., :half]
    second = tensor[..., half:]
    return jnp.concatenate(
        [first * cosine - second * sine, second * cosine + first * sine], axis=-1
    )


def feature_sum(values):
    return lax.psum(values, "col")


def gather_features(rows_in):
    return lax.all_gather(rows_in, "col", axis=1, tiled=True)


def sum_features(partials):
    return lax.psum_scatter(
        partials.astype(jnp.bfloat16), "col", scatter_dimension=1, tiled=True
    ).astype(jnp.float32)


def add_rows(left, piece):
    return jnp.dot(left, piece, preferred_element_type=jnp.float32)


def project_in(left, shard):
    return add_rows(left, lax.all_gather(shard, "row", axis=0, tiled=True))


def columns_of(left, piece):
    return jnp.einsum("tj,dj->td", left, piece, preferred_element_type=jnp.float32)


def project_out(left, shard):
    return columns_of(left, lax.all_gather(shard, "row", axis=0, tiled=True))


def weight_grad(left, right):
    return lax.psum_scatter(
        lax.dot_general(
            left, right, (((0,), (0,)), ((), ())), preferred_element_type=jnp.float32
        ).astype(jnp.bfloat16),
        "row",
        scatter_dimension=0,
        tiled=True,
    ).astype(jnp.float32)


def norm_forward(values, gain):
    total = feature_sum(jnp.sum(values * values, axis=1))
    factor = lax.rsqrt(total / D + EPS)
    normed = values * factor[:, None]
    return (normed, factor, (normed * gain).astype(jnp.bfloat16))


def norm_backward(grad_normed, normed, factor, gain):
    scaled = grad_normed * gain
    inner = feature_sum(jnp.sum(scaled * normed, axis=1))
    grad_in = factor[:, None] * (scaled - normed * (inner / D)[:, None])
    return (grad_in, jnp.sum(grad_normed * normed, axis=0))


def masked_scores(queries, keys, query_pos, key_pos):
    scores = jnp.einsum("qgd,kd->gqk", queries, keys, preferred_element_type=jnp.float32) * (
        1.0 / math.sqrt(queries.shape[-1])
    )
    return jnp.where(key_pos[None, None, :] <= query_pos[None, :, None], scores, -1e30)


def local(stream, grad_out, wqkv, wo, wgu, wd, gain_attn, gain_ffn):
    tok = stream.shape[0]
    layers = wqkv.shape[0]
    count_rows = wqkv.shape[1]
    head = HEAD
    query_cols = GROUP * head
    seq_len = lax.axis_size("row") * tok
    query_pos = lax.axis_index("row") * tok + jnp.arange(tok, dtype=jnp.int32)
    key_pos = jnp.arange(seq_len, dtype=jnp.int32)
    freq = THETA ** (-(jnp.arange(head // 2, dtype=jnp.float32) * 2.0 / head))
    angle = query_pos.astype(jnp.float32)[:, None] * freq[None, :]
    cosine = jnp.cos(angle)
    sine = jnp.sin(angle)
    saved = []
    current = stream
    for index in range(layers):
        weight_qkv = wqkv[index].reshape(count_rows, -1)
        weight_out = wo[index]
        weight_gu = wgu[index].reshape(count_rows, -1)
        weight_down = wd[index]
        wholes = (None, None, None, None)
        normed_a, factor_a, xnormed = norm_forward(current, gain_attn[index])
        xfull = gather_features(xnormed)
        qkv = project_in(xfull, weight_qkv)
        queries = rope_turn(
            qkv[:, :query_cols].reshape(tok, GROUP, head), cosine[:, None, :], sine[:, None, :]
        ).astype(jnp.bfloat16)
        keys = rope_turn(qkv[:, query_cols : query_cols + head], cosine, sine).astype(jnp.bfloat16)
        values = qkv[:, query_cols + head :].astype(jnp.bfloat16)
        seqkv = lax.all_gather(jnp.concatenate([keys, values], axis=1), "row", axis=0, tiled=True)
        seq_keys = seqkv[:, :head]
        seq_values = seqkv[:, head:]
        scores = masked_scores(queries, seq_keys, query_pos, key_pos)
        top = jnp.max(scores, axis=2, keepdims=True)
        expo = jnp.exp(scores - top)
        denom = jnp.sum(expo, axis=2, keepdims=True)
        probs = (expo / denom).astype(jnp.bfloat16)
        log_total = top + jnp.log(denom)
        mixed = (
            jnp.einsum("gqk,kd->qgd", probs, seq_values, preferred_element_type=jnp.float32)
            .reshape(tok, query_cols)
            .astype(jnp.bfloat16)
        )
        hidden_in = current + sum_features(project_out(mixed, weight_out))
        normed_f, factor_f, hnormed = norm_forward(hidden_in, gain_ffn[index])
        hfull = gather_features(hnormed)
        gate_up = project_in(hfull, weight_gu)
        hidden_cols = gate_up.shape[1] // 2
        gate = gate_up[:, :hidden_cols]
        upper = gate_up[:, hidden_cols:]
        active = (jax.nn.silu(gate) * upper).astype(jnp.bfloat16)
        current = hidden_in + sum_features(project_out(active, weight_down))
        saved.append(
            (
                weight_qkv,
                weight_out,
                weight_gu,
                weight_down,
                wholes,
                normed_a,
                factor_a,
                xfull,
                queries,
                seq_keys,
                seq_values,
                log_total,
                mixed,
                normed_f,
                factor_f,
                hfull,
                gate,
                upper,
                active,
            )
        )
    grad_now = grad_out
    list_qkv, list_out, list_gu, list_down, list_ga, list_gf = ([], [], [], [], [], [])
    for index in reversed(range(layers)):
        (
            weight_qkv,
            weight_out,
            weight_gu,
            weight_down,
            wholes,
            normed_a,
            factor_a,
            xfull,
            queries,
            seq_keys,
            seq_values,
            log_total,
            mixed,
            normed_f,
            factor_f,
            hfull,
            gate,
            upper,
            active,
        ) = saved[index]
        grad_full = gather_features(grad_now.astype(jnp.bfloat16))
        grad_active = project_in(grad_full, weight_down)
        list_down.append(weight_grad(grad_full, active))
        sig = jax.nn.sigmoid(gate)
        grad_gate = grad_active * upper * sig * (1.0 + gate * (1.0 - sig))
        grad_up = grad_active * gate * sig
        grad_gu = jnp.concatenate([grad_gate, grad_up], axis=1).astype(jnp.bfloat16)
        grad_hn = sum_features(project_out(grad_gu, weight_gu))
        list_gu.append(weight_grad(hfull, grad_gu).reshape(count_rows, 2, -1))
        grad_mid, gain_f_grad = norm_backward(grad_hn, normed_f, factor_f, gain_ffn[index])
        list_gf.append(gain_f_grad)
        grad_hidden = grad_now + grad_mid
        hidden_full = gather_features(grad_hidden.astype(jnp.bfloat16))
        grad_mixed = project_in(hidden_full, weight_out).astype(jnp.bfloat16)
        list_out.append(weight_grad(hidden_full, mixed))
        grad_heads = grad_mixed.reshape(tok, GROUP, head)
        scores = masked_scores(queries, seq_keys, query_pos, key_pos)
        probs_full = jnp.exp(scores - log_total)
        probs = probs_full.astype(jnp.bfloat16)
        grad_probs = jnp.einsum(
            "qgd,kd->gqk", grad_heads, seq_values, preferred_element_type=jnp.float32
        )
        delta = jnp.sum(probs_full * grad_probs, axis=2, keepdims=True)
        grad_scores = (probs_full * (grad_probs - delta)).astype(jnp.bfloat16)
        inverse = 1.0 / math.sqrt(head)
        grad_queries = (
            jnp.einsum("gqk,kd->qgd", grad_scores, seq_keys, preferred_element_type=jnp.float32)
            * inverse
        )
        grad_keys = (
            jnp.einsum("gqk,qgd->kd", grad_scores, queries, preferred_element_type=jnp.float32)
            * inverse
        )
        grad_values = jnp.einsum(
            "gqk,qgd->kd", probs, grad_heads, preferred_element_type=jnp.float32
        )
        grad_kv = lax.psum_scatter(
            jnp.concatenate([grad_keys, grad_values], axis=1).astype(jnp.bfloat16),
            "row",
            scatter_dimension=0,
            tiled=True,
        ).astype(jnp.float32)
        grad_k = rope_turn(grad_kv[:, :head], cosine, -sine)
        grad_v = grad_kv[:, head:]
        grad_q = rope_turn(grad_queries, cosine[:, None, :], -sine[:, None, :]).reshape(
            tok, query_cols
        )
        grad_qkv = jnp.concatenate([grad_q, grad_k, grad_v], axis=1).astype(jnp.bfloat16)
        grad_xn = sum_features(project_out(grad_qkv, weight_qkv))
        list_qkv.append(weight_grad(xfull, grad_qkv).reshape(count_rows, 1, -1))
        grad_in, gain_a_grad = norm_backward(grad_xn, normed_a, factor_a, gain_attn[index])
        list_ga.append(gain_a_grad)
        grad_now = grad_hidden + grad_in
    gains_a, gains_f = lax.psum((jnp.stack(list_ga[::-1]), jnp.stack(list_gf[::-1])), "row")
    return (
        current,
        grad_now,
        jnp.stack(list_qkv[::-1]),
        jnp.stack(list_out[::-1]),
        jnp.stack(list_gu[::-1]),
        jnp.stack(list_down[::-1]),
        gains_a,
        gains_f,
    )


def share_out(mesh):
    rows, cols = mesh.shape["row"], mesh.shape["col"]
    return Mesh(
        mesh.devices.reshape(rows // 2, 2, cols // 2, 2), ("z", "x", "y", "c")
    )


def swap_grid(values, depth):
    pairs = [(z * depth + g, g * depth + z) for z in range(depth) for g in range(depth)]
    return lax.ppermute(values, ("z", "y", "c"), pairs)


MESH_ID = pl.DeviceIdType.MESH
ROWS = 16
SKEW = 3
GROUP_CHUNKS = 4
EXTRA = 128


def spread(column):
    high = column.astype(jnp.bfloat16)
    low = (column - high.astype(jnp.float32)).astype(jnp.bfloat16)
    lane = lax.broadcasted_iota(jnp.int32, (column.shape[0], EXTRA), 1)
    wide = jnp.where(lane == 0, high.astype(jnp.float32), jnp.where(lane == 1, low.astype(jnp.float32), 0.0))
    return wide.astype(jnp.bfloat16)


def unspread(block):
    return jnp.sum(block.astype(jnp.float32), axis=1, keepdims=True)


def transposed_dot(left, right):
    return lax.dot_general(left, right, (((1,), (1,)), ((), ())), preferred_element_type=jnp.float32)


class Side:
    def __init__(self, send, recv):
        self.peer = {"x": 1 - lax.axis_index("x")}
        self.send, self.recv, self.copies = send, recv, []

    def start(self, source, target):
        at = len(self.copies)
        copy = remote(source, target, self.send.at[at], self.recv.at[at], self.peer)
        copy.start()
        self.copies.append(copy)
        return copy

    def later(self, source, target):
        at = len(self.copies)
        copy = remote(source, target, self.send.at[at], self.recv.at[at], self.peer)
        self.copies.append(copy)
        return copy

    def finish(self, taken=()):
        for copy in self.copies:
            copy.wait_send()
            if not any(copy is item for item in taken):
                copy.wait_recv()


def remote(src, dst, send, recv, device):
    return pltpu.make_async_remote_copy(
        src_ref=src, dst_ref=dst, send_sem=send, recv_sem=recv, device_id=device, device_id_type=MESH_ID
    )


def halves(features):
    half = features // 2
    x = lax.axis_index("x")
    own = pl.ds(pl.multiple_of(x * half, half), half)
    other = pl.ds(pl.multiple_of((1 - x) * half, half), half)
    return own, other


def flip(block):
    return jnp.transpose(block.astype(jnp.float32)).astype(jnp.bfloat16)


def grad_tile(turned, features, right, cols, kept, given):
    own, other = halves(features)
    value = right[:, cols]
    kept[:, cols] = jnp.dot(turned[own, :], value, preferred_element_type=jnp.float32).astype(jnp.bfloat16)
    given[:, cols] = jnp.dot(turned[other, :], value, preferred_element_type=jnp.float32).astype(jnp.bfloat16)


def sem(*shape):
    return pltpu.SemaphoreType.DMA(shape)


class Link:
    def __init__(self, part, at, shape, dtype):
        self.part, self.at, self.shape, self.dtype = part, at, shape, dtype


class Part:
    def __init__(self, kernel, operands, shapes, staged_in, staged_out, scratch, aliases, flops, name, early=None):
        self.kernel, self.operands, self.shapes = kernel, operands, shapes
        self.staged_in, self.staged_out, self.scratch = staged_in, staged_out, scratch
        self.aliases, self.flops, self.name = aliases, flops, name
        self.early, self.private = early, ()

    def link(self, at, part=0):
        return Link(part, at, self.shapes[at].shape, self.shapes[at].dtype)


class Done:
    def start(self):
        pass

    def wait(self):
        pass


class Later:
    def __init__(self, copy):
        self.start = copy.start

    def wait(self):
        pass


def launch(parts, greet, ident):
    operands, aliases, shapes, scratch = [], {}, [], []
    for part in parts:
        base = len(shapes)
        for at, item in enumerate(part.operands):
            if not isinstance(item, Link):
                if at in part.aliases:
                    aliases[len(operands)] = base + part.aliases[at]
                operands.append(item)
        shapes += part.shapes
        for item in part.operands[: part.staged_in]:
            if not (isinstance(item, Link) and item.at < parts[item.part].staged_out):
                scratch.append(pltpu.VMEM(item.shape, item.dtype))
        scratch += [pltpu.VMEM(item.shape, item.dtype) for item in part.shapes[: part.staged_out]]
        scratch += [sem(part.staged_in), sem(part.staged_out)] + part.scratch

    def body(*refs):
        given, made, rest = refs[: len(operands)], refs[len(operands) : len(operands) + len(shapes)], list(
            refs[len(operands) + len(shapes) :]
        )
        given, made = list(given), list(made)
        ready, results, held = [], [], []
        for part in parts:
            outs = [made.pop(0) for _ in part.shapes]
            inner, sources, late = [], [], []
            for at, item in enumerate(part.operands):
                if isinstance(item, Link):
                    staged, whole = results[item.part]
                    near = item.at < parts[item.part].staged_out
                    source = None if near else whole[item.at]
                    late.append(at)
                else:
                    near, source = False, given.pop(0)
                if at >= part.staged_in:
                    inner.append(staged[item.at] if near else source)
                elif near:
                    inner.append(staged[item.at])
                else:
                    inner.append(rest.pop(0))
                sources.append(source)
            results_in = [rest.pop(0) for _ in range(part.staged_out)]
            load_s, store_s = rest.pop(0), rest.pop(0)
            own = [rest.pop(0) for _ in part.scratch]
            loads = [
                Done() if sources[k] is None else pltpu.make_async_copy(sources[k], inner[k], load_s.at[k])
                for k in range(part.staged_in)
            ]
            stores = [
                Done() if k in part.private else pltpu.make_async_copy(results_in[k], outs[k], store_s.at[k])
                for k in range(part.staged_out)
            ]
            for k, copy in enumerate(loads):
                if k not in late:
                    copy.start()
            results.append((results_in, outs))
            ready.append((loads, stores, late, inner, results_in + outs[part.staged_out :], own))
        for at, part in enumerate(parts):
            loads, stores, late, inner, outs, own = ready[at]
            for k in late:
                if k < part.staged_in:
                    loads[k].start()
            last = at == len(parts) - 1
            if not last:
                held += stores
                stores = [Later(copy) for copy in stores]
            hook = lambda: None
            if not last and parts[at + 1].early:
                following = ready[at + 1]
                hook = lambda: parts[at + 1].early(following[0], *following[3], *following[4], *following[5])
            part.kernel(loads, stores, greet if at == 0 else lambda: None, hook, *inner, *outs, *own)
        for copy in held:
            copy.wait()

    outside = pl.BlockSpec(memory_space=pl.ANY)
    out = pl.pallas_call(
        body,
        out_shape=tuple(shapes),
        in_specs=[outside] * len(operands),
        out_specs=[outside] * len(shapes),
        input_output_aliases=aliases,
        scratch_shapes=scratch,
        compiler_params=pltpu.CompilerParams(collective_id=ident, has_side_effects=True, vmem_limit_bytes=62 << 20),
        cost_estimate=pl.CostEstimate(
            flops=sum(part.flops for part in parts), bytes_accessed=8_000_000, transcendentals=0
        ),
        name="_".join(part.name for part in parts),
    )(*operands)
    out = list(out)
    return [[out.pop(0) for _ in part.shapes] for part in parts]


class Line:
    def __init__(self, tok, depth):
        self.z, self.x = lax.axis_index("z"), lax.axis_index("x")
        self.y, self.c = lax.axis_index("y"), lax.axis_index("c")
        self.tok, self.depth = tok, depth
        self.half = 2 * tok
        self.chunks = self.half // ROWS
        self.own = pl.multiple_of((2 * self.y + self.c) * tok, tok)
        self.peers = (
            {"y": self.y, "c": 1 - self.c},
            {"y": 1 - self.y, "c": self.c},
            {"y": 1 - self.y, "c": 1 - self.c},
        )

    def place(self, stream):
        return self.z if stream == 0 else self.depth - 1 - self.z

    def onward(self, stream):
        return {"z": self.z + 1} if stream == 0 else {"z": self.z - 1}

    def backward(self, stream):
        return {"z": self.z - 1} if stream == 0 else {"z": self.z + 1}

    def row_of(self, stream, chunk):
        per = self.chunks // 2
        far = chunk // per
        y = self.y + far * (1 - 2 * self.y)
        return pl.multiple_of((2 * y + stream) * self.tok + lax.rem(chunk, per) * ROWS, ROWS)


def make_line(tok, depth, width_in, width_out, carry_in, carry_out, features):
    chunks = 2 * tok // ROWS
    groups = chunks // GROUP_CHUNKS
    span = GROUP_CHUNKS * ROWS
    half_groups = groups // 2

    def run(line, greet, started, taken, begin, prepare, beside, finish, second, settle, close, product, carried, chain_out, chain_in, wide, own_part, rs_out, rs_in,
            ag_s, ag_r, ch_s, ch_r, bc_s, bc_r, rs_s, rs_r):
        greet()
        gather = [
            pltpu.make_async_remote_copy(
                src_ref=taken.at[pl.ds(line.own, tok)],
                dst_ref=taken.at[pl.ds(line.own, tok)],
                send_sem=ag_s.at[at],
                recv_sem=ag_r.at[at],
                device_id=peer,
                device_id_type=MESH_ID,
            )
            for at, peer in enumerate(line.peers)
        ]
        if not started:
            for copy in gather:
                copy.start()
        begin()
        gather[0].wait_recv()
        prepare(pl.multiple_of(line.y * 2 * tok, 2 * tok))

        def chain_copy(stream, chunk):
            return pltpu.make_async_remote_copy(
                src_ref=chain_out.at[stream, chunk],
                dst_ref=chain_in.at[stream, chunk],
                send_sem=ch_s.at[stream, chunk],
                recv_sem=ch_r.at[stream, chunk],
                device_id=line.onward(stream),
                device_id_type=MESH_ID,
            )

        def wide_copy(stream, chunk):
            rows = pl.ds(line.row_of(stream, chunk), ROWS)
            return pltpu.make_async_remote_copy(
                src_ref=wide.at[rows],
                dst_ref=wide.at[rows],
                send_sem=bc_s.at[stream, chunk],
                recv_sem=bc_r.at[stream, chunk],
                device_id=line.backward(stream),
                device_id_type=MESH_ID,
            )

        def sum_copy(stream, group):
            far = group // half_groups
            y = line.y + far * (1 - 2 * line.y)
            other = stream + line.c - 2 * stream * line.c
            slot = 2 * far + other - 1
            part = lax.rem(group, half_groups)
            return (slot >= 0, part, pltpu.make_async_remote_copy(
                src_ref=rs_out.at[stream, group],
                dst_ref=rs_in.at[jnp.maximum(slot, 0), pl.ds(pl.multiple_of(part * span, span), span)],
                send_sem=rs_s.at[stream, group],
                recv_sem=rs_r.at[jnp.maximum(slot, 0), part],
                device_id={"y": y, "c": stream},
                device_id_type=MESH_ID,
            ))

        def step(i, _):
            @pl.when(i == SKEW)
            def _():
                gather[1].wait_recv()
                gather[2].wait_recv()
                prepare(pl.multiple_of((1 - line.y) * 2 * tok, 2 * tok))

            beside(i)
            for stream in (0, 1):
                place = line.place(stream)
                chunk = i - SKEW * place

                @pl.when((chunk >= 0) & (chunk < chunks))
                def _():
                    row = line.row_of(stream, chunk)

                    @pl.when(place > 0)
                    def _():
                        chain_copy(stream, chunk).wait_recv()

                    @pl.when(place == 0)
                    def _():
                        chain_out[stream, chunk, :, :width_in] = product[pl.ds(row, ROWS), :].astype(jnp.bfloat16)
                        if carry_in:
                            chain_out[stream, chunk, :, width_in:] = spread(carried[pl.ds(row, ROWS), :1])

                    @pl.when((place > 0) & (place < depth - 1))
                    def _():
                        chain_out[stream, chunk, :, :width_in] = (
                            product[pl.ds(row, ROWS), :] + chain_in[stream, chunk, :, :width_in].astype(jnp.float32)
                        ).astype(jnp.bfloat16)
                        if carry_in:
                            chain_out[stream, chunk, :, width_in:] = spread(
                                carried[pl.ds(row, ROWS), :1] + unspread(chain_in[stream, chunk, :, width_in:])
                            )

                    @pl.when(place < depth - 1)
                    def _():
                        chain_copy(stream, chunk).start()

                    @pl.when(place == depth - 1)
                    def _():
                        total = product[pl.ds(row, ROWS), :] + chain_in[stream, chunk, :, :width_in].astype(jnp.float32)
                        extra = None
                        if carry_in:
                            extra = carried[pl.ds(row, ROWS), :1] + unspread(chain_in[stream, chunk, :, width_in:])
                        finish(row, pl.multiple_of(chunk * ROWS, ROWS), total, extra)
                        wide_copy(stream, chunk).start()

                ready = i - SKEW * (2 * (depth - 1) - place)

                @pl.when((ready >= 0) & (ready < chunks))
                def _():
                    @pl.when(place < depth - 1)
                    def _():
                        wide_copy(stream, ready).wait_recv()

                        @pl.when(place > 0)
                        def _():
                            wide_copy(stream, ready).start()

                    @pl.when(lax.rem(ready, GROUP_CHUNKS) == GROUP_CHUNKS - 1)
                    def _():
                        group = ready // GROUP_CHUNKS
                        row = pl.multiple_of(line.row_of(stream, ready) - (span - ROWS), span)
                        away, part, copy = sum_copy(stream, group)
                        value = second(row, span)

                        @pl.when(away)
                        def _():
                            rs_out[stream, group, :, :features] = value.astype(jnp.bfloat16)
                            if carry_out:
                                rs_out[stream, group, :, features:] = wide[pl.ds(row, span), width_out:]
                            copy.start()

                        @pl.when(jnp.logical_not(away))
                        def _():
                            own_part[pl.ds(pl.multiple_of(part * span, span), span), :] = value

            return 0

        lax.fori_loop(0, chunks + 2 * SKEW * (depth - 1), step, 0)

        def drain(i, _):
            for stream in (0, 1):
                place = line.place(stream)

                @pl.when(place < depth - 1)
                def _():
                    chain_copy(stream, i).wait_send()

                @pl.when(place > 0)
                def _():
                    wide_copy(stream, i).wait_send()

            return 0

        def drain_sums(i, _):
            for stream in (0, 1):
                away, part, copy = sum_copy(stream, i)

                @pl.when(away)
                def _():
                    copy.wait_send()
            return 0

        settle()
        for slot in range(3):
            for part in range(half_groups):
                pltpu.make_async_remote_copy(
                    src_ref=rs_out.at[0, 0],
                    dst_ref=rs_in.at[slot, pl.ds(part * span, span)],
                    send_sem=rs_s.at[0, 0],
                    recv_sem=rs_r.at[slot, part],
                    device_id=line.peers[slot],
                    device_id_type=MESH_ID,
                ).wait_recv()
        close()
        for copy in gather:
            copy.wait_send()
        lax.fori_loop(0, chunks, drain, 0)
        lax.fori_loop(0, groups, drain_sums, 0)

    wide_in = width_in + (EXTRA if carry_in else 0)
    scratch = [
        pltpu.VMEM((4 * tok, width_in), jnp.float32),
        pltpu.VMEM((4 * tok, EXTRA), jnp.float32),
        pltpu.VMEM((2, chunks, ROWS, wide_in), jnp.bfloat16),
        pltpu.VMEM((2, chunks, ROWS, wide_in), jnp.bfloat16),
        pltpu.VMEM((tok, features), jnp.float32),
        pltpu.VMEM((2, groups, span, features + (EXTRA if carry_out else 0)), jnp.bfloat16),
        pltpu.VMEM((3, tok, features + (EXTRA if carry_out else 0)), jnp.bfloat16),
        pltpu.SemaphoreType.DMA((3,)),
        pltpu.SemaphoreType.DMA((3,)),
        pltpu.SemaphoreType.DMA((2, chunks)),
        pltpu.SemaphoreType.DMA((2, chunks)),
        pltpu.SemaphoreType.DMA((2, chunks)),
        pltpu.SemaphoreType.DMA((2, chunks)),
        pltpu.SemaphoreType.DMA((2, groups)),
        pltpu.SemaphoreType.DMA((3, half_groups)),
    ]
    return run, scratch


TILE = 256


def ffn_forward(hidden, gain, gu_own, gu_peer, down_own, shipped, depth):
    tok, features = hidden.shape
    width = down_own.shape[1]
    run, scratch = make_line(tok, depth, 2 * width, width, True, False, features)
    chunks = 2 * tok // ROWS
    started = False
    count = len(shipped)

    def kernel(loads, stores, greet, hook, h_ref, gain_ref, w1_own, w1_peer, w2_own, *rest):
        leave, rest = rest[:count], rest[count:]
        (out_ref, normed_t, kept, wide, w2_peer), rest = rest[:5], rest[5:]
        landed, rest = rest[:count], rest[count:]
        (taken, scaled, pieces, side_s, side_r, product, carried, chain_out, chain_in, own_part, rs_out, rs_in), sems = (
            rest[:12], rest[12:])
        line = Line(tok, depth)
        side = Side(side_s, side_r)
        own, other = halves(features)
        loads[0].wait()
        taken[pl.ds(line.own, tok), :] = h_ref[...].astype(jnp.bfloat16)
        at_end = (line.z == 0) | (line.z == depth - 1)

        def begin():
            for copy in loads[1:]:
                copy.wait()
            side.start(w2_own, w2_peer)
            for source, target in zip(leave, landed):
                side.start(source, target)

        def prepare(row):
            rows = pl.ds(row, 2 * tok)
            block = taken[rows, :].astype(jnp.float32)
            carried[rows, :] = jnp.broadcast_to(jnp.sum(block * block, axis=1, keepdims=True), (2 * tok, EXTRA))
            scaled[...] = (block * gain_ref[...]).astype(jnp.bfloat16)

            def tile(j, _):
                cols = pl.ds(pl.multiple_of(j * TILE, TILE), TILE)
                product[rows, cols] = jnp.dot(
                    scaled[:, own], w1_own[:, cols], preferred_element_type=jnp.float32
                ) + jnp.dot(scaled[:, other], w1_peer[:, cols], preferred_element_type=jnp.float32)
                return 0

            lax.fori_loop(0, 2 * width // TILE, tile, 0)

        def beside(i):
            @pl.when(i == SKEW * (depth - 1))
            def _():
                side.copies[0].wait_recv()
                stores[4].start()

            @pl.when(i == chunks // 2)
            def _():
                hook()

        def finish(row, at, total, extra):
            factor = lax.rsqrt(extra / D + EPS)
            gate = total[:, :width] * factor
            upper = total[:, width:] * factor
            kept[pl.ds(at, ROWS), :width] = gate
            kept[pl.ds(at, ROWS), width:] = upper
            active = gate * jax.nn.sigmoid(gate) * upper
            wide[pl.ds(row, ROWS), :width] = active.astype(jnp.bfloat16)
            wide[pl.ds(row, ROWS), width:] = spread(factor)

        def second(row, span):
            value = wide[pl.ds(row, span), :width]
            pieces[:, own] = transposed_dot(value, w2_own[...])
            pieces[:, other] = transposed_dot(value, w2_peer[...])
            return pieces[...]

        def settle():
            stores[3].start()

            @pl.when(at_end)
            def _():
                stores[2].start()

            normed = taken[...].astype(jnp.float32) * unspread(wide[:, width:]) * gain_ref[...]
            normed_t[...] = jnp.transpose(normed).astype(jnp.bfloat16)
            stores[1].start()

        def close():
            total = own_part[...]
            for slot in range(3):
                total = total + rs_in[slot].astype(jnp.float32)
            out_ref[...] = h_ref[...] + total
            stores[0].start()
            side.finish(side.copies[:1])
            for at in (0, 1, 3, 4):
                stores[at].wait()

            @pl.when(at_end)
            def _():
                stores[2].wait()

        run(line, greet, started, taken, begin, prepare, beside, finish, second, settle, close, product, carried, chain_out, chain_in, wide,
            own_part, rs_out, rs_in, *sems)

    low, full = jnp.bfloat16, jnp.float32
    shapes = (
        jax.ShapeDtypeStruct((tok, features), full),
        jax.ShapeDtypeStruct((features, 4 * tok), low),
        jax.ShapeDtypeStruct((2 * tok, 2 * width), full),
        jax.ShapeDtypeStruct((4 * tok, width + EXTRA), low),
        jax.ShapeDtypeStruct(down_own.shape, low),
    ) + tuple(jax.ShapeDtypeStruct(item.shape, item.dtype) for item in shipped)
    return Part(
        kernel, (hidden, gain.reshape(1, -1), gu_own, gu_peer, down_own, *shipped), shapes, 5, 5,
        [
            pltpu.VMEM((4 * tok, features), low),
            pltpu.VMEM((2 * tok, features), low),
            pltpu.VMEM((GROUP_CHUNKS * ROWS, features), full),
            sem(1 + count), sem(1 + count),
        ] + scratch,
        {}, 60_000_000_000, "ffn_forward",
    )


def ffn_backward(
    grad, hidden, gain, kept, wide_forward, gu_own, gu_peer, down_own, down_peer, shipped, stacks, index, layers, depth, started
):
    tok, features = hidden.shape
    width = down_own.shape[1]
    run, scratch = make_line(tok, depth, width, 2 * width, False, True, features)
    count = len(shipped)
    first_tile = SKEW + 1
    tiles = width // EXTRA

    def kernel(loads, stores, greet, hook, dy_ref, h_ref, gain_ref, kept_ref, before_ref, w1_own, w1_peer, w2_own, w2_peer, *rest):
        leave, rest = rest[:count], rest[count:]
        rest = rest[len(stacks):]
        (out_ref, wide, gain_out, kept_all, got_all), rest = rest[:5], rest[5:]
        landed, rest = rest[:count], rest[count:]
        (taken, turned, down_kept, down_given, keep_s, pieces, side_s, side_r, product, carried, chain_out, chain_in, own_part,
         rs_out, rs_in), sems = rest[:15], rest[15:]
        line = Line(tok, depth)
        side = Side(side_s, side_r)
        own, other = halves(features)
        if not started:
            loads[0].wait()
            taken[pl.ds(line.own, tok), :] = dy_ref[...].astype(jnp.bfloat16)
        give = side.later(down_given, got_all.at[index])
        keep = pltpu.make_async_copy(down_kept, kept_all.at[index], keep_s)

        def begin():
            for source, target in zip(leave, landed):
                side.start(source, target)
            loads[7].wait()
            loads[8].wait()

        def prepare(row):
            rows = pl.ds(row, 2 * tok)

            def tile(j, _):
                cols = pl.ds(pl.multiple_of(j * EXTRA, EXTRA), EXTRA)
                product[rows, cols] = jnp.dot(
                    taken[rows, own], w2_own[:, cols], preferred_element_type=jnp.float32
                ) + jnp.dot(taken[rows, other], w2_peer[:, cols], preferred_element_type=jnp.float32)
                return 0

            lax.fori_loop(0, width // EXTRA, tile, 0)

        def beside(i):
            @pl.when(i == 1)
            def _():
                for copy in loads[1:7]:
                    copy.wait()

            @pl.when(i == first_tile)
            def _():
                turned[...] = flip(taken[...])

            @pl.when((i >= first_tile) & (i < first_tile + tiles))
            def _():
                cols = pl.ds(pl.multiple_of((i - first_tile) * EXTRA, EXTRA), EXTRA)
                grad_tile(turned, features, before_ref, cols, down_kept, down_given)

            @pl.when(i == first_tile + tiles)
            def _():
                give.start()
                keep.start()

        def finish(row, at, total, extra):
            gate = kept_ref[pl.ds(at, ROWS), :width]
            upper = kept_ref[pl.ds(at, ROWS), width:]
            sig = jax.nn.sigmoid(gate)
            silu = gate * sig
            grad_gate = total * upper * (sig + silu * (1.0 - sig))
            grad_up = total * silu
            wide[pl.ds(row, ROWS), :width] = grad_gate.astype(jnp.bfloat16)
            wide[pl.ds(row, ROWS), width : 2 * width] = grad_up.astype(jnp.bfloat16)
            inner = jnp.sum(grad_gate * gate + grad_up * upper, axis=1, keepdims=True)
            wide[pl.ds(row, ROWS), 2 * width :] = spread(inner)

        def second(row, span):
            value = wide[pl.ds(row, span), : 2 * width]
            pieces[:, own] = transposed_dot(value, w1_own[...])
            pieces[:, other] = transposed_dot(value, w1_peer[...])
            return pieces[...]

        def settle():
            stores[1].start()

        def close():
            total = own_part[...]
            inner = unspread(wide[pl.ds(line.own, tok), 2 * width :])
            for slot in range(3):
                total = total + rs_in[slot, :, :features].astype(jnp.float32)
                inner = inner + unspread(rs_in[slot, :, features:])
            factor = unspread(before_ref[pl.ds(line.own, tok), width:])
            normed = h_ref[...] * factor
            gain_out[...] = jnp.broadcast_to(jnp.sum(total * normed, axis=0, keepdims=True), gain_out.shape)
            out_ref[...] = dy_ref[...] + factor * (total * gain_ref[...] - normed * (inner / D))
            stores[2].start()
            stores[0].start()
            keep.wait()
            side.finish()
            for copy in stores:
                copy.wait()

        run(line, greet, started, taken, begin, prepare, beside, finish, second, settle, close, product, carried, chain_out, chain_in,
            wide, own_part, rs_out, rs_in, *sems)

    low, full = jnp.bfloat16, jnp.float32
    shapes = (
        jax.ShapeDtypeStruct((tok, features), full),
        jax.ShapeDtypeStruct((4 * tok, 2 * width + EXTRA), low),
        jax.ShapeDtypeStruct((8, features), full),
        jax.ShapeDtypeStruct((layers,) + down_own.shape, low),
        jax.ShapeDtypeStruct((layers,) + down_own.shape, low),
    ) + tuple(jax.ShapeDtypeStruct(item.shape, item.dtype) for item in shipped)
    def early(loads, dy_ref, *rest):
        line = Line(tok, depth)
        own = rest[-len(own_scratch) :]
        taken, ag_s, ag_r = own[0], own[15], own[16]
        loads[0].wait()
        here = pl.ds(line.own, tok)
        taken[here, :] = dy_ref[...].astype(jnp.bfloat16)
        for at, peer in enumerate(line.peers):
            remote(taken.at[here], taken.at[here], ag_s.at[at], ag_r.at[at], peer).start()

    own_scratch = [
        pltpu.VMEM((4 * tok, features), low),
        pltpu.VMEM((features, 4 * tok), low),
        pltpu.VMEM(down_own.shape, low),
        pltpu.VMEM(down_own.shape, low),
        pltpu.SemaphoreType.DMA,
        pltpu.VMEM((GROUP_CHUNKS * ROWS, features), full),
        sem(1 + count), sem(1 + count),
    ] + scratch
    return Part(
        kernel,
        (grad, hidden, gain.reshape(1, -1), kept, wide_forward, gu_own, gu_peer, down_own, down_peer, *shipped, *stacks),
        shapes, 9, 3,
        own_scratch,
        {9 + count + at: 3 + at for at in range(len(stacks))}, 60_000_000_000, "ffn_backward", early if started else None,
    )


def to_row(column):
    return jnp.transpose(jnp.broadcast_to(column, (column.shape[0], EXTRA)))[:8]


def to_column(row):
    return jnp.transpose(jnp.broadcast_to(row[:1], (row.shape[1], row.shape[1])))[:, :1]


def turn(values, cosine, sine):
    lane = lax.broadcasted_iota(jnp.int32, values.shape, 1)
    width = values.shape[1]
    back = pltpu.roll(values, width - HEAD // 2, 1)
    forth = pltpu.roll(values, HEAD // 2, 1)
    partner = jnp.where(lax.rem(lane, HEAD) < HEAD // 2, back, forth)
    return values * cosine + partner * sine


def split_pair(block):
    lane = lax.broadcasted_iota(jnp.int32, block.shape, 1)
    zero = jnp.zeros_like(block)
    return jnp.concatenate([jnp.where(lane < HEAD, block, zero), jnp.where(lane < HEAD, zero, block)], axis=0)


def join_pair(turned, tok):
    return jnp.transpose(jnp.concatenate([turned[:HEAD, :tok], turned[HEAD:, tok:]], axis=0))


def twice(kv):
    wide = kv.astype(jnp.float32)
    lane = lax.broadcasted_iota(jnp.int32, wide.shape, 1)
    other = pltpu.roll(wide, HEAD, 1)
    return jnp.where(lane < HEAD, wide, other), jnp.where(lane < HEAD, other, wide)


class Square:
    def __init__(self, tok, depth):
        self.z, self.x = lax.axis_index("z"), lax.axis_index("x")
        self.y, self.c = lax.axis_index("y"), lax.axis_index("c")
        self.tok, self.depth = tok, depth
        self.g = 2 * self.y + self.c
        self.row = 2 * self.z + self.x
        self.own = pl.multiple_of(self.g * tok, tok)
        self.mine = pl.multiple_of(self.z * tok, tok)
        self.peers = (
            {"y": self.y, "c": 1 - self.c},
            {"y": 1 - self.y, "c": self.c},
            {"y": 1 - self.y, "c": 1 - self.c},
        )

    def row_peer(self, step):
        at = lax.rem(self.row + step, 2 * self.depth)
        return {"z": at // 2, "x": lax.rem(at, 2)}

    def greet(self, extra=0):
        barrier = pltpu.get_barrier_semaphore()
        for peer in self.peers:
            pl.semaphore_signal(barrier, 1, device_id=peer, device_id_type=MESH_ID)
        for step in range(1, 2 * self.depth):
            pl.semaphore_signal(barrier, 1, device_id=self.row_peer(step), device_id_type=MESH_ID)
        pl.semaphore_wait(barrier, 3 + 2 * self.depth - 1 + extra)


def start_gather(square, taken, send, recv):
    copies = [
        remote(taken.at[pl.ds(square.own, square.tok)], taken.at[pl.ds(square.own, square.tok)], send.at[at], recv.at[at], peer)
        for at, peer in enumerate(square.peers)
    ]
    for copy in copies:
        copy.start()
    return copies


def line_sum(square, gather, product, own, own_row, outs, ins, row_outs, row_ins, send, recv, row_send, row_recv, between):
    tok, depth = square.tok, square.depth

    def one(order):
        block = lax.rem(2 * square.y + order, depth)
        step = lax.rem(block - square.z + depth, depth)
        slot = jnp.maximum(depth - 1 - step, 0)
        value, column = product(pl.multiple_of(block * tok, tok))

        @pl.when(step == 0)
        def _():
            own[...] = value
            if column is not None:
                own_row[...] = to_row(column)

        copy = remote(outs.at[order], ins.at[slot], send.at[order], recv.at[slot], {"z": block})
        row_copy = None
        if column is not None:
            row_copy = remote(row_outs.at[order], row_ins.at[slot], row_send.at[order], row_recv.at[slot], {"z": block})

        @pl.when(step != 0)
        def _():
            outs[order] = value.astype(jnp.bfloat16)
            copy.start()
            if column is not None:
                row_outs[order] = to_row(column)
                row_copy.start()

        return step, copy, row_copy

    gather[0].wait_recv()
    sent = [one(0), one(1)]
    gather[1].wait_recv()
    gather[2].wait_recv()
    sent += [one(2), one(3)]
    between()
    for slot in range(depth - 1):
        remote(outs.at[0], ins.at[slot], send.at[0], recv.at[slot], {"z": square.z}).wait_recv()
        if row_ins is not None:
            remote(row_outs.at[0], row_ins.at[slot], row_send.at[0], row_recv.at[slot], {"z": square.z}).wait_recv()
    return sent


def send_part(square, array, part, send, recv):
    lanes = pl.ds(pl.multiple_of(part * EXTRA, EXTRA), EXTRA)
    here = array.at[pl.ds(square.mine, square.tok), lanes]
    depth = square.depth
    return [
        remote(here, here, send.at[step - 1, part], recv.at[depth - 1 - step, part], {"z": lax.rem(square.z + step, depth)})
        for step in range(1, depth)
    ]


def send_row(square, rows, send, recv):
    line = rows.at[square.z]
    depth = square.depth
    return [
        remote(line, line, send.at[step - 1], recv.at[depth - 1 - step], {"z": lax.rem(square.z + step, depth)})
        for step in range(1, depth)
    ]


def grid_sum(square, array, rows, second, settle, own, outs, ins, row_ins, arrive, row_arrive, send, recv, row_send, row_recv):
    tok, depth = square.tok, square.depth
    sent = []
    for step in range(depth):
        block = lax.rem(square.z + step, depth)
        if step:
            for part in range(array.shape[1] // EXTRA):
                rows_of = array.at[pl.ds(pl.multiple_of(block * tok, tok), tok), pl.ds(part * EXTRA, EXTRA)]
                remote(rows_of, rows_of, send.at[0], arrive.at[step - 1, part], {"z": square.z}).wait_recv()
            remote(rows.at[block], rows.at[block], send.at[0], row_arrive.at[step - 1], {"z": square.z}).wait_recv()
        value = second(pl.multiple_of(block * tok, tok))
        away = lax.rem(block - square.g + depth, depth)
        slot = jnp.maximum(depth - 1 - away, 0)
        device = {"y": block // 2, "c": lax.rem(block, 2)}
        copy = remote(outs.at[step], ins.at[slot], send.at[step], recv.at[slot], device)
        row_copy = None
        if row_ins is not None:
            row_copy = remote(rows.at[block], row_ins.at[slot], row_send.at[step], row_recv.at[slot], device)

        @pl.when(away == 0)
        def _():
            own[...] = value

        @pl.when(away != 0)
        def _():
            outs[step] = value.astype(jnp.bfloat16)
            copy.start()
            if row_ins is not None:
                row_copy.start()

        sent.append((away, copy, row_copy))
    settle()
    for slot in range(depth - 1):
        remote(outs.at[0], ins.at[slot], send.at[0], recv.at[slot], square.peers[0]).wait_recv()
        if row_ins is not None:
            remote(rows.at[0], row_ins.at[slot], row_send.at[0], row_recv.at[slot], square.peers[0]).wait_recv()
    return sent


def drain(sent):
    for away, copy, row_copy in sent:

        @pl.when(away != 0)
        def _():
            copy.wait_send()
            if row_copy is not None:
                row_copy.wait_send()


def attention_forward(hidden, gain, qkv_own, out_own, qkv_peer, out_peer, shipped, cosine, sine, depth):
    tok, features = hidden.shape
    cols = qkv_own.shape[1]
    fetch = qkv_peer is None
    extra = 2 if fetch else 0
    count = len(shipped)
    sides = extra + 2 * count
    query_cols = GROUP * HEAD
    seq = 2 * depth * tok
    pairs = query_cols // EXTRA
    scale = 1.0 / math.sqrt(HEAD)

    def kernel(loads, stores, greet, hook, h_ref, gain_ref, wqkv_own, wo_own, cos_ref, sin_ref, *rest):
        if not fetch:
            (wqkv_peer, wo_peer), rest = rest[:2], rest[2:]
        leave, rest = rest[:count], rest[count:]
        (out_ref, normed_t, queries, kv, lse, mixed, factors), rest = rest[:7], rest[7:]
        if fetch:
            (wqkv_peer, wo_peer), rest = rest[:2], rest[2:]
        landed, rest = rest[:count], rest[count:]
        (taken, scaled, pieces, own, own_row, z_out, z_in, zr_out, zr_in, values_t, g_own, g_out, g_in,
         ag_s, ag_r, zs_s, zs_r, zr_s, zr_r, kv_s, kv_r, zg_s, zg_r, zgr_s, zgr_r, gs_s, gs_r), rest = rest[:27], rest[27:]
        square = Square(tok, depth)
        side = Side(*rest) if sides else None
        mine, other = halves(features)
        loads[0].wait()
        taken[pl.ds(square.own, tok), :] = h_ref[...].astype(jnp.bfloat16)
        greet()
        gather = start_gather(square, taken, ag_s, ag_r)
        for copy in loads[1:]:
            copy.wait()
        urgent = []
        if fetch:
            urgent = [side.start(wqkv_own, wqkv_peer), side.start(wo_own, wo_peer)]
        held = []
        for source, target in zip(leave, landed):
            most = source.shape[0] // 2
            rest_of = pl.ds(most, source.shape[0] - most)
            side.start(source.at[pl.ds(0, most)], target.at[pl.ds(0, most)])
            held.append(side.later(source.at[rest_of], target.at[rest_of]))
        for copy in urgent[:1]:
            copy.wait_recv()
            stores[7].start()

        def product(row):
            block = taken[pl.ds(row, tok), :].astype(jnp.float32)
            scaled[...] = (block * gain_ref[...]).astype(jnp.bfloat16)
            return (
                jnp.dot(scaled[:, mine], wqkv_own[...], preferred_element_type=jnp.float32)
                + jnp.dot(scaled[:, other], wqkv_peer[...], preferred_element_type=jnp.float32),
                jnp.sum(block * block, axis=1, keepdims=True),
            )

        sent = line_sum(square, gather, product, own, own_row, z_out, z_in, zr_out, zr_in, zs_s, zs_r, zr_s, zr_r, lambda: None)
        total, squares = own[...], own_row[...]
        for slot in range(depth - 1):
            total = total + z_in[slot].astype(jnp.float32)
            squares = squares + zr_in[slot]
        factor_row = lax.rsqrt(squares / D + EPS)
        factors[square.z] = factor_row
        given = send_row(square, factors, zgr_s, zgr_r)
        for copy in given:
            copy.start()
        first = lax.broadcasted_iota(jnp.int32, (tok, EXTRA), 1) < HEAD
        cosine_row, sine_row = cos_ref[...], sin_ref[...]
        turned = turn(
            total * to_column(factor_row),
            jnp.concatenate([cosine_row] * pairs + [jnp.where(first, cosine_row, 1.0)], axis=1),
            jnp.concatenate([sine_row] * pairs + [jnp.where(first, sine_row, 0.0)], axis=1),
        )
        here = pl.ds(pl.multiple_of(square.row * tok, tok), tok)
        kv[here, :] = turned[:, query_cols:].astype(jnp.bfloat16)
        queries[...] = turned[:, :query_cols].astype(jnp.bfloat16)
        stores[2].start()
        spreads = []
        for step in range(1, 2 * depth):
            copy = remote(kv.at[here], kv.at[here], kv_s.at[step - 1], kv_r.at[2 * depth - 1 - step], square.row_peer(step))
            copy.start()
            spreads.append(copy)
        for copy in spreads:
            copy.wait_recv()
        stores[3].start()
        for copy in held:
            copy.start()
        keys, both = twice(kv[...])
        values_t[...] = jnp.transpose(both).astype(jnp.bfloat16)
        keys = keys.astype(jnp.bfloat16)

        def pair(t, _):
            lanes = pl.ds(pl.multiple_of(t * EXTRA, EXTRA), EXTRA)
            scores = transposed_dot(keys, split_pair(queries[:, lanes])) * scale
            key_at = lax.broadcasted_iota(jnp.int32, scores.shape, 0)
            query_at = lax.rem(lax.broadcasted_iota(jnp.int32, scores.shape, 1), tok) + square.row * tok
            scores = jnp.where(key_at <= query_at, scores, -1e30)
            top = jnp.max(scores, axis=0, keepdims=True)
            expo = jnp.exp(scores - top)
            denom = jnp.sum(expo, axis=0, keepdims=True)
            lse[t] = jnp.broadcast_to(top + jnp.log(denom), (8, 2 * tok))
            probs = (expo * (1.0 / denom)).astype(jnp.bfloat16)
            out_t = jnp.dot(values_t[...], probs, preferred_element_type=jnp.float32)
            mixed[pl.ds(square.mine, tok), lanes] = join_pair(out_t, tok).astype(jnp.bfloat16)
            for copy in send_part(square, mixed, t, zg_s, zg_r):
                copy.start()
            return 0

        lax.fori_loop(0, pairs, pair, 0)
        given += [copy for part in range(pairs) for copy in send_part(square, mixed, part, zg_s, zg_r)]

        stores[4].start()
        for copy in urgent[1:]:
            copy.wait_recv()
            stores[8].start()

        def second(row):
            value = mixed[pl.ds(row, tok), :]
            pieces[:, mine] = transposed_dot(value, wo_own[...])
            pieces[:, other] = transposed_dot(value, wo_peer[...])
            return pieces[...]

        def settle():
            stores[5].start()
            stores[6].start()
            for block in range(depth):
                rows = pl.ds(block * tok, tok)
                normed = taken[rows, :].astype(jnp.float32) * to_column(factors[block]) * gain_ref[...]
                normed_t[:, rows] = jnp.transpose(normed).astype(jnp.bfloat16)
            stores[1].start()

        sums = grid_sum(square, mixed, factors, second, settle, g_own, g_out, g_in, None, zg_r, zgr_r, gs_s, gs_r, None, None)
        total = g_own[...]
        for slot in range(depth - 1):
            total = total + g_in[slot].astype(jnp.float32)
        out_ref[...] = h_ref[...] + total
        stores[0].start()
        drain(sent)
        drain(sums)
        for copy in gather + spreads + given:
            copy.wait_send()
        if side:
            side.finish(urgent)
        for copy in stores:
            copy.wait()

    low, full = jnp.bfloat16, jnp.float32
    shapes = (
        jax.ShapeDtypeStruct((tok, features), full),
        jax.ShapeDtypeStruct((features, depth * tok), low),
        jax.ShapeDtypeStruct((tok, query_cols), low),
        jax.ShapeDtypeStruct((seq, 2 * HEAD), low),
        jax.ShapeDtypeStruct((pairs, 8, 2 * tok), full),
        jax.ShapeDtypeStruct((depth * tok, query_cols), low),
        jax.ShapeDtypeStruct((depth, 8, tok), full),
    )
    if fetch:
        shapes += (jax.ShapeDtypeStruct(qkv_own.shape, low), jax.ShapeDtypeStruct(out_own.shape, low))
    shapes += tuple(jax.ShapeDtypeStruct(item.shape, item.dtype) for item in shipped)
    peers = () if fetch else (qkv_peer, out_peer)
    operands = (hidden, gain.reshape(1, -1), qkv_own, out_own, cosine, sine, *peers, *shipped)
    return Part(
        kernel, operands, shapes, 6 + len(peers), 7 + extra,
        [
            pltpu.VMEM((depth * tok, features), low),
            pltpu.VMEM((tok, features), low),
            pltpu.VMEM((tok, features), full),
            pltpu.VMEM((tok, cols), full),
            pltpu.VMEM((8, tok), full),
            pltpu.VMEM((depth, tok, cols), low),
            pltpu.VMEM((depth - 1, tok, cols), low),
            pltpu.VMEM((depth, 8, tok), full),
            pltpu.VMEM((depth - 1, 8, tok), full),
            pltpu.VMEM((2 * HEAD, seq), low),
            pltpu.VMEM((tok, features), full),
            pltpu.VMEM((depth, tok, features), low),
            pltpu.VMEM((depth - 1, tok, features), low),
            sem(3), sem(3), sem(depth), sem(depth - 1), sem(depth), sem(depth - 1),
            sem(2 * depth - 1), sem(2 * depth - 1), sem(depth - 1, pairs), sem(depth - 1, pairs), sem(depth - 1), sem(depth - 1),
            sem(depth), sem(depth - 1),
        ] + ([sem(sides), sem(sides)] if sides else []),
        {}, 50_000_000_000, "attention_forward",
    )


def attention_backward(
    grad, hidden, gain, qkv_own, qkv_peer, out_own, out_peer, cosine, sine, queries, kv, lse, factors, mixed, normed_a, normed_f,
    grad_gu, stacks, index, layers, depth,
):
    tok, features = hidden.shape
    cols = qkv_own.shape[1]
    wide = grad_gu.shape[1] - EXTRA
    query_cols = GROUP * HEAD
    seq = 2 * depth * tok
    pairs = query_cols // EXTRA
    scale = 1.0 / math.sqrt(HEAD)

    def kernel(loads, stores, greet, hook, dy_ref, h_ref, gain_ref, wqkv_own, wqkv_peer, wo_own, wo_peer, cos_ref, sin_ref, q_ref, kv_ref, lse_ref,
               factor_ref, mixed_ref, normed_a_ref, normed_f_ref, gu_ref, *rest_refs):
        (out_ref, gain_out, qkv_given, gu_kept_all, gu_got_all, out_kept_all, out_got_all, qkv_kept_all,
               taken, spun, turned, pieces, gu_kept, gu_given, out_kept, out_given, qkv_kept, keep_s,
               own, heads, z_out, z_in, keys_t, dk, dv, kv_out, kv_in, dq, inner_rows, g_own, g_out, g_in, g_rows,
               ag_s, ag_r, zs_s, zs_r, kv_s, kv_r, zg_s, zg_r, zgr_s, zgr_r, gs_s, gs_r, gr_s, gr_r, side_s, side_r) = rest_refs[len(stacks):]
        square = Square(tok, depth)
        side = Side(side_s, side_r)
        mine, other = halves(features)
        loads[0].wait()
        taken[pl.ds(square.own, tok), :] = dy_ref[...].astype(jnp.bfloat16)
        greet()
        gather = start_gather(square, taken, ag_s, ag_r)
        for copy in loads[1:]:
            copy.wait()

        def gu_tiles(start, stop):
            def tile(j, _):
                grad_tile(normed_f_ref, features, gu_ref, pl.ds(pl.multiple_of(j * EXTRA, EXTRA), EXTRA), gu_kept, gu_given)
                return 0

            lax.fori_loop(start, stop, tile, 0)

        gu_got = gu_got_all.at[index]
        keeps = [
            pltpu.make_async_copy(gu_kept, gu_kept_all.at[index], keep_s.at[0]),
            pltpu.make_async_copy(out_kept, out_kept_all.at[index], keep_s.at[1]),
            pltpu.make_async_copy(qkv_kept, qkv_kept_all.at[index], keep_s.at[2]),
        ]
        every = wide // EXTRA
        middle, late = every // 2, every * 3 // 4
        gu_tiles(0, middle)
        front, rest = pl.ds(0, middle * EXTRA), pl.ds(late * EXTRA, wide - late * EXTRA)
        inner_part = pl.ds(middle * EXTRA, (late - middle) * EXTRA)
        side.start(gu_given.at[:, front], gu_got.at[:, front])

        def between():
            turned[...] = flip(taken[...])
            for t in range(query_cols // EXTRA):
                grad_tile(turned, features, mixed_ref, pl.ds(t * EXTRA, EXTRA), out_kept, out_given)
            side.start(out_given, out_got_all.at[index])
            gu_tiles(middle, late)
            side.start(gu_given.at[:, inner_part], gu_got.at[:, inner_part])
            gu_tiles(late, every)
            keeps[0].start()
            keeps[1].start()

        def product(row):
            rows = pl.ds(row, tok)
            value = jnp.dot(taken[rows, mine], wo_own[...], preferred_element_type=jnp.float32) + jnp.dot(
                taken[rows, other], wo_peer[...], preferred_element_type=jnp.float32
            )
            return value, None

        sent = line_sum(square, gather, product, own, None, z_out, z_in, None, None, zs_s, zs_r, None, None, between)
        total = own[...]
        for slot in range(depth - 1):
            total = total + z_in[slot].astype(jnp.float32)
        heads[...] = total.astype(jnp.bfloat16)
        keys, both = twice(kv_ref[...])
        keys_t[...] = jnp.transpose(keys).astype(jnp.bfloat16)
        keys = keys.astype(jnp.bfloat16)
        both = both.astype(jnp.bfloat16)
        dk[...] = jnp.zeros_like(dk)
        dv[...] = jnp.zeros_like(dv)

        def pair(t, _):
            lanes = pl.ds(pl.multiple_of(t * EXTRA, EXTRA), EXTRA)
            query = split_pair(q_ref[:, lanes])
            head = split_pair(heads[:, lanes])
            scores = transposed_dot(keys, query) * scale
            key_at = lax.broadcasted_iota(jnp.int32, scores.shape, 0)
            query_at = lax.rem(lax.broadcasted_iota(jnp.int32, scores.shape, 1), tok) + square.row * tok
            probs = jnp.exp(jnp.where(key_at <= query_at, scores, -1e30) - lse_ref[t, :1, :])
            grad_probs = transposed_dot(both, head)
            delta = jnp.sum(probs * grad_probs, axis=0, keepdims=True)
            grad_scores = (probs * (grad_probs - delta)).astype(jnp.bfloat16)
            dk[...] += jnp.dot(grad_scores, query, preferred_element_type=jnp.float32)
            dv[...] += jnp.dot(probs.astype(jnp.bfloat16), head, preferred_element_type=jnp.float32)
            back = jnp.dot(keys_t[...], grad_scores, preferred_element_type=jnp.float32)
            value = join_pair(back, tok) * scale
            dq[...] += jnp.broadcast_to(
                jnp.sum(value * q_ref[:, lanes].astype(jnp.float32), axis=1, keepdims=True), dq.shape
            )
            spun[pl.ds(square.mine, tok), lanes] = turn(value, cos_ref[...], -sin_ref[...]).astype(jnp.bfloat16)
            for copy in send_part(square, spun, t, zg_s, zg_r):
                copy.start()
            return 0

        dq[...] = jnp.zeros_like(dq)
        lax.fori_loop(0, pairs, pair, 0)
        lane = lax.broadcasted_iota(jnp.int32, (seq, EXTRA), 1)
        left = dk[...]
        right = dv[...]
        both_kv = jnp.where(
            lane < HEAD, (left + pltpu.roll(left, HEAD, 1)) * scale, right + pltpu.roll(right, HEAD, 1)
        )
        dk[...] = both_kv
        kv_out[...] = both_kv.astype(jnp.bfloat16)
        here = pl.ds(pl.multiple_of(square.row * tok, tok), tok)
        spreads = []
        for step in range(1, 2 * depth):
            at = lax.rem(square.row + step, 2 * depth)
            copy = remote(
                kv_out.at[pl.ds(pl.multiple_of(at * tok, tok), tok)],
                kv_in.at[2 * depth - 1 - step],
                kv_s.at[step - 1],
                kv_r.at[2 * depth - 1 - step],
                square.row_peer(step),
            )
            copy.start()
            spreads.append(copy)
        total_kv = dk[here, :]
        for copy in spreads:
            copy.wait_recv()
        side.start(gu_given.at[:, rest], gu_got.at[:, rest])
        for slot in range(2 * depth - 1):
            total_kv = total_kv + kv_in[slot].astype(jnp.float32)
        first = lax.broadcasted_iota(jnp.int32, (tok, EXTRA), 1) < HEAD
        spun[pl.ds(square.mine, tok), query_cols:] = turn(
            total_kv, jnp.where(first, cos_ref[...], 1.0), jnp.where(first, -sin_ref[...], 0.0)
        ).astype(jnp.bfloat16)
        inner = dq[:, :1] + jnp.sum(total_kv * kv_ref[here, :].astype(jnp.float32), axis=1, keepdims=True)
        inner_rows[square.z] = to_row(inner)
        given = send_part(square, spun, pairs, zg_s, zg_r) + send_row(square, inner_rows, zgr_s, zgr_r)
        for copy in given:
            copy.start()
        given += [copy for part in range(pairs) for copy in send_part(square, spun, part, zg_s, zg_r)]

        def second(row):
            value = spun[pl.ds(row, tok), :]
            pieces[:, mine] = transposed_dot(value, wqkv_own[...])
            pieces[:, other] = transposed_dot(value, wqkv_peer[...])
            return pieces[...]

        def settle():
            for t in range(cols // EXTRA):
                grad_tile(normed_a_ref, features, spun, pl.ds(t * EXTRA, EXTRA), qkv_kept, qkv_given)
            keeps[2].start()
            stores[2].start()
            hook()

        sums = grid_sum(
            square, spun, inner_rows, second, settle, g_own, g_out, g_in, g_rows, zg_r, zgr_r, gs_s, gs_r, gr_s, gr_r
        )
        total = g_own[...]
        inner = inner_rows[square.g]
        for slot in range(depth - 1):
            total = total + g_in[slot].astype(jnp.float32)
            inner = inner + g_rows[slot]
        factor = to_column(factor_ref[square.g])
        normed = h_ref[...] * factor
        gain_out[...] = jnp.broadcast_to(jnp.sum(total * normed, axis=0, keepdims=True), gain_out.shape)
        out_ref[...] = dy_ref[...] + factor * (total * gain_ref[...] - normed * (to_column(inner) / D))
        stores[0].start()
        stores[1].start()
        drain(sent)
        drain(sums)
        for copy in gather + spreads + given:
            copy.wait_send()
        for copy in keeps + stores:
            copy.wait()
        side.finish()

    low, full = jnp.bfloat16, jnp.float32
    shapes = (
        jax.ShapeDtypeStruct((tok, features), full),
        jax.ShapeDtypeStruct((8, features), full),
        jax.ShapeDtypeStruct(qkv_own.shape, low),
        jax.ShapeDtypeStruct((layers, features // 2, wide), low),
        jax.ShapeDtypeStruct((layers, features // 2, wide), low),
        jax.ShapeDtypeStruct((layers,) + out_own.shape, low),
        jax.ShapeDtypeStruct((layers,) + out_own.shape, low),
        jax.ShapeDtypeStruct((layers,) + qkv_own.shape, low),
    )
    operands = (
        grad, hidden, gain.reshape(1, -1), qkv_own, qkv_peer, out_own, out_peer, cosine, sine, queries, kv, lse, factors,
        mixed, normed_a, normed_f, grad_gu, *stacks,
    )
    return Part(
        kernel, operands, shapes, 17, 3,
        [
            pltpu.VMEM((depth * tok, features), low),
            pltpu.VMEM((depth * tok, cols), low),
            pltpu.VMEM((features, depth * tok), low),
            pltpu.VMEM((tok, features), full),
            pltpu.VMEM((features // 2, wide), low),
            pltpu.VMEM((features // 2, wide), low),
            pltpu.VMEM(out_own.shape, low),
            pltpu.VMEM(out_own.shape, low),
            pltpu.VMEM(qkv_own.shape, low),
            sem(3),
            pltpu.VMEM((tok, query_cols), full),
            pltpu.VMEM((tok, query_cols), low),
            pltpu.VMEM((depth, tok, query_cols), low),
            pltpu.VMEM((depth - 1, tok, query_cols), low),
            pltpu.VMEM((2 * HEAD, seq), low),
            pltpu.VMEM((seq, 2 * HEAD), full),
            pltpu.VMEM((seq, 2 * HEAD), full),
            pltpu.VMEM((seq, 2 * HEAD), low),
            pltpu.VMEM((2 * depth - 1, tok, 2 * HEAD), low),
            pltpu.VMEM((tok, EXTRA), full),
            pltpu.VMEM((depth, 8, tok), full),
            pltpu.VMEM((tok, features), full),
            pltpu.VMEM((depth, tok, features), low),
            pltpu.VMEM((depth - 1, tok, features), low),
            pltpu.VMEM((depth - 1, 8, tok), full),
            sem(3), sem(3), sem(depth), sem(depth - 1),
            sem(2 * depth - 1), sem(2 * depth - 1), sem(depth - 1, pairs + 1), sem(depth - 1, pairs + 1), sem(depth - 1),
            sem(depth - 1), sem(depth), sem(depth - 1), sem(depth), sem(depth - 1), sem(4), sem(4),
        ],
        {17 + at: 3 + at for at in range(len(stacks))}, 50_000_000_000, "attention_backward",
    )


def greet_last(tok, depth):
    square = Square(tok, depth)
    barrier = pltpu.get_barrier_semaphore()
    for slot in range(2 * depth):
        here = (square.z == square.g) & (slot == square.x * depth + square.g)

        @pl.when(jnp.logical_not(here))
        def _():
            source = {"z": square.g, "x": slot // depth, "y": (slot % depth) // 2, "c": slot % 2}
            pl.semaphore_signal(barrier, 1, device_id=source, device_id_type=MESH_ID)

    square.greet(2 * depth - jnp.where(square.z == square.g, 1, 0))


def finish(grad, gains, qkv_given, depth):
    tok, features = grad.shape
    count = len(gains)
    members = 2 * depth

    def kernel(loads, stores, greet, hook, grad_ref, *rest):
        gain_refs, rest = rest[:count], rest[count:]
        (given, out_ref, gain_out, got, packed, parts, sent, home, part_s, part_r, move_s, move_r, side_s, side_r) = rest
        z, x = lax.axis_index("z"), lax.axis_index("x")
        y, c = lax.axis_index("y"), lax.axis_index("c")
        g = 2 * y + c
        self_at = x * depth + g

        def target(at):
            return {"z": at // 2, "x": at % 2, "y": z // 2, "c": lax.rem(z, 2)}

        def is_source_me(slot):
            return (z == g) & (slot == self_at)

        def is_target_me(at):
            return (z == g) & (at == 2 * z + x)

        for copy in loads:
            copy.wait()
        for at, ref in enumerate(gain_refs):
            packed[at : at + 1, :] = ref[:1, :]
        sent[...] = grad_ref[...].astype(jnp.bfloat16)
        side = Side(side_s, side_r)
        side.later(given, got)
        move = remote(sent, home, move_s, move_r, {"z": g, "y": z // 2, "c": lax.rem(z, 2)})

        @pl.when(z != g)
        def _():
            move.start()

        def part(at):
            return remote(packed, parts.at[self_at], part_s.at[at], part_r.at[self_at], target(at))

        for at in range(members):

            @pl.when(jnp.logical_not(is_target_me(at)))
            def _():
                part(at).start()

        @pl.when(z == g)
        def _():
            parts[self_at] = packed[...]

        for slot in range(members):

            @pl.when(jnp.logical_not(is_source_me(slot)))
            def _():
                remote(packed, parts.at[slot], part_s.at[0], part_r.at[slot], target(0)).wait_recv()

        total = parts[0]
        for slot in range(1, members):
            total = total + parts[slot]
        gain_out[...] = total
        stores[1].start()

        @pl.when(z == g)
        def _():
            out_ref[...] = grad_ref[...]

        @pl.when(z != g)
        def _():
            move.wait_recv()
            out_ref[...] = home[...].astype(jnp.float32)
            move.wait_send()

        stores[0].start()
        for at in range(members):

            @pl.when(jnp.logical_not(is_target_me(at)))
            def _():
                part(at).wait_send()

        side.finish()
        for copy in stores:
            copy.wait()

    low, full = jnp.bfloat16, jnp.float32
    shapes = (
        jax.ShapeDtypeStruct((tok, features), full),
        jax.ShapeDtypeStruct((count, features), full),
        jax.ShapeDtypeStruct(qkv_given.shape, low),
    )
    def early(loads, *refs):
        given, got, side_s, side_r = refs[1 + count], refs[4 + count], refs[-2], refs[-1]
        Side(side_s, side_r).start(given, got)

    return Part(
        kernel, (grad, *gains, qkv_given), shapes, 1 + count, 2,
        [
            pltpu.VMEM((count, features), full),
            pltpu.VMEM((members, count, features), full),
            pltpu.VMEM((tok, features), low),
            pltpu.VMEM((tok, features), low),
            sem(members), sem(members),
            pltpu.SemaphoreType.DMA, pltpu.SemaphoreType.DMA,
            sem(1), sem(1),
        ],
        {}, 5_000_000_000, "finish", early,
    )


def combine(rests, downs, got_qkv):
    gu_kept, gu_got, out_kept, out_got, qkv_kept = rests
    layers, rows, wide = gu_kept.shape
    half = wide // 2
    step = rows // 2

    def kernel(gu_k, gu_g, out_k, out_g, down_k, down_g, qkv_k, *rest):
        got, (qkv_o, out_o, gu_o, down_o) = rest[:layers], rest[layers:]
        total = gu_k[0].astype(jnp.float32) + gu_g[0].astype(jnp.float32)
        gu_o[0, :, 0, :] = total[:, :half]
        gu_o[0, :, 1, :] = total[:, half:]
        out_o[...] = out_k[...].astype(jnp.float32) + out_g[...].astype(jnp.float32)
        down_o[...] = down_k[...].astype(jnp.float32) + down_g[...].astype(jnp.float32)
        for index in range(layers):

            @pl.when(pl.program_id(0) == index)
            def _():
                qkv_o[0, :, 0, :] = qkv_k[0].astype(jnp.float32) + got[index][...].astype(jnp.float32)

    def spec(item):
        return pl.BlockSpec((1, step, item.shape[2]), lambda layer, at: (layer, at, 0))

    operands = (gu_kept, gu_got, out_kept, out_got, *downs, qkv_kept)
    cols = qkv_kept.shape[2]
    full = jnp.float32
    return pl.pallas_call(
        kernel,
        grid=(layers, rows // step),
        in_specs=[spec(item) for item in operands]
        + [pl.BlockSpec((step, cols), lambda layer, at: (at, 0)) for _ in range(layers)],
        out_specs=[
            pl.BlockSpec((1, step, 1, cols), lambda layer, at: (layer, at, 0, 0)),
            spec(out_kept),
            pl.BlockSpec((1, step, 2, half), lambda layer, at: (layer, at, 0, 0)),
            spec(downs[0]),
        ],
        out_shape=[
            jax.ShapeDtypeStruct((layers, rows, 1, cols), full),
            jax.ShapeDtypeStruct(out_kept.shape, full),
            jax.ShapeDtypeStruct((layers, rows, 2, half), full),
            jax.ShapeDtypeStruct(downs[0].shape, full),
        ],
        compiler_params=pltpu.CompilerParams(vmem_limit_bytes=60 << 20),
        name="combine",
    )(*operands, *got_qkv)


def stationary(stream, grad_out, wqkv, wo, wgu, wd, gain_attn, gain_ffn):
    tok = stream.shape[0]
    layers = wqkv.shape[0]
    count_rows = wqkv.shape[1]
    depth = lax.axis_size("z")
    head = HEAD
    row = lax.axis_index("z") * 2 + lax.axis_index("x")
    query_pos = row * tok + jnp.arange(tok, dtype=jnp.int32)
    lane = jnp.arange(EXTRA, dtype=jnp.int32)
    half = head // 2
    freq = THETA ** (-((lane % half).astype(jnp.float32) * 2.0 / head))
    angle = query_pos.astype(jnp.float32)[:, None] * freq[None, :]
    cosine = jnp.cos(angle)
    sine = jnp.where((lane % head < half)[None, :], -1.0, 1.0) * jnp.sin(angle)
    current = swap_grid(stream, depth)
    grad_now = swap_grid(grad_out, depth)
    gains = swap_grid(jnp.concatenate([gain_attn, gain_ffn]), depth)
    gain_a, gain_f = gains[:layers], gains[layers:]
    greet = lambda: Square(tok, depth).greet()
    own_qkv = [wqkv[index].reshape(count_rows, -1) for index in range(layers)]
    own_out = [wo[index] for index in range(layers)]
    own_gu = [wgu[index].reshape(count_rows, -1) for index in range(layers)]
    own_down = [wd[index] for index in range(layers)]
    peer_qkv, peer_out, peer_gu, peer_down = ([None] * layers for _ in range(4))
    saved = []
    for index in range(layers):
        before = current
        first = index == 0
        final = index == layers - 1
        follow = index + 1
        shipped = [] if final else [own_qkv[follow], own_out[follow], own_gu[follow]]
        attend = attention_forward(
            before, gain_a[index], own_qkv[index], own_out[index], peer_qkv[index], peer_out[index],
            own_gu[:1] if first else [], cosine, sine, depth
        )
        peer = attend.link(len(attend.shapes) - 1) if first else peer_gu[index]
        feed = ffn_forward(attend.link(0), gain_f[index], own_gu[index], peer, own_down[index], shipped, depth)
        parts = [attend, feed]
        if final:
            feed.private = (2, 3, 4)
            parts.append(
                ffn_backward(
                    grad_now, attend.link(0), gain_f[index], feed.link(2, 1), feed.link(3, 1), own_gu[index], peer,
                    own_down[index], feed.link(4, 1), [], [], index, layers, depth, True
                )
            )
        made, fed, *back = launch(parts, greet, 2 * index)
        hidden_in, normed_a, queries, kv, lse, mixed, factors = made[:7]
        if first:
            peer_qkv[0], peer_out[0], peer_gu[0] = made[7:]
        current, normed_f, kept, active, peer_down[index] = fed[:5]
        if shipped:
            peer_qkv[follow], peer_out[follow], peer_gu[follow] = fed[5:]
        saved.append((before, normed_a, queries, kv, lse, mixed, factors, hidden_in, normed_f, kept, active))
    list_ga, list_gf, got_qkv, rest_stack = ([], [], [], [])
    grad_hidden, grad_gu, gain_f_grad, *down_stack = back[0]
    for index in reversed(range(layers)):
        list_gf.append(gain_f_grad)
        before, normed_a, queries, kv, lse, mixed, factors, _, normed_f, _, _ = saved[index]
        attend = attention_backward(
            grad_hidden, before, gain_a[index], own_qkv[index], peer_qkv[index], own_out[index], peer_out[index],
            cosine, sine, queries, kv, lse, factors, mixed, normed_a, normed_f, grad_gu, rest_stack, index, layers, depth
        )
        attend.private = (2,)
        if index:
            _, _, _, _, _, _, _, hidden_in, _, kept, active = saved[index - 1]
            feed = ffn_backward(
                attend.link(0), hidden_in, gain_f[index - 1], kept, active, own_gu[index - 1], peer_gu[index - 1],
                own_down[index - 1], peer_down[index - 1], [attend.link(2)], down_stack, index - 1, layers, depth, False
            )
            made, (grad_hidden, grad_gu, gain_f_grad, *down_stack, landed) = launch([attend, feed], greet, 2 * index + 1)
            got_qkv.append(landed)
        else:
            tail = finish(attend.link(0), [attend.link(1)] + list_ga[::-1] + list_gf[::-1], attend.link(2), depth)
            made, (grad_in, gains, landed) = launch([attend, tail], lambda: greet_last(tok, depth), 1)
            got_qkv.append(landed)
        list_ga.append(made[1])
        rest_stack = made[3:]
    grads = combine(rest_stack, down_stack, got_qkv[::-1])
    return (swap_grid(current, depth), grad_in, *grads, gains[:layers], gains[layers:])


def solution(mesh):
    rows, cols = ("row", "col")
    body = local
    if (mesh.shape["row"], mesh.shape["col"]) == (8, 4):
        mesh = share_out(mesh)
        rows, cols = (("z", "x"), ("y", "c"))
        body = stationary
    in_specs = (
        P(rows, cols),
        P(rows, cols),
        P(None, rows, cols, None),
        P(None, rows, cols),
        P(None, rows, None, cols),
        P(None, rows, cols),
        P(None, cols),
        P(None, cols),
    )
    out_specs = (
        P(rows, cols),
        P(rows, cols),
        P(None, rows, cols, None),
        P(None, rows, cols),
        P(None, rows, None, cols),
        P(None, rows, cols),
        P(None, cols),
        P(None, cols),
    )
    return jax.shard_map(body, mesh=mesh, in_specs=in_specs, out_specs=out_specs, check_vma=False)
```

```python
import math

import jax
import jax.numpy as jnp
from jax import lax
from jax.experimental import pallas as pl
from jax.experimental.pallas import tpu as pltpu
from jax.sharding import Mesh
from jax.sharding import PartitionSpec as P

D = 2048
HEAD = 64
GROUP = 8


EPS = 1e-05
THETA = 10000.0


def rope_turn(tensor, cosine, sine):
    half = tensor.shape[-1] // 2
    first = tensor[..., :half]
    second = tensor[..., half:]
    return jnp.concatenate(
        [first * cosine - second * sine, second * cosine + first * sine], axis=-1
    )


def feature_sum(values):
    return lax.psum(values, "col")


def gather_features(rows_in):
    return lax.all_gather(rows_in, "col", axis=1, tiled=True)


def sum_features(partials):
    return lax.psum_scatter(
        partials.astype(jnp.bfloat16), "col", scatter_dimension=1, tiled=True
    ).astype(jnp.float32)


def add_rows(left, piece):
    return jnp.dot(left, piece, preferred_element_type=jnp.float32)


def project_in(left, shard):
    return add_rows(left, lax.all_gather(shard, "row", axis=0, tiled=True))


def columns_of(left, piece):
    return jnp.einsum("tj,dj->td", left, piece, preferred_element_type=jnp.float32)


def project_out(left, shard):
    return columns_of(left, lax.all_gather(shard, "row", axis=0, tiled=True))


def weight_grad(left, right):
    return lax.psum_scatter(
        lax.dot_general(
            left, right, (((0,), (0,)), ((), ())), preferred_element_type=jnp.float32
        ).astype(jnp.bfloat16),
        "row",
        scatter_dimension=0,
        tiled=True,
    ).astype(jnp.float32)


def norm_forward(values, gain):
    total = feature_sum(jnp.sum(values * values, axis=1))
    factor = lax.rsqrt(total / D + EPS)
    normed = values * factor[:, None]
    return (normed, factor, (normed * gain).astype(jnp.bfloat16))


def norm_backward(grad_normed, normed, factor, gain):
    scaled = grad_normed * gain
    inner = feature_sum(jnp.sum(scaled * normed, axis=1))
    grad_in = factor[:, None] * (scaled - normed * (inner / D)[:, None])
    return (grad_in, jnp.sum(grad_normed * normed, axis=0))


def masked_scores(queries, keys, query_pos, key_pos):
    scores = jnp.einsum("qgd,kd->gqk", queries, keys, preferred_element_type=jnp.float32) * (
        1.0 / math.sqrt(queries.shape[-1])
    )
    return jnp.where(key_pos[None, None, :] <= query_pos[None, :, None], scores, -1e30)


def local(stream, grad_out, wqkv, wo, wgu, wd, gain_attn, gain_ffn):
    tok = stream.shape[0]
    layers = wqkv.shape[0]
    count_rows = wqkv.shape[1]
    head = HEAD
    query_cols = GROUP * head
    seq_len = lax.axis_size("row") * tok
    query_pos = lax.axis_index("row") * tok + jnp.arange(tok, dtype=jnp.int32)
    key_pos = jnp.arange(seq_len, dtype=jnp.int32)
    freq = THETA ** (-(jnp.arange(head // 2, dtype=jnp.float32) * 2.0 / head))
    angle = query_pos.astype(jnp.float32)[:, None] * freq[None, :]
    cosine = jnp.cos(angle)
    sine = jnp.sin(angle)
    saved = []
    current = stream
    for index in range(layers):
        weight_qkv = wqkv[index].reshape(count_rows, -1)
        weight_out = wo[index]
        weight_gu = wgu[index].reshape(count_rows, -1)
        weight_down = wd[index]
        wholes = (None, None, None, None)
        normed_a, factor_a, xnormed = norm_forward(current, gain_attn[index])
        xfull = gather_features(xnormed)
        qkv = project_in(xfull, weight_qkv)
        queries = rope_turn(
            qkv[:, :query_cols].reshape(tok, GROUP, head), cosine[:, None, :], sine[:, None, :]
        ).astype(jnp.bfloat16)
        keys = rope_turn(qkv[:, query_cols : query_cols + head], cosine, sine).astype(jnp.bfloat16)
        values = qkv[:, query_cols + head :].astype(jnp.bfloat16)
        seqkv = lax.all_gather(jnp.concatenate([keys, values], axis=1), "row", axis=0, tiled=True)
        seq_keys = seqkv[:, :head]
        seq_values = seqkv[:, head:]
        scores = masked_scores(queries, seq_keys, query_pos, key_pos)
        top = jnp.max(scores, axis=2, keepdims=True)
        expo = jnp.exp(scores - top)
        denom = jnp.sum(expo, axis=2, keepdims=True)
        probs = (expo / denom).astype(jnp.bfloat16)
        log_total = top + jnp.log(denom)
        mixed = (
            jnp.einsum("gqk,kd->qgd", probs, seq_values, preferred_element_type=jnp.float32)
            .reshape(tok, query_cols)
            .astype(jnp.bfloat16)
        )
        hidden_in = current + sum_features(project_out(mixed, weight_out))
        normed_f, factor_f, hnormed = norm_forward(hidden_in, gain_ffn[index])
        hfull = gather_features(hnormed)
        gate_up = project_in(hfull, weight_gu)
        hidden_cols = gate_up.shape[1] // 2
        gate = gate_up[:, :hidden_cols]
        upper = gate_up[:, hidden_cols:]
        active = (jax.nn.silu(gate) * upper).astype(jnp.bfloat16)
        current = hidden_in + sum_features(project_out(active, weight_down))
        saved.append(
            (
                weight_qkv,
                weight_out,
                weight_gu,
                weight_down,
                wholes,
                normed_a,
                factor_a,
                xfull,
                queries,
                seq_keys,
                seq_values,
                log_total,
                mixed,
                normed_f,
                factor_f,
                hfull,
                gate,
                upper,
                active,
            )
        )
    grad_now = grad_out
    list_qkv, list_out, list_gu, list_down, list_ga, list_gf = ([], [], [], [], [], [])
    for index in reversed(range(layers)):
        (
            weight_qkv,
            weight_out,
            weight_gu,
            weight_down,
            wholes,
            normed_a,
            factor_a,
            xfull,
            queries,
            seq_keys,
            seq_values,
            log_total,
            mixed,
            normed_f,
            factor_f,
            hfull,
            gate,
            upper,
            active,
        ) = saved[index]
        grad_full = gather_features(grad_now.astype(jnp.bfloat16))
        grad_active = project_in(grad_full, weight_down)
        list_down.append(weight_grad(grad_full, active))
        sig = jax.nn.sigmoid(gate)
        grad_gate = grad_active * upper * sig * (1.0 + gate * (1.0 - sig))
        grad_up = grad_active * gate * sig
        grad_gu = jnp.concatenate([grad_gate, grad_up], axis=1).astype(jnp.bfloat16)
        grad_hn = sum_features(project_out(grad_gu, weight_gu))
        list_gu.append(weight_grad(hfull, grad_gu).reshape(count_rows, 2, -1))
        grad_mid, gain_f_grad = norm_backward(grad_hn, normed_f, factor_f, gain_ffn[index])
        list_gf.append(gain_f_grad)
        grad_hidden = grad_now + grad_mid
        hidden_full = gather_features(grad_hidden.astype(jnp.bfloat16))
        grad_mixed = project_in(hidden_full, weight_out).astype(jnp.bfloat16)
        list_out.append(weight_grad(hidden_full, mixed))
        grad_heads = grad_mixed.reshape(tok, GROUP, head)
        scores = masked_scores(queries, seq_keys, query_pos, key_pos)
        probs_full = jnp.exp(scores - log_total)
        probs = probs_full.astype(jnp.bfloat16)
        grad_probs = jnp.einsum(
            "qgd,kd->gqk", grad_heads, seq_values, preferred_element_type=jnp.float32
        )
        delta = jnp.sum(probs_full * grad_probs, axis=2, keepdims=True)
        grad_scores = (probs_full * (grad_probs - delta)).astype(jnp.bfloat16)
        inverse = 1.0 / math.sqrt(head)
        grad_queries = (
            jnp.einsum("gqk,kd->qgd", grad_scores, seq_keys, preferred_element_type=jnp.float32)
            * inverse
        )
        grad_keys = (
            jnp.einsum("gqk,qgd->kd", grad_scores, queries, preferred_element_type=jnp.float32)
            * inverse
        )
        grad_values = jnp.einsum(
            "gqk,qgd->kd", probs, grad_heads, preferred_element_type=jnp.float32
        )
        grad_kv = lax.psum_scatter(
            jnp.concatenate([grad_keys, grad_values], axis=1).astype(jnp.bfloat16),
            "row",
            scatter_dimension=0,
            tiled=True,
        ).astype(jnp.float32)
        grad_k = rope_turn(grad_kv[:, :head], cosine, -sine)
        grad_v = grad_kv[:, head:]
        grad_q = rope_turn(grad_queries, cosine[:, None, :], -sine[:, None, :]).reshape(
            tok, query_cols
        )
        grad_qkv = jnp.concatenate([grad_q, grad_k, grad_v], axis=1).astype(jnp.bfloat16)
        grad_xn = sum_features(project_out(grad_qkv, weight_qkv))
        list_qkv.append(weight_grad(xfull, grad_qkv).reshape(count_rows, 1, -1))
        grad_in, gain_a_grad = norm_backward(grad_xn, normed_a, factor_a, gain_attn[index])
        list_ga.append(gain_a_grad)
        grad_now = grad_hidden + grad_in
    gains_a, gains_f = lax.psum((jnp.stack(list_ga[::-1]), jnp.stack(list_gf[::-1])), "row")
    return (
        current,
        grad_now,
        jnp.stack(list_qkv[::-1]),
        jnp.stack(list_out[::-1]),
        jnp.stack(list_gu[::-1]),
        jnp.stack(list_down[::-1]),
        gains_a,
        gains_f,
    )


def share_out(mesh):
    rows, cols = mesh.shape["row"], mesh.shape["col"]
    return Mesh(
        mesh.devices.reshape(rows // 2, 2, cols // 2, 2), ("z", "x", "y", "c")
    )


def swap_grid(values, depth):
    pairs = [(z * depth + g, g * depth + z) for z in range(depth) for g in range(depth)]
    return lax.ppermute(values, ("z", "y", "c"), pairs)


MESH_ID = pl.DeviceIdType.MESH
ROWS = 16
SKEW = 3
OFFSET = 18
GROUP_CHUNKS = 4
EXTRA = 128


def spread(column):
    high = column.astype(jnp.bfloat16)
    low = (column - high.astype(jnp.float32)).astype(jnp.bfloat16)
    lane = lax.broadcasted_iota(jnp.int32, (column.shape[0], EXTRA), 1)
    wide = jnp.where(lane == 0, high.astype(jnp.float32), jnp.where(lane == 1, low.astype(jnp.float32), 0.0))
    return wide.astype(jnp.bfloat16)


def unspread(block):
    return jnp.sum(block.astype(jnp.float32), axis=1, keepdims=True)


def transposed_dot(left, right):
    return lax.dot_general(left, right, (((1,), (1,)), ((), ())), preferred_element_type=jnp.float32)


class Side:
    def __init__(self, send, recv):
        self.peer = {"x": 1 - lax.axis_index("x")}
        self.send, self.recv, self.copies = send, recv, []

    def start(self, source, target):
        at = len(self.copies)
        copy = remote(source, target, self.send.at[at], self.recv.at[at], self.peer)
        copy.start()
        self.copies.append(copy)
        return copy

    def later(self, source, target):
        at = len(self.copies)
        copy = remote(source, target, self.send.at[at], self.recv.at[at], self.peer)
        self.copies.append(copy)
        return copy

    def finish(self, taken=()):
        for copy in self.copies:
            copy.wait_send()
            if not any(copy is item for item in taken):
                copy.wait_recv()


def remote(src, dst, send, recv, device):
    return pltpu.make_async_remote_copy(
        src_ref=src, dst_ref=dst, send_sem=send, recv_sem=recv, device_id=device, device_id_type=MESH_ID
    )


def halves(features):
    half = features // 2
    x = lax.axis_index("x")
    own = pl.ds(pl.multiple_of(x * half, half), half)
    other = pl.ds(pl.multiple_of((1 - x) * half, half), half)
    return own, other


def flip(block):
    return jnp.transpose(block.astype(jnp.float32)).astype(jnp.bfloat16)


def grad_tile(turned, features, right, cols, kept, given):
    own, other = halves(features)
    value = right[:, cols]
    kept[:, cols] = jnp.dot(turned[own, :], value, preferred_element_type=jnp.float32).astype(jnp.bfloat16)
    given[:, cols] = jnp.dot(turned[other, :], value, preferred_element_type=jnp.float32).astype(jnp.bfloat16)


def sem(*shape):
    return pltpu.SemaphoreType.DMA(shape)


class Link:
    def __init__(self, part, at, shape, dtype):
        self.part, self.at, self.shape, self.dtype = part, at, shape, dtype


class Part:
    def __init__(self, kernel, operands, shapes, staged_in, staged_out, scratch, aliases, flops, name, early=None):
        self.kernel, self.operands, self.shapes = kernel, operands, shapes
        self.staged_in, self.staged_out, self.scratch = staged_in, staged_out, scratch
        self.aliases, self.flops, self.name = aliases, flops, name
        self.early, self.private, self.woven = early, (), False

    def link(self, at, part=0):
        return Link(part, at, self.shapes[at].shape, self.shapes[at].dtype)


class Done:
    def start(self):
        pass

    def wait(self):
        pass


class Later:
    def __init__(self, copy):
        self.start = copy.start

    def wait(self):
        pass


def weave(step, count, later_step, later_post, later_count, post):
    def both(i, _):
        @pl.when(i < count)
        def _():
            step(i, 0)

        @pl.when(i >= OFFSET)
        def _():
            later_step(i - OFFSET, 0)

        return 0

    lax.fori_loop(0, OFFSET + later_count, both, 0)
    post()
    later_post()


def launch(parts, greet, ident):
    operands, aliases, shapes, scratch = [], {}, [], []
    for part in parts:
        base = len(shapes)
        for at, item in enumerate(part.operands):
            if not isinstance(item, Link):
                if at in part.aliases:
                    aliases[len(operands)] = base + part.aliases[at]
                operands.append(item)
        shapes += part.shapes
        for item in part.operands[: part.staged_in]:
            if not (isinstance(item, Link) and item.at < parts[item.part].staged_out):
                scratch.append(pltpu.VMEM(item.shape, item.dtype))
        scratch += [pltpu.VMEM(item.shape, item.dtype) for item in part.shapes[: part.staged_out]]
        scratch += [sem(part.staged_in), sem(part.staged_out)] + part.scratch

    def body(*refs):
        given, made, rest = refs[: len(operands)], refs[len(operands) : len(operands) + len(shapes)], list(
            refs[len(operands) + len(shapes) :]
        )
        given, made = list(given), list(made)
        ready, results, held = [], [], []
        for part in parts:
            outs = [made.pop(0) for _ in part.shapes]
            inner, sources, late = [], [], []
            for at, item in enumerate(part.operands):
                if isinstance(item, Link):
                    staged, whole = results[item.part]
                    near = item.at < parts[item.part].staged_out
                    source = None if near else whole[item.at]
                    late.append(at)
                else:
                    near, source = False, given.pop(0)
                if at >= part.staged_in:
                    inner.append(staged[item.at] if near else source)
                elif near:
                    inner.append(staged[item.at])
                else:
                    inner.append(rest.pop(0))
                sources.append(source)
            results_in = [rest.pop(0) for _ in range(part.staged_out)]
            load_s, store_s = rest.pop(0), rest.pop(0)
            own = [rest.pop(0) for _ in part.scratch]
            loads = [
                Done() if sources[k] is None else pltpu.make_async_copy(sources[k], inner[k], load_s.at[k])
                for k in range(part.staged_in)
            ]
            stores = [
                Done() if k in part.private else pltpu.make_async_copy(results_in[k], outs[k], store_s.at[k])
                for k in range(part.staged_out)
            ]
            for k, copy in enumerate(loads):
                if k not in late:
                    copy.start()
            results.append((results_in, outs))
            ready.append((loads, stores, late, inner, results_in + outs[part.staged_out :], own))
        begun = {}

        def begin(at):
            part = parts[at]
            loads, stores, late, inner, outs, own = ready[at]
            for k in late:
                if k < part.staged_in:
                    loads[k].start()
            if at < len(parts) - 1:
                held.extend(copy for copy in stores if not isinstance(copy, Done))
                stores = [copy if isinstance(copy, Done) else Later(copy) for copy in stores]
            hook = lambda: None
            if at + 2 < len(parts) and parts[at + 2].woven:
                hook = lambda: begin(at + 2)
            elif at + 1 < len(parts) and parts[at + 1].early:
                following = ready[at + 1]
                hook = lambda: parts[at + 1].early(following[0], *following[3], *following[4], *following[5])
            begun[at] = part.kernel(loads, stores, greet if at == 0 else lambda: None, hook, *inner, *outs, *own)

        for at, part in enumerate(parts):
            if part.woven:
                continue
            begin(at)
            if begun[at] is None:
                continue
            step, post, count = begun[at]
            if at + 1 < len(parts) and parts[at + 1].woven:
                weave(step, count, *begun[at + 1], post)
            else:
                lax.fori_loop(0, count, step, 0)
                post()
        for copy in held:
            copy.wait()

    outside = pl.BlockSpec(memory_space=pl.ANY)
    out = pl.pallas_call(
        body,
        out_shape=tuple(shapes),
        in_specs=[outside] * len(operands),
        out_specs=[outside] * len(shapes),
        input_output_aliases=aliases,
        scratch_shapes=scratch,
        compiler_params=pltpu.CompilerParams(collective_id=ident, has_side_effects=True, vmem_limit_bytes=62 << 20),
        cost_estimate=pl.CostEstimate(
            flops=sum(part.flops for part in parts), bytes_accessed=8_000_000, transcendentals=0
        ),
        name="_".join(part.name for part in parts),
    )(*operands)
    out = list(out)
    return [[out.pop(0) for _ in part.shapes] for part in parts]


class Line:
    def __init__(self, tok, depth):
        self.z, self.x = lax.axis_index("z"), lax.axis_index("x")
        self.y, self.c = lax.axis_index("y"), lax.axis_index("c")
        self.tok, self.depth = tok, depth
        self.half = 2 * tok
        self.chunks = self.half // ROWS
        self.own = pl.multiple_of((2 * self.y + self.c) * tok, tok)
        self.peers = (
            {"y": self.y, "c": 1 - self.c},
            {"y": 1 - self.y, "c": self.c},
            {"y": 1 - self.y, "c": 1 - self.c},
        )

    def place(self, stream):
        return self.z if stream == 0 else self.depth - 1 - self.z

    def onward(self, stream):
        return {"z": self.z + 1} if stream == 0 else {"z": self.z - 1}

    def backward(self, stream):
        return {"z": self.z - 1} if stream == 0 else {"z": self.z + 1}

    def row_of(self, stream, chunk):
        per = self.chunks // 2
        far = chunk // per
        y = self.y + far * (1 - 2 * self.y)
        return pl.multiple_of((2 * y + stream) * self.tok + lax.rem(chunk, per) * ROWS, ROWS)


def make_line(tok, depth, width_in, width_out, carry_in, carry_out, features):
    chunks = 2 * tok // ROWS
    groups = chunks // GROUP_CHUNKS
    span = GROUP_CHUNKS * ROWS
    half_groups = groups // 2

    def run(line, greet, taken, begin, prepare, beside, finish, second, settle, close, product, carried, chain_out, chain_in, wide, own_part, rs_out, rs_in,
            ag_s, ag_r, ch_s, ch_r, bc_s, bc_r, rs_s, rs_r):
        greet()
        gather = [
            pltpu.make_async_remote_copy(
                src_ref=taken.at[pl.ds(line.own, tok)],
                dst_ref=taken.at[pl.ds(line.own, tok)],
                send_sem=ag_s.at[at],
                recv_sem=ag_r.at[at],
                device_id=peer,
                device_id_type=MESH_ID,
            )
            for at, peer in enumerate(line.peers)
        ]
        for copy in gather:
            copy.start()
        begin()
        gather[0].wait_recv()
        prepare(pl.multiple_of(line.y * 2 * tok, 2 * tok))

        def chain_copy(stream, chunk):
            return pltpu.make_async_remote_copy(
                src_ref=chain_out.at[stream, chunk],
                dst_ref=chain_in.at[stream, chunk],
                send_sem=ch_s.at[stream, chunk],
                recv_sem=ch_r.at[stream, chunk],
                device_id=line.onward(stream),
                device_id_type=MESH_ID,
            )

        def wide_copy(stream, chunk):
            rows = pl.ds(line.row_of(stream, chunk), ROWS)
            return pltpu.make_async_remote_copy(
                src_ref=wide.at[rows],
                dst_ref=wide.at[rows],
                send_sem=bc_s.at[stream, chunk],
                recv_sem=bc_r.at[stream, chunk],
                device_id=line.backward(stream),
                device_id_type=MESH_ID,
            )

        def sum_copy(stream, group):
            far = group // half_groups
            y = line.y + far * (1 - 2 * line.y)
            other = stream + line.c - 2 * stream * line.c
            slot = 2 * far + other - 1
            part = lax.rem(group, half_groups)
            return (slot >= 0, part, pltpu.make_async_remote_copy(
                src_ref=rs_out.at[stream, group],
                dst_ref=rs_in.at[jnp.maximum(slot, 0), pl.ds(pl.multiple_of(part * span, span), span)],
                send_sem=rs_s.at[stream, group],
                recv_sem=rs_r.at[jnp.maximum(slot, 0), part],
                device_id={"y": y, "c": stream},
                device_id_type=MESH_ID,
            ))

        def step(i, _):
            @pl.when(i == SKEW)
            def _():
                gather[1].wait_recv()
                gather[2].wait_recv()
                prepare(pl.multiple_of((1 - line.y) * 2 * tok, 2 * tok))

            for stream in (0, 1):
                place = line.place(stream)
                chunk = i - SKEW * place

                @pl.when((chunk >= 0) & (chunk < chunks))
                def _():
                    row = line.row_of(stream, chunk)

                    @pl.when(place > 0)
                    def _():
                        chain_copy(stream, chunk).wait_recv()

                    @pl.when(place == 0)
                    def _():
                        chain_out[stream, chunk, :, :width_in] = product[pl.ds(row, ROWS), :].astype(jnp.bfloat16)
                        if carry_in:
                            chain_out[stream, chunk, :, width_in:] = spread(carried[pl.ds(row, ROWS), :1])

                    @pl.when((place > 0) & (place < depth - 1))
                    def _():
                        chain_out[stream, chunk, :, :width_in] = (
                            product[pl.ds(row, ROWS), :] + chain_in[stream, chunk, :, :width_in].astype(jnp.float32)
                        ).astype(jnp.bfloat16)
                        if carry_in:
                            chain_out[stream, chunk, :, width_in:] = spread(
                                carried[pl.ds(row, ROWS), :1] + unspread(chain_in[stream, chunk, :, width_in:])
                            )

                    @pl.when(place < depth - 1)
                    def _():
                        chain_copy(stream, chunk).start()

                    @pl.when(place == depth - 1)
                    def _():
                        total = product[pl.ds(row, ROWS), :] + chain_in[stream, chunk, :, :width_in].astype(jnp.float32)
                        extra = None
                        if carry_in:
                            extra = carried[pl.ds(row, ROWS), :1] + unspread(chain_in[stream, chunk, :, width_in:])
                        finish(row, pl.multiple_of(chunk * ROWS, ROWS), total, extra)
                        wide_copy(stream, chunk).start()

            for stream in (0, 1):
                place = line.place(stream)
                ready = i - SKEW * (2 * (depth - 1) - place)

                @pl.when((ready >= 0) & (ready < chunks))
                def _():
                    @pl.when(place < depth - 1)
                    def _():
                        wide_copy(stream, ready).wait_recv()

                        @pl.when(place > 0)
                        def _():
                            wide_copy(stream, ready).start()

            beside(i)
            for stream in (0, 1):
                place = line.place(stream)
                ready = i - SKEW * (2 * (depth - 1) - place)

                @pl.when((ready >= 0) & (ready < chunks))
                def _():
                    @pl.when(lax.rem(ready, GROUP_CHUNKS) == GROUP_CHUNKS - 1)
                    def _():
                        group = ready // GROUP_CHUNKS
                        row = pl.multiple_of(line.row_of(stream, ready) - (span - ROWS), span)
                        away, part, copy = sum_copy(stream, group)
                        value = second(row, span)

                        @pl.when(away)
                        def _():
                            rs_out[stream, group, :, :features] = value.astype(jnp.bfloat16)
                            if carry_out:
                                rs_out[stream, group, :, features:] = wide[pl.ds(row, span), width_out:]
                            copy.start()

                        @pl.when(jnp.logical_not(away))
                        def _():
                            own_part[pl.ds(pl.multiple_of(part * span, span), span), :] = value

            return 0

        def drain(i, _):
            for stream in (0, 1):
                place = line.place(stream)

                @pl.when(place < depth - 1)
                def _():
                    chain_copy(stream, i).wait_send()

                @pl.when(place > 0)
                def _():
                    wide_copy(stream, i).wait_send()

            return 0

        def drain_sums(i, _):
            for stream in (0, 1):
                away, part, copy = sum_copy(stream, i)

                @pl.when(away)
                def _():
                    copy.wait_send()
            return 0

        def post():
            settle()
            for slot in range(3):
                for part in range(half_groups):
                    pltpu.make_async_remote_copy(
                        src_ref=rs_out.at[0, 0],
                        dst_ref=rs_in.at[slot, pl.ds(part * span, span)],
                        send_sem=rs_s.at[0, 0],
                        recv_sem=rs_r.at[slot, part],
                        device_id=line.peers[slot],
                        device_id_type=MESH_ID,
                    ).wait_recv()
            close()
            for copy in gather:
                copy.wait_send()
            lax.fori_loop(0, chunks, drain, 0)
            lax.fori_loop(0, groups, drain_sums, 0)

        return step, post, chunks + 2 * SKEW * (depth - 1)

    wide_in = width_in + (EXTRA if carry_in else 0)
    scratch = [
        pltpu.VMEM((4 * tok, width_in), jnp.float32),
        pltpu.VMEM((4 * tok, EXTRA), jnp.float32),
        pltpu.VMEM((2, chunks, ROWS, wide_in), jnp.bfloat16),
        pltpu.VMEM((2, chunks, ROWS, wide_in), jnp.bfloat16),
        pltpu.VMEM((tok, features), jnp.float32),
        pltpu.VMEM((2, groups, span, features + (EXTRA if carry_out else 0)), jnp.bfloat16),
        pltpu.VMEM((3, tok, features + (EXTRA if carry_out else 0)), jnp.bfloat16),
        pltpu.SemaphoreType.DMA((3,)),
        pltpu.SemaphoreType.DMA((3,)),
        pltpu.SemaphoreType.DMA((2, chunks)),
        pltpu.SemaphoreType.DMA((2, chunks)),
        pltpu.SemaphoreType.DMA((2, chunks)),
        pltpu.SemaphoreType.DMA((2, chunks)),
        pltpu.SemaphoreType.DMA((2, groups)),
        pltpu.SemaphoreType.DMA((3, half_groups)),
    ]
    return run, scratch


TILE = 256


def ffn_forward(hidden, gain, gu_own, gu_peer, down_own, down_peer, shipped, depth):
    tok, features = hidden.shape
    width = down_own.shape[1]
    run, scratch = make_line(tok, depth, 2 * width, width, True, False, features)
    fetch = down_peer is None
    count = len(shipped)
    sides = count + (1 if fetch else 0)

    def kernel(loads, stores, greet, hook, h_ref, gain_ref, w1_own, w1_peer, w2_own, *rest):
        if not fetch:
            w2_peer, rest = rest[0], rest[1:]
        leave, rest = rest[:count], rest[count:]
        (out_ref, normed_t, kept, wide), rest = rest[:4], rest[4:]
        if fetch:
            w2_peer, rest = rest[0], rest[1:]
        landed, rest = rest[:count], rest[count:]
        (taken, scaled, pieces, side_s, side_r, product, carried, chain_out, chain_in, own_part, rs_out, rs_in), sems = (
            rest[:12], rest[12:])
        line = Line(tok, depth)
        side = Side(side_s, side_r)
        own, other = halves(features)
        loads[0].wait()
        taken[pl.ds(line.own, tok), :] = h_ref[...].astype(jnp.bfloat16)
        at_end = (line.z == 0) | (line.z == depth - 1)

        def begin():
            for copy in loads[1:]:
                copy.wait()
            if fetch:
                side.start(w2_own, w2_peer)
            for source, target in zip(leave, landed):
                side.start(source, target)

        def prepare(row):
            rows = pl.ds(row, 2 * tok)
            block = taken[rows, :].astype(jnp.float32)
            carried[rows, :] = jnp.broadcast_to(jnp.sum(block * block, axis=1, keepdims=True), (2 * tok, EXTRA))
            scaled[...] = (block * gain_ref[...]).astype(jnp.bfloat16)

            def tile(j, _):
                cols = pl.ds(pl.multiple_of(j * TILE, TILE), TILE)
                product[rows, cols] = jnp.dot(
                    scaled[:, own], w1_own[:, cols], preferred_element_type=jnp.float32
                ) + jnp.dot(scaled[:, other], w1_peer[:, cols], preferred_element_type=jnp.float32)
                return 0

            lax.fori_loop(0, 2 * width // TILE, tile, 0)

        def beside(i):
            if fetch:

                @pl.when(i == SKEW * (depth - 1))
                def _():
                    side.copies[0].wait_recv()
                    stores[4].start()

        def finish(row, at, total, extra):
            factor = lax.rsqrt(extra / D + EPS)
            gate = total[:, :width] * factor
            upper = total[:, width:] * factor
            kept[pl.ds(at, ROWS), :width] = gate
            kept[pl.ds(at, ROWS), width:] = upper
            active = gate * jax.nn.sigmoid(gate) * upper
            wide[pl.ds(row, ROWS), :width] = active.astype(jnp.bfloat16)
            wide[pl.ds(row, ROWS), width:] = spread(factor)

        def second(row, span):
            value = wide[pl.ds(row, span), :width]
            pieces[:, own] = transposed_dot(value, w2_own[...])
            pieces[:, other] = transposed_dot(value, w2_peer[...])
            return pieces[...]

        def settle():
            stores[3].start()

            @pl.when(at_end)
            def _():
                stores[2].start()

            normed = taken[...].astype(jnp.float32) * unspread(wide[:, width:]) * gain_ref[...]
            normed_t[...] = jnp.transpose(normed).astype(jnp.bfloat16)
            stores[1].start()

        def close():
            total = own_part[...]
            for slot in range(3):
                total = total + rs_in[slot].astype(jnp.float32)
            out_ref[...] = h_ref[...] + total
            stores[0].start()
            side.finish(side.copies[:1] if fetch else ())
            for at in (0, 1, 3, 4)[: 4 if fetch else 3]:
                stores[at].wait()

            @pl.when(at_end)
            def _():
                stores[2].wait()

        return run(line, greet, taken, begin, prepare, beside, finish, second, settle, close, product, carried, chain_out, chain_in, wide,
            own_part, rs_out, rs_in, *sems)

    low, full = jnp.bfloat16, jnp.float32
    shapes = (
        jax.ShapeDtypeStruct((tok, features), full),
        jax.ShapeDtypeStruct((features, 4 * tok), low),
        jax.ShapeDtypeStruct((2 * tok, 2 * width), full),
        jax.ShapeDtypeStruct((4 * tok, width + EXTRA), low),
    ) + ((jax.ShapeDtypeStruct(down_own.shape, low),) if fetch else ()) + tuple(jax.ShapeDtypeStruct(item.shape, item.dtype) for item in shipped)
    return Part(
        kernel, (hidden, gain.reshape(1, -1), gu_own, gu_peer, down_own, *(() if fetch else (down_peer,)), *shipped), shapes,
        5 if fetch else 6, 5 if fetch else 4,
        [
            pltpu.VMEM((4 * tok, features), low),
            pltpu.VMEM((2 * tok, features), low),
            pltpu.VMEM((GROUP_CHUNKS * ROWS, features), full),
            sem(max(sides, 1)), sem(max(sides, 1)),
        ] + scratch,
        {}, 60_000_000_000, "ffn_forward",
    )


def ffn_backward(
    grad, hidden, gain, kept, wide_forward, gu_own, gu_peer, down_own, down_peer, shipped, stacks, index, layers, depth, woven=False
):
    tok, features = hidden.shape
    width = down_own.shape[1]
    run, scratch = make_line(tok, depth, width, 2 * width, False, True, features)
    count = len(shipped)
    tiles = width // EXTRA
    every = 2 if woven else 1
    first_tile = 2 * tok // ROWS + 2 * SKEW * (depth - 1) - OFFSET if woven else SKEW + 1
    turns = (tiles + every - 1) // every

    def kernel(loads, stores, greet, hook, dy_ref, h_ref, gain_ref, kept_ref, before_ref, w1_own, w1_peer, w2_own, w2_peer, *rest):
        leave, rest = rest[:count], rest[count:]
        rest = rest[len(stacks):]
        (out_ref, wide, gain_out, kept_all, got_all), rest = rest[:5], rest[5:]
        landed, rest = rest[:count], rest[count:]
        (taken, turned, down_kept, down_given, keep_s, pieces, side_s, side_r, product, carried, chain_out, chain_in, own_part,
         rs_out, rs_in), sems = rest[:15], rest[15:]
        line = Line(tok, depth)
        side = Side(side_s, side_r)
        own, other = halves(features)
        loads[0].wait()
        taken[pl.ds(line.own, tok), :] = dy_ref[...].astype(jnp.bfloat16)
        give = side.later(down_given, got_all.at[index])
        keep = pltpu.make_async_copy(down_kept, kept_all.at[index], keep_s)

        def begin():
            for source, target in zip(leave, landed):
                side.start(source, target)
            loads[7].wait()
            loads[8].wait()

        def prepare(row):
            rows = pl.ds(row, 2 * tok)

            def tile(j, _):
                cols = pl.ds(pl.multiple_of(j * EXTRA, EXTRA), EXTRA)
                product[rows, cols] = jnp.dot(
                    taken[rows, own], w2_own[:, cols], preferred_element_type=jnp.float32
                ) + jnp.dot(taken[rows, other], w2_peer[:, cols], preferred_element_type=jnp.float32)
                return 0

            lax.fori_loop(0, width // EXTRA, tile, 0)

        def beside(i):
            @pl.when(i == 1)
            def _():
                for copy in loads[1:7]:
                    copy.wait()

            @pl.when(i == first_tile)
            def _():
                turned[...] = flip(taken[...])

            for turn_at in range(every):
                at = (i - first_tile) * every + turn_at

                @pl.when((at >= 0) & (at < tiles))
                def _():
                    cols = pl.ds(pl.multiple_of(at * EXTRA, EXTRA), EXTRA)
                    grad_tile(turned, features, before_ref, cols, down_kept, down_given)

            @pl.when(i == first_tile + turns)
            def _():
                give.start()
                keep.start()

        def finish(row, at, total, extra):
            gate = kept_ref[pl.ds(at, ROWS), :width]
            upper = kept_ref[pl.ds(at, ROWS), width:]
            sig = jax.nn.sigmoid(gate)
            silu = gate * sig
            grad_gate = total * upper * (sig + silu * (1.0 - sig))
            grad_up = total * silu
            wide[pl.ds(row, ROWS), :width] = grad_gate.astype(jnp.bfloat16)
            wide[pl.ds(row, ROWS), width : 2 * width] = grad_up.astype(jnp.bfloat16)
            inner = jnp.sum(grad_gate * gate + grad_up * upper, axis=1, keepdims=True)
            wide[pl.ds(row, ROWS), 2 * width :] = spread(inner)

        def second(row, span):
            value = wide[pl.ds(row, span), : 2 * width]
            pieces[:, own] = transposed_dot(value, w1_own[...])
            pieces[:, other] = transposed_dot(value, w1_peer[...])
            return pieces[...]

        def settle():
            stores[1].start()

        def close():
            total = own_part[...]
            inner = unspread(wide[pl.ds(line.own, tok), 2 * width :])
            for slot in range(3):
                total = total + rs_in[slot, :, :features].astype(jnp.float32)
                inner = inner + unspread(rs_in[slot, :, features:])
            factor = unspread(before_ref[pl.ds(line.own, tok), width:])
            normed = h_ref[...] * factor
            gain_out[...] = jnp.broadcast_to(jnp.sum(total * normed, axis=0, keepdims=True), gain_out.shape)
            out_ref[...] = dy_ref[...] + factor * (total * gain_ref[...] - normed * (inner / D))
            stores[2].start()
            stores[0].start()
            keep.wait()
            side.finish()
            for copy in stores:
                copy.wait()

        return run(line, greet, taken, begin, prepare, beside, finish, second, settle, close, product, carried, chain_out, chain_in,
            wide, own_part, rs_out, rs_in, *sems)

    low, full = jnp.bfloat16, jnp.float32
    shapes = (
        jax.ShapeDtypeStruct((tok, features), full),
        jax.ShapeDtypeStruct((4 * tok, 2 * width + EXTRA), low),
        jax.ShapeDtypeStruct((8, features), full),
        jax.ShapeDtypeStruct((layers,) + down_own.shape, low),
        jax.ShapeDtypeStruct((layers,) + down_own.shape, low),
    ) + tuple(jax.ShapeDtypeStruct(item.shape, item.dtype) for item in shipped)
    own_scratch = [
        pltpu.VMEM((4 * tok, features), low),
        pltpu.VMEM((features, 4 * tok), low),
        pltpu.VMEM(down_own.shape, low),
        pltpu.VMEM(down_own.shape, low),
        pltpu.SemaphoreType.DMA,
        pltpu.VMEM((GROUP_CHUNKS * ROWS, features), full),
        sem(1 + count), sem(1 + count),
    ] + scratch
    return Part(
        kernel,
        (grad, hidden, gain.reshape(1, -1), kept, wide_forward, gu_own, gu_peer, down_own, down_peer, *shipped, *stacks),
        shapes, 9, 3,
        own_scratch,
        {9 + count + at: 3 + at for at in range(len(stacks))}, 60_000_000_000, "ffn_backward",
    )


def to_row(column):
    return jnp.transpose(jnp.broadcast_to(column, (column.shape[0], EXTRA)))[:8]


def to_column(row):
    return jnp.transpose(jnp.broadcast_to(row[:1], (row.shape[1], row.shape[1])))[:, :1]


def turn(values, cosine, sine):
    lane = lax.broadcasted_iota(jnp.int32, values.shape, 1)
    width = values.shape[1]
    back = pltpu.roll(values, width - HEAD // 2, 1)
    forth = pltpu.roll(values, HEAD // 2, 1)
    partner = jnp.where(lax.rem(lane, HEAD) < HEAD // 2, back, forth)
    return values * cosine + partner * sine


def split_pair(block):
    lane = lax.broadcasted_iota(jnp.int32, block.shape, 1)
    zero = jnp.zeros_like(block)
    return jnp.concatenate([jnp.where(lane < HEAD, block, zero), jnp.where(lane < HEAD, zero, block)], axis=0)


def join_pair(turned, tok):
    return jnp.transpose(jnp.concatenate([turned[:HEAD, :tok], turned[HEAD:, tok:]], axis=0))


def twice(kv):
    wide = kv.astype(jnp.float32)
    lane = lax.broadcasted_iota(jnp.int32, wide.shape, 1)
    other = pltpu.roll(wide, HEAD, 1)
    return jnp.where(lane < HEAD, wide, other), jnp.where(lane < HEAD, other, wide)


class Square:
    def __init__(self, tok, depth):
        self.z, self.x = lax.axis_index("z"), lax.axis_index("x")
        self.y, self.c = lax.axis_index("y"), lax.axis_index("c")
        self.tok, self.depth = tok, depth
        self.g = 2 * self.y + self.c
        self.row = 2 * self.z + self.x
        self.own = pl.multiple_of(self.g * tok, tok)
        self.mine = pl.multiple_of(self.z * tok, tok)
        self.peers = (
            {"y": self.y, "c": 1 - self.c},
            {"y": 1 - self.y, "c": self.c},
            {"y": 1 - self.y, "c": 1 - self.c},
        )

    def row_peer(self, step):
        at = lax.rem(self.row + step, 2 * self.depth)
        return {"z": at // 2, "x": lax.rem(at, 2)}

    def greet(self, extra=0):
        barrier = pltpu.get_barrier_semaphore()
        for peer in self.peers:
            pl.semaphore_signal(barrier, 1, device_id=peer, device_id_type=MESH_ID)
        for step in range(1, 2 * self.depth):
            pl.semaphore_signal(barrier, 1, device_id=self.row_peer(step), device_id_type=MESH_ID)
        pl.semaphore_wait(barrier, 3 + 2 * self.depth - 1 + extra)


def start_gather(square, taken, send, recv):
    copies = [
        remote(taken.at[pl.ds(square.own, square.tok)], taken.at[pl.ds(square.own, square.tok)], send.at[at], recv.at[at], peer)
        for at, peer in enumerate(square.peers)
    ]
    for copy in copies:
        copy.start()
    return copies


def line_sum(square, gather, product, own, own_row, outs, ins, row_outs, row_ins, send, recv, row_send, row_recv, between):
    tok, depth = square.tok, square.depth

    def one(order):
        block = lax.rem(2 * square.y + order, depth)
        step = lax.rem(block - square.z + depth, depth)
        slot = jnp.maximum(depth - 1 - step, 0)
        value, column = product(pl.multiple_of(block * tok, tok))

        @pl.when(step == 0)
        def _():
            own[...] = value
            if column is not None:
                own_row[...] = to_row(column)

        copy = remote(outs.at[order], ins.at[slot], send.at[order], recv.at[slot], {"z": block})
        row_copy = None
        if column is not None:
            row_copy = remote(row_outs.at[order], row_ins.at[slot], row_send.at[order], row_recv.at[slot], {"z": block})

        @pl.when(step != 0)
        def _():
            outs[order] = value.astype(jnp.bfloat16)
            copy.start()
            if column is not None:
                row_outs[order] = to_row(column)
                row_copy.start()

        return step, copy, row_copy

    gather[0].wait_recv()
    sent = [one(0), one(1)]
    gather[1].wait_recv()
    gather[2].wait_recv()
    sent += [one(2), one(3)]
    between()
    for slot in range(depth - 1):
        remote(outs.at[0], ins.at[slot], send.at[0], recv.at[slot], {"z": square.z}).wait_recv()
        if row_ins is not None:
            remote(row_outs.at[0], row_ins.at[slot], row_send.at[0], row_recv.at[slot], {"z": square.z}).wait_recv()
    return sent


def send_part(square, array, part, send, recv):
    lanes = pl.ds(pl.multiple_of(part * EXTRA, EXTRA), EXTRA)
    here = array.at[pl.ds(square.mine, square.tok), lanes]
    depth = square.depth
    return [
        remote(here, here, send.at[step - 1, part], recv.at[depth - 1 - step, part], {"z": lax.rem(square.z + step, depth)})
        for step in range(1, depth)
    ]


def send_row(square, rows, send, recv):
    line = rows.at[square.z]
    depth = square.depth
    return [
        remote(line, line, send.at[step - 1], recv.at[depth - 1 - step], {"z": lax.rem(square.z + step, depth)})
        for step in range(1, depth)
    ]


def grid_sum(square, array, rows, second, settle, own, outs, ins, row_ins, arrive, row_arrive, send, recv, row_send, row_recv):
    tok, depth = square.tok, square.depth
    sent = []
    for step in range(depth):
        block = lax.rem(square.z + step, depth)
        if step:
            for part in range(array.shape[1] // EXTRA):
                rows_of = array.at[pl.ds(pl.multiple_of(block * tok, tok), tok), pl.ds(part * EXTRA, EXTRA)]
                remote(rows_of, rows_of, send.at[0], arrive.at[step - 1, part], {"z": square.z}).wait_recv()
            remote(rows.at[block], rows.at[block], send.at[0], row_arrive.at[step - 1], {"z": square.z}).wait_recv()
        value = second(pl.multiple_of(block * tok, tok))
        away = lax.rem(block - square.g + depth, depth)
        slot = jnp.maximum(depth - 1 - away, 0)
        device = {"y": block // 2, "c": lax.rem(block, 2)}
        copy = remote(outs.at[step], ins.at[slot], send.at[step], recv.at[slot], device)
        row_copy = None
        if row_ins is not None:
            row_copy = remote(rows.at[block], row_ins.at[slot], row_send.at[step], row_recv.at[slot], device)

        @pl.when(away == 0)
        def _():
            own[...] = value

        @pl.when(away != 0)
        def _():
            outs[step] = value.astype(jnp.bfloat16)
            copy.start()
            if row_ins is not None:
                row_copy.start()

        sent.append((away, copy, row_copy))
    settle()
    for slot in range(depth - 1):
        remote(outs.at[0], ins.at[slot], send.at[0], recv.at[slot], square.peers[0]).wait_recv()
        if row_ins is not None:
            remote(rows.at[0], row_ins.at[slot], row_send.at[0], row_recv.at[slot], square.peers[0]).wait_recv()
    return sent


def drain(sent):
    for away, copy, row_copy in sent:

        @pl.when(away != 0)
        def _():
            copy.wait_send()
            if row_copy is not None:
                row_copy.wait_send()


def attention_forward(hidden, gain, qkv_own, out_own, qkv_peer, out_peer, shipped, cosine, sine, depth):
    tok, features = hidden.shape
    cols = qkv_own.shape[1]
    fetch = qkv_peer is None
    extra = 2 if fetch else 0
    count = len(shipped)
    sides = extra + 2 * count
    query_cols = GROUP * HEAD
    seq = 2 * depth * tok
    pairs = query_cols // EXTRA
    scale = 1.0 / math.sqrt(HEAD)

    def kernel(loads, stores, greet, hook, h_ref, gain_ref, wqkv_own, wo_own, cos_ref, sin_ref, *rest):
        if not fetch:
            (wqkv_peer, wo_peer), rest = rest[:2], rest[2:]
        leave, rest = rest[:count], rest[count:]
        (out_ref, normed_t, queries, kv, lse, mixed, factors), rest = rest[:7], rest[7:]
        if fetch:
            (wqkv_peer, wo_peer), rest = rest[:2], rest[2:]
        landed, rest = rest[:count], rest[count:]
        (taken, scaled, pieces, own, own_row, z_out, z_in, zr_out, zr_in, values_t, g_own, g_out, g_in,
         ag_s, ag_r, zs_s, zs_r, zr_s, zr_r, kv_s, kv_r, zg_s, zg_r, zgr_s, zgr_r, gs_s, gs_r), rest = rest[:27], rest[27:]
        square = Square(tok, depth)
        side = Side(*rest) if sides else None
        mine, other = halves(features)
        loads[0].wait()
        taken[pl.ds(square.own, tok), :] = h_ref[...].astype(jnp.bfloat16)
        greet()
        gather = start_gather(square, taken, ag_s, ag_r)
        for copy in loads[1:]:
            copy.wait()
        urgent = []
        if fetch:
            urgent = [side.start(wqkv_own, wqkv_peer), side.start(wo_own, wo_peer)]
        held = []
        for source, target in zip(leave, landed):
            most = source.shape[0] // 2
            rest_of = pl.ds(most, source.shape[0] - most)
            side.start(source.at[pl.ds(0, most)], target.at[pl.ds(0, most)])
            held.append(side.later(source.at[rest_of], target.at[rest_of]))
        for copy in urgent[:1]:
            copy.wait_recv()
            stores[7].start()

        def product(row):
            block = taken[pl.ds(row, tok), :].astype(jnp.float32)
            scaled[...] = (block * gain_ref[...]).astype(jnp.bfloat16)
            return (
                jnp.dot(scaled[:, mine], wqkv_own[...], preferred_element_type=jnp.float32)
                + jnp.dot(scaled[:, other], wqkv_peer[...], preferred_element_type=jnp.float32),
                jnp.sum(block * block, axis=1, keepdims=True),
            )

        sent = line_sum(square, gather, product, own, own_row, z_out, z_in, zr_out, zr_in, zs_s, zs_r, zr_s, zr_r, hook)
        total, squares = own[...], own_row[...]
        for slot in range(depth - 1):
            total = total + z_in[slot].astype(jnp.float32)
            squares = squares + zr_in[slot]
        factor_row = lax.rsqrt(squares / D + EPS)
        factors[square.z] = factor_row
        given = send_row(square, factors, zgr_s, zgr_r)
        for copy in given:
            copy.start()
        first = lax.broadcasted_iota(jnp.int32, (tok, EXTRA), 1) < HEAD
        cosine_row, sine_row = cos_ref[...], sin_ref[...]
        turned = turn(
            total * to_column(factor_row),
            jnp.concatenate([cosine_row] * pairs + [jnp.where(first, cosine_row, 1.0)], axis=1),
            jnp.concatenate([sine_row] * pairs + [jnp.where(first, sine_row, 0.0)], axis=1),
        )
        here = pl.ds(pl.multiple_of(square.row * tok, tok), tok)
        kv[here, :] = turned[:, query_cols:].astype(jnp.bfloat16)
        queries[...] = turned[:, :query_cols].astype(jnp.bfloat16)
        stores[2].start()
        spreads = []
        for step in range(1, 2 * depth):
            copy = remote(kv.at[here], kv.at[here], kv_s.at[step - 1], kv_r.at[2 * depth - 1 - step], square.row_peer(step))
            copy.start()
            spreads.append(copy)
        for copy in spreads:
            copy.wait_recv()
        stores[3].start()
        for copy in held:
            copy.start()
        keys, both = twice(kv[...])
        values_t[...] = jnp.transpose(both).astype(jnp.bfloat16)
        keys = keys.astype(jnp.bfloat16)

        def pair(t, _):
            lanes = pl.ds(pl.multiple_of(t * EXTRA, EXTRA), EXTRA)
            scores = transposed_dot(keys, split_pair(queries[:, lanes])) * scale
            key_at = lax.broadcasted_iota(jnp.int32, scores.shape, 0)
            query_at = lax.rem(lax.broadcasted_iota(jnp.int32, scores.shape, 1), tok) + square.row * tok
            scores = jnp.where(key_at <= query_at, scores, -1e30)
            top = jnp.max(scores, axis=0, keepdims=True)
            expo = jnp.exp(scores - top)
            denom = jnp.sum(expo, axis=0, keepdims=True)
            lse[t] = jnp.broadcast_to(top + jnp.log(denom), (8, 2 * tok))
            probs = (expo * (1.0 / denom)).astype(jnp.bfloat16)
            out_t = jnp.dot(values_t[...], probs, preferred_element_type=jnp.float32)
            mixed[pl.ds(square.mine, tok), lanes] = join_pair(out_t, tok).astype(jnp.bfloat16)
            for copy in send_part(square, mixed, t, zg_s, zg_r):
                copy.start()
            return 0

        lax.fori_loop(0, pairs, pair, 0)
        given += [copy for part in range(pairs) for copy in send_part(square, mixed, part, zg_s, zg_r)]

        stores[4].start()
        for copy in urgent[1:]:
            copy.wait_recv()
            stores[8].start()

        def second(row):
            value = mixed[pl.ds(row, tok), :]
            pieces[:, mine] = transposed_dot(value, wo_own[...])
            pieces[:, other] = transposed_dot(value, wo_peer[...])
            return pieces[...]

        def settle():
            stores[5].start()
            stores[6].start()
            for block in range(depth):
                rows = pl.ds(block * tok, tok)
                normed = taken[rows, :].astype(jnp.float32) * to_column(factors[block]) * gain_ref[...]
                normed_t[:, rows] = jnp.transpose(normed).astype(jnp.bfloat16)
            stores[1].start()

        sums = grid_sum(square, mixed, factors, second, settle, g_own, g_out, g_in, None, zg_r, zgr_r, gs_s, gs_r, None, None)
        total = g_own[...]
        for slot in range(depth - 1):
            total = total + g_in[slot].astype(jnp.float32)
        out_ref[...] = h_ref[...] + total
        stores[0].start()
        drain(sent)
        drain(sums)
        for copy in gather + spreads + given:
            copy.wait_send()
        if side:
            side.finish(urgent)
        for copy in stores:
            copy.wait()

    low, full = jnp.bfloat16, jnp.float32
    shapes = (
        jax.ShapeDtypeStruct((tok, features), full),
        jax.ShapeDtypeStruct((features, depth * tok), low),
        jax.ShapeDtypeStruct((tok, query_cols), low),
        jax.ShapeDtypeStruct((seq, 2 * HEAD), low),
        jax.ShapeDtypeStruct((pairs, 8, 2 * tok), full),
        jax.ShapeDtypeStruct((depth * tok, query_cols), low),
        jax.ShapeDtypeStruct((depth, 8, tok), full),
    )
    if fetch:
        shapes += (jax.ShapeDtypeStruct(qkv_own.shape, low), jax.ShapeDtypeStruct(out_own.shape, low))
    shapes += tuple(jax.ShapeDtypeStruct(item.shape, item.dtype) for item in shipped)
    peers = () if fetch else (qkv_peer, out_peer)
    operands = (hidden, gain.reshape(1, -1), qkv_own, out_own, cosine, sine, *peers, *shipped)
    return Part(
        kernel, operands, shapes, 6 + len(peers), 7 + extra,
        [
            pltpu.VMEM((depth * tok, features), low),
            pltpu.VMEM((tok, features), low),
            pltpu.VMEM((tok, features), full),
            pltpu.VMEM((tok, cols), full),
            pltpu.VMEM((8, tok), full),
            pltpu.VMEM((depth, tok, cols), low),
            pltpu.VMEM((depth - 1, tok, cols), low),
            pltpu.VMEM((depth, 8, tok), full),
            pltpu.VMEM((depth - 1, 8, tok), full),
            pltpu.VMEM((2 * HEAD, seq), low),
            pltpu.VMEM((tok, features), full),
            pltpu.VMEM((depth, tok, features), low),
            pltpu.VMEM((depth - 1, tok, features), low),
            sem(3), sem(3), sem(depth), sem(depth - 1), sem(depth), sem(depth - 1),
            sem(2 * depth - 1), sem(2 * depth - 1), sem(depth - 1, pairs), sem(depth - 1, pairs), sem(depth - 1), sem(depth - 1),
            sem(depth), sem(depth - 1),
        ] + ([sem(sides), sem(sides)] if sides else []),
        {}, 50_000_000_000, "attention_forward",
    )


def attention_backward(
    grad, hidden, gain, qkv_own, qkv_peer, out_own, out_peer, cosine, sine, queries, kv, lse, factors, mixed, normed_a, normed_f,
    grad_gu, stacks, index, layers, depth,
):
    tok, features = hidden.shape
    cols = qkv_own.shape[1]
    wide = grad_gu.shape[1] - EXTRA
    query_cols = GROUP * HEAD
    seq = 2 * depth * tok
    pairs = query_cols // EXTRA
    scale = 1.0 / math.sqrt(HEAD)

    def kernel(loads, stores, greet, hook, dy_ref, h_ref, gain_ref, wqkv_own, wqkv_peer, wo_own, wo_peer, cos_ref, sin_ref, q_ref, kv_ref, lse_ref,
               factor_ref, mixed_ref, normed_a_ref, normed_f_ref, gu_ref, *rest_refs):
        (out_ref, gain_out, qkv_given, gu_kept_all, gu_got_all, out_kept_all, out_got_all, qkv_kept_all,
               taken, spun, turned, pieces, gu_kept, gu_given, out_kept, out_given, qkv_kept, keep_s,
               own, heads, z_out, z_in, keys_t, dk, dv, kv_out, kv_in, dq, inner_rows, g_own, g_out, g_in, g_rows,
               ag_s, ag_r, zs_s, zs_r, kv_s, kv_r, zg_s, zg_r, zgr_s, zgr_r, gs_s, gs_r, gr_s, gr_r, side_s, side_r) = rest_refs[len(stacks):]
        square = Square(tok, depth)
        side = Side(side_s, side_r)
        mine, other = halves(features)
        loads[0].wait()
        taken[pl.ds(square.own, tok), :] = dy_ref[...].astype(jnp.bfloat16)
        greet()
        gather = start_gather(square, taken, ag_s, ag_r)
        for copy in loads[1:]:
            copy.wait()

        def gu_tiles(start, stop):
            def tile(j, _):
                grad_tile(normed_f_ref, features, gu_ref, pl.ds(pl.multiple_of(j * EXTRA, EXTRA), EXTRA), gu_kept, gu_given)
                return 0

            lax.fori_loop(start, stop, tile, 0)

        gu_got = gu_got_all.at[index]
        keeps = [
            pltpu.make_async_copy(gu_kept, gu_kept_all.at[index], keep_s.at[0]),
            pltpu.make_async_copy(out_kept, out_kept_all.at[index], keep_s.at[1]),
            pltpu.make_async_copy(qkv_kept, qkv_kept_all.at[index], keep_s.at[2]),
        ]
        every = wide // EXTRA
        middle, late = every // 2, every * 3 // 4
        gu_tiles(0, middle)
        front, rest = pl.ds(0, middle * EXTRA), pl.ds(late * EXTRA, wide - late * EXTRA)
        inner_part = pl.ds(middle * EXTRA, (late - middle) * EXTRA)
        side.start(gu_given.at[:, front], gu_got.at[:, front])

        def between():
            turned[...] = flip(taken[...])
            for t in range(query_cols // EXTRA):
                grad_tile(turned, features, mixed_ref, pl.ds(t * EXTRA, EXTRA), out_kept, out_given)
            side.start(out_given, out_got_all.at[index])
            gu_tiles(middle, late)
            side.start(gu_given.at[:, inner_part], gu_got.at[:, inner_part])
            gu_tiles(late, every)
            keeps[0].start()
            keeps[1].start()

        def product(row):
            rows = pl.ds(row, tok)
            value = jnp.dot(taken[rows, mine], wo_own[...], preferred_element_type=jnp.float32) + jnp.dot(
                taken[rows, other], wo_peer[...], preferred_element_type=jnp.float32
            )
            return value, None

        sent = line_sum(square, gather, product, own, None, z_out, z_in, None, None, zs_s, zs_r, None, None, between)
        total = own[...]
        for slot in range(depth - 1):
            total = total + z_in[slot].astype(jnp.float32)
        heads[...] = total.astype(jnp.bfloat16)
        keys, both = twice(kv_ref[...])
        keys_t[...] = jnp.transpose(keys).astype(jnp.bfloat16)
        keys = keys.astype(jnp.bfloat16)
        both = both.astype(jnp.bfloat16)
        dk[...] = jnp.zeros_like(dk)
        dv[...] = jnp.zeros_like(dv)

        def pair(t, _):
            lanes = pl.ds(pl.multiple_of(t * EXTRA, EXTRA), EXTRA)
            query = split_pair(q_ref[:, lanes])
            head = split_pair(heads[:, lanes])
            scores = transposed_dot(keys, query) * scale
            key_at = lax.broadcasted_iota(jnp.int32, scores.shape, 0)
            query_at = lax.rem(lax.broadcasted_iota(jnp.int32, scores.shape, 1), tok) + square.row * tok
            probs = jnp.exp(jnp.where(key_at <= query_at, scores, -1e30) - lse_ref[t, :1, :])
            grad_probs = transposed_dot(both, head)
            delta = jnp.sum(probs * grad_probs, axis=0, keepdims=True)
            grad_scores = (probs * (grad_probs - delta)).astype(jnp.bfloat16)
            dk[...] += jnp.dot(grad_scores, query, preferred_element_type=jnp.float32)
            dv[...] += jnp.dot(probs.astype(jnp.bfloat16), head, preferred_element_type=jnp.float32)
            back = jnp.dot(keys_t[...], grad_scores, preferred_element_type=jnp.float32)
            value = join_pair(back, tok) * scale
            dq[...] += jnp.broadcast_to(
                jnp.sum(value * q_ref[:, lanes].astype(jnp.float32), axis=1, keepdims=True), dq.shape
            )
            spun[pl.ds(square.mine, tok), lanes] = turn(value, cos_ref[...], -sin_ref[...]).astype(jnp.bfloat16)
            for copy in send_part(square, spun, t, zg_s, zg_r):
                copy.start()
            return 0

        dq[...] = jnp.zeros_like(dq)
        lax.fori_loop(0, pairs, pair, 0)
        lane = lax.broadcasted_iota(jnp.int32, (seq, EXTRA), 1)
        left = dk[...]
        right = dv[...]
        both_kv = jnp.where(
            lane < HEAD, (left + pltpu.roll(left, HEAD, 1)) * scale, right + pltpu.roll(right, HEAD, 1)
        )
        dk[...] = both_kv
        kv_out[...] = both_kv.astype(jnp.bfloat16)
        here = pl.ds(pl.multiple_of(square.row * tok, tok), tok)
        spreads = []
        for step in range(1, 2 * depth):
            at = lax.rem(square.row + step, 2 * depth)
            copy = remote(
                kv_out.at[pl.ds(pl.multiple_of(at * tok, tok), tok)],
                kv_in.at[2 * depth - 1 - step],
                kv_s.at[step - 1],
                kv_r.at[2 * depth - 1 - step],
                square.row_peer(step),
            )
            copy.start()
            spreads.append(copy)
        total_kv = dk[here, :]
        for copy in spreads:
            copy.wait_recv()
        side.start(gu_given.at[:, rest], gu_got.at[:, rest])
        for slot in range(2 * depth - 1):
            total_kv = total_kv + kv_in[slot].astype(jnp.float32)
        first = lax.broadcasted_iota(jnp.int32, (tok, EXTRA), 1) < HEAD
        spun[pl.ds(square.mine, tok), query_cols:] = turn(
            total_kv, jnp.where(first, cos_ref[...], 1.0), jnp.where(first, -sin_ref[...], 0.0)
        ).astype(jnp.bfloat16)
        inner = dq[:, :1] + jnp.sum(total_kv * kv_ref[here, :].astype(jnp.float32), axis=1, keepdims=True)
        inner_rows[square.z] = to_row(inner)
        given = send_part(square, spun, pairs, zg_s, zg_r) + send_row(square, inner_rows, zgr_s, zgr_r)
        for copy in given:
            copy.start()
        given += [copy for part in range(pairs) for copy in send_part(square, spun, part, zg_s, zg_r)]

        def second(row):
            value = spun[pl.ds(row, tok), :]
            pieces[:, mine] = transposed_dot(value, wqkv_own[...])
            pieces[:, other] = transposed_dot(value, wqkv_peer[...])
            return pieces[...]

        def settle():
            for t in range(cols // EXTRA):
                grad_tile(normed_a_ref, features, spun, pl.ds(t * EXTRA, EXTRA), qkv_kept, qkv_given)
            keeps[2].start()
            stores[2].start()
            hook()

        sums = grid_sum(
            square, spun, inner_rows, second, settle, g_own, g_out, g_in, g_rows, zg_r, zgr_r, gs_s, gs_r, gr_s, gr_r
        )
        total = g_own[...]
        inner = inner_rows[square.g]
        for slot in range(depth - 1):
            total = total + g_in[slot].astype(jnp.float32)
            inner = inner + g_rows[slot]
        factor = to_column(factor_ref[square.g])
        normed = h_ref[...] * factor
        gain_out[...] = jnp.broadcast_to(jnp.sum(total * normed, axis=0, keepdims=True), gain_out.shape)
        out_ref[...] = dy_ref[...] + factor * (total * gain_ref[...] - normed * (to_column(inner) / D))
        stores[0].start()
        stores[1].start()
        drain(sent)
        drain(sums)
        for copy in gather + spreads + given:
            copy.wait_send()
        for copy in keeps + stores:
            copy.wait()
        side.finish()

    low, full = jnp.bfloat16, jnp.float32
    shapes = (
        jax.ShapeDtypeStruct((tok, features), full),
        jax.ShapeDtypeStruct((8, features), full),
        jax.ShapeDtypeStruct(qkv_own.shape, low),
        jax.ShapeDtypeStruct((layers, features // 2, wide), low),
        jax.ShapeDtypeStruct((layers, features // 2, wide), low),
        jax.ShapeDtypeStruct((layers,) + out_own.shape, low),
        jax.ShapeDtypeStruct((layers,) + out_own.shape, low),
        jax.ShapeDtypeStruct((layers,) + qkv_own.shape, low),
    )
    operands = (
        grad, hidden, gain.reshape(1, -1), qkv_own, qkv_peer, out_own, out_peer, cosine, sine, queries, kv, lse, factors,
        mixed, normed_a, normed_f, grad_gu, *stacks,
    )
    return Part(
        kernel, operands, shapes, 17, 3,
        [
            pltpu.VMEM((depth * tok, features), low),
            pltpu.VMEM((depth * tok, cols), low),
            pltpu.VMEM((features, depth * tok), low),
            pltpu.VMEM((tok, features), full),
            pltpu.VMEM((features // 2, wide), low),
            pltpu.VMEM((features // 2, wide), low),
            pltpu.VMEM(out_own.shape, low),
            pltpu.VMEM(out_own.shape, low),
            pltpu.VMEM(qkv_own.shape, low),
            sem(3),
            pltpu.VMEM((tok, query_cols), full),
            pltpu.VMEM((tok, query_cols), low),
            pltpu.VMEM((depth, tok, query_cols), low),
            pltpu.VMEM((depth - 1, tok, query_cols), low),
            pltpu.VMEM((2 * HEAD, seq), low),
            pltpu.VMEM((seq, 2 * HEAD), full),
            pltpu.VMEM((seq, 2 * HEAD), full),
            pltpu.VMEM((seq, 2 * HEAD), low),
            pltpu.VMEM((2 * depth - 1, tok, 2 * HEAD), low),
            pltpu.VMEM((tok, EXTRA), full),
            pltpu.VMEM((depth, 8, tok), full),
            pltpu.VMEM((tok, features), full),
            pltpu.VMEM((depth, tok, features), low),
            pltpu.VMEM((depth - 1, tok, features), low),
            pltpu.VMEM((depth - 1, 8, tok), full),
            sem(3), sem(3), sem(depth), sem(depth - 1),
            sem(2 * depth - 1), sem(2 * depth - 1), sem(depth - 1, pairs + 1), sem(depth - 1, pairs + 1), sem(depth - 1),
            sem(depth - 1), sem(depth), sem(depth - 1), sem(depth), sem(depth - 1), sem(4), sem(4),
        ],
        {17 + at: 3 + at for at in range(len(stacks))}, 50_000_000_000, "attention_backward",
    )


def greet_last(tok, depth):
    square = Square(tok, depth)
    barrier = pltpu.get_barrier_semaphore()
    for slot in range(2 * depth):
        here = (square.z == square.g) & (slot == square.x * depth + square.g)

        @pl.when(jnp.logical_not(here))
        def _():
            source = {"z": square.g, "x": slot // depth, "y": (slot % depth) // 2, "c": slot % 2}
            pl.semaphore_signal(barrier, 1, device_id=source, device_id_type=MESH_ID)

    square.greet(2 * depth - jnp.where(square.z == square.g, 1, 0))


def finish(grad, gains, qkv_given, depth):
    tok, features = grad.shape
    count = len(gains)
    members = 2 * depth

    def kernel(loads, stores, greet, hook, grad_ref, *rest):
        gain_refs, rest = rest[:count], rest[count:]
        (given, out_ref, gain_out, got, packed, parts, sent, home, part_s, part_r, move_s, move_r, side_s, side_r) = rest
        z, x = lax.axis_index("z"), lax.axis_index("x")
        y, c = lax.axis_index("y"), lax.axis_index("c")
        g = 2 * y + c
        self_at = x * depth + g

        def target(at):
            return {"z": at // 2, "x": at % 2, "y": z // 2, "c": lax.rem(z, 2)}

        def is_source_me(slot):
            return (z == g) & (slot == self_at)

        def is_target_me(at):
            return (z == g) & (at == 2 * z + x)

        for copy in loads:
            copy.wait()
        for at, ref in enumerate(gain_refs):
            packed[at : at + 1, :] = ref[:1, :]
        sent[...] = grad_ref[...].astype(jnp.bfloat16)
        side = Side(side_s, side_r)
        side.later(given, got)
        move = remote(sent, home, move_s, move_r, {"z": g, "y": z // 2, "c": lax.rem(z, 2)})

        @pl.when(z != g)
        def _():
            move.start()

        def part(at):
            return remote(packed, parts.at[self_at], part_s.at[at], part_r.at[self_at], target(at))

        for at in range(members):

            @pl.when(jnp.logical_not(is_target_me(at)))
            def _():
                part(at).start()

        @pl.when(z == g)
        def _():
            parts[self_at] = packed[...]

        for slot in range(members):

            @pl.when(jnp.logical_not(is_source_me(slot)))
            def _():
                remote(packed, parts.at[slot], part_s.at[0], part_r.at[slot], target(0)).wait_recv()

        total = parts[0]
        for slot in range(1, members):
            total = total + parts[slot]
        gain_out[...] = total
        stores[1].start()

        @pl.when(z == g)
        def _():
            out_ref[...] = grad_ref[...]

        @pl.when(z != g)
        def _():
            move.wait_recv()
            out_ref[...] = home[...].astype(jnp.float32)
            move.wait_send()

        stores[0].start()
        for at in range(members):

            @pl.when(jnp.logical_not(is_target_me(at)))
            def _():
                part(at).wait_send()

        side.finish()
        for copy in stores:
            copy.wait()

    low, full = jnp.bfloat16, jnp.float32
    shapes = (
        jax.ShapeDtypeStruct((tok, features), full),
        jax.ShapeDtypeStruct((count, features), full),
        jax.ShapeDtypeStruct(qkv_given.shape, low),
    )
    def early(loads, *refs):
        given, got, side_s, side_r = refs[1 + count], refs[4 + count], refs[-2], refs[-1]
        Side(side_s, side_r).start(given, got)

    return Part(
        kernel, (grad, *gains, qkv_given), shapes, 1 + count, 2,
        [
            pltpu.VMEM((count, features), full),
            pltpu.VMEM((members, count, features), full),
            pltpu.VMEM((tok, features), low),
            pltpu.VMEM((tok, features), low),
            sem(members), sem(members),
            pltpu.SemaphoreType.DMA, pltpu.SemaphoreType.DMA,
            sem(1), sem(1),
        ],
        {}, 5_000_000_000, "finish", early,
    )


def combine(rests, downs, got_qkv):
    gu_kept, gu_got, out_kept, out_got, qkv_kept = rests
    layers, rows, wide = gu_kept.shape
    half = wide // 2
    step = rows // 2

    def kernel(gu_k, gu_g, out_k, out_g, down_k, down_g, qkv_k, *rest):
        got, (qkv_o, out_o, gu_o, down_o) = rest[:layers], rest[layers:]
        total = gu_k[0].astype(jnp.float32) + gu_g[0].astype(jnp.float32)
        gu_o[0, :, 0, :] = total[:, :half]
        gu_o[0, :, 1, :] = total[:, half:]
        out_o[...] = out_k[...].astype(jnp.float32) + out_g[...].astype(jnp.float32)
        down_o[...] = down_k[...].astype(jnp.float32) + down_g[...].astype(jnp.float32)
        for index in range(layers):

            @pl.when(pl.program_id(0) == index)
            def _():
                qkv_o[0, :, 0, :] = qkv_k[0].astype(jnp.float32) + got[index][...].astype(jnp.float32)

    def spec(item):
        return pl.BlockSpec((1, step, item.shape[2]), lambda layer, at: (layer, at, 0))

    operands = (gu_kept, gu_got, out_kept, out_got, *downs, qkv_kept)
    cols = qkv_kept.shape[2]
    full = jnp.float32
    return pl.pallas_call(
        kernel,
        grid=(layers, rows // step),
        in_specs=[spec(item) for item in operands]
        + [pl.BlockSpec((step, cols), lambda layer, at: (at, 0)) for _ in range(layers)],
        out_specs=[
            pl.BlockSpec((1, step, 1, cols), lambda layer, at: (layer, at, 0, 0)),
            spec(out_kept),
            pl.BlockSpec((1, step, 2, half), lambda layer, at: (layer, at, 0, 0)),
            spec(downs[0]),
        ],
        out_shape=[
            jax.ShapeDtypeStruct((layers, rows, 1, cols), full),
            jax.ShapeDtypeStruct(out_kept.shape, full),
            jax.ShapeDtypeStruct((layers, rows, 2, half), full),
            jax.ShapeDtypeStruct(downs[0].shape, full),
        ],
        compiler_params=pltpu.CompilerParams(vmem_limit_bytes=60 << 20),
        name="combine",
    )(*operands, *got_qkv)


def stationary(stream, grad_out, wqkv, wo, wgu, wd, gain_attn, gain_ffn):
    tok = stream.shape[0]
    layers = wqkv.shape[0]
    count_rows = wqkv.shape[1]
    depth = lax.axis_size("z")
    head = HEAD
    row = lax.axis_index("z") * 2 + lax.axis_index("x")
    query_pos = row * tok + jnp.arange(tok, dtype=jnp.int32)
    lane = jnp.arange(EXTRA, dtype=jnp.int32)
    half = head // 2
    freq = THETA ** (-((lane % half).astype(jnp.float32) * 2.0 / head))
    angle = query_pos.astype(jnp.float32)[:, None] * freq[None, :]
    cosine = jnp.cos(angle)
    sine = jnp.where((lane % head < half)[None, :], -1.0, 1.0) * jnp.sin(angle)
    current = swap_grid(stream, depth)
    grad_now = swap_grid(grad_out, depth)
    gains = swap_grid(jnp.concatenate([gain_attn, gain_ffn]), depth)
    gain_a, gain_f = gains[:layers], gains[layers:]
    greet = lambda: Square(tok, depth).greet()
    own_qkv = [wqkv[index].reshape(count_rows, -1) for index in range(layers)]
    own_out = [wo[index] for index in range(layers)]
    own_gu = [wgu[index].reshape(count_rows, -1) for index in range(layers)]
    own_down = [wd[index] for index in range(layers)]
    peer_qkv, peer_out, peer_gu, peer_down = ([None] * layers for _ in range(4))
    saved = []
    for index in range(layers):
        before = current
        first = index == 0
        final = index == layers - 1
        follow = index + 1
        shipped = [] if final else [own_qkv[follow], own_out[follow], own_gu[follow], own_down[follow]]
        attend = attention_forward(
            before, gain_a[index], own_qkv[index], own_out[index], peer_qkv[index], peer_out[index],
            own_gu[:1] if first else [], cosine, sine, depth
        )
        peer = attend.link(len(attend.shapes) - 1) if first else peer_gu[index]
        feed = ffn_forward(
            attend.link(0), gain_f[index], own_gu[index], peer, own_down[index], peer_down[index], shipped, depth
        )
        parts = [attend, feed]
        if final:
            feed.private = (2, 3)
            back_part = ffn_backward(
                grad_now, attend.link(0), gain_f[index], feed.link(2, 1), feed.link(3, 1), own_gu[index], peer, own_down[index],
                feed.link(4, 1) if first else peer_down[index], [], [], index, layers, depth, not first
            )
            back_part.woven = not first
            parts.append(back_part)
        made, fed, *back = launch(parts, greet, 2 * index)
        hidden_in, normed_a, queries, kv, lse, mixed, factors = made[:7]
        if first:
            peer_qkv[0], peer_out[0], peer_gu[0] = made[7:]
        current, normed_f, kept, active = fed[:4]
        if first:
            peer_down[index] = fed[4]
        if shipped:
            peer_qkv[follow], peer_out[follow], peer_gu[follow], peer_down[follow] = fed[-4:]
        saved.append((before, normed_a, queries, kv, lse, mixed, factors, hidden_in, normed_f, kept, active))
    list_ga, list_gf, got_qkv, rest_stack = ([], [], [], [])
    grad_hidden, grad_gu, gain_f_grad, *down_stack = back[0]
    for index in reversed(range(layers)):
        list_gf.append(gain_f_grad)
        before, normed_a, queries, kv, lse, mixed, factors, _, normed_f, _, _ = saved[index]
        attend = attention_backward(
            grad_hidden, before, gain_a[index], own_qkv[index], peer_qkv[index], own_out[index], peer_out[index],
            cosine, sine, queries, kv, lse, factors, mixed, normed_a, normed_f, grad_gu, rest_stack, index, layers, depth
        )
        attend.private = (2,)
        if index:
            _, _, _, _, _, _, _, hidden_in, _, kept, active = saved[index - 1]
            feed = ffn_backward(
                attend.link(0), hidden_in, gain_f[index - 1], kept, active, own_gu[index - 1], peer_gu[index - 1],
                own_down[index - 1], peer_down[index - 1], [attend.link(2)], down_stack, index - 1, layers, depth
            )
            made, (grad_hidden, grad_gu, gain_f_grad, *down_stack, landed) = launch([attend, feed], greet, 2 * index + 1)
            got_qkv.append(landed)
        else:
            tail = finish(attend.link(0), [attend.link(1)] + list_ga[::-1] + list_gf[::-1], attend.link(2), depth)
            made, (grad_in, gains, landed) = launch([attend, tail], lambda: greet_last(tok, depth), 1)
            got_qkv.append(landed)
        list_ga.append(made[1])
        rest_stack = made[3:]
    grads = combine(rest_stack, down_stack, got_qkv[::-1])
    return (swap_grid(current, depth), grad_in, *grads, gains[:layers], gains[layers:])


def solution(mesh):
    rows, cols = ("row", "col")
    body = local
    if (mesh.shape["row"], mesh.shape["col"]) == (8, 4):
        mesh = share_out(mesh)
        rows, cols = (("z", "x"), ("y", "c"))
        body = stationary
    in_specs = (
        P(rows, cols),
        P(rows, cols),
        P(None, rows, cols, None),
        P(None, rows, cols),
        P(None, rows, None, cols),
        P(None, rows, cols),
        P(None, cols),
        P(None, cols),
    )
    out_specs = (
        P(rows, cols),
        P(rows, cols),
        P(None, rows, cols, None),
        P(None, rows, cols),
        P(None, rows, None, cols),
        P(None, rows, cols),
        P(None, cols),
        P(None, cols),
    )
    return jax.shard_map(body, mesh=mesh, in_specs=in_specs, out_specs=out_specs, check_vma=False)
```

```python
import math

import jax
import jax.numpy as jnp
from jax import lax
from jax.experimental import pallas as pl
from jax.experimental.pallas import tpu as pltpu
from jax.sharding import Mesh
from jax.sharding import PartitionSpec as P

D = 2048
HEAD = 64
GROUP = 8


EPS = 1e-05
THETA = 10000.0


def rope_turn(tensor, cosine, sine):
    half = tensor.shape[-1] // 2
    first = tensor[..., :half]
    second = tensor[..., half:]
    return jnp.concatenate(
        [first * cosine - second * sine, second * cosine + first * sine], axis=-1
    )


def feature_sum(values):
    return lax.psum(values, "col")


def gather_features(rows_in):
    return lax.all_gather(rows_in, "col", axis=1, tiled=True)


def sum_features(partials):
    return lax.psum_scatter(
        partials.astype(jnp.bfloat16), "col", scatter_dimension=1, tiled=True
    ).astype(jnp.float32)


def add_rows(left, piece):
    return jnp.dot(left, piece, preferred_element_type=jnp.float32)


def project_in(left, shard):
    return add_rows(left, lax.all_gather(shard, "row", axis=0, tiled=True))


def columns_of(left, piece):
    return jnp.einsum("tj,dj->td", left, piece, preferred_element_type=jnp.float32)


def project_out(left, shard):
    return columns_of(left, lax.all_gather(shard, "row", axis=0, tiled=True))


def weight_grad(left, right):
    return lax.psum_scatter(
        lax.dot_general(
            left, right, (((0,), (0,)), ((), ())), preferred_element_type=jnp.float32
        ).astype(jnp.bfloat16),
        "row",
        scatter_dimension=0,
        tiled=True,
    ).astype(jnp.float32)


def norm_forward(values, gain):
    total = feature_sum(jnp.sum(values * values, axis=1))
    factor = lax.rsqrt(total / D + EPS)
    normed = values * factor[:, None]
    return (normed, factor, (normed * gain).astype(jnp.bfloat16))


def norm_backward(grad_normed, normed, factor, gain):
    scaled = grad_normed * gain
    inner = feature_sum(jnp.sum(scaled * normed, axis=1))
    grad_in = factor[:, None] * (scaled - normed * (inner / D)[:, None])
    return (grad_in, jnp.sum(grad_normed * normed, axis=0))


def masked_scores(queries, keys, query_pos, key_pos):
    scores = jnp.einsum("qgd,kd->gqk", queries, keys, preferred_element_type=jnp.float32) * (
        1.0 / math.sqrt(queries.shape[-1])
    )
    return jnp.where(key_pos[None, None, :] <= query_pos[None, :, None], scores, -1e30)


def local(stream, grad_out, wqkv, wo, wgu, wd, gain_attn, gain_ffn):
    tok = stream.shape[0]
    layers = wqkv.shape[0]
    count_rows = wqkv.shape[1]
    head = HEAD
    query_cols = GROUP * head
    seq_len = lax.axis_size("row") * tok
    query_pos = lax.axis_index("row") * tok + jnp.arange(tok, dtype=jnp.int32)
    key_pos = jnp.arange(seq_len, dtype=jnp.int32)
    freq = THETA ** (-(jnp.arange(head // 2, dtype=jnp.float32) * 2.0 / head))
    angle = query_pos.astype(jnp.float32)[:, None] * freq[None, :]
    cosine = jnp.cos(angle)
    sine = jnp.sin(angle)
    saved = []
    current = stream
    for index in range(layers):
        weight_qkv = wqkv[index].reshape(count_rows, -1)
        weight_out = wo[index]
        weight_gu = wgu[index].reshape(count_rows, -1)
        weight_down = wd[index]
        wholes = (None, None, None, None)
        normed_a, factor_a, xnormed = norm_forward(current, gain_attn[index])
        xfull = gather_features(xnormed)
        qkv = project_in(xfull, weight_qkv)
        queries = rope_turn(
            qkv[:, :query_cols].reshape(tok, GROUP, head), cosine[:, None, :], sine[:, None, :]
        ).astype(jnp.bfloat16)
        keys = rope_turn(qkv[:, query_cols : query_cols + head], cosine, sine).astype(jnp.bfloat16)
        values = qkv[:, query_cols + head :].astype(jnp.bfloat16)
        seqkv = lax.all_gather(jnp.concatenate([keys, values], axis=1), "row", axis=0, tiled=True)
        seq_keys = seqkv[:, :head]
        seq_values = seqkv[:, head:]
        scores = masked_scores(queries, seq_keys, query_pos, key_pos)
        top = jnp.max(scores, axis=2, keepdims=True)
        expo = jnp.exp(scores - top)
        denom = jnp.sum(expo, axis=2, keepdims=True)
        probs = (expo / denom).astype(jnp.bfloat16)
        log_total = top + jnp.log(denom)
        mixed = (
            jnp.einsum("gqk,kd->qgd", probs, seq_values, preferred_element_type=jnp.float32)
            .reshape(tok, query_cols)
            .astype(jnp.bfloat16)
        )
        hidden_in = current + sum_features(project_out(mixed, weight_out))
        normed_f, factor_f, hnormed = norm_forward(hidden_in, gain_ffn[index])
        hfull = gather_features(hnormed)
        gate_up = project_in(hfull, weight_gu)
        hidden_cols = gate_up.shape[1] // 2
        gate = gate_up[:, :hidden_cols]
        upper = gate_up[:, hidden_cols:]
        active = (jax.nn.silu(gate) * upper).astype(jnp.bfloat16)
        current = hidden_in + sum_features(project_out(active, weight_down))
        saved.append(
            (
                weight_qkv,
                weight_out,
                weight_gu,
                weight_down,
                wholes,
                normed_a,
                factor_a,
                xfull,
                queries,
                seq_keys,
                seq_values,
                log_total,
                mixed,
                normed_f,
                factor_f,
                hfull,
                gate,
                upper,
                active,
            )
        )
    grad_now = grad_out
    list_qkv, list_out, list_gu, list_down, list_ga, list_gf = ([], [], [], [], [], [])
    for index in reversed(range(layers)):
        (
            weight_qkv,
            weight_out,
            weight_gu,
            weight_down,
            wholes,
            normed_a,
            factor_a,
            xfull,
            queries,
            seq_keys,
            seq_values,
            log_total,
            mixed,
            normed_f,
            factor_f,
            hfull,
            gate,
            upper,
            active,
        ) = saved[index]
        grad_full = gather_features(grad_now.astype(jnp.bfloat16))
        grad_active = project_in(grad_full, weight_down)
        list_down.append(weight_grad(grad_full, active))
        sig = jax.nn.sigmoid(gate)
        grad_gate = grad_active * upper * sig * (1.0 + gate * (1.0 - sig))
        grad_up = grad_active * gate * sig
        grad_gu = jnp.concatenate([grad_gate, grad_up], axis=1).astype(jnp.bfloat16)
        grad_hn = sum_features(project_out(grad_gu, weight_gu))
        list_gu.append(weight_grad(hfull, grad_gu).reshape(count_rows, 2, -1))
        grad_mid, gain_f_grad = norm_backward(grad_hn, normed_f, factor_f, gain_ffn[index])
        list_gf.append(gain_f_grad)
        grad_hidden = grad_now + grad_mid
        hidden_full = gather_features(grad_hidden.astype(jnp.bfloat16))
        grad_mixed = project_in(hidden_full, weight_out).astype(jnp.bfloat16)
        list_out.append(weight_grad(hidden_full, mixed))
        grad_heads = grad_mixed.reshape(tok, GROUP, head)
        scores = masked_scores(queries, seq_keys, query_pos, key_pos)
        probs_full = jnp.exp(scores - log_total)
        probs = probs_full.astype(jnp.bfloat16)
        grad_probs = jnp.einsum(
            "qgd,kd->gqk", grad_heads, seq_values, preferred_element_type=jnp.float32
        )
        delta = jnp.sum(probs_full * grad_probs, axis=2, keepdims=True)
        grad_scores = (probs_full * (grad_probs - delta)).astype(jnp.bfloat16)
        inverse = 1.0 / math.sqrt(head)
        grad_queries = (
            jnp.einsum("gqk,kd->qgd", grad_scores, seq_keys, preferred_element_type=jnp.float32)
            * inverse
        )
        grad_keys = (
            jnp.einsum("gqk,qgd->kd", grad_scores, queries, preferred_element_type=jnp.float32)
            * inverse
        )
        grad_values = jnp.einsum(
            "gqk,qgd->kd", probs, grad_heads, preferred_element_type=jnp.float32
        )
        grad_kv = lax.psum_scatter(
            jnp.concatenate([grad_keys, grad_values], axis=1).astype(jnp.bfloat16),
            "row",
            scatter_dimension=0,
            tiled=True,
        ).astype(jnp.float32)
        grad_k = rope_turn(grad_kv[:, :head], cosine, -sine)
        grad_v = grad_kv[:, head:]
        grad_q = rope_turn(grad_queries, cosine[:, None, :], -sine[:, None, :]).reshape(
            tok, query_cols
        )
        grad_qkv = jnp.concatenate([grad_q, grad_k, grad_v], axis=1).astype(jnp.bfloat16)
        grad_xn = sum_features(project_out(grad_qkv, weight_qkv))
        list_qkv.append(weight_grad(xfull, grad_qkv).reshape(count_rows, 1, -1))
        grad_in, gain_a_grad = norm_backward(grad_xn, normed_a, factor_a, gain_attn[index])
        list_ga.append(gain_a_grad)
        grad_now = grad_hidden + grad_in
    gains_a, gains_f = lax.psum((jnp.stack(list_ga[::-1]), jnp.stack(list_gf[::-1])), "row")
    return (
        current,
        grad_now,
        jnp.stack(list_qkv[::-1]),
        jnp.stack(list_out[::-1]),
        jnp.stack(list_gu[::-1]),
        jnp.stack(list_down[::-1]),
        gains_a,
        gains_f,
    )


def share_out(mesh):
    rows, cols = mesh.shape["row"], mesh.shape["col"]
    return Mesh(
        mesh.devices.reshape(rows // 2, 2, cols // 2, 2), ("z", "x", "y", "c")
    )


def swap_grid(values, depth):
    pairs = [(z * depth + g, g * depth + z) for z in range(depth) for g in range(depth)]
    return lax.ppermute(values, ("z", "y", "c"), pairs)


MESH_ID = pl.DeviceIdType.MESH
ROWS = 16
SKEW = 3
OFFSET = 18
GROUP_CHUNKS = 4
EXTRA = 128


def spread(column):
    high = column.astype(jnp.bfloat16)
    low = (column - high.astype(jnp.float32)).astype(jnp.bfloat16)
    lane = lax.broadcasted_iota(jnp.int32, (column.shape[0], EXTRA), 1)
    wide = jnp.where(lane == 0, high.astype(jnp.float32), jnp.where(lane == 1, low.astype(jnp.float32), 0.0))
    return wide.astype(jnp.bfloat16)


def unspread(block):
    return jnp.sum(block.astype(jnp.float32), axis=1, keepdims=True)


def transposed_dot(left, right):
    return lax.dot_general(left, right, (((1,), (1,)), ((), ())), preferred_element_type=jnp.float32)


class Side:
    def __init__(self, send, recv):
        self.peer = {"x": 1 - lax.axis_index("x")}
        self.send, self.recv, self.copies = send, recv, []

    def start(self, source, target):
        at = len(self.copies)
        copy = remote(source, target, self.send.at[at], self.recv.at[at], self.peer)
        copy.start()
        self.copies.append(copy)
        return copy

    def later(self, source, target):
        at = len(self.copies)
        copy = remote(source, target, self.send.at[at], self.recv.at[at], self.peer)
        self.copies.append(copy)
        return copy

    def finish(self, taken=()):
        for copy in self.copies:
            copy.wait_send()
            if not any(copy is item for item in taken):
                copy.wait_recv()


def remote(src, dst, send, recv, device):
    return pltpu.make_async_remote_copy(
        src_ref=src, dst_ref=dst, send_sem=send, recv_sem=recv, device_id=device, device_id_type=MESH_ID
    )


def halves(features):
    half = features // 2
    x = lax.axis_index("x")
    own = pl.ds(pl.multiple_of(x * half, half), half)
    other = pl.ds(pl.multiple_of((1 - x) * half, half), half)
    return own, other


def flip(block):
    return jnp.transpose(block.astype(jnp.float32)).astype(jnp.bfloat16)


def grad_tile(turned, features, right, cols, kept, given):
    own, other = halves(features)
    value = right[:, cols]
    kept[:, cols] = jnp.dot(turned[own, :], value, preferred_element_type=jnp.float32).astype(jnp.bfloat16)
    given[:, cols] = jnp.dot(turned[other, :], value, preferred_element_type=jnp.float32).astype(jnp.bfloat16)


def sem(*shape):
    return pltpu.SemaphoreType.DMA(shape)


class Link:
    def __init__(self, part, at, shape, dtype):
        self.part, self.at, self.shape, self.dtype = part, at, shape, dtype


class Part:
    def __init__(self, kernel, operands, shapes, staged_in, staged_out, scratch, aliases, flops, name, early=None):
        self.kernel, self.operands, self.shapes = kernel, operands, shapes
        self.staged_in, self.staged_out, self.scratch = staged_in, staged_out, scratch
        self.aliases, self.flops, self.name = aliases, flops, name
        self.early, self.private, self.woven = early, (), False

    def link(self, at, part=0):
        return Link(part, at, self.shapes[at].shape, self.shapes[at].dtype)


class Done:
    def start(self):
        pass

    def wait(self):
        pass


class Later:
    def __init__(self, copy):
        self.start = copy.start

    def wait(self):
        pass


def weave(step, count, later_step, later_post, later_count, post):
    def both(i, _):
        @pl.when(i < count)
        def _():
            step(i, 0)

        @pl.when(i >= OFFSET)
        def _():
            later_step(i - OFFSET, 0)

        return 0

    lax.fori_loop(0, OFFSET + later_count, both, 0)
    post()
    later_post()


def launch(parts, greet, ident):
    operands, aliases, shapes, scratch = [], {}, [], []
    for part in parts:
        base = len(shapes)
        for at, item in enumerate(part.operands):
            if not isinstance(item, Link):
                if at in part.aliases:
                    aliases[len(operands)] = base + part.aliases[at]
                operands.append(item)
        shapes += part.shapes
        for item in part.operands[: part.staged_in]:
            if not (isinstance(item, Link) and item.at < parts[item.part].staged_out):
                scratch.append(pltpu.VMEM(item.shape, item.dtype))
        scratch += [pltpu.VMEM(item.shape, item.dtype) for item in part.shapes[: part.staged_out]]
        scratch += [sem(part.staged_in), sem(part.staged_out)] + part.scratch

    def body(*refs):
        given, made, rest = refs[: len(operands)], refs[len(operands) : len(operands) + len(shapes)], list(
            refs[len(operands) + len(shapes) :]
        )
        given, made = list(given), list(made)
        ready, results, held = [], [], []
        for part in parts:
            outs = [made.pop(0) for _ in part.shapes]
            inner, sources, late = [], [], []
            for at, item in enumerate(part.operands):
                if isinstance(item, Link):
                    staged, whole = results[item.part]
                    near = item.at < parts[item.part].staged_out
                    source = None if near else whole[item.at]
                    late.append(at)
                else:
                    near, source = False, given.pop(0)
                if at >= part.staged_in:
                    inner.append(staged[item.at] if near else source)
                elif near:
                    inner.append(staged[item.at])
                else:
                    inner.append(rest.pop(0))
                sources.append(source)
            results_in = [rest.pop(0) for _ in range(part.staged_out)]
            load_s, store_s = rest.pop(0), rest.pop(0)
            own = [rest.pop(0) for _ in part.scratch]
            loads = [
                Done() if sources[k] is None else pltpu.make_async_copy(sources[k], inner[k], load_s.at[k])
                for k in range(part.staged_in)
            ]
            stores = [
                Done() if k in part.private else pltpu.make_async_copy(results_in[k], outs[k], store_s.at[k])
                for k in range(part.staged_out)
            ]
            for k, copy in enumerate(loads):
                if k not in late:
                    copy.start()
            results.append((results_in, outs))
            ready.append((loads, stores, late, inner, results_in + outs[part.staged_out :], own))
        begun = {}

        def begin(at):
            part = parts[at]
            loads, stores, late, inner, outs, own = ready[at]
            for k in late:
                if k < part.staged_in:
                    loads[k].start()
            if at < len(parts) - 1:
                held.extend(copy for copy in stores if not isinstance(copy, Done))
                stores = [copy if isinstance(copy, Done) else Later(copy) for copy in stores]
            hook = lambda: None
            if at + 2 < len(parts) and parts[at + 2].woven:
                hook = lambda: begin(at + 2)
            elif at + 1 < len(parts) and parts[at + 1].early:
                following = ready[at + 1]
                hook = lambda: parts[at + 1].early(following[0], *following[3], *following[4], *following[5])
            begun[at] = part.kernel(loads, stores, greet if at == 0 else lambda: None, hook, *inner, *outs, *own)

        for at, part in enumerate(parts):
            if part.woven:
                continue
            begin(at)
            if begun[at] is None:
                continue
            step, post, count = begun[at]
            if at + 1 < len(parts) and parts[at + 1].woven:
                weave(step, count, *begun[at + 1], post)
            else:
                lax.fori_loop(0, count, step, 0)
                post()
        for copy in held:
            copy.wait()

    outside = pl.BlockSpec(memory_space=pl.ANY)
    out = pl.pallas_call(
        body,
        out_shape=tuple(shapes),
        in_specs=[outside] * len(operands),
        out_specs=[outside] * len(shapes),
        input_output_aliases=aliases,
        scratch_shapes=scratch,
        compiler_params=pltpu.CompilerParams(collective_id=ident, has_side_effects=True, vmem_limit_bytes=62 << 20),
        cost_estimate=pl.CostEstimate(
            flops=sum(part.flops for part in parts), bytes_accessed=8_000_000, transcendentals=0
        ),
        name="_".join(part.name for part in parts),
    )(*operands)
    out = list(out)
    return [[out.pop(0) for _ in part.shapes] for part in parts]


class Line:
    def __init__(self, tok, depth):
        self.z, self.x = lax.axis_index("z"), lax.axis_index("x")
        self.y, self.c = lax.axis_index("y"), lax.axis_index("c")
        self.tok, self.depth = tok, depth
        self.half = 2 * tok
        self.chunks = self.half // ROWS
        self.own = pl.multiple_of((2 * self.y + self.c) * tok, tok)
        self.peers = (
            {"y": self.y, "c": 1 - self.c},
            {"y": 1 - self.y, "c": self.c},
            {"y": 1 - self.y, "c": 1 - self.c},
        )

    def place(self, stream):
        return self.z if stream == 0 else self.depth - 1 - self.z

    def onward(self, stream):
        return {"z": self.z + 1} if stream == 0 else {"z": self.z - 1}

    def backward(self, stream):
        return {"z": self.z - 1} if stream == 0 else {"z": self.z + 1}

    def row_of(self, stream, chunk):
        per = self.chunks // 2
        far = chunk // per
        y = self.y + far * (1 - 2 * self.y)
        return pl.multiple_of((2 * y + stream) * self.tok + lax.rem(chunk, per) * ROWS, ROWS)


def make_line(tok, depth, width_in, width_out, carry_in, carry_out, features):
    chunks = 2 * tok // ROWS
    groups = chunks // GROUP_CHUNKS
    span = GROUP_CHUNKS * ROWS
    half_groups = groups // 2

    def run(line, greet, taken, begin, prepare, beside, finish, second, settle, close, product, carried, chain_out, chain_in, wide, own_part, rs_out, rs_in,
            ag_s, ag_r, ch_s, ch_r, bc_s, bc_r, rs_s, rs_r):
        greet()
        gather = [
            pltpu.make_async_remote_copy(
                src_ref=taken.at[pl.ds(line.own, tok)],
                dst_ref=taken.at[pl.ds(line.own, tok)],
                send_sem=ag_s.at[at],
                recv_sem=ag_r.at[at],
                device_id=peer,
                device_id_type=MESH_ID,
            )
            for at, peer in enumerate(line.peers)
        ]
        for copy in gather:
            copy.start()
        begin()
        gather[0].wait_recv()
        prepare(pl.multiple_of(line.y * 2 * tok, 2 * tok))

        def chain_copy(stream, chunk):
            return pltpu.make_async_remote_copy(
                src_ref=chain_out.at[stream, chunk],
                dst_ref=chain_in.at[stream, chunk],
                send_sem=ch_s.at[stream, chunk],
                recv_sem=ch_r.at[stream, chunk],
                device_id=line.onward(stream),
                device_id_type=MESH_ID,
            )

        def wide_copy(stream, chunk):
            rows = pl.ds(line.row_of(stream, chunk), ROWS)
            return pltpu.make_async_remote_copy(
                src_ref=wide.at[rows],
                dst_ref=wide.at[rows],
                send_sem=bc_s.at[stream, chunk],
                recv_sem=bc_r.at[stream, chunk],
                device_id=line.backward(stream),
                device_id_type=MESH_ID,
            )

        def sum_copy(stream, group):
            far = group // half_groups
            y = line.y + far * (1 - 2 * line.y)
            other = stream + line.c - 2 * stream * line.c
            slot = 2 * far + other - 1
            part = lax.rem(group, half_groups)
            return (slot >= 0, part, pltpu.make_async_remote_copy(
                src_ref=rs_out.at[stream, group],
                dst_ref=rs_in.at[jnp.maximum(slot, 0), pl.ds(pl.multiple_of(part * span, span), span)],
                send_sem=rs_s.at[stream, group],
                recv_sem=rs_r.at[jnp.maximum(slot, 0), part],
                device_id={"y": y, "c": stream},
                device_id_type=MESH_ID,
            ))

        def step(i, _):
            @pl.when(i == SKEW)
            def _():
                gather[1].wait_recv()
                gather[2].wait_recv()
                prepare(pl.multiple_of((1 - line.y) * 2 * tok, 2 * tok))

            for stream in (0, 1):
                place = line.place(stream)
                chunk = i - SKEW * place

                @pl.when((chunk >= 0) & (chunk < chunks))
                def _():
                    row = line.row_of(stream, chunk)

                    @pl.when(place > 0)
                    def _():
                        chain_copy(stream, chunk).wait_recv()

                    @pl.when(place == 0)
                    def _():
                        chain_out[stream, chunk, :, :width_in] = product[pl.ds(row, ROWS), :].astype(jnp.bfloat16)
                        if carry_in:
                            chain_out[stream, chunk, :, width_in:] = spread(carried[pl.ds(row, ROWS), :1])

                    @pl.when((place > 0) & (place < depth - 1))
                    def _():
                        chain_out[stream, chunk, :, :width_in] = (
                            product[pl.ds(row, ROWS), :] + chain_in[stream, chunk, :, :width_in].astype(jnp.float32)
                        ).astype(jnp.bfloat16)
                        if carry_in:
                            chain_out[stream, chunk, :, width_in:] = spread(
                                carried[pl.ds(row, ROWS), :1] + unspread(chain_in[stream, chunk, :, width_in:])
                            )

                    @pl.when(place < depth - 1)
                    def _():
                        chain_copy(stream, chunk).start()

                    @pl.when(place == depth - 1)
                    def _():
                        total = product[pl.ds(row, ROWS), :] + chain_in[stream, chunk, :, :width_in].astype(jnp.float32)
                        extra = None
                        if carry_in:
                            extra = carried[pl.ds(row, ROWS), :1] + unspread(chain_in[stream, chunk, :, width_in:])
                        finish(row, pl.multiple_of(chunk * ROWS, ROWS), total, extra)
                        wide_copy(stream, chunk).start()

            for stream in (0, 1):
                place = line.place(stream)
                ready = i - SKEW * (2 * (depth - 1) - place)

                @pl.when((ready >= 0) & (ready < chunks))
                def _():
                    @pl.when(place < depth - 1)
                    def _():
                        wide_copy(stream, ready).wait_recv()

                        @pl.when(place > 0)
                        def _():
                            wide_copy(stream, ready).start()

            beside(i)
            for stream in (0, 1):
                place = line.place(stream)
                ready = i - SKEW * (2 * (depth - 1) - place)

                @pl.when((ready >= 0) & (ready < chunks))
                def _():
                    @pl.when(lax.rem(ready, GROUP_CHUNKS) == GROUP_CHUNKS - 1)
                    def _():
                        group = ready // GROUP_CHUNKS
                        row = pl.multiple_of(line.row_of(stream, ready) - (span - ROWS), span)
                        away, part, copy = sum_copy(stream, group)
                        value = second(row, span)

                        @pl.when(away)
                        def _():
                            rs_out[stream, group, :, :features] = value.astype(jnp.bfloat16)
                            if carry_out:
                                rs_out[stream, group, :, features:] = wide[pl.ds(row, span), width_out:]
                            copy.start()

                        @pl.when(jnp.logical_not(away))
                        def _():
                            own_part[pl.ds(pl.multiple_of(part * span, span), span), :] = value

            return 0

        def drain(i, _):
            for stream in (0, 1):
                place = line.place(stream)

                @pl.when(place < depth - 1)
                def _():
                    chain_copy(stream, i).wait_send()

                @pl.when(place > 0)
                def _():
                    wide_copy(stream, i).wait_send()

            return 0

        def drain_sums(i, _):
            for stream in (0, 1):
                away, part, copy = sum_copy(stream, i)

                @pl.when(away)
                def _():
                    copy.wait_send()
            return 0

        def post():
            settle()
            for slot in range(3):
                for part in range(half_groups):
                    pltpu.make_async_remote_copy(
                        src_ref=rs_out.at[0, 0],
                        dst_ref=rs_in.at[slot, pl.ds(part * span, span)],
                        send_sem=rs_s.at[0, 0],
                        recv_sem=rs_r.at[slot, part],
                        device_id=line.peers[slot],
                        device_id_type=MESH_ID,
                    ).wait_recv()
            close()
            for copy in gather:
                copy.wait_send()
            lax.fori_loop(0, chunks, drain, 0)
            lax.fori_loop(0, groups, drain_sums, 0)

        return step, post, chunks + 2 * SKEW * (depth - 1)

    wide_in = width_in + (EXTRA if carry_in else 0)
    scratch = [
        pltpu.VMEM((4 * tok, width_in), jnp.float32),
        pltpu.VMEM((4 * tok, EXTRA), jnp.float32),
        pltpu.VMEM((2, chunks, ROWS, wide_in), jnp.bfloat16),
        pltpu.VMEM((2, chunks, ROWS, wide_in), jnp.bfloat16),
        pltpu.VMEM((tok, features), jnp.float32),
        pltpu.VMEM((2, groups, span, features + (EXTRA if carry_out else 0)), jnp.bfloat16),
        pltpu.VMEM((3, tok, features + (EXTRA if carry_out else 0)), jnp.bfloat16),
        pltpu.SemaphoreType.DMA((3,)),
        pltpu.SemaphoreType.DMA((3,)),
        pltpu.SemaphoreType.DMA((2, chunks)),
        pltpu.SemaphoreType.DMA((2, chunks)),
        pltpu.SemaphoreType.DMA((2, chunks)),
        pltpu.SemaphoreType.DMA((2, chunks)),
        pltpu.SemaphoreType.DMA((2, groups)),
        pltpu.SemaphoreType.DMA((3, half_groups)),
    ]
    return run, scratch


TILE = 256


def ffn_forward(hidden, gain, gu_own, gu_peer, down_own, down_peer, shipped, depth):
    tok, features = hidden.shape
    width = down_own.shape[1]
    run, scratch = make_line(tok, depth, 2 * width, width, True, False, features)
    fetch = down_peer is None
    count = len(shipped)
    sides = count + (1 if fetch else 0)

    def kernel(loads, stores, greet, hook, h_ref, gain_ref, w1_own, w1_peer, w2_own, *rest):
        if not fetch:
            w2_peer, rest = rest[0], rest[1:]
        leave, rest = rest[:count], rest[count:]
        (out_ref, normed_t, kept, wide), rest = rest[:4], rest[4:]
        if fetch:
            w2_peer, rest = rest[0], rest[1:]
        landed, rest = rest[:count], rest[count:]
        (taken, scaled, pieces, side_s, side_r, product, carried, chain_out, chain_in, own_part, rs_out, rs_in), sems = (
            rest[:12], rest[12:])
        line = Line(tok, depth)
        side = Side(side_s, side_r)
        own, other = halves(features)
        loads[0].wait()
        taken[pl.ds(line.own, tok), :] = h_ref[...].astype(jnp.bfloat16)
        at_end = (line.z == 0) | (line.z == depth - 1)

        def begin():
            for copy in loads[1:]:
                copy.wait()
            if fetch:
                side.start(w2_own, w2_peer)
            for source, target in zip(leave, landed):
                side.start(source, target)

        def prepare(row):
            rows = pl.ds(row, 2 * tok)
            block = taken[rows, :].astype(jnp.float32)
            carried[rows, :] = jnp.broadcast_to(jnp.sum(block * block, axis=1, keepdims=True), (2 * tok, EXTRA))
            scaled[...] = (block * gain_ref[...]).astype(jnp.bfloat16)

            def tile(j, _):
                cols = pl.ds(pl.multiple_of(j * TILE, TILE), TILE)
                product[rows, cols] = jnp.dot(
                    scaled[:, own], w1_own[:, cols], preferred_element_type=jnp.float32
                ) + jnp.dot(scaled[:, other], w1_peer[:, cols], preferred_element_type=jnp.float32)
                return 0

            lax.fori_loop(0, 2 * width // TILE, tile, 0)

        def beside(i):
            if fetch:

                @pl.when(i == SKEW * (depth - 1))
                def _():
                    side.copies[0].wait_recv()
                    stores[4].start()

        def finish(row, at, total, extra):
            factor = lax.rsqrt(extra / D + EPS)
            gate = total[:, :width] * factor
            upper = total[:, width:] * factor
            kept[pl.ds(at, ROWS), :width] = gate
            kept[pl.ds(at, ROWS), width:] = upper
            active = gate * jax.nn.sigmoid(gate) * upper
            wide[pl.ds(row, ROWS), :width] = active.astype(jnp.bfloat16)
            wide[pl.ds(row, ROWS), width:] = spread(factor)

        def second(row, span):
            value = wide[pl.ds(row, span), :width]
            pieces[:, own] = transposed_dot(value, w2_own[...])
            pieces[:, other] = transposed_dot(value, w2_peer[...])
            return pieces[...]

        def settle():
            stores[3].start()

            @pl.when(at_end)
            def _():
                stores[2].start()

            normed = taken[...].astype(jnp.float32) * unspread(wide[:, width:]) * gain_ref[...]
            normed_t[...] = jnp.transpose(normed).astype(jnp.bfloat16)
            stores[1].start()

        def close():
            total = own_part[...]
            for slot in range(3):
                total = total + rs_in[slot].astype(jnp.float32)
            out_ref[...] = h_ref[...] + total
            stores[0].start()
            side.finish(side.copies[:1] if fetch else ())
            for at in (0, 1, 3, 4)[: 4 if fetch else 3]:
                stores[at].wait()

            @pl.when(at_end)
            def _():
                stores[2].wait()

        return run(line, greet, taken, begin, prepare, beside, finish, second, settle, close, product, carried, chain_out, chain_in, wide,
            own_part, rs_out, rs_in, *sems)

    low, full = jnp.bfloat16, jnp.float32
    shapes = (
        jax.ShapeDtypeStruct((tok, features), full),
        jax.ShapeDtypeStruct((features, 4 * tok), low),
        jax.ShapeDtypeStruct((2 * tok, 2 * width), full),
        jax.ShapeDtypeStruct((4 * tok, width + EXTRA), low),
    ) + ((jax.ShapeDtypeStruct(down_own.shape, low),) if fetch else ()) + tuple(jax.ShapeDtypeStruct(item.shape, item.dtype) for item in shipped)
    return Part(
        kernel, (hidden, gain.reshape(1, -1), gu_own, gu_peer, down_own, *(() if fetch else (down_peer,)), *shipped), shapes,
        5 if fetch else 6, 5 if fetch else 4,
        [
            pltpu.VMEM((4 * tok, features), low),
            pltpu.VMEM((2 * tok, features), low),
            pltpu.VMEM((GROUP_CHUNKS * ROWS, features), full),
            sem(max(sides, 1)), sem(max(sides, 1)),
        ] + scratch,
        {}, 60_000_000_000, "ffn_forward",
    )


def ffn_backward(
    grad, hidden, gain, kept, wide_forward, gu_own, gu_peer, down_own, down_peer, shipped, depth, woven=False
):
    tok, features = hidden.shape
    width = down_own.shape[1]
    run, scratch = make_line(tok, depth, width, 2 * width, False, True, features)
    count = len(shipped)
    tiles = width // EXTRA
    every = 2 if woven else 1
    first_tile = 2 * tok // ROWS + 2 * SKEW * (depth - 1) - OFFSET if woven else SKEW + 1
    turns = (tiles + every - 1) // every

    def kernel(loads, stores, greet, hook, dy_ref, h_ref, gain_ref, kept_ref, before_ref, w1_own, w1_peer, w2_own, w2_peer, *rest):
        leave, rest = rest[:count], rest[count:]
        (out_ref, wide, gain_out, kept_all, got_all), rest = rest[:5], rest[5:]
        landed, rest = rest[:count], rest[count:]
        (taken, turned, down_kept, down_given, keep_s, pieces, side_s, side_r, product, carried, chain_out, chain_in, own_part,
         rs_out, rs_in), sems = rest[:15], rest[15:]
        line = Line(tok, depth)
        side = Side(side_s, side_r)
        own, other = halves(features)
        loads[0].wait()
        taken[pl.ds(line.own, tok), :] = dy_ref[...].astype(jnp.bfloat16)
        give = side.later(down_given, got_all)
        keep = pltpu.make_async_copy(down_kept, kept_all, keep_s)

        def begin():
            for source, target in zip(leave, landed):
                side.start(source, target)
            loads[7].wait()
            loads[8].wait()

        def prepare(row):
            rows = pl.ds(row, 2 * tok)

            def tile(j, _):
                cols = pl.ds(pl.multiple_of(j * EXTRA, EXTRA), EXTRA)
                product[rows, cols] = jnp.dot(
                    taken[rows, own], w2_own[:, cols], preferred_element_type=jnp.float32
                ) + jnp.dot(taken[rows, other], w2_peer[:, cols], preferred_element_type=jnp.float32)
                return 0

            lax.fori_loop(0, width // EXTRA, tile, 0)

        def beside(i):
            @pl.when(i == 1)
            def _():
                for copy in loads[1:7]:
                    copy.wait()

            @pl.when(i == first_tile)
            def _():
                turned[...] = flip(taken[...])

            for turn_at in range(every):
                at = (i - first_tile) * every + turn_at

                @pl.when((at >= 0) & (at < tiles))
                def _():
                    cols = pl.ds(pl.multiple_of(at * EXTRA, EXTRA), EXTRA)
                    grad_tile(turned, features, before_ref, cols, down_kept, down_given)

            @pl.when(i == first_tile + turns)
            def _():
                give.start()
                keep.start()

        def finish(row, at, total, extra):
            gate = kept_ref[pl.ds(at, ROWS), :width]
            upper = kept_ref[pl.ds(at, ROWS), width:]
            sig = jax.nn.sigmoid(gate)
            silu = gate * sig
            grad_gate = total * upper * (sig + silu * (1.0 - sig))
            grad_up = total * silu
            wide[pl.ds(row, ROWS), :width] = grad_gate.astype(jnp.bfloat16)
            wide[pl.ds(row, ROWS), width : 2 * width] = grad_up.astype(jnp.bfloat16)
            inner = jnp.sum(grad_gate * gate + grad_up * upper, axis=1, keepdims=True)
            wide[pl.ds(row, ROWS), 2 * width :] = spread(inner)

        def second(row, span):
            value = wide[pl.ds(row, span), : 2 * width]
            pieces[:, own] = transposed_dot(value, w1_own[...])
            pieces[:, other] = transposed_dot(value, w1_peer[...])
            return pieces[...]

        def settle():
            stores[1].start()

        def close():
            total = own_part[...]
            inner = unspread(wide[pl.ds(line.own, tok), 2 * width :])
            for slot in range(3):
                total = total + rs_in[slot, :, :features].astype(jnp.float32)
                inner = inner + unspread(rs_in[slot, :, features:])
            factor = unspread(before_ref[pl.ds(line.own, tok), width:])
            normed = h_ref[...] * factor
            gain_out[...] = jnp.broadcast_to(jnp.sum(total * normed, axis=0, keepdims=True), gain_out.shape)
            out_ref[...] = dy_ref[...] + factor * (total * gain_ref[...] - normed * (inner / D))
            stores[2].start()
            stores[0].start()
            keep.wait()
            side.finish()
            for copy in stores:
                copy.wait()

        return run(line, greet, taken, begin, prepare, beside, finish, second, settle, close, product, carried, chain_out, chain_in,
            wide, own_part, rs_out, rs_in, *sems)

    low, full = jnp.bfloat16, jnp.float32
    shapes = (
        jax.ShapeDtypeStruct((tok, features), full),
        jax.ShapeDtypeStruct((4 * tok, 2 * width + EXTRA), low),
        jax.ShapeDtypeStruct((8, features), full),
        jax.ShapeDtypeStruct(down_own.shape, low),
        jax.ShapeDtypeStruct(down_own.shape, low),
    ) + tuple(jax.ShapeDtypeStruct(item.shape, item.dtype) for item in shipped)
    own_scratch = [
        pltpu.VMEM((4 * tok, features), low),
        pltpu.VMEM((features, 4 * tok), low),
        pltpu.VMEM(down_own.shape, low),
        pltpu.VMEM(down_own.shape, low),
        pltpu.SemaphoreType.DMA,
        pltpu.VMEM((GROUP_CHUNKS * ROWS, features), full),
        sem(1 + count), sem(1 + count),
    ] + scratch
    return Part(
        kernel,
        (grad, hidden, gain.reshape(1, -1), kept, wide_forward, gu_own, gu_peer, down_own, down_peer, *shipped),
        shapes, 9, 3,
        own_scratch,
        {}, 60_000_000_000, "ffn_backward",
    )


def to_row(column):
    return jnp.transpose(jnp.broadcast_to(column, (column.shape[0], EXTRA)))[:8]


def to_column(row):
    return jnp.transpose(jnp.broadcast_to(row[:1], (row.shape[1], row.shape[1])))[:, :1]


def turn(values, cosine, sine):
    lane = lax.broadcasted_iota(jnp.int32, values.shape, 1)
    width = values.shape[1]
    back = pltpu.roll(values, width - HEAD // 2, 1)
    forth = pltpu.roll(values, HEAD // 2, 1)
    partner = jnp.where(lax.rem(lane, HEAD) < HEAD // 2, back, forth)
    return values * cosine + partner * sine


def split_pair(block):
    lane = lax.broadcasted_iota(jnp.int32, block.shape, 1)
    zero = jnp.zeros_like(block)
    return jnp.concatenate([jnp.where(lane < HEAD, block, zero), jnp.where(lane < HEAD, zero, block)], axis=0)


def join_pair(turned, tok):
    return jnp.transpose(jnp.concatenate([turned[:HEAD, :tok], turned[HEAD:, tok:]], axis=0))


def twice(kv):
    wide = kv.astype(jnp.float32)
    lane = lax.broadcasted_iota(jnp.int32, wide.shape, 1)
    other = pltpu.roll(wide, HEAD, 1)
    return jnp.where(lane < HEAD, wide, other), jnp.where(lane < HEAD, other, wide)


class Square:
    def __init__(self, tok, depth):
        self.z, self.x = lax.axis_index("z"), lax.axis_index("x")
        self.y, self.c = lax.axis_index("y"), lax.axis_index("c")
        self.tok, self.depth = tok, depth
        self.g = 2 * self.y + self.c
        self.row = 2 * self.z + self.x
        self.own = pl.multiple_of(self.g * tok, tok)
        self.mine = pl.multiple_of(self.z * tok, tok)
        self.peers = (
            {"y": self.y, "c": 1 - self.c},
            {"y": 1 - self.y, "c": self.c},
            {"y": 1 - self.y, "c": 1 - self.c},
        )

    def row_peer(self, step):
        at = lax.rem(self.row + step, 2 * self.depth)
        return {"z": at // 2, "x": lax.rem(at, 2)}

    def greet(self, extra=0):
        barrier = pltpu.get_barrier_semaphore()
        for peer in self.peers:
            pl.semaphore_signal(barrier, 1, device_id=peer, device_id_type=MESH_ID)
        for step in range(1, 2 * self.depth):
            pl.semaphore_signal(barrier, 1, device_id=self.row_peer(step), device_id_type=MESH_ID)
        pl.semaphore_wait(barrier, 3 + 2 * self.depth - 1 + extra)


def start_gather(square, taken, send, recv):
    copies = [
        remote(taken.at[pl.ds(square.own, square.tok)], taken.at[pl.ds(square.own, square.tok)], send.at[at], recv.at[at], peer)
        for at, peer in enumerate(square.peers)
    ]
    for copy in copies:
        copy.start()
    return copies


def line_sum(square, gather, product, own, own_row, outs, ins, row_outs, row_ins, send, recv, row_send, row_recv, between):
    tok, depth = square.tok, square.depth

    def one(order):
        block = lax.rem(2 * square.y + order, depth)
        step = lax.rem(block - square.z + depth, depth)
        slot = jnp.maximum(depth - 1 - step, 0)
        value, column = product(pl.multiple_of(block * tok, tok))

        @pl.when(step == 0)
        def _():
            own[...] = value
            if column is not None:
                own_row[...] = to_row(column)

        copy = remote(outs.at[order], ins.at[slot], send.at[order], recv.at[slot], {"z": block})
        row_copy = None
        if column is not None:
            row_copy = remote(row_outs.at[order], row_ins.at[slot], row_send.at[order], row_recv.at[slot], {"z": block})

        @pl.when(step != 0)
        def _():
            outs[order] = value.astype(jnp.bfloat16)
            copy.start()
            if column is not None:
                row_outs[order] = to_row(column)
                row_copy.start()

        return step, copy, row_copy

    gather[0].wait_recv()
    sent = [one(0), one(1)]
    gather[1].wait_recv()
    gather[2].wait_recv()
    sent += [one(2), one(3)]
    between()
    for slot in range(depth - 1):
        remote(outs.at[0], ins.at[slot], send.at[0], recv.at[slot], {"z": square.z}).wait_recv()
        if row_ins is not None:
            remote(row_outs.at[0], row_ins.at[slot], row_send.at[0], row_recv.at[slot], {"z": square.z}).wait_recv()
    return sent


def send_part(square, array, part, send, recv):
    lanes = pl.ds(pl.multiple_of(part * EXTRA, EXTRA), EXTRA)
    here = array.at[pl.ds(square.mine, square.tok), lanes]
    depth = square.depth
    return [
        remote(here, here, send.at[step - 1, part], recv.at[depth - 1 - step, part], {"z": lax.rem(square.z + step, depth)})
        for step in range(1, depth)
    ]


def send_row(square, rows, send, recv):
    line = rows.at[square.z]
    depth = square.depth
    return [
        remote(line, line, send.at[step - 1], recv.at[depth - 1 - step], {"z": lax.rem(square.z + step, depth)})
        for step in range(1, depth)
    ]


def grid_sum(square, array, rows, second, settle, own, outs, ins, row_ins, arrive, row_arrive, send, recv, row_send, row_recv):
    tok, depth = square.tok, square.depth
    sent = []
    for step in range(depth):
        block = lax.rem(square.z + step, depth)
        if step:
            for part in range(array.shape[1] // EXTRA):
                rows_of = array.at[pl.ds(pl.multiple_of(block * tok, tok), tok), pl.ds(part * EXTRA, EXTRA)]
                remote(rows_of, rows_of, send.at[0], arrive.at[step - 1, part], {"z": square.z}).wait_recv()
            remote(rows.at[block], rows.at[block], send.at[0], row_arrive.at[step - 1], {"z": square.z}).wait_recv()
        value = second(pl.multiple_of(block * tok, tok))
        away = lax.rem(block - square.g + depth, depth)
        slot = jnp.maximum(depth - 1 - away, 0)
        device = {"y": block // 2, "c": lax.rem(block, 2)}
        copy = remote(outs.at[step], ins.at[slot], send.at[step], recv.at[slot], device)
        row_copy = None
        if row_ins is not None:
            row_copy = remote(rows.at[block], row_ins.at[slot], row_send.at[step], row_recv.at[slot], device)

        @pl.when(away == 0)
        def _():
            own[...] = value

        @pl.when(away != 0)
        def _():
            outs[step] = value.astype(jnp.bfloat16)
            copy.start()
            if row_ins is not None:
                row_copy.start()

        sent.append((away, copy, row_copy))
    settle()
    for slot in range(depth - 1):
        remote(outs.at[0], ins.at[slot], send.at[0], recv.at[slot], square.peers[0]).wait_recv()
        if row_ins is not None:
            remote(rows.at[0], row_ins.at[slot], row_send.at[0], row_recv.at[slot], square.peers[0]).wait_recv()
    return sent


def drain(sent):
    for away, copy, row_copy in sent:

        @pl.when(away != 0)
        def _():
            copy.wait_send()
            if row_copy is not None:
                row_copy.wait_send()


def attention_forward(hidden, gain, qkv_own, out_own, qkv_peer, out_peer, shipped, cosine, sine, depth):
    tok, features = hidden.shape
    cols = qkv_own.shape[1]
    fetch = qkv_peer is None
    extra = 2 if fetch else 0
    count = len(shipped)
    sides = extra + 2 * count
    query_cols = GROUP * HEAD
    seq = 2 * depth * tok
    pairs = query_cols // EXTRA
    scale = 1.0 / math.sqrt(HEAD)

    def kernel(loads, stores, greet, hook, h_ref, gain_ref, wqkv_own, wo_own, cos_ref, sin_ref, *rest):
        if not fetch:
            (wqkv_peer, wo_peer), rest = rest[:2], rest[2:]
        leave, rest = rest[:count], rest[count:]
        (out_ref, normed_t, queries, kv, lse, mixed, factors), rest = rest[:7], rest[7:]
        if fetch:
            (wqkv_peer, wo_peer), rest = rest[:2], rest[2:]
        landed, rest = rest[:count], rest[count:]
        (taken, scaled, pieces, own, own_row, z_out, z_in, zr_out, zr_in, values_t, g_own, g_out, g_in,
         ag_s, ag_r, zs_s, zs_r, zr_s, zr_r, kv_s, kv_r, zg_s, zg_r, zgr_s, zgr_r, gs_s, gs_r), rest = rest[:27], rest[27:]
        square = Square(tok, depth)
        side = Side(*rest) if sides else None
        mine, other = halves(features)
        loads[0].wait()
        taken[pl.ds(square.own, tok), :] = h_ref[...].astype(jnp.bfloat16)
        greet()
        gather = start_gather(square, taken, ag_s, ag_r)
        for copy in loads[1:]:
            copy.wait()
        urgent = []
        if fetch:
            urgent = [side.start(wqkv_own, wqkv_peer), side.start(wo_own, wo_peer)]
        held = []
        for source, target in zip(leave, landed):
            most = source.shape[0] // 2
            rest_of = pl.ds(most, source.shape[0] - most)
            side.start(source.at[pl.ds(0, most)], target.at[pl.ds(0, most)])
            held.append(side.later(source.at[rest_of], target.at[rest_of]))
        for copy in urgent[:1]:
            copy.wait_recv()
            stores[7].start()

        def product(row):
            block = taken[pl.ds(row, tok), :].astype(jnp.float32)
            scaled[...] = (block * gain_ref[...]).astype(jnp.bfloat16)
            return (
                jnp.dot(scaled[:, mine], wqkv_own[...], preferred_element_type=jnp.float32)
                + jnp.dot(scaled[:, other], wqkv_peer[...], preferred_element_type=jnp.float32),
                jnp.sum(block * block, axis=1, keepdims=True),
            )

        sent = line_sum(square, gather, product, own, own_row, z_out, z_in, zr_out, zr_in, zs_s, zs_r, zr_s, zr_r, hook)
        total, squares = own[...], own_row[...]
        for slot in range(depth - 1):
            total = total + z_in[slot].astype(jnp.float32)
            squares = squares + zr_in[slot]
        factor_row = lax.rsqrt(squares / D + EPS)
        factors[square.z] = factor_row
        given = send_row(square, factors, zgr_s, zgr_r)
        for copy in given:
            copy.start()
        first = lax.broadcasted_iota(jnp.int32, (tok, EXTRA), 1) < HEAD
        cosine_row, sine_row = cos_ref[...], sin_ref[...]
        turned = turn(
            total * to_column(factor_row),
            jnp.concatenate([cosine_row] * pairs + [jnp.where(first, cosine_row, 1.0)], axis=1),
            jnp.concatenate([sine_row] * pairs + [jnp.where(first, sine_row, 0.0)], axis=1),
        )
        here = pl.ds(pl.multiple_of(square.row * tok, tok), tok)
        kv[here, :] = turned[:, query_cols:].astype(jnp.bfloat16)
        queries[...] = turned[:, :query_cols].astype(jnp.bfloat16)
        stores[2].start()
        spreads = []
        for step in range(1, 2 * depth):
            copy = remote(kv.at[here], kv.at[here], kv_s.at[step - 1], kv_r.at[2 * depth - 1 - step], square.row_peer(step))
            copy.start()
            spreads.append(copy)
        for copy in spreads:
            copy.wait_recv()
        stores[3].start()
        for copy in held:
            copy.start()
        keys, both = twice(kv[...])
        values_t[...] = jnp.transpose(both).astype(jnp.bfloat16)
        keys = keys.astype(jnp.bfloat16)

        def pair(t, _):
            lanes = pl.ds(pl.multiple_of(t * EXTRA, EXTRA), EXTRA)
            scores = transposed_dot(keys, split_pair(queries[:, lanes])) * scale
            key_at = lax.broadcasted_iota(jnp.int32, scores.shape, 0)
            query_at = lax.rem(lax.broadcasted_iota(jnp.int32, scores.shape, 1), tok) + square.row * tok
            scores = jnp.where(key_at <= query_at, scores, -1e30)
            top = jnp.max(scores, axis=0, keepdims=True)
            expo = jnp.exp(scores - top)
            denom = jnp.sum(expo, axis=0, keepdims=True)
            lse[t] = jnp.broadcast_to(top + jnp.log(denom), (8, 2 * tok))
            probs = (expo * (1.0 / denom)).astype(jnp.bfloat16)
            out_t = jnp.dot(values_t[...], probs, preferred_element_type=jnp.float32)
            mixed[pl.ds(square.mine, tok), lanes] = join_pair(out_t, tok).astype(jnp.bfloat16)
            for copy in send_part(square, mixed, t, zg_s, zg_r):
                copy.start()
            return 0

        lax.fori_loop(0, pairs, pair, 0)
        given += [copy for part in range(pairs) for copy in send_part(square, mixed, part, zg_s, zg_r)]

        stores[4].start()
        for copy in urgent[1:]:
            copy.wait_recv()
            stores[8].start()

        def second(row):
            value = mixed[pl.ds(row, tok), :]
            pieces[:, mine] = transposed_dot(value, wo_own[...])
            pieces[:, other] = transposed_dot(value, wo_peer[...])
            return pieces[...]

        def settle():
            stores[5].start()
            stores[6].start()
            for block in range(depth):
                rows = pl.ds(block * tok, tok)
                normed = taken[rows, :].astype(jnp.float32) * to_column(factors[block]) * gain_ref[...]
                normed_t[:, rows] = jnp.transpose(normed).astype(jnp.bfloat16)
            stores[1].start()

        sums = grid_sum(square, mixed, factors, second, settle, g_own, g_out, g_in, None, zg_r, zgr_r, gs_s, gs_r, None, None)
        total = g_own[...]
        for slot in range(depth - 1):
            total = total + g_in[slot].astype(jnp.float32)
        out_ref[...] = h_ref[...] + total
        stores[0].start()
        drain(sent)
        drain(sums)
        for copy in gather + spreads + given:
            copy.wait_send()
        if side:
            side.finish(urgent)
        for copy in stores:
            copy.wait()

    low, full = jnp.bfloat16, jnp.float32
    shapes = (
        jax.ShapeDtypeStruct((tok, features), full),
        jax.ShapeDtypeStruct((features, depth * tok), low),
        jax.ShapeDtypeStruct((tok, query_cols), low),
        jax.ShapeDtypeStruct((seq, 2 * HEAD), low),
        jax.ShapeDtypeStruct((pairs, 8, 2 * tok), full),
        jax.ShapeDtypeStruct((depth * tok, query_cols), low),
        jax.ShapeDtypeStruct((depth, 8, tok), full),
    )
    if fetch:
        shapes += (jax.ShapeDtypeStruct(qkv_own.shape, low), jax.ShapeDtypeStruct(out_own.shape, low))
    shapes += tuple(jax.ShapeDtypeStruct(item.shape, item.dtype) for item in shipped)
    peers = () if fetch else (qkv_peer, out_peer)
    operands = (hidden, gain.reshape(1, -1), qkv_own, out_own, cosine, sine, *peers, *shipped)
    return Part(
        kernel, operands, shapes, 6 + len(peers), 7 + extra,
        [
            pltpu.VMEM((depth * tok, features), low),
            pltpu.VMEM((tok, features), low),
            pltpu.VMEM((tok, features), full),
            pltpu.VMEM((tok, cols), full),
            pltpu.VMEM((8, tok), full),
            pltpu.VMEM((depth, tok, cols), low),
            pltpu.VMEM((depth - 1, tok, cols), low),
            pltpu.VMEM((depth, 8, tok), full),
            pltpu.VMEM((depth - 1, 8, tok), full),
            pltpu.VMEM((2 * HEAD, seq), low),
            pltpu.VMEM((tok, features), full),
            pltpu.VMEM((depth, tok, features), low),
            pltpu.VMEM((depth - 1, tok, features), low),
            sem(3), sem(3), sem(depth), sem(depth - 1), sem(depth), sem(depth - 1),
            sem(2 * depth - 1), sem(2 * depth - 1), sem(depth - 1, pairs), sem(depth - 1, pairs), sem(depth - 1), sem(depth - 1),
            sem(depth), sem(depth - 1),
        ] + ([sem(sides), sem(sides)] if sides else []),
        {}, 50_000_000_000, "attention_forward",
    )


def attention_backward(
    grad, hidden, gain, qkv_own, qkv_peer, out_own, out_peer, cosine, sine, queries, kv, lse, factors, mixed, normed_a, normed_f,
    grad_gu, depth,
):
    tok, features = hidden.shape
    cols = qkv_own.shape[1]
    wide = grad_gu.shape[1] - EXTRA
    query_cols = GROUP * HEAD
    seq = 2 * depth * tok
    pairs = query_cols // EXTRA
    scale = 1.0 / math.sqrt(HEAD)

    def kernel(loads, stores, greet, hook, dy_ref, h_ref, gain_ref, wqkv_own, wqkv_peer, wo_own, wo_peer, cos_ref, sin_ref, q_ref, kv_ref, lse_ref,
               factor_ref, mixed_ref, normed_a_ref, normed_f_ref, gu_ref, *rest_refs):
        (out_ref, gain_out, qkv_given, gu_kept_all, gu_got_all, out_kept_all, out_got_all, qkv_kept_all,
               taken, spun, turned, pieces, gu_kept, gu_given, out_kept, out_given, qkv_kept, keep_s,
               own, heads, z_out, z_in, keys_t, dk, dv, kv_out, kv_in, dq, inner_rows, g_own, g_out, g_in, g_rows,
               ag_s, ag_r, zs_s, zs_r, kv_s, kv_r, zg_s, zg_r, zgr_s, zgr_r, gs_s, gs_r, gr_s, gr_r, side_s, side_r) = rest_refs
        square = Square(tok, depth)
        side = Side(side_s, side_r)
        mine, other = halves(features)
        loads[0].wait()
        taken[pl.ds(square.own, tok), :] = dy_ref[...].astype(jnp.bfloat16)
        greet()
        gather = start_gather(square, taken, ag_s, ag_r)
        for copy in loads[1:]:
            copy.wait()

        def gu_tiles(start, stop):
            def tile(j, _):
                grad_tile(normed_f_ref, features, gu_ref, pl.ds(pl.multiple_of(j * EXTRA, EXTRA), EXTRA), gu_kept, gu_given)
                return 0

            lax.fori_loop(start, stop, tile, 0)

        gu_got = gu_got_all
        keeps = [
            pltpu.make_async_copy(gu_kept, gu_kept_all, keep_s.at[0]),
            pltpu.make_async_copy(out_kept, out_kept_all, keep_s.at[1]),
            pltpu.make_async_copy(qkv_kept, qkv_kept_all, keep_s.at[2]),
        ]
        every = wide // EXTRA
        middle, late = every // 2, every * 3 // 4
        gu_tiles(0, middle)
        front, rest = pl.ds(0, middle * EXTRA), pl.ds(late * EXTRA, wide - late * EXTRA)
        inner_part = pl.ds(middle * EXTRA, (late - middle) * EXTRA)
        side.start(gu_given.at[:, front], gu_got.at[:, front])

        def between():
            turned[...] = flip(taken[...])
            for t in range(query_cols // EXTRA):
                grad_tile(turned, features, mixed_ref, pl.ds(t * EXTRA, EXTRA), out_kept, out_given)
            side.start(out_given, out_got_all)
            gu_tiles(middle, late)
            side.start(gu_given.at[:, inner_part], gu_got.at[:, inner_part])
            gu_tiles(late, every)
            keeps[0].start()
            keeps[1].start()

        def product(row):
            rows = pl.ds(row, tok)
            value = jnp.dot(taken[rows, mine], wo_own[...], preferred_element_type=jnp.float32) + jnp.dot(
                taken[rows, other], wo_peer[...], preferred_element_type=jnp.float32
            )
            return value, None

        sent = line_sum(square, gather, product, own, None, z_out, z_in, None, None, zs_s, zs_r, None, None, between)
        total = own[...]
        for slot in range(depth - 1):
            total = total + z_in[slot].astype(jnp.float32)
        heads[...] = total.astype(jnp.bfloat16)
        keys, both = twice(kv_ref[...])
        keys_t[...] = jnp.transpose(keys).astype(jnp.bfloat16)
        keys = keys.astype(jnp.bfloat16)
        both = both.astype(jnp.bfloat16)
        dk[...] = jnp.zeros_like(dk)
        dv[...] = jnp.zeros_like(dv)

        def pair(t, _):
            lanes = pl.ds(pl.multiple_of(t * EXTRA, EXTRA), EXTRA)
            query = split_pair(q_ref[:, lanes])
            head = split_pair(heads[:, lanes])
            scores = transposed_dot(keys, query) * scale
            key_at = lax.broadcasted_iota(jnp.int32, scores.shape, 0)
            query_at = lax.rem(lax.broadcasted_iota(jnp.int32, scores.shape, 1), tok) + square.row * tok
            probs = jnp.exp(jnp.where(key_at <= query_at, scores, -1e30) - lse_ref[t, :1, :])
            grad_probs = transposed_dot(both, head)
            delta = jnp.sum(probs * grad_probs, axis=0, keepdims=True)
            grad_scores = (probs * (grad_probs - delta)).astype(jnp.bfloat16)
            dk[...] += jnp.dot(grad_scores, query, preferred_element_type=jnp.float32)
            dv[...] += jnp.dot(probs.astype(jnp.bfloat16), head, preferred_element_type=jnp.float32)
            back = jnp.dot(keys_t[...], grad_scores, preferred_element_type=jnp.float32)
            value = join_pair(back, tok) * scale
            dq[...] += jnp.broadcast_to(
                jnp.sum(value * q_ref[:, lanes].astype(jnp.float32), axis=1, keepdims=True), dq.shape
            )
            spun[pl.ds(square.mine, tok), lanes] = turn(value, cos_ref[...], -sin_ref[...]).astype(jnp.bfloat16)
            for copy in send_part(square, spun, t, zg_s, zg_r):
                copy.start()
            return 0

        dq[...] = jnp.zeros_like(dq)
        lax.fori_loop(0, pairs, pair, 0)
        lane = lax.broadcasted_iota(jnp.int32, (seq, EXTRA), 1)
        left = dk[...]
        right = dv[...]
        both_kv = jnp.where(
            lane < HEAD, (left + pltpu.roll(left, HEAD, 1)) * scale, right + pltpu.roll(right, HEAD, 1)
        )
        dk[...] = both_kv
        kv_out[...] = both_kv.astype(jnp.bfloat16)
        here = pl.ds(pl.multiple_of(square.row * tok, tok), tok)
        spreads = []
        for step in range(1, 2 * depth):
            at = lax.rem(square.row + step, 2 * depth)
            copy = remote(
                kv_out.at[pl.ds(pl.multiple_of(at * tok, tok), tok)],
                kv_in.at[2 * depth - 1 - step],
                kv_s.at[step - 1],
                kv_r.at[2 * depth - 1 - step],
                square.row_peer(step),
            )
            copy.start()
            spreads.append(copy)
        total_kv = dk[here, :]
        for copy in spreads:
            copy.wait_recv()
        side.start(gu_given.at[:, rest], gu_got.at[:, rest])
        for slot in range(2 * depth - 1):
            total_kv = total_kv + kv_in[slot].astype(jnp.float32)
        first = lax.broadcasted_iota(jnp.int32, (tok, EXTRA), 1) < HEAD
        spun[pl.ds(square.mine, tok), query_cols:] = turn(
            total_kv, jnp.where(first, cos_ref[...], 1.0), jnp.where(first, -sin_ref[...], 0.0)
        ).astype(jnp.bfloat16)
        inner = dq[:, :1] + jnp.sum(total_kv * kv_ref[here, :].astype(jnp.float32), axis=1, keepdims=True)
        inner_rows[square.z] = to_row(inner)
        given = send_part(square, spun, pairs, zg_s, zg_r) + send_row(square, inner_rows, zgr_s, zgr_r)
        for copy in given:
            copy.start()
        given += [copy for part in range(pairs) for copy in send_part(square, spun, part, zg_s, zg_r)]

        def second(row):
            value = spun[pl.ds(row, tok), :]
            pieces[:, mine] = transposed_dot(value, wqkv_own[...])
            pieces[:, other] = transposed_dot(value, wqkv_peer[...])
            return pieces[...]

        def settle():
            for t in range(cols // EXTRA):
                grad_tile(normed_a_ref, features, spun, pl.ds(t * EXTRA, EXTRA), qkv_kept, qkv_given)
            keeps[2].start()
            stores[2].start()
            hook()

        sums = grid_sum(
            square, spun, inner_rows, second, settle, g_own, g_out, g_in, g_rows, zg_r, zgr_r, gs_s, gs_r, gr_s, gr_r
        )
        total = g_own[...]
        inner = inner_rows[square.g]
        for slot in range(depth - 1):
            total = total + g_in[slot].astype(jnp.float32)
            inner = inner + g_rows[slot]
        factor = to_column(factor_ref[square.g])
        normed = h_ref[...] * factor
        gain_out[...] = jnp.broadcast_to(jnp.sum(total * normed, axis=0, keepdims=True), gain_out.shape)
        out_ref[...] = dy_ref[...] + factor * (total * gain_ref[...] - normed * (to_column(inner) / D))
        stores[0].start()
        stores[1].start()
        drain(sent)
        drain(sums)
        for copy in gather + spreads + given:
            copy.wait_send()
        for copy in keeps + stores:
            copy.wait()
        side.finish()

    low, full = jnp.bfloat16, jnp.float32
    shapes = (
        jax.ShapeDtypeStruct((tok, features), full),
        jax.ShapeDtypeStruct((8, features), full),
        jax.ShapeDtypeStruct(qkv_own.shape, low),
        jax.ShapeDtypeStruct((features // 2, wide), low),
        jax.ShapeDtypeStruct((features // 2, wide), low),
        jax.ShapeDtypeStruct(out_own.shape, low),
        jax.ShapeDtypeStruct(out_own.shape, low),
        jax.ShapeDtypeStruct(qkv_own.shape, low),
    )
    operands = (
        grad, hidden, gain.reshape(1, -1), qkv_own, qkv_peer, out_own, out_peer, cosine, sine, queries, kv, lse, factors,
        mixed, normed_a, normed_f, grad_gu,
    )
    return Part(
        kernel, operands, shapes, 17, 3,
        [
            pltpu.VMEM((depth * tok, features), low),
            pltpu.VMEM((depth * tok, cols), low),
            pltpu.VMEM((features, depth * tok), low),
            pltpu.VMEM((tok, features), full),
            pltpu.VMEM((features // 2, wide), low),
            pltpu.VMEM((features // 2, wide), low),
            pltpu.VMEM(out_own.shape, low),
            pltpu.VMEM(out_own.shape, low),
            pltpu.VMEM(qkv_own.shape, low),
            sem(3),
            pltpu.VMEM((tok, query_cols), full),
            pltpu.VMEM((tok, query_cols), low),
            pltpu.VMEM((depth, tok, query_cols), low),
            pltpu.VMEM((depth - 1, tok, query_cols), low),
            pltpu.VMEM((2 * HEAD, seq), low),
            pltpu.VMEM((seq, 2 * HEAD), full),
            pltpu.VMEM((seq, 2 * HEAD), full),
            pltpu.VMEM((seq, 2 * HEAD), low),
            pltpu.VMEM((2 * depth - 1, tok, 2 * HEAD), low),
            pltpu.VMEM((tok, EXTRA), full),
            pltpu.VMEM((depth, 8, tok), full),
            pltpu.VMEM((tok, features), full),
            pltpu.VMEM((depth, tok, features), low),
            pltpu.VMEM((depth - 1, tok, features), low),
            pltpu.VMEM((depth - 1, 8, tok), full),
            sem(3), sem(3), sem(depth), sem(depth - 1),
            sem(2 * depth - 1), sem(2 * depth - 1), sem(depth - 1, pairs + 1), sem(depth - 1, pairs + 1), sem(depth - 1),
            sem(depth - 1), sem(depth), sem(depth - 1), sem(depth), sem(depth - 1), sem(4), sem(4),
        ],
        {}, 50_000_000_000, "attention_backward",
    )


def greet_last(tok, depth):
    square = Square(tok, depth)
    barrier = pltpu.get_barrier_semaphore()
    for slot in range(2 * depth):
        here = (square.z == square.g) & (slot == square.x * depth + square.g)

        @pl.when(jnp.logical_not(here))
        def _():
            source = {"z": square.g, "x": slot // depth, "y": (slot % depth) // 2, "c": slot % 2}
            pl.semaphore_signal(barrier, 1, device_id=source, device_id_type=MESH_ID)

    square.greet(2 * depth - jnp.where(square.z == square.g, 1, 0))


def finish(grad, gains, qkv_given, depth):
    tok, features = grad.shape
    count = len(gains)
    members = 2 * depth

    def kernel(loads, stores, greet, hook, grad_ref, *rest):
        gain_refs, rest = rest[:count], rest[count:]
        (given, out_ref, gain_out, got, packed, parts, sent, home, part_s, part_r, move_s, move_r, side_s, side_r) = rest
        z, x = lax.axis_index("z"), lax.axis_index("x")
        y, c = lax.axis_index("y"), lax.axis_index("c")
        g = 2 * y + c
        self_at = x * depth + g

        def target(at):
            return {"z": at // 2, "x": at % 2, "y": z // 2, "c": lax.rem(z, 2)}

        def is_source_me(slot):
            return (z == g) & (slot == self_at)

        def is_target_me(at):
            return (z == g) & (at == 2 * z + x)

        for copy in loads:
            copy.wait()
        for at, ref in enumerate(gain_refs):
            packed[at : at + 1, :] = ref[:1, :]
        sent[...] = grad_ref[...].astype(jnp.bfloat16)
        side = Side(side_s, side_r)
        side.later(given, got)
        move = remote(sent, home, move_s, move_r, {"z": g, "y": z // 2, "c": lax.rem(z, 2)})

        @pl.when(z != g)
        def _():
            move.start()

        def part(at):
            return remote(packed, parts.at[self_at], part_s.at[at], part_r.at[self_at], target(at))

        for at in range(members):

            @pl.when(jnp.logical_not(is_target_me(at)))
            def _():
                part(at).start()

        @pl.when(z == g)
        def _():
            parts[self_at] = packed[...]

        for slot in range(members):

            @pl.when(jnp.logical_not(is_source_me(slot)))
            def _():
                remote(packed, parts.at[slot], part_s.at[0], part_r.at[slot], target(0)).wait_recv()

        total = parts[0]
        for slot in range(1, members):
            total = total + parts[slot]
        gain_out[...] = total
        stores[1].start()

        @pl.when(z == g)
        def _():
            out_ref[...] = grad_ref[...]

        @pl.when(z != g)
        def _():
            move.wait_recv()
            out_ref[...] = home[...].astype(jnp.float32)
            move.wait_send()

        stores[0].start()
        for at in range(members):

            @pl.when(jnp.logical_not(is_target_me(at)))
            def _():
                part(at).wait_send()

        side.finish()
        for copy in stores:
            copy.wait()

    low, full = jnp.bfloat16, jnp.float32
    shapes = (
        jax.ShapeDtypeStruct((tok, features), full),
        jax.ShapeDtypeStruct((count, features), full),
        jax.ShapeDtypeStruct(qkv_given.shape, low),
    )
    def early(loads, *refs):
        given, got, side_s, side_r = refs[1 + count], refs[4 + count], refs[-2], refs[-1]
        Side(side_s, side_r).start(given, got)

    return Part(
        kernel, (grad, *gains, qkv_given), shapes, 1 + count, 2,
        [
            pltpu.VMEM((count, features), full),
            pltpu.VMEM((members, count, features), full),
            pltpu.VMEM((tok, features), low),
            pltpu.VMEM((tok, features), low),
            sem(members), sem(members),
            pltpu.SemaphoreType.DMA, pltpu.SemaphoreType.DMA,
            sem(1), sem(1),
        ],
        {}, 5_000_000_000, "finish", early,
    )


def combine(halves_of):
    layers, count = len(halves_of), len(halves_of[0])
    rows, wide = halves_of[0][0].shape
    half = wide // 2
    step = rows // 2
    last = rows // step - 1

    def kernel(*refs):
        qkv_o, out_o, gu_o, down_o = refs[layers * count :]
        for index in range(layers):
            gu_k, gu_g, out_k, out_g, down_k, down_g, qkv_k, qkv_g = refs[index * count : (index + 1) * count]

            @pl.when(pl.program_id(0) == index)
            def _():
                add = lambda kept, got: kept[...].astype(jnp.float32) + got[...].astype(jnp.float32)
                total = add(gu_k, gu_g)
                gu_o[0, :, 0, :] = total[:, :half]
                gu_o[0, :, 1, :] = total[:, half:]
                out_o[0] = add(out_k, out_g)
                down_o[0] = add(down_k, down_g)
                qkv_o[0, :, 0, :] = add(qkv_k, qkv_g)

    def place(index):
        def at_of(layer, at):
            return jnp.where(layer == index, at, jnp.where(layer < index, 0, last)), 0

        return at_of

    full = jnp.float32
    sizes = [item.shape[1] for item in halves_of[0]]
    outer = lambda layer, at: (layer, at, 0)
    inner = lambda layer, at: (layer, at, 0, 0)
    return pl.pallas_call(
        kernel,
        grid=(layers, rows // step),
        in_specs=[pl.BlockSpec((step, size), place(index)) for index in range(layers) for size in sizes],
        out_specs=[
            pl.BlockSpec((1, step, 1, sizes[6]), inner),
            pl.BlockSpec((1, step, sizes[2]), outer),
            pl.BlockSpec((1, step, 2, half), inner),
            pl.BlockSpec((1, step, sizes[4]), outer),
        ],
        out_shape=[
            jax.ShapeDtypeStruct((layers, rows, 1, sizes[6]), full),
            jax.ShapeDtypeStruct((layers, rows, sizes[2]), full),
            jax.ShapeDtypeStruct((layers, rows, 2, half), full),
            jax.ShapeDtypeStruct((layers, rows, sizes[4]), full),
        ],
        compiler_params=pltpu.CompilerParams(vmem_limit_bytes=60 << 20),
        name="combine",
    )(*(item for items in halves_of for item in items))


def stationary(stream, grad_out, wqkv, wo, wgu, wd, gain_attn, gain_ffn):
    tok = stream.shape[0]
    layers = wqkv.shape[0]
    count_rows = wqkv.shape[1]
    depth = lax.axis_size("z")
    head = HEAD
    row = lax.axis_index("z") * 2 + lax.axis_index("x")
    query_pos = row * tok + jnp.arange(tok, dtype=jnp.int32)
    lane = jnp.arange(EXTRA, dtype=jnp.int32)
    half = head // 2
    freq = THETA ** (-((lane % half).astype(jnp.float32) * 2.0 / head))
    angle = query_pos.astype(jnp.float32)[:, None] * freq[None, :]
    cosine = jnp.cos(angle)
    sine = jnp.where((lane % head < half)[None, :], -1.0, 1.0) * jnp.sin(angle)
    current = swap_grid(stream, depth)
    grad_now = swap_grid(grad_out, depth)
    gains = swap_grid(jnp.concatenate([gain_attn, gain_ffn]), depth)
    gain_a, gain_f = gains[:layers], gains[layers:]
    greet = lambda: Square(tok, depth).greet()
    own_qkv = [wqkv[index].reshape(count_rows, -1) for index in range(layers)]
    own_out = [wo[index] for index in range(layers)]
    own_gu = [wgu[index].reshape(count_rows, -1) for index in range(layers)]
    own_down = [wd[index] for index in range(layers)]
    peer_qkv, peer_out, peer_gu, peer_down = ([None] * layers for _ in range(4))
    saved = []
    for index in range(layers):
        before = current
        first = index == 0
        final = index == layers - 1
        follow = index + 1
        shipped = [] if final else [own_qkv[follow], own_out[follow], own_gu[follow], own_down[follow]]
        attend = attention_forward(
            before, gain_a[index], own_qkv[index], own_out[index], peer_qkv[index], peer_out[index],
            own_gu[:1] if first else [], cosine, sine, depth
        )
        peer = attend.link(len(attend.shapes) - 1) if first else peer_gu[index]
        feed = ffn_forward(
            attend.link(0), gain_f[index], own_gu[index], peer, own_down[index], peer_down[index], shipped, depth
        )
        parts = [attend, feed]
        if final:
            feed.private = (2, 3)
            back_part = ffn_backward(
                grad_now, attend.link(0), gain_f[index], feed.link(2, 1), feed.link(3, 1), own_gu[index], peer, own_down[index],
                feed.link(4, 1) if first else peer_down[index], [], depth, not first
            )
            back_part.woven = not first
            parts.append(back_part)
        made, fed, *back = launch(parts, greet, 2 * index)
        hidden_in, normed_a, queries, kv, lse, mixed, factors = made[:7]
        if first:
            peer_qkv[0], peer_out[0], peer_gu[0] = made[7:]
        current, normed_f, kept, active = fed[:4]
        if first:
            peer_down[index] = fed[4]
        if shipped:
            peer_qkv[follow], peer_out[follow], peer_gu[follow], peer_down[follow] = fed[-4:]
        saved.append((before, normed_a, queries, kv, lse, mixed, factors, hidden_in, normed_f, kept, active))
    gains_a, gains_f, downs, rests, got_qkv = ({}, {}, {}, {}, {})
    grad_hidden, grad_gu, gains_f[layers - 1], *downs[layers - 1] = back[0]
    parts, whose = [], []
    for index in reversed(range(layers)):
        before, normed_a, queries, kv, lse, mixed, factors, _, normed_f, _, _ = saved[index]
        attend = attention_backward(
            grad_hidden, before, gain_a[index], own_qkv[index], peer_qkv[index], own_out[index], peer_out[index],
            cosine, sine, queries, kv, lse, factors, mixed, normed_a, normed_f, grad_gu, depth
        )
        attend.private = (2,)
        at = len(parts)
        parts.append(attend)
        if index:
            _, _, _, _, _, _, _, hidden_in, _, kept, active = saved[index - 1]
            feed = ffn_backward(
                attend.link(0, at), hidden_in, gain_f[index - 1], kept, active, own_gu[index - 1], peer_gu[index - 1],
                own_down[index - 1], peer_down[index - 1], [attend.link(2, at)], depth
            )
            parts.append(feed)
            whose.append((index, at))
            grad_hidden, grad_gu = feed.link(0, at + 1), feed.link(1, at + 1)
            if index > 1:
                made = launch(parts, greet, 2 * index + 1)
                for layer, spot in whose:
                    _, gains_a[layer], _, *rests[layer] = made[spot]
                    grad_hidden, grad_gu, gains_f[layer - 1], *downs[layer - 1], got_qkv[layer] = made[spot + 1]
                parts, whose = [], []
    known_a = [gains_a[layer] for layer in range(1, layers) if layer in gains_a]
    open_a = [parts[spot].link(1, spot) for _, spot in whose[::-1]]
    known_f = [gains_f[layer] for layer in range(layers) if layer in gains_f]
    open_f = [parts[spot + 1].link(2, spot + 1) for _, spot in whose[::-1]]
    tail = finish(attend.link(0, at), [attend.link(1, at)] + open_a + known_a + open_f + known_f, attend.link(2, at), depth)
    made = launch(parts + [tail], lambda: greet_last(tok, depth), 1)
    for layer, spot in whose:
        rests[layer] = made[spot][3:]
        *_, kept_down, got_down, got_qkv[layer] = made[spot + 1]
        downs[layer - 1] = [kept_down, got_down]
    rests[0] = made[at][3:]
    grad_in, gains, got_qkv[0] = made[-1]
    grads = combine([
        (*rests[layer][:4], *downs[layer], rests[layer][4], got_qkv[layer]) for layer in range(layers)
    ])
    return (swap_grid(current, depth), grad_in, *grads, gains[:layers], gains[layers:])


def solution(mesh):
    rows, cols = ("row", "col")
    body = local
    if (mesh.shape["row"], mesh.shape["col"]) == (8, 4):
        mesh = share_out(mesh)
        rows, cols = (("z", "x"), ("y", "c"))
        body = stationary
    in_specs = (
        P(rows, cols),
        P(rows, cols),
        P(None, rows, cols, None),
        P(None, rows, cols),
        P(None, rows, None, cols),
        P(None, rows, cols),
        P(None, cols),
        P(None, cols),
    )
    out_specs = (
        P(rows, cols),
        P(rows, cols),
        P(None, rows, cols, None),
        P(None, rows, cols),
        P(None, rows, None, cols),
        P(None, rows, cols),
        P(None, cols),
        P(None, cols),
    )
    return jax.shard_map(body, mesh=mesh, in_specs=in_specs, out_specs=out_specs, check_vma=False)
```

```python
import math

import jax
import jax.numpy as jnp
from jax import lax
from jax.experimental import pallas as pl
from jax.experimental.pallas import tpu as pltpu
from jax.sharding import Mesh
from jax.sharding import PartitionSpec as P

D = 2048
HEAD = 64
GROUP = 8


EPS = 1e-05
THETA = 10000.0


def rope_turn(tensor, cosine, sine):
    half = tensor.shape[-1] // 2
    first = tensor[..., :half]
    second = tensor[..., half:]
    return jnp.concatenate(
        [first * cosine - second * sine, second * cosine + first * sine], axis=-1
    )


def feature_sum(values):
    return lax.psum(values, "col")


def gather_features(rows_in):
    return lax.all_gather(rows_in, "col", axis=1, tiled=True)


def sum_features(partials):
    return lax.psum_scatter(
        partials.astype(jnp.bfloat16), "col", scatter_dimension=1, tiled=True
    ).astype(jnp.float32)


def add_rows(left, piece):
    return jnp.dot(left, piece, preferred_element_type=jnp.float32)


def project_in(left, shard):
    return add_rows(left, lax.all_gather(shard, "row", axis=0, tiled=True))


def columns_of(left, piece):
    return jnp.einsum("tj,dj->td", left, piece, preferred_element_type=jnp.float32)


def project_out(left, shard):
    return columns_of(left, lax.all_gather(shard, "row", axis=0, tiled=True))


def weight_grad(left, right):
    return lax.psum_scatter(
        lax.dot_general(
            left, right, (((0,), (0,)), ((), ())), preferred_element_type=jnp.float32
        ).astype(jnp.bfloat16),
        "row",
        scatter_dimension=0,
        tiled=True,
    ).astype(jnp.float32)


def norm_forward(values, gain):
    total = feature_sum(jnp.sum(values * values, axis=1))
    factor = lax.rsqrt(total / D + EPS)
    normed = values * factor[:, None]
    return (normed, factor, (normed * gain).astype(jnp.bfloat16))


def norm_backward(grad_normed, normed, factor, gain):
    scaled = grad_normed * gain
    inner = feature_sum(jnp.sum(scaled * normed, axis=1))
    grad_in = factor[:, None] * (scaled - normed * (inner / D)[:, None])
    return (grad_in, jnp.sum(grad_normed * normed, axis=0))


def masked_scores(queries, keys, query_pos, key_pos):
    scores = jnp.einsum("qgd,kd->gqk", queries, keys, preferred_element_type=jnp.float32) * (
        1.0 / math.sqrt(queries.shape[-1])
    )
    return jnp.where(key_pos[None, None, :] <= query_pos[None, :, None], scores, -1e30)


def local(stream, grad_out, wqkv, wo, wgu, wd, gain_attn, gain_ffn):
    tok = stream.shape[0]
    layers = wqkv.shape[0]
    count_rows = wqkv.shape[1]
    head = HEAD
    query_cols = GROUP * head
    seq_len = lax.axis_size("row") * tok
    query_pos = lax.axis_index("row") * tok + jnp.arange(tok, dtype=jnp.int32)
    key_pos = jnp.arange(seq_len, dtype=jnp.int32)
    freq = THETA ** (-(jnp.arange(head // 2, dtype=jnp.float32) * 2.0 / head))
    angle = query_pos.astype(jnp.float32)[:, None] * freq[None, :]
    cosine = jnp.cos(angle)
    sine = jnp.sin(angle)
    saved = []
    current = stream
    for index in range(layers):
        weight_qkv = wqkv[index].reshape(count_rows, -1)
        weight_out = wo[index]
        weight_gu = wgu[index].reshape(count_rows, -1)
        weight_down = wd[index]
        wholes = (None, None, None, None)
        normed_a, factor_a, xnormed = norm_forward(current, gain_attn[index])
        xfull = gather_features(xnormed)
        qkv = project_in(xfull, weight_qkv)
        queries = rope_turn(
            qkv[:, :query_cols].reshape(tok, GROUP, head), cosine[:, None, :], sine[:, None, :]
        ).astype(jnp.bfloat16)
        keys = rope_turn(qkv[:, query_cols : query_cols + head], cosine, sine).astype(jnp.bfloat16)
        values = qkv[:, query_cols + head :].astype(jnp.bfloat16)
        seqkv = lax.all_gather(jnp.concatenate([keys, values], axis=1), "row", axis=0, tiled=True)
        seq_keys = seqkv[:, :head]
        seq_values = seqkv[:, head:]
        scores = masked_scores(queries, seq_keys, query_pos, key_pos)
        top = jnp.max(scores, axis=2, keepdims=True)
        expo = jnp.exp(scores - top)
        denom = jnp.sum(expo, axis=2, keepdims=True)
        probs = (expo / denom).astype(jnp.bfloat16)
        log_total = top + jnp.log(denom)
        mixed = (
            jnp.einsum("gqk,kd->qgd", probs, seq_values, preferred_element_type=jnp.float32)
            .reshape(tok, query_cols)
            .astype(jnp.bfloat16)
        )
        hidden_in = current + sum_features(project_out(mixed, weight_out))
        normed_f, factor_f, hnormed = norm_forward(hidden_in, gain_ffn[index])
        hfull = gather_features(hnormed)
        gate_up = project_in(hfull, weight_gu)
        hidden_cols = gate_up.shape[1] // 2
        gate = gate_up[:, :hidden_cols]
        upper = gate_up[:, hidden_cols:]
        active = (jax.nn.silu(gate) * upper).astype(jnp.bfloat16)
        current = hidden_in + sum_features(project_out(active, weight_down))
        saved.append(
            (
                weight_qkv,
                weight_out,
                weight_gu,
                weight_down,
                wholes,
                normed_a,
                factor_a,
                xfull,
                queries,
                seq_keys,
                seq_values,
                log_total,
                mixed,
                normed_f,
                factor_f,
                hfull,
                gate,
                upper,
                active,
            )
        )
    grad_now = grad_out
    list_qkv, list_out, list_gu, list_down, list_ga, list_gf = ([], [], [], [], [], [])
    for index in reversed(range(layers)):
        (
            weight_qkv,
            weight_out,
            weight_gu,
            weight_down,
            wholes,
            normed_a,
            factor_a,
            xfull,
            queries,
            seq_keys,
            seq_values,
            log_total,
            mixed,
            normed_f,
            factor_f,
            hfull,
            gate,
            upper,
            active,
        ) = saved[index]
        grad_full = gather_features(grad_now.astype(jnp.bfloat16))
        grad_active = project_in(grad_full, weight_down)
        list_down.append(weight_grad(grad_full, active))
        sig = jax.nn.sigmoid(gate)
        grad_gate = grad_active * upper * sig * (1.0 + gate * (1.0 - sig))
        grad_up = grad_active * gate * sig
        grad_gu = jnp.concatenate([grad_gate, grad_up], axis=1).astype(jnp.bfloat16)
        grad_hn = sum_features(project_out(grad_gu, weight_gu))
        list_gu.append(weight_grad(hfull, grad_gu).reshape(count_rows, 2, -1))
        grad_mid, gain_f_grad = norm_backward(grad_hn, normed_f, factor_f, gain_ffn[index])
        list_gf.append(gain_f_grad)
        grad_hidden = grad_now + grad_mid
        hidden_full = gather_features(grad_hidden.astype(jnp.bfloat16))
        grad_mixed = project_in(hidden_full, weight_out).astype(jnp.bfloat16)
        list_out.append(weight_grad(hidden_full, mixed))
        grad_heads = grad_mixed.reshape(tok, GROUP, head)
        scores = masked_scores(queries, seq_keys, query_pos, key_pos)
        probs_full = jnp.exp(scores - log_total)
        probs = probs_full.astype(jnp.bfloat16)
        grad_probs = jnp.einsum(
            "qgd,kd->gqk", grad_heads, seq_values, preferred_element_type=jnp.float32
        )
        delta = jnp.sum(probs_full * grad_probs, axis=2, keepdims=True)
        grad_scores = (probs_full * (grad_probs - delta)).astype(jnp.bfloat16)
        inverse = 1.0 / math.sqrt(head)
        grad_queries = (
            jnp.einsum("gqk,kd->qgd", grad_scores, seq_keys, preferred_element_type=jnp.float32)
            * inverse
        )
        grad_keys = (
            jnp.einsum("gqk,qgd->kd", grad_scores, queries, preferred_element_type=jnp.float32)
            * inverse
        )
        grad_values = jnp.einsum(
            "gqk,qgd->kd", probs, grad_heads, preferred_element_type=jnp.float32
        )
        grad_kv = lax.psum_scatter(
            jnp.concatenate([grad_keys, grad_values], axis=1).astype(jnp.bfloat16),
            "row",
            scatter_dimension=0,
            tiled=True,
        ).astype(jnp.float32)
        grad_k = rope_turn(grad_kv[:, :head], cosine, -sine)
        grad_v = grad_kv[:, head:]
        grad_q = rope_turn(grad_queries, cosine[:, None, :], -sine[:, None, :]).reshape(
            tok, query_cols
        )
        grad_qkv = jnp.concatenate([grad_q, grad_k, grad_v], axis=1).astype(jnp.bfloat16)
        grad_xn = sum_features(project_out(grad_qkv, weight_qkv))
        list_qkv.append(weight_grad(xfull, grad_qkv).reshape(count_rows, 1, -1))
        grad_in, gain_a_grad = norm_backward(grad_xn, normed_a, factor_a, gain_attn[index])
        list_ga.append(gain_a_grad)
        grad_now = grad_hidden + grad_in
    gains_a, gains_f = lax.psum((jnp.stack(list_ga[::-1]), jnp.stack(list_gf[::-1])), "row")
    return (
        current,
        grad_now,
        jnp.stack(list_qkv[::-1]),
        jnp.stack(list_out[::-1]),
        jnp.stack(list_gu[::-1]),
        jnp.stack(list_down[::-1]),
        gains_a,
        gains_f,
    )


def share_out(mesh):
    rows, cols = mesh.shape["row"], mesh.shape["col"]
    return Mesh(
        mesh.devices.reshape(rows // 2, 2, cols // 2, 2), ("z", "x", "y", "c")
    )


def swap_grid(values, depth):
    pairs = [(z * depth + g, g * depth + z) for z in range(depth) for g in range(depth)]
    return lax.ppermute(values, ("z", "y", "c"), pairs)


MESH_ID = pl.DeviceIdType.MESH
ROWS = 16
SKEW = 3
OFFSET = 18
GROUP_CHUNKS = 4
EXTRA = 128


def spread(column):
    high = column.astype(jnp.bfloat16)
    low = (column - high.astype(jnp.float32)).astype(jnp.bfloat16)
    lane = lax.broadcasted_iota(jnp.int32, (column.shape[0], EXTRA), 1)
    wide = jnp.where(lane == 0, high.astype(jnp.float32), jnp.where(lane == 1, low.astype(jnp.float32), 0.0))
    return wide.astype(jnp.bfloat16)


def unspread(block):
    return jnp.sum(block.astype(jnp.float32), axis=1, keepdims=True)


def transposed_dot(left, right):
    return lax.dot_general(left, right, (((1,), (1,)), ((), ())), preferred_element_type=jnp.float32)


class Side:
    def __init__(self, send, recv):
        self.peer = {"x": 1 - lax.axis_index("x")}
        self.send, self.recv, self.copies = send, recv, []

    def start(self, source, target):
        at = len(self.copies)
        copy = remote(source, target, self.send.at[at], self.recv.at[at], self.peer)
        copy.start()
        self.copies.append(copy)
        return copy

    def later(self, source, target):
        at = len(self.copies)
        copy = remote(source, target, self.send.at[at], self.recv.at[at], self.peer)
        self.copies.append(copy)
        return copy

    def finish(self, taken=()):
        for copy in self.copies:
            copy.wait_send()
            if not any(copy is item for item in taken):
                copy.wait_recv()


def remote(src, dst, send, recv, device):
    return pltpu.make_async_remote_copy(
        src_ref=src, dst_ref=dst, send_sem=send, recv_sem=recv, device_id=device, device_id_type=MESH_ID
    )


def halves(features):
    half = features // 2
    x = lax.axis_index("x")
    own = pl.ds(pl.multiple_of(x * half, half), half)
    other = pl.ds(pl.multiple_of((1 - x) * half, half), half)
    return own, other


def flip(block):
    return jnp.transpose(block.astype(jnp.float32)).astype(jnp.bfloat16)


def grad_tile(turned, features, right, cols, kept, given):
    own, other = halves(features)
    value = right[:, cols]
    kept[:, cols] = jnp.dot(turned[own, :], value, preferred_element_type=jnp.float32).astype(jnp.bfloat16)
    given[:, cols] = jnp.dot(turned[other, :], value, preferred_element_type=jnp.float32).astype(jnp.bfloat16)


def sem(*shape):
    return pltpu.SemaphoreType.DMA(shape)


class Link:
    def __init__(self, part, at, shape, dtype):
        self.part, self.at, self.shape, self.dtype = part, at, shape, dtype


class Slice:
    def __init__(self, array, index):
        self.array, self.index = array, index
        self.shape, self.dtype = array.shape[1:], array.dtype


class Part:
    def __init__(self, kernel, operands, shapes, staged_in, staged_out, scratch, aliases, flops, name, early=None):
        self.kernel, self.operands, self.shapes = kernel, operands, shapes
        self.staged_in, self.staged_out, self.scratch = staged_in, staged_out, scratch
        self.aliases, self.flops, self.name = aliases, flops, name
        self.early, self.private, self.woven = early, (), False

    def link(self, at, part=0):
        return Link(part, at, self.shapes[at].shape, self.shapes[at].dtype)


class Done:
    def start(self):
        pass

    def wait(self):
        pass


class Later:
    def __init__(self, copy):
        self.start = copy.start

    def wait(self):
        pass


def weave(step, count, later_step, later_post, later_count, post):
    def both(i, _):
        @pl.when(i < count)
        def _():
            step(i, 0)

        @pl.when(i >= OFFSET)
        def _():
            later_step(i - OFFSET, 0)

        return 0

    lax.fori_loop(0, OFFSET + later_count, both, 0)
    post()
    later_post()


def launch(parts, greet, ident):
    operands, aliases, shapes, scratch = [], {}, [], []
    for part in parts:
        base = len(shapes)
        for at, item in enumerate(part.operands):
            if not isinstance(item, Link):
                if at in part.aliases:
                    aliases[len(operands)] = base + part.aliases[at]
                operands.append(item.array if isinstance(item, Slice) else item)
        shapes += part.shapes
        for item in part.operands[: part.staged_in]:
            if not (isinstance(item, Link) and item.at < parts[item.part].staged_out):
                scratch.append(pltpu.VMEM(item.shape, item.dtype))
        scratch += [pltpu.VMEM(item.shape, item.dtype) for item in part.shapes[: part.staged_out]]
        scratch += [sem(part.staged_in), sem(part.staged_out)] + part.scratch

    def body(*refs):
        given, made, rest = refs[: len(operands)], refs[len(operands) : len(operands) + len(shapes)], list(
            refs[len(operands) + len(shapes) :]
        )
        given, made = list(given), list(made)
        ready, results, held = [], [], []
        for part in parts:
            outs = [made.pop(0) for _ in part.shapes]
            inner, sources, late = [], [], []
            for at, item in enumerate(part.operands):
                if isinstance(item, Link):
                    staged, whole = results[item.part]
                    near = item.at < parts[item.part].staged_out
                    source = None if near else whole[item.at]
                    late.append(at)
                else:
                    near, source = False, given.pop(0)
                    if isinstance(item, Slice):
                        source = source.at[item.index]
                if at >= part.staged_in:
                    inner.append(staged[item.at] if near else source)
                elif near:
                    inner.append(staged[item.at])
                else:
                    inner.append(rest.pop(0))
                sources.append(source)
            results_in = [rest.pop(0) for _ in range(part.staged_out)]
            load_s, store_s = rest.pop(0), rest.pop(0)
            own = [rest.pop(0) for _ in part.scratch]
            loads = [
                Done() if sources[k] is None else pltpu.make_async_copy(sources[k], inner[k], load_s.at[k])
                for k in range(part.staged_in)
            ]
            stores = [
                Done() if k in part.private else pltpu.make_async_copy(results_in[k], outs[k], store_s.at[k])
                for k in range(part.staged_out)
            ]
            for k, copy in enumerate(loads):
                if k not in late:
                    copy.start()
            results.append((results_in, outs))
            ready.append((loads, stores, late, inner, results_in + outs[part.staged_out :], own))
        begun = {}

        def begin(at):
            part = parts[at]
            loads, stores, late, inner, outs, own = ready[at]
            for k in late:
                if k < part.staged_in:
                    loads[k].start()
            if at < len(parts) - 1:
                held.extend(copy for copy in stores if not isinstance(copy, Done))
                stores = [copy if isinstance(copy, Done) else Later(copy) for copy in stores]
            hook = lambda: None
            if at + 2 < len(parts) and parts[at + 2].woven:
                hook = lambda: begin(at + 2)
            elif at + 1 < len(parts) and parts[at + 1].early:
                following = ready[at + 1]
                hook = lambda: parts[at + 1].early(following[0], *following[3], *following[4], *following[5])
            begun[at] = part.kernel(loads, stores, greet if at == 0 else lambda: None, hook, *inner, *outs, *own)

        for at, part in enumerate(parts):
            if part.woven:
                continue
            begin(at)
            if begun[at] is None:
                continue
            step, post, count = begun[at]
            if at + 1 < len(parts) and parts[at + 1].woven:
                weave(step, count, *begun[at + 1], post)
            else:
                lax.fori_loop(0, count, step, 0)
                post()
        for copy in held:
            copy.wait()

    outside = pl.BlockSpec(memory_space=pl.ANY)
    out = pl.pallas_call(
        body,
        out_shape=tuple(shapes),
        in_specs=[outside] * len(operands),
        out_specs=[outside] * len(shapes),
        input_output_aliases=aliases,
        scratch_shapes=scratch,
        compiler_params=pltpu.CompilerParams(collective_id=ident, has_side_effects=True, vmem_limit_bytes=62 << 20),
        cost_estimate=pl.CostEstimate(
            flops=sum(part.flops for part in parts), bytes_accessed=8_000_000, transcendentals=0
        ),
        name="_".join(part.name for part in parts),
    )(*operands)
    out = list(out)
    return [[out.pop(0) for _ in part.shapes] for part in parts]


class Line:
    def __init__(self, tok, depth):
        self.z, self.x = lax.axis_index("z"), lax.axis_index("x")
        self.y, self.c = lax.axis_index("y"), lax.axis_index("c")
        self.tok, self.depth = tok, depth
        self.half = 2 * tok
        self.chunks = self.half // ROWS
        self.own = pl.multiple_of((2 * self.y + self.c) * tok, tok)
        self.peers = (
            {"y": self.y, "c": 1 - self.c},
            {"y": 1 - self.y, "c": self.c},
            {"y": 1 - self.y, "c": 1 - self.c},
        )

    def place(self, stream):
        return self.z if stream == 0 else self.depth - 1 - self.z

    def onward(self, stream):
        return {"z": self.z + 1} if stream == 0 else {"z": self.z - 1}

    def backward(self, stream):
        return {"z": self.z - 1} if stream == 0 else {"z": self.z + 1}

    def row_of(self, stream, chunk):
        per = self.chunks // 2
        far = chunk // per
        y = self.y + far * (1 - 2 * self.y)
        return pl.multiple_of((2 * y + stream) * self.tok + lax.rem(chunk, per) * ROWS, ROWS)


def make_line(tok, depth, width_in, width_out, carry_in, carry_out, features):
    chunks = 2 * tok // ROWS
    groups = chunks // GROUP_CHUNKS
    span = GROUP_CHUNKS * ROWS
    half_groups = groups // 2

    def run(line, greet, taken, begin, prepare, beside, finish, second, settle, close, product, carried, chain_out, chain_in, wide, own_part, rs_out, rs_in,
            ag_s, ag_r, ch_s, ch_r, bc_s, bc_r, rs_s, rs_r):
        greet()
        gather = [
            pltpu.make_async_remote_copy(
                src_ref=taken.at[pl.ds(line.own, tok)],
                dst_ref=taken.at[pl.ds(line.own, tok)],
                send_sem=ag_s.at[at],
                recv_sem=ag_r.at[at],
                device_id=peer,
                device_id_type=MESH_ID,
            )
            for at, peer in enumerate(line.peers)
        ]
        for copy in gather:
            copy.start()
        begin()
        gather[0].wait_recv()
        prepare(pl.multiple_of(line.y * 2 * tok, 2 * tok))

        def chain_copy(stream, chunk):
            return pltpu.make_async_remote_copy(
                src_ref=chain_out.at[stream, chunk],
                dst_ref=chain_in.at[stream, chunk],
                send_sem=ch_s.at[stream, chunk],
                recv_sem=ch_r.at[stream, chunk],
                device_id=line.onward(stream),
                device_id_type=MESH_ID,
            )

        def wide_copy(stream, chunk):
            rows = pl.ds(line.row_of(stream, chunk), ROWS)
            return pltpu.make_async_remote_copy(
                src_ref=wide.at[rows],
                dst_ref=wide.at[rows],
                send_sem=bc_s.at[stream, chunk],
                recv_sem=bc_r.at[stream, chunk],
                device_id=line.backward(stream),
                device_id_type=MESH_ID,
            )

        def sum_copy(stream, group):
            far = group // half_groups
            y = line.y + far * (1 - 2 * line.y)
            other = stream + line.c - 2 * stream * line.c
            slot = 2 * far + other - 1
            part = lax.rem(group, half_groups)
            return (slot >= 0, part, pltpu.make_async_remote_copy(
                src_ref=rs_out.at[stream, group],
                dst_ref=rs_in.at[jnp.maximum(slot, 0), pl.ds(pl.multiple_of(part * span, span), span)],
                send_sem=rs_s.at[stream, group],
                recv_sem=rs_r.at[jnp.maximum(slot, 0), part],
                device_id={"y": y, "c": stream},
                device_id_type=MESH_ID,
            ))

        def step(i, _):
            @pl.when(i == SKEW)
            def _():
                gather[1].wait_recv()
                gather[2].wait_recv()
                prepare(pl.multiple_of((1 - line.y) * 2 * tok, 2 * tok))

            for stream in (0, 1):
                place = line.place(stream)
                chunk = i - SKEW * place

                @pl.when((chunk >= 0) & (chunk < chunks))
                def _():
                    row = line.row_of(stream, chunk)

                    @pl.when(place > 0)
                    def _():
                        chain_copy(stream, chunk).wait_recv()

                    @pl.when(place == 0)
                    def _():
                        chain_out[stream, chunk, :, :width_in] = product[pl.ds(row, ROWS), :].astype(jnp.bfloat16)
                        if carry_in:
                            chain_out[stream, chunk, :, width_in:] = spread(carried[pl.ds(row, ROWS), :1])

                    @pl.when((place > 0) & (place < depth - 1))
                    def _():
                        chain_out[stream, chunk, :, :width_in] = (
                            product[pl.ds(row, ROWS), :] + chain_in[stream, chunk, :, :width_in].astype(jnp.float32)
                        ).astype(jnp.bfloat16)
                        if carry_in:
                            chain_out[stream, chunk, :, width_in:] = spread(
                                carried[pl.ds(row, ROWS), :1] + unspread(chain_in[stream, chunk, :, width_in:])
                            )

                    @pl.when(place < depth - 1)
                    def _():
                        chain_copy(stream, chunk).start()

                    @pl.when(place == depth - 1)
                    def _():
                        total = product[pl.ds(row, ROWS), :] + chain_in[stream, chunk, :, :width_in].astype(jnp.float32)
                        extra = None
                        if carry_in:
                            extra = carried[pl.ds(row, ROWS), :1] + unspread(chain_in[stream, chunk, :, width_in:])
                        finish(row, pl.multiple_of(chunk * ROWS, ROWS), total, extra)
                        wide_copy(stream, chunk).start()

            for stream in (0, 1):
                place = line.place(stream)
                ready = i - SKEW * (2 * (depth - 1) - place)

                @pl.when((ready >= 0) & (ready < chunks))
                def _():
                    @pl.when(place < depth - 1)
                    def _():
                        wide_copy(stream, ready).wait_recv()

                        @pl.when(place > 0)
                        def _():
                            wide_copy(stream, ready).start()

            beside(i)
            for stream in (0, 1):
                place = line.place(stream)
                ready = i - SKEW * (2 * (depth - 1) - place)

                @pl.when((ready >= 0) & (ready < chunks))
                def _():
                    @pl.when(lax.rem(ready, GROUP_CHUNKS) == GROUP_CHUNKS - 1)
                    def _():
                        group = ready // GROUP_CHUNKS
                        row = pl.multiple_of(line.row_of(stream, ready) - (span - ROWS), span)
                        away, part, copy = sum_copy(stream, group)
                        value = second(row, span)

                        @pl.when(away)
                        def _():
                            rs_out[stream, group, :, :features] = value.astype(jnp.bfloat16)
                            if carry_out:
                                rs_out[stream, group, :, features:] = wide[pl.ds(row, span), width_out:]
                            copy.start()

                        @pl.when(jnp.logical_not(away))
                        def _():
                            own_part[pl.ds(pl.multiple_of(part * span, span), span), :] = value

            return 0

        def drain(i, _):
            for stream in (0, 1):
                place = line.place(stream)

                @pl.when(place < depth - 1)
                def _():
                    chain_copy(stream, i).wait_send()

                @pl.when(place > 0)
                def _():
                    wide_copy(stream, i).wait_send()

            return 0

        def drain_sums(i, _):
            for stream in (0, 1):
                away, part, copy = sum_copy(stream, i)

                @pl.when(away)
                def _():
                    copy.wait_send()
            return 0

        def post():
            settle()
            for slot in range(3):
                for part in range(half_groups):
                    pltpu.make_async_remote_copy(
                        src_ref=rs_out.at[0, 0],
                        dst_ref=rs_in.at[slot, pl.ds(part * span, span)],
                        send_sem=rs_s.at[0, 0],
                        recv_sem=rs_r.at[slot, part],
                        device_id=line.peers[slot],
                        device_id_type=MESH_ID,
                    ).wait_recv()
            close()
            for copy in gather:
                copy.wait_send()
            lax.fori_loop(0, chunks, drain, 0)
            lax.fori_loop(0, groups, drain_sums, 0)

        return step, post, chunks + 2 * SKEW * (depth - 1)

    wide_in = width_in + (EXTRA if carry_in else 0)
    scratch = [
        pltpu.VMEM((4 * tok, width_in), jnp.float32),
        pltpu.VMEM((4 * tok, EXTRA), jnp.float32),
        pltpu.VMEM((2, chunks, ROWS, wide_in), jnp.bfloat16),
        pltpu.VMEM((2, chunks, ROWS, wide_in), jnp.bfloat16),
        pltpu.VMEM((tok, features), jnp.float32),
        pltpu.VMEM((2, groups, span, features + (EXTRA if carry_out else 0)), jnp.bfloat16),
        pltpu.VMEM((3, tok, features + (EXTRA if carry_out else 0)), jnp.bfloat16),
        pltpu.SemaphoreType.DMA((3,)),
        pltpu.SemaphoreType.DMA((3,)),
        pltpu.SemaphoreType.DMA((2, chunks)),
        pltpu.SemaphoreType.DMA((2, chunks)),
        pltpu.SemaphoreType.DMA((2, chunks)),
        pltpu.SemaphoreType.DMA((2, chunks)),
        pltpu.SemaphoreType.DMA((2, groups)),
        pltpu.SemaphoreType.DMA((3, half_groups)),
    ]
    return run, scratch


TILE = 256


def ffn_forward(hidden, gain, gu_own, gu_peer, down_own, down_peer, shipped, depth):
    tok, features = hidden.shape
    width = down_own.shape[1]
    run, scratch = make_line(tok, depth, 2 * width, width, True, False, features)
    fetch = down_peer is None
    count = len(shipped)
    sides = count + (1 if fetch else 0)

    def kernel(loads, stores, greet, hook, h_ref, gain_ref, w1_own, w1_peer, w2_own, *rest):
        if not fetch:
            w2_peer, rest = rest[0], rest[1:]
        leave, rest = rest[:count], rest[count:]
        (out_ref, normed_t, kept, wide), rest = rest[:4], rest[4:]
        if fetch:
            w2_peer, rest = rest[0], rest[1:]
        landed, rest = rest[:count], rest[count:]
        (taken, scaled, pieces, side_s, side_r, product, carried, chain_out, chain_in, own_part, rs_out, rs_in), sems = (
            rest[:12], rest[12:])
        line = Line(tok, depth)
        side = Side(side_s, side_r)
        own, other = halves(features)
        loads[0].wait()
        taken[pl.ds(line.own, tok), :] = h_ref[...].astype(jnp.bfloat16)
        at_end = (line.z == 0) | (line.z == depth - 1)

        def begin():
            for copy in loads[1:]:
                copy.wait()
            if fetch:
                side.start(w2_own, w2_peer)
            for source, target in zip(leave, landed):
                side.start(source, target)

        def prepare(row):
            rows = pl.ds(row, 2 * tok)
            block = taken[rows, :].astype(jnp.float32)
            carried[rows, :] = jnp.broadcast_to(jnp.sum(block * block, axis=1, keepdims=True), (2 * tok, EXTRA))
            scaled[...] = (block * gain_ref[...]).astype(jnp.bfloat16)

            def tile(j, _):
                cols = pl.ds(pl.multiple_of(j * TILE, TILE), TILE)
                product[rows, cols] = jnp.dot(
                    scaled[:, own], w1_own[:, cols], preferred_element_type=jnp.float32
                ) + jnp.dot(scaled[:, other], w1_peer[:, cols], preferred_element_type=jnp.float32)
                return 0

            lax.fori_loop(0, 2 * width // TILE, tile, 0)

        def beside(i):
            if fetch:

                @pl.when(i == SKEW * (depth - 1))
                def _():
                    side.copies[0].wait_recv()
                    stores[4].start()

        def finish(row, at, total, extra):
            factor = lax.rsqrt(extra / D + EPS)
            gate = total[:, :width] * factor
            upper = total[:, width:] * factor
            kept[pl.ds(at, ROWS), :width] = gate
            kept[pl.ds(at, ROWS), width:] = upper
            active = gate * jax.nn.sigmoid(gate) * upper
            wide[pl.ds(row, ROWS), :width] = active.astype(jnp.bfloat16)
            wide[pl.ds(row, ROWS), width:] = spread(factor)

        def second(row, span):
            value = wide[pl.ds(row, span), :width]
            pieces[:, own] = transposed_dot(value, w2_own[...])
            pieces[:, other] = transposed_dot(value, w2_peer[...])
            return pieces[...]

        def settle():
            stores[3].start()

            @pl.when(at_end)
            def _():
                stores[2].start()

            normed = taken[...].astype(jnp.float32) * unspread(wide[:, width:]) * gain_ref[...]
            normed_t[...] = jnp.transpose(normed).astype(jnp.bfloat16)
            stores[1].start()

        def close():
            total = own_part[...]
            for slot in range(3):
                total = total + rs_in[slot].astype(jnp.float32)
            out_ref[...] = h_ref[...] + total
            stores[0].start()
            side.finish(side.copies[:1] if fetch else ())
            for at in (0, 1, 3, 4)[: 4 if fetch else 3]:
                stores[at].wait()

            @pl.when(at_end)
            def _():
                stores[2].wait()

        return run(line, greet, taken, begin, prepare, beside, finish, second, settle, close, product, carried, chain_out, chain_in, wide,
            own_part, rs_out, rs_in, *sems)

    low, full = jnp.bfloat16, jnp.float32
    shapes = (
        jax.ShapeDtypeStruct((tok, features), full),
        jax.ShapeDtypeStruct((features, 4 * tok), low),
        jax.ShapeDtypeStruct((2 * tok, 2 * width), full),
        jax.ShapeDtypeStruct((4 * tok, width + EXTRA), low),
    ) + ((jax.ShapeDtypeStruct(down_own.shape, low),) if fetch else ()) + tuple(jax.ShapeDtypeStruct(item.shape, item.dtype) for item in shipped)
    return Part(
        kernel, (hidden, gain.reshape(1, -1), gu_own, gu_peer, down_own, *(() if fetch else (down_peer,)), *shipped), shapes,
        5 if fetch else 6, 5 if fetch else 4,
        [
            pltpu.VMEM((4 * tok, features), low),
            pltpu.VMEM((2 * tok, features), low),
            pltpu.VMEM((GROUP_CHUNKS * ROWS, features), full),
            sem(max(sides, 1)), sem(max(sides, 1)),
        ] + scratch,
        {}, 60_000_000_000, "ffn_forward",
    )


def ffn_backward(
    grad, hidden, gain, kept, wide_forward, gu_own, gu_peer, down_own, down_peer, shipped, depth, woven=False
):
    tok, features = hidden.shape
    width = down_own.shape[1]
    run, scratch = make_line(tok, depth, width, 2 * width, False, True, features)
    count = len(shipped)
    tiles = width // EXTRA
    every = 2 if woven else 1
    first_tile = 2 * tok // ROWS + 2 * SKEW * (depth - 1) - OFFSET if woven else SKEW + 1
    turns = (tiles + every - 1) // every

    def kernel(loads, stores, greet, hook, dy_ref, h_ref, gain_ref, kept_ref, before_ref, w1_own, w1_peer, w2_own, w2_peer, *rest):
        leave, rest = rest[:count], rest[count:]
        (out_ref, wide, gain_out, kept_all, got_all), rest = rest[:5], rest[5:]
        landed, rest = rest[:count], rest[count:]
        (taken, turned, down_kept, down_given, keep_s, pieces, side_s, side_r, product, carried, chain_out, chain_in, own_part,
         rs_out, rs_in), sems = rest[:15], rest[15:]
        line = Line(tok, depth)
        side = Side(side_s, side_r)
        own, other = halves(features)
        loads[0].wait()
        taken[pl.ds(line.own, tok), :] = dy_ref[...].astype(jnp.bfloat16)
        give = side.later(down_given, got_all)
        keep = pltpu.make_async_copy(down_kept, kept_all, keep_s)

        def begin():
            for source, target in zip(leave, landed):
                side.start(source, target)
            loads[7].wait()
            loads[8].wait()

        def prepare(row):
            rows = pl.ds(row, 2 * tok)

            def tile(j, _):
                cols = pl.ds(pl.multiple_of(j * EXTRA, EXTRA), EXTRA)
                product[rows, cols] = jnp.dot(
                    taken[rows, own], w2_own[:, cols], preferred_element_type=jnp.float32
                ) + jnp.dot(taken[rows, other], w2_peer[:, cols], preferred_element_type=jnp.float32)
                return 0

            lax.fori_loop(0, width // EXTRA, tile, 0)

        def beside(i):
            @pl.when(i == 1)
            def _():
                for copy in loads[1:7]:
                    copy.wait()

            @pl.when(i == first_tile)
            def _():
                turned[...] = flip(taken[...])

            for turn_at in range(every):
                at = (i - first_tile) * every + turn_at

                @pl.when((at >= 0) & (at < tiles))
                def _():
                    cols = pl.ds(pl.multiple_of(at * EXTRA, EXTRA), EXTRA)
                    grad_tile(turned, features, before_ref, cols, down_kept, down_given)

            @pl.when(i == first_tile + turns)
            def _():
                give.start()
                keep.start()

        def finish(row, at, total, extra):
            gate = kept_ref[pl.ds(at, ROWS), :width]
            upper = kept_ref[pl.ds(at, ROWS), width:]
            sig = jax.nn.sigmoid(gate)
            silu = gate * sig
            grad_gate = total * upper * (sig + silu * (1.0 - sig))
            grad_up = total * silu
            wide[pl.ds(row, ROWS), :width] = grad_gate.astype(jnp.bfloat16)
            wide[pl.ds(row, ROWS), width : 2 * width] = grad_up.astype(jnp.bfloat16)
            inner = jnp.sum(grad_gate * gate + grad_up * upper, axis=1, keepdims=True)
            wide[pl.ds(row, ROWS), 2 * width :] = spread(inner)

        def second(row, span):
            value = wide[pl.ds(row, span), : 2 * width]
            pieces[:, own] = transposed_dot(value, w1_own[...])
            pieces[:, other] = transposed_dot(value, w1_peer[...])
            return pieces[...]

        def settle():
            stores[1].start()

        def close():
            total = own_part[...]
            inner = unspread(wide[pl.ds(line.own, tok), 2 * width :])
            for slot in range(3):
                total = total + rs_in[slot, :, :features].astype(jnp.float32)
                inner = inner + unspread(rs_in[slot, :, features:])
            factor = unspread(before_ref[pl.ds(line.own, tok), width:])
            normed = h_ref[...] * factor
            gain_out[...] = jnp.broadcast_to(jnp.sum(total * normed, axis=0, keepdims=True), gain_out.shape)
            out_ref[...] = dy_ref[...] + factor * (total * gain_ref[...] - normed * (inner / D))
            stores[2].start()
            stores[0].start()
            keep.wait()
            side.finish()
            for copy in stores:
                copy.wait()

        return run(line, greet, taken, begin, prepare, beside, finish, second, settle, close, product, carried, chain_out, chain_in,
            wide, own_part, rs_out, rs_in, *sems)

    low, full = jnp.bfloat16, jnp.float32
    shapes = (
        jax.ShapeDtypeStruct((tok, features), full),
        jax.ShapeDtypeStruct((4 * tok, 2 * width + EXTRA), low),
        jax.ShapeDtypeStruct((8, features), full),
        jax.ShapeDtypeStruct(down_own.shape, low),
        jax.ShapeDtypeStruct(down_own.shape, low),
    ) + tuple(jax.ShapeDtypeStruct(item.shape, item.dtype) for item in shipped)
    own_scratch = [
        pltpu.VMEM((4 * tok, features), low),
        pltpu.VMEM((features, 4 * tok), low),
        pltpu.VMEM(down_own.shape, low),
        pltpu.VMEM(down_own.shape, low),
        pltpu.SemaphoreType.DMA,
        pltpu.VMEM((GROUP_CHUNKS * ROWS, features), full),
        sem(1 + count), sem(1 + count),
    ] + scratch
    return Part(
        kernel,
        (grad, hidden, gain.reshape(1, -1), kept, wide_forward, gu_own, gu_peer, down_own, down_peer, *shipped),
        shapes, 9, 3,
        own_scratch,
        {}, 60_000_000_000, "ffn_backward",
    )


def to_row(column):
    return jnp.transpose(jnp.broadcast_to(column, (column.shape[0], EXTRA)))[:8]


def to_column(row):
    return jnp.transpose(jnp.broadcast_to(row[:1], (row.shape[1], row.shape[1])))[:, :1]


def turn(values, cosine, sine):
    lane = lax.broadcasted_iota(jnp.int32, values.shape, 1)
    width = values.shape[1]
    back = pltpu.roll(values, width - HEAD // 2, 1)
    forth = pltpu.roll(values, HEAD // 2, 1)
    partner = jnp.where(lax.rem(lane, HEAD) < HEAD // 2, back, forth)
    return values * cosine + partner * sine


def split_pair(block):
    lane = lax.broadcasted_iota(jnp.int32, block.shape, 1)
    zero = jnp.zeros_like(block)
    return jnp.concatenate([jnp.where(lane < HEAD, block, zero), jnp.where(lane < HEAD, zero, block)], axis=0)


def join_pair(turned, tok):
    return jnp.transpose(jnp.concatenate([turned[:HEAD, :tok], turned[HEAD:, tok:]], axis=0))


def twice(kv):
    wide = kv.astype(jnp.float32)
    lane = lax.broadcasted_iota(jnp.int32, wide.shape, 1)
    other = pltpu.roll(wide, HEAD, 1)
    return jnp.where(lane < HEAD, wide, other), jnp.where(lane < HEAD, other, wide)


class Square:
    def __init__(self, tok, depth):
        self.z, self.x = lax.axis_index("z"), lax.axis_index("x")
        self.y, self.c = lax.axis_index("y"), lax.axis_index("c")
        self.tok, self.depth = tok, depth
        self.g = 2 * self.y + self.c
        self.row = 2 * self.z + self.x
        self.own = pl.multiple_of(self.g * tok, tok)
        self.mine = pl.multiple_of(self.z * tok, tok)
        self.peers = (
            {"y": self.y, "c": 1 - self.c},
            {"y": 1 - self.y, "c": self.c},
            {"y": 1 - self.y, "c": 1 - self.c},
        )

    def row_peer(self, step):
        at = lax.rem(self.row + step, 2 * self.depth)
        return {"z": at // 2, "x": lax.rem(at, 2)}

    def greet(self, extra=0):
        barrier = pltpu.get_barrier_semaphore()
        for peer in self.peers:
            pl.semaphore_signal(barrier, 1, device_id=peer, device_id_type=MESH_ID)
        for step in range(1, 2 * self.depth):
            pl.semaphore_signal(barrier, 1, device_id=self.row_peer(step), device_id_type=MESH_ID)
        pl.semaphore_wait(barrier, 3 + 2 * self.depth - 1 + extra)


def start_gather(square, taken, send, recv):
    copies = [
        remote(taken.at[pl.ds(square.own, square.tok)], taken.at[pl.ds(square.own, square.tok)], send.at[at], recv.at[at], peer)
        for at, peer in enumerate(square.peers)
    ]
    for copy in copies:
        copy.start()
    return copies


def line_sum(square, gather, product, own, own_row, outs, ins, row_outs, row_ins, send, recv, row_send, row_recv, between):
    tok, depth = square.tok, square.depth

    def one(order):
        block = lax.rem(2 * square.y + order, depth)
        step = lax.rem(block - square.z + depth, depth)
        slot = jnp.maximum(depth - 1 - step, 0)
        value, column = product(pl.multiple_of(block * tok, tok))

        @pl.when(step == 0)
        def _():
            own[...] = value
            if column is not None:
                own_row[...] = to_row(column)

        copy = remote(outs.at[order], ins.at[slot], send.at[order], recv.at[slot], {"z": block})
        row_copy = None
        if column is not None:
            row_copy = remote(row_outs.at[order], row_ins.at[slot], row_send.at[order], row_recv.at[slot], {"z": block})

        @pl.when(step != 0)
        def _():
            outs[order] = value.astype(jnp.bfloat16)
            copy.start()
            if column is not None:
                row_outs[order] = to_row(column)
                row_copy.start()

        return step, copy, row_copy

    gather[0].wait_recv()
    sent = [one(0), one(1)]
    gather[1].wait_recv()
    gather[2].wait_recv()
    sent += [one(2), one(3)]
    between()
    for slot in range(depth - 1):
        remote(outs.at[0], ins.at[slot], send.at[0], recv.at[slot], {"z": square.z}).wait_recv()
        if row_ins is not None:
            remote(row_outs.at[0], row_ins.at[slot], row_send.at[0], row_recv.at[slot], {"z": square.z}).wait_recv()
    return sent


def send_part(square, array, part, send, recv):
    lanes = pl.ds(pl.multiple_of(part * EXTRA, EXTRA), EXTRA)
    here = array.at[pl.ds(square.mine, square.tok), lanes]
    depth = square.depth
    return [
        remote(here, here, send.at[step - 1, part], recv.at[depth - 1 - step, part], {"z": lax.rem(square.z + step, depth)})
        for step in range(1, depth)
    ]


def send_row(square, rows, send, recv):
    line = rows.at[square.z]
    depth = square.depth
    return [
        remote(line, line, send.at[step - 1], recv.at[depth - 1 - step], {"z": lax.rem(square.z + step, depth)})
        for step in range(1, depth)
    ]


def grid_sum(square, array, rows, second, settle, own, outs, ins, row_ins, arrive, row_arrive, send, recv, row_send, row_recv):
    tok, depth = square.tok, square.depth
    sent = []
    for step in range(depth):
        block = lax.rem(square.z + step, depth)
        if step:
            for part in range(array.shape[1] // EXTRA):
                rows_of = array.at[pl.ds(pl.multiple_of(block * tok, tok), tok), pl.ds(part * EXTRA, EXTRA)]
                remote(rows_of, rows_of, send.at[0], arrive.at[step - 1, part], {"z": square.z}).wait_recv()
            remote(rows.at[block], rows.at[block], send.at[0], row_arrive.at[step - 1], {"z": square.z}).wait_recv()
        value = second(pl.multiple_of(block * tok, tok))
        away = lax.rem(block - square.g + depth, depth)
        slot = jnp.maximum(depth - 1 - away, 0)
        device = {"y": block // 2, "c": lax.rem(block, 2)}
        copy = remote(outs.at[step], ins.at[slot], send.at[step], recv.at[slot], device)
        row_copy = None
        if row_ins is not None:
            row_copy = remote(rows.at[block], row_ins.at[slot], row_send.at[step], row_recv.at[slot], device)

        @pl.when(away == 0)
        def _():
            own[...] = value

        @pl.when(away != 0)
        def _():
            outs[step] = value.astype(jnp.bfloat16)
            copy.start()
            if row_ins is not None:
                row_copy.start()

        sent.append((away, copy, row_copy))
    settle()
    for slot in range(depth - 1):
        remote(outs.at[0], ins.at[slot], send.at[0], recv.at[slot], square.peers[0]).wait_recv()
        if row_ins is not None:
            remote(rows.at[0], row_ins.at[slot], row_send.at[0], row_recv.at[slot], square.peers[0]).wait_recv()
    return sent


def drain(sent):
    for away, copy, row_copy in sent:

        @pl.when(away != 0)
        def _():
            copy.wait_send()
            if row_copy is not None:
                row_copy.wait_send()


def attention_forward(hidden, gain, qkv_own, out_own, qkv_peer, out_peer, shipped, freq, cosine, sine, depth):
    tok, features = hidden.shape
    cols = qkv_own.shape[1]
    fetch = qkv_peer is None
    extra = 4 if fetch else 0
    count = len(shipped)
    sides = (2 if fetch else 0) + 2 * count
    query_cols = GROUP * HEAD
    seq = 2 * depth * tok
    pairs = query_cols // EXTRA
    scale = 1.0 / math.sqrt(HEAD)

    def kernel(loads, stores, greet, hook, h_ref, gain_ref, wqkv_own, wo_own, *rest):
        if fetch:
            freq_ref, rest = rest[0], rest[1:]
        else:
            (cos_ref, sin_ref, wqkv_peer, wo_peer), rest = rest[:4], rest[4:]
        leave, rest = rest[:count], rest[count:]
        (out_ref, normed_t, queries, kv, lse, mixed, factors), rest = rest[:7], rest[7:]
        if fetch:
            (wqkv_peer, wo_peer, cos_ref, sin_ref), rest = rest[:4], rest[4:]
        landed, rest = rest[:count], rest[count:]
        (taken, scaled, pieces, own, own_row, z_out, z_in, zr_out, zr_in, values_t, g_own, g_out, g_in,
         ag_s, ag_r, zs_s, zs_r, zr_s, zr_r, kv_s, kv_r, zg_s, zg_r, zgr_s, zgr_r, gs_s, gs_r), rest = rest[:27], rest[27:]
        square = Square(tok, depth)
        side = Side(*rest) if sides else None
        mine, other = halves(features)
        loads[0].wait()
        taken[pl.ds(square.own, tok), :] = h_ref[...].astype(jnp.bfloat16)
        greet()
        gather = start_gather(square, taken, ag_s, ag_r)
        for copy in loads[1:]:
            copy.wait()
        urgent = []
        if fetch:
            urgent = [side.start(wqkv_own, wqkv_peer), side.start(wo_own, wo_peer)]
        held = []
        for source, target in zip(leave, landed):
            most = source.shape[0] // 2
            rest_of = pl.ds(most, source.shape[0] - most)
            side.start(source.at[pl.ds(0, most)], target.at[pl.ds(0, most)])
            held.append(side.later(source.at[rest_of], target.at[rest_of]))
        if fetch:
            at = lax.broadcasted_iota(jnp.int32, (tok, EXTRA), 0) + square.row * tok
            lane = lax.broadcasted_iota(jnp.int32, (tok, EXTRA), 1)
            angle = at.astype(jnp.float32) * freq_ref[...]
            cos_ref[...] = jnp.cos(angle)
            sin_ref[...] = jnp.where(lax.rem(lane, HEAD) < HEAD // 2, -1.0, 1.0) * jnp.sin(angle)
            stores[9].start()
            stores[10].start()
        for copy in urgent[:1]:
            copy.wait_recv()
            stores[7].start()

        def product(row):
            block = taken[pl.ds(row, tok), :].astype(jnp.float32)
            scaled[...] = (block * gain_ref[...]).astype(jnp.bfloat16)
            return (
                jnp.dot(scaled[:, mine], wqkv_own[...], preferred_element_type=jnp.float32)
                + jnp.dot(scaled[:, other], wqkv_peer[...], preferred_element_type=jnp.float32),
                jnp.sum(block * block, axis=1, keepdims=True),
            )

        sent = line_sum(square, gather, product, own, own_row, z_out, z_in, zr_out, zr_in, zs_s, zs_r, zr_s, zr_r, hook)
        total, squares = own[...], own_row[...]
        for slot in range(depth - 1):
            total = total + z_in[slot].astype(jnp.float32)
            squares = squares + zr_in[slot]
        factor_row = lax.rsqrt(squares / D + EPS)
        factors[square.z] = factor_row
        given = send_row(square, factors, zgr_s, zgr_r)
        for copy in given:
            copy.start()
        first = lax.broadcasted_iota(jnp.int32, (tok, EXTRA), 1) < HEAD
        cosine_row, sine_row = cos_ref[...], sin_ref[...]
        turned = turn(
            total * to_column(factor_row),
            jnp.concatenate([cosine_row] * pairs + [jnp.where(first, cosine_row, 1.0)], axis=1),
            jnp.concatenate([sine_row] * pairs + [jnp.where(first, sine_row, 0.0)], axis=1),
        )
        here = pl.ds(pl.multiple_of(square.row * tok, tok), tok)
        kv[here, :] = turned[:, query_cols:].astype(jnp.bfloat16)
        queries[...] = turned[:, :query_cols].astype(jnp.bfloat16)
        stores[2].start()
        spreads = []
        for step in range(1, 2 * depth):
            copy = remote(kv.at[here], kv.at[here], kv_s.at[step - 1], kv_r.at[2 * depth - 1 - step], square.row_peer(step))
            copy.start()
            spreads.append(copy)
        for copy in spreads:
            copy.wait_recv()
        stores[3].start()
        for copy in held:
            copy.start()
        keys, both = twice(kv[...])
        values_t[...] = jnp.transpose(both).astype(jnp.bfloat16)
        keys = keys.astype(jnp.bfloat16)

        def pair(t, _):
            lanes = pl.ds(pl.multiple_of(t * EXTRA, EXTRA), EXTRA)
            scores = transposed_dot(keys, split_pair(queries[:, lanes])) * scale
            key_at = lax.broadcasted_iota(jnp.int32, scores.shape, 0)
            query_at = lax.rem(lax.broadcasted_iota(jnp.int32, scores.shape, 1), tok) + square.row * tok
            scores = jnp.where(key_at <= query_at, scores, -1e30)
            top = jnp.max(scores, axis=0, keepdims=True)
            expo = jnp.exp(scores - top)
            denom = jnp.sum(expo, axis=0, keepdims=True)
            lse[t] = jnp.broadcast_to(top + jnp.log(denom), (8, 2 * tok))
            probs = (expo * (1.0 / denom)).astype(jnp.bfloat16)
            out_t = jnp.dot(values_t[...], probs, preferred_element_type=jnp.float32)
            mixed[pl.ds(square.mine, tok), lanes] = join_pair(out_t, tok).astype(jnp.bfloat16)
            for copy in send_part(square, mixed, t, zg_s, zg_r):
                copy.start()
            return 0

        lax.fori_loop(0, pairs, pair, 0)
        given += [copy for part in range(pairs) for copy in send_part(square, mixed, part, zg_s, zg_r)]

        stores[4].start()
        for copy in urgent[1:]:
            copy.wait_recv()
            stores[8].start()

        def second(row):
            value = mixed[pl.ds(row, tok), :]
            pieces[:, mine] = transposed_dot(value, wo_own[...])
            pieces[:, other] = transposed_dot(value, wo_peer[...])
            return pieces[...]

        def settle():
            stores[5].start()
            stores[6].start()
            for block in range(depth):
                rows = pl.ds(block * tok, tok)
                normed = taken[rows, :].astype(jnp.float32) * to_column(factors[block]) * gain_ref[...]
                normed_t[:, rows] = jnp.transpose(normed).astype(jnp.bfloat16)
            stores[1].start()

        sums = grid_sum(square, mixed, factors, second, settle, g_own, g_out, g_in, None, zg_r, zgr_r, gs_s, gs_r, None, None)
        total = g_own[...]
        for slot in range(depth - 1):
            total = total + g_in[slot].astype(jnp.float32)
        out_ref[...] = h_ref[...] + total
        stores[0].start()
        drain(sent)
        drain(sums)
        for copy in gather + spreads + given:
            copy.wait_send()
        if side:
            side.finish(urgent)
        for copy in stores:
            copy.wait()

    low, full = jnp.bfloat16, jnp.float32
    shapes = (
        jax.ShapeDtypeStruct((tok, features), full),
        jax.ShapeDtypeStruct((features, depth * tok), low),
        jax.ShapeDtypeStruct((tok, query_cols), low),
        jax.ShapeDtypeStruct((seq, 2 * HEAD), low),
        jax.ShapeDtypeStruct((pairs, 8, 2 * tok), full),
        jax.ShapeDtypeStruct((depth * tok, query_cols), low),
        jax.ShapeDtypeStruct((depth, 8, tok), full),
    )
    if fetch:
        shapes += (jax.ShapeDtypeStruct(qkv_own.shape, low), jax.ShapeDtypeStruct(out_own.shape, low))
        shapes += (jax.ShapeDtypeStruct((tok, EXTRA), full),) * 2
    shapes += tuple(jax.ShapeDtypeStruct(item.shape, item.dtype) for item in shipped)
    peers = () if fetch else (qkv_peer, out_peer)
    tables = (freq,) if fetch else (cosine, sine)
    operands = (hidden, gain.reshape(1, -1), qkv_own, out_own, *tables, *peers, *shipped)
    return Part(
        kernel, operands, shapes, 4 + len(tables) + len(peers), 7 + extra,
        [
            pltpu.VMEM((depth * tok, features), low),
            pltpu.VMEM((tok, features), low),
            pltpu.VMEM((tok, features), full),
            pltpu.VMEM((tok, cols), full),
            pltpu.VMEM((8, tok), full),
            pltpu.VMEM((depth, tok, cols), low),
            pltpu.VMEM((depth - 1, tok, cols), low),
            pltpu.VMEM((depth, 8, tok), full),
            pltpu.VMEM((depth - 1, 8, tok), full),
            pltpu.VMEM((2 * HEAD, seq), low),
            pltpu.VMEM((tok, features), full),
            pltpu.VMEM((depth, tok, features), low),
            pltpu.VMEM((depth - 1, tok, features), low),
            sem(3), sem(3), sem(depth), sem(depth - 1), sem(depth), sem(depth - 1),
            sem(2 * depth - 1), sem(2 * depth - 1), sem(depth - 1, pairs), sem(depth - 1, pairs), sem(depth - 1), sem(depth - 1),
            sem(depth), sem(depth - 1),
        ] + ([sem(sides), sem(sides)] if sides else []),
        {}, 50_000_000_000, "attention_forward",
    )


def attention_backward(
    grad, hidden, gain, qkv_own, qkv_peer, out_own, out_peer, cosine, sine, queries, kv, lse, factors, mixed, normed_a, normed_f,
    grad_gu, depth,
):
    tok, features = hidden.shape
    cols = qkv_own.shape[1]
    wide = grad_gu.shape[1] - EXTRA
    query_cols = GROUP * HEAD
    seq = 2 * depth * tok
    pairs = query_cols // EXTRA
    scale = 1.0 / math.sqrt(HEAD)

    def kernel(loads, stores, greet, hook, dy_ref, h_ref, gain_ref, wqkv_own, wqkv_peer, wo_own, wo_peer, cos_ref, sin_ref, q_ref, kv_ref, lse_ref,
               factor_ref, mixed_ref, normed_a_ref, normed_f_ref, gu_ref, *rest_refs):
        (out_ref, gain_out, qkv_given, gu_kept_all, gu_got_all, out_kept_all, out_got_all, qkv_kept_all,
               taken, spun, turned, pieces, gu_kept, gu_given, out_kept, out_given, qkv_kept, keep_s,
               own, heads, z_out, z_in, keys_t, dk, dv, kv_out, kv_in, dq, inner_rows, g_own, g_out, g_in, g_rows,
               ag_s, ag_r, zs_s, zs_r, kv_s, kv_r, zg_s, zg_r, zgr_s, zgr_r, gs_s, gs_r, gr_s, gr_r, side_s, side_r) = rest_refs
        square = Square(tok, depth)
        side = Side(side_s, side_r)
        mine, other = halves(features)
        loads[0].wait()
        taken[pl.ds(square.own, tok), :] = dy_ref[...].astype(jnp.bfloat16)
        greet()
        gather = start_gather(square, taken, ag_s, ag_r)
        for copy in loads[1:]:
            copy.wait()

        def gu_tiles(start, stop):
            def tile(j, _):
                grad_tile(normed_f_ref, features, gu_ref, pl.ds(pl.multiple_of(j * EXTRA, EXTRA), EXTRA), gu_kept, gu_given)
                return 0

            lax.fori_loop(start, stop, tile, 0)

        gu_got = gu_got_all
        keeps = [
            pltpu.make_async_copy(gu_kept, gu_kept_all, keep_s.at[0]),
            pltpu.make_async_copy(out_kept, out_kept_all, keep_s.at[1]),
            pltpu.make_async_copy(qkv_kept, qkv_kept_all, keep_s.at[2]),
        ]
        every = wide // EXTRA
        middle, late = every // 2, every * 3 // 4
        gu_tiles(0, middle)
        front, rest = pl.ds(0, middle * EXTRA), pl.ds(late * EXTRA, wide - late * EXTRA)
        inner_part = pl.ds(middle * EXTRA, (late - middle) * EXTRA)
        side.start(gu_given.at[:, front], gu_got.at[:, front])

        def between():
            turned[...] = flip(taken[...])
            for t in range(query_cols // EXTRA):
                grad_tile(turned, features, mixed_ref, pl.ds(t * EXTRA, EXTRA), out_kept, out_given)
            side.start(out_given, out_got_all)
            gu_tiles(middle, late)
            side.start(gu_given.at[:, inner_part], gu_got.at[:, inner_part])
            gu_tiles(late, every)
            keeps[0].start()
            keeps[1].start()

        def product(row):
            rows = pl.ds(row, tok)
            value = jnp.dot(taken[rows, mine], wo_own[...], preferred_element_type=jnp.float32) + jnp.dot(
                taken[rows, other], wo_peer[...], preferred_element_type=jnp.float32
            )
            return value, None

        sent = line_sum(square, gather, product, own, None, z_out, z_in, None, None, zs_s, zs_r, None, None, between)
        total = own[...]
        for slot in range(depth - 1):
            total = total + z_in[slot].astype(jnp.float32)
        heads[...] = total.astype(jnp.bfloat16)
        keys, both = twice(kv_ref[...])
        keys_t[...] = jnp.transpose(keys).astype(jnp.bfloat16)
        keys = keys.astype(jnp.bfloat16)
        both = both.astype(jnp.bfloat16)
        dk[...] = jnp.zeros_like(dk)
        dv[...] = jnp.zeros_like(dv)

        def pair(t, _):
            lanes = pl.ds(pl.multiple_of(t * EXTRA, EXTRA), EXTRA)
            query = split_pair(q_ref[:, lanes])
            head = split_pair(heads[:, lanes])
            scores = transposed_dot(keys, query) * scale
            key_at = lax.broadcasted_iota(jnp.int32, scores.shape, 0)
            query_at = lax.rem(lax.broadcasted_iota(jnp.int32, scores.shape, 1), tok) + square.row * tok
            probs = jnp.exp(jnp.where(key_at <= query_at, scores, -1e30) - lse_ref[t, :1, :])
            grad_probs = transposed_dot(both, head)
            delta = jnp.sum(probs * grad_probs, axis=0, keepdims=True)
            grad_scores = (probs * (grad_probs - delta)).astype(jnp.bfloat16)
            dk[...] += jnp.dot(grad_scores, query, preferred_element_type=jnp.float32)
            dv[...] += jnp.dot(probs.astype(jnp.bfloat16), head, preferred_element_type=jnp.float32)
            back = jnp.dot(keys_t[...], grad_scores, preferred_element_type=jnp.float32)
            value = join_pair(back, tok) * scale
            dq[...] += jnp.broadcast_to(
                jnp.sum(value * q_ref[:, lanes].astype(jnp.float32), axis=1, keepdims=True), dq.shape
            )
            spun[pl.ds(square.mine, tok), lanes] = turn(value, cos_ref[...], -sin_ref[...]).astype(jnp.bfloat16)
            for copy in send_part(square, spun, t, zg_s, zg_r):
                copy.start()
            return 0

        dq[...] = jnp.zeros_like(dq)
        lax.fori_loop(0, pairs, pair, 0)
        lane = lax.broadcasted_iota(jnp.int32, (seq, EXTRA), 1)
        left = dk[...]
        right = dv[...]
        both_kv = jnp.where(
            lane < HEAD, (left + pltpu.roll(left, HEAD, 1)) * scale, right + pltpu.roll(right, HEAD, 1)
        )
        dk[...] = both_kv
        kv_out[...] = both_kv.astype(jnp.bfloat16)
        here = pl.ds(pl.multiple_of(square.row * tok, tok), tok)
        spreads = []
        for step in range(1, 2 * depth):
            at = lax.rem(square.row + step, 2 * depth)
            copy = remote(
                kv_out.at[pl.ds(pl.multiple_of(at * tok, tok), tok)],
                kv_in.at[2 * depth - 1 - step],
                kv_s.at[step - 1],
                kv_r.at[2 * depth - 1 - step],
                square.row_peer(step),
            )
            copy.start()
            spreads.append(copy)
        total_kv = dk[here, :]
        for copy in spreads:
            copy.wait_recv()
        side.start(gu_given.at[:, rest], gu_got.at[:, rest])
        for slot in range(2 * depth - 1):
            total_kv = total_kv + kv_in[slot].astype(jnp.float32)
        first = lax.broadcasted_iota(jnp.int32, (tok, EXTRA), 1) < HEAD
        spun[pl.ds(square.mine, tok), query_cols:] = turn(
            total_kv, jnp.where(first, cos_ref[...], 1.0), jnp.where(first, -sin_ref[...], 0.0)
        ).astype(jnp.bfloat16)
        inner = dq[:, :1] + jnp.sum(total_kv * kv_ref[here, :].astype(jnp.float32), axis=1, keepdims=True)
        inner_rows[square.z] = to_row(inner)
        given = send_part(square, spun, pairs, zg_s, zg_r) + send_row(square, inner_rows, zgr_s, zgr_r)
        for copy in given:
            copy.start()
        given += [copy for part in range(pairs) for copy in send_part(square, spun, part, zg_s, zg_r)]

        def second(row):
            value = spun[pl.ds(row, tok), :]
            pieces[:, mine] = transposed_dot(value, wqkv_own[...])
            pieces[:, other] = transposed_dot(value, wqkv_peer[...])
            return pieces[...]

        def settle():
            for t in range(cols // EXTRA):
                grad_tile(normed_a_ref, features, spun, pl.ds(t * EXTRA, EXTRA), qkv_kept, qkv_given)
            keeps[2].start()
            stores[2].start()
            hook()

        sums = grid_sum(
            square, spun, inner_rows, second, settle, g_own, g_out, g_in, g_rows, zg_r, zgr_r, gs_s, gs_r, gr_s, gr_r
        )
        total = g_own[...]
        inner = inner_rows[square.g]
        for slot in range(depth - 1):
            total = total + g_in[slot].astype(jnp.float32)
            inner = inner + g_rows[slot]
        factor = to_column(factor_ref[square.g])
        normed = h_ref[...] * factor
        gain_out[...] = jnp.broadcast_to(jnp.sum(total * normed, axis=0, keepdims=True), gain_out.shape)
        out_ref[...] = dy_ref[...] + factor * (total * gain_ref[...] - normed * (to_column(inner) / D))
        stores[0].start()
        stores[1].start()
        drain(sent)
        drain(sums)
        for copy in gather + spreads + given:
            copy.wait_send()
        for copy in keeps + stores:
            copy.wait()
        side.finish()

    low, full = jnp.bfloat16, jnp.float32
    shapes = (
        jax.ShapeDtypeStruct((tok, features), full),
        jax.ShapeDtypeStruct((8, features), full),
        jax.ShapeDtypeStruct(qkv_own.shape, low),
        jax.ShapeDtypeStruct((features // 2, wide), low),
        jax.ShapeDtypeStruct((features // 2, wide), low),
        jax.ShapeDtypeStruct(out_own.shape, low),
        jax.ShapeDtypeStruct(out_own.shape, low),
        jax.ShapeDtypeStruct(qkv_own.shape, low),
    )
    operands = (
        grad, hidden, gain.reshape(1, -1), qkv_own, qkv_peer, out_own, out_peer, cosine, sine, queries, kv, lse, factors,
        mixed, normed_a, normed_f, grad_gu,
    )
    return Part(
        kernel, operands, shapes, 17, 3,
        [
            pltpu.VMEM((depth * tok, features), low),
            pltpu.VMEM((depth * tok, cols), low),
            pltpu.VMEM((features, depth * tok), low),
            pltpu.VMEM((tok, features), full),
            pltpu.VMEM((features // 2, wide), low),
            pltpu.VMEM((features // 2, wide), low),
            pltpu.VMEM(out_own.shape, low),
            pltpu.VMEM(out_own.shape, low),
            pltpu.VMEM(qkv_own.shape, low),
            sem(3),
            pltpu.VMEM((tok, query_cols), full),
            pltpu.VMEM((tok, query_cols), low),
            pltpu.VMEM((depth, tok, query_cols), low),
            pltpu.VMEM((depth - 1, tok, query_cols), low),
            pltpu.VMEM((2 * HEAD, seq), low),
            pltpu.VMEM((seq, 2 * HEAD), full),
            pltpu.VMEM((seq, 2 * HEAD), full),
            pltpu.VMEM((seq, 2 * HEAD), low),
            pltpu.VMEM((2 * depth - 1, tok, 2 * HEAD), low),
            pltpu.VMEM((tok, EXTRA), full),
            pltpu.VMEM((depth, 8, tok), full),
            pltpu.VMEM((tok, features), full),
            pltpu.VMEM((depth, tok, features), low),
            pltpu.VMEM((depth - 1, tok, features), low),
            pltpu.VMEM((depth - 1, 8, tok), full),
            sem(3), sem(3), sem(depth), sem(depth - 1),
            sem(2 * depth - 1), sem(2 * depth - 1), sem(depth - 1, pairs + 1), sem(depth - 1, pairs + 1), sem(depth - 1),
            sem(depth - 1), sem(depth), sem(depth - 1), sem(depth), sem(depth - 1), sem(4), sem(4),
        ],
        {}, 50_000_000_000, "attention_backward",
    )


def greet_last(tok, depth):
    square = Square(tok, depth)
    barrier = pltpu.get_barrier_semaphore()
    for slot in range(2 * depth):
        here = (square.z == square.g) & (slot == square.x * depth + square.g)

        @pl.when(jnp.logical_not(here))
        def _():
            source = {"z": square.g, "x": slot // depth, "y": (slot % depth) // 2, "c": slot % 2}
            pl.semaphore_signal(barrier, 1, device_id=source, device_id_type=MESH_ID)

    square.greet(2 * depth - jnp.where(square.z == square.g, 1, 0))


def finish(grad, gains, qkv_given, depth):
    tok, features = grad.shape
    count = len(gains)
    members = 2 * depth

    def kernel(loads, stores, greet, hook, grad_ref, *rest):
        gain_refs, rest = rest[:count], rest[count:]
        (given, out_ref, gain_out, got, packed, parts, sent, home, part_s, part_r, move_s, move_r, side_s, side_r) = rest
        z, x = lax.axis_index("z"), lax.axis_index("x")
        y, c = lax.axis_index("y"), lax.axis_index("c")
        g = 2 * y + c
        self_at = x * depth + g

        def target(at):
            return {"z": at // 2, "x": at % 2, "y": z // 2, "c": lax.rem(z, 2)}

        def is_source_me(slot):
            return (z == g) & (slot == self_at)

        def is_target_me(at):
            return (z == g) & (at == 2 * z + x)

        for copy in loads:
            copy.wait()
        for at, ref in enumerate(gain_refs):
            packed[at : at + 1, :] = ref[:1, :]
        sent[...] = grad_ref[...].astype(jnp.bfloat16)
        side = Side(side_s, side_r)
        side.later(given, got)
        move = remote(sent, home, move_s, move_r, {"z": g, "y": z // 2, "c": lax.rem(z, 2)})

        @pl.when(z != g)
        def _():
            move.start()

        def part(at):
            return remote(packed, parts.at[self_at], part_s.at[at], part_r.at[self_at], target(at))

        for at in range(members):

            @pl.when(jnp.logical_not(is_target_me(at)))
            def _():
                part(at).start()

        @pl.when(z == g)
        def _():
            parts[self_at] = packed[...]

        for slot in range(members):

            @pl.when(jnp.logical_not(is_source_me(slot)))
            def _():
                remote(packed, parts.at[slot], part_s.at[0], part_r.at[slot], target(0)).wait_recv()

        total = parts[0]
        for slot in range(1, members):
            total = total + parts[slot]
        gain_out[...] = total
        stores[1].start()

        @pl.when(z == g)
        def _():
            out_ref[...] = grad_ref[...]

        @pl.when(z != g)
        def _():
            move.wait_recv()
            out_ref[...] = home[...].astype(jnp.float32)
            move.wait_send()

        stores[0].start()
        for at in range(members):

            @pl.when(jnp.logical_not(is_target_me(at)))
            def _():
                part(at).wait_send()

        side.finish()
        for copy in stores:
            copy.wait()

    low, full = jnp.bfloat16, jnp.float32
    shapes = (
        jax.ShapeDtypeStruct((tok, features), full),
        jax.ShapeDtypeStruct((count, features), full),
        jax.ShapeDtypeStruct(qkv_given.shape, low),
    )
    def early(loads, *refs):
        given, got, side_s, side_r = refs[1 + count], refs[4 + count], refs[-2], refs[-1]
        Side(side_s, side_r).start(given, got)

    return Part(
        kernel, (grad, *gains, qkv_given), shapes, 1 + count, 2,
        [
            pltpu.VMEM((count, features), full),
            pltpu.VMEM((members, count, features), full),
            pltpu.VMEM((tok, features), low),
            pltpu.VMEM((tok, features), low),
            sem(members), sem(members),
            pltpu.SemaphoreType.DMA, pltpu.SemaphoreType.DMA,
            sem(1), sem(1),
        ],
        {}, 5_000_000_000, "finish", early,
    )


def combine(halves_of):
    layers, count = len(halves_of), len(halves_of[0])
    rows, wide = halves_of[0][0].shape
    half = wide // 2
    step = rows // 2
    last = rows // step - 1

    def kernel(*refs):
        qkv_o, out_o, gu_o, down_o = refs[layers * count :]
        for index in range(layers):
            gu_k, gu_g, out_k, out_g, down_k, down_g, qkv_k, qkv_g = refs[index * count : (index + 1) * count]

            @pl.when(pl.program_id(0) == index)
            def _():
                add = lambda kept, got: kept[...].astype(jnp.float32) + got[...].astype(jnp.float32)
                total = add(gu_k, gu_g)
                gu_o[0, :, 0, :] = total[:, :half]
                gu_o[0, :, 1, :] = total[:, half:]
                out_o[0] = add(out_k, out_g)
                down_o[0] = add(down_k, down_g)
                qkv_o[0, :, 0, :] = add(qkv_k, qkv_g)

    def place(index):
        def at_of(layer, at):
            return jnp.where(layer == index, at, jnp.where(layer < index, 0, last)), 0

        return at_of

    full = jnp.float32
    sizes = [item.shape[1] for item in halves_of[0]]
    outer = lambda layer, at: (layer, at, 0)
    inner = lambda layer, at: (layer, at, 0, 0)
    return pl.pallas_call(
        kernel,
        grid=(layers, rows // step),
        in_specs=[pl.BlockSpec((step, size), place(index)) for index in range(layers) for size in sizes],
        out_specs=[
            pl.BlockSpec((1, step, 1, sizes[6]), inner),
            pl.BlockSpec((1, step, sizes[2]), outer),
            pl.BlockSpec((1, step, 2, half), inner),
            pl.BlockSpec((1, step, sizes[4]), outer),
        ],
        out_shape=[
            jax.ShapeDtypeStruct((layers, rows, 1, sizes[6]), full),
            jax.ShapeDtypeStruct((layers, rows, sizes[2]), full),
            jax.ShapeDtypeStruct((layers, rows, 2, half), full),
            jax.ShapeDtypeStruct((layers, rows, sizes[4]), full),
        ],
        compiler_params=pltpu.CompilerParams(vmem_limit_bytes=60 << 20),
        name="combine",
    )(*(item for items in halves_of for item in items))


def stationary(stream, grad_out, wqkv, wo, wgu, wd, gain_attn, gain_ffn):
    tok = stream.shape[0]
    layers = wqkv.shape[0]
    count_rows = wqkv.shape[1]
    depth = lax.axis_size("z")
    half = HEAD // 2
    lane = jnp.arange(EXTRA, dtype=jnp.int32)
    freq = (THETA ** (-((lane % half).astype(jnp.float32) * 2.0 / HEAD))).reshape(1, -1)
    cosine = sine = None
    current = swap_grid(stream, depth)
    grad_now = swap_grid(grad_out, depth)
    gains = swap_grid(jnp.concatenate([gain_attn, gain_ffn]), depth)
    gain_a, gain_f = gains[:layers], gains[layers:]
    greet = lambda: Square(tok, depth).greet()
    flat_qkv = wqkv.reshape(layers, count_rows, -1)
    own_qkv = [Slice(flat_qkv, index) for index in range(layers)]
    own_out = [Slice(wo, index) for index in range(layers)]
    own_gu = [wgu[index].reshape(count_rows, -1) for index in range(layers)]
    own_down = [Slice(wd, index) for index in range(layers)]
    peer_qkv, peer_out, peer_gu, peer_down = ([None] * layers for _ in range(4))
    saved = []
    for index in range(layers):
        before = current
        first = index == 0
        final = index == layers - 1
        follow = index + 1
        shipped = [] if final else [own_qkv[follow], own_out[follow], own_gu[follow], own_down[follow]]
        attend = attention_forward(
            before, gain_a[index], own_qkv[index], own_out[index], peer_qkv[index], peer_out[index],
            own_gu[:1] if first else [], freq, cosine, sine, depth
        )
        peer = attend.link(len(attend.shapes) - 1) if first else peer_gu[index]
        feed = ffn_forward(
            attend.link(0), gain_f[index], own_gu[index], peer, own_down[index], peer_down[index], shipped, depth
        )
        parts = [attend, feed]
        if final:
            feed.private = (2, 3)
            back_part = ffn_backward(
                grad_now, attend.link(0), gain_f[index], feed.link(2, 1), feed.link(3, 1), own_gu[index], peer, own_down[index],
                feed.link(4, 1) if first else peer_down[index], [], depth, not first
            )
            back_part.woven = not first
            parts.append(back_part)
        made, fed, *back = launch(parts, greet, 2 * index)
        hidden_in, normed_a, queries, kv, lse, mixed, factors = made[:7]
        if first:
            peer_qkv[0], peer_out[0], cosine, sine, peer_gu[0] = made[7:]
        current, normed_f, kept, active = fed[:4]
        if first:
            peer_down[index] = fed[4]
        if shipped:
            peer_qkv[follow], peer_out[follow], peer_gu[follow], peer_down[follow] = fed[-4:]
        saved.append((before, normed_a, queries, kv, lse, mixed, factors, hidden_in, normed_f, kept, active))
    gains_a, gains_f, downs, rests, got_qkv = ({}, {}, {}, {}, {})
    grad_hidden, grad_gu, gains_f[layers - 1], *downs[layers - 1] = back[0]
    parts, whose = [], []
    for index in reversed(range(layers)):
        before, normed_a, queries, kv, lse, mixed, factors, _, normed_f, _, _ = saved[index]
        attend = attention_backward(
            grad_hidden, before, gain_a[index], own_qkv[index], peer_qkv[index], own_out[index], peer_out[index],
            cosine, sine, queries, kv, lse, factors, mixed, normed_a, normed_f, grad_gu, depth
        )
        attend.private = (2,)
        at = len(parts)
        parts.append(attend)
        if index:
            _, _, _, _, _, _, _, hidden_in, _, kept, active = saved[index - 1]
            feed = ffn_backward(
                attend.link(0, at), hidden_in, gain_f[index - 1], kept, active, own_gu[index - 1], peer_gu[index - 1],
                own_down[index - 1], peer_down[index - 1], [attend.link(2, at)], depth
            )
            parts.append(feed)
            whose.append((index, at))
            grad_hidden, grad_gu = feed.link(0, at + 1), feed.link(1, at + 1)
            if index > 1:
                made = launch(parts, greet, 2 * index + 1)
                for layer, spot in whose:
                    _, gains_a[layer], _, *rests[layer] = made[spot]
                    grad_hidden, grad_gu, gains_f[layer - 1], *downs[layer - 1], got_qkv[layer] = made[spot + 1]
                parts, whose = [], []
    known_a = [gains_a[layer] for layer in range(1, layers) if layer in gains_a]
    open_a = [parts[spot].link(1, spot) for _, spot in whose[::-1]]
    known_f = [gains_f[layer] for layer in range(layers) if layer in gains_f]
    open_f = [parts[spot + 1].link(2, spot + 1) for _, spot in whose[::-1]]
    tail = finish(attend.link(0, at), [attend.link(1, at)] + open_a + known_a + open_f + known_f, attend.link(2, at), depth)
    made = launch(parts + [tail], lambda: greet_last(tok, depth), 1)
    for layer, spot in whose:
        rests[layer] = made[spot][3:]
        *_, kept_down, got_down, got_qkv[layer] = made[spot + 1]
        downs[layer - 1] = [kept_down, got_down]
    rests[0] = made[at][3:]
    grad_in, gains, got_qkv[0] = made[-1]
    grads = combine([
        (*rests[layer][:4], *downs[layer], rests[layer][4], got_qkv[layer]) for layer in range(layers)
    ])
    return (swap_grid(current, depth), grad_in, *grads, gains[:layers], gains[layers:])


def solution(mesh):
    rows, cols = ("row", "col")
    body = local
    if (mesh.shape["row"], mesh.shape["col"]) == (8, 4):
        mesh = share_out(mesh)
        rows, cols = (("z", "x"), ("y", "c"))
        body = stationary
    in_specs = (
        P(rows, cols),
        P(rows, cols),
        P(None, rows, cols, None),
        P(None, rows, cols),
        P(None, rows, None, cols),
        P(None, rows, cols),
        P(None, cols),
        P(None, cols),
    )
    out_specs = (
        P(rows, cols),
        P(rows, cols),
        P(None, rows, cols, None),
        P(None, rows, cols),
        P(None, rows, None, cols),
        P(None, rows, cols),
        P(None, cols),
        P(None, cols),
    )
    return jax.shard_map(body, mesh=mesh, in_specs=in_specs, out_specs=out_specs, check_vma=False)
```
